128 devices in a mesh: gx: 4 (over z_hi, core), gy: 4 (over x), gz: 8 (over y, z_lo).
Axes of the slice: x: 4, y: 4, z: 4 (z_hi: 2, z_lo: 2; z = z_hi * 2 + z_lo), core: 2. Of those that a mesh axis runs over, the one named last changes fastest.
Arguments:
- x_a: bfloat16 [32, 8, 64, 1024], P(None, 'gx', 'gy', 'gz'), may hold values from -12 to 12
- x_b: bfloat16 [32, 8, 64, 1024], P(None, 'gx', 'gy', 'gz'), may hold values from -12 to 12
- w_first: bfloat16 [3, 3, 3, 32, 32], replicated, may hold values from -0.21875 to 0.21875
- w_second: bfloat16 [3, 3, 3, 32, 32], replicated, may hold values from -0.21875 to 0.21875
- gain_first: float32 [32], replicated, may hold values from 0.1 to 1.9
- bias_first: float32 [32], replicated, may hold values from -2 to 2
- gain_second: float32 [32], replicated, may hold values from 0.1 to 1.9
- bias_second: float32 [32], replicated, may hold values from -2 to 2
- grad_out: bfloat16 [32, 8, 64, 1024], P(None, 'gx', 'gy', 'gz'), may hold values from -6 to 6
Outputs:
- y_a: bfloat16 [32, 8, 64, 1024], P(None, 'gx', 'gy', 'gz')
- dx_b: bfloat16 [32, 8, 64, 1024], P(None, 'gx', 'gy', 'gz')
- grad_w_first: float32 [3, 3, 3, 32, 32], replicated
- grad_w_second: float32 [3, 3, 3, 32, 32], replicated
- grad_norm: float32 [4, 32], replicated
The draws below stay inside these ranges and needn't reach their ends.
All inputs are finite; a program needn't handle non-finite values.
Results may differ from the reference program's by a relative error of at most 0.0063.
Values may be sent and summed in bfloat16 or wider, within the bound.
A program may use at most 128 MiB of HBM per device.

```python
import math
import jax
import jax.numpy as jnp
from jax import lax

C = 32
NX = 8
NY = 64
NZ = 1024
VOXELS = 524288


def draw_volume(key, salt):
    folded = jax.random.fold_in(key, salt)
    depth = jnp.arange(NX, dtype=jnp.float32) / max(NX - 1, 1)
    base = jnp.clip(jax.random.normal(folded, (C, NX, NY, NZ), jnp.float32), -4.0, 4.0)
    ramp = 1.0 + 2.0 * depth
    value = base * ramp[None, :, None, None]
    return value.astype(jnp.bfloat16)


def draw_x_a(key, part):
    return draw_volume(key, 11)


def draw_x_b(key, part):
    return draw_volume(key, 23)


def block_levels(key, extent, cuts, smallest, high):
    level = 1.0
    for axis_at, blocks in cuts:
        draws = jax.random.uniform(jax.random.fold_in(jax.random.fold_in(key, 6), axis_at), (blocks,), jnp.float32, smallest / len(cuts), high / len(cuts))
        level = level * jnp.repeat(jnp.exp(draws), extent[axis_at] // blocks).reshape((-1,) + (1,) * (len(extent) - 1 - axis_at))
    return level


def bell_draw(own_key, extent, scale, bound, cuts=(), kind=jnp.bfloat16):
    result = jax.random.normal(own_key, extent, jnp.float32) * scale
    if len(cuts) > 0:
        result = block_levels(own_key, extent, cuts, -0.22, 0.18) * result
    return jnp.clip(result, min=-bound, max=bound).astype(kind)


def setup_inputs(seed: int = 0) -> dict:
    arg_keys = jax.random.split(jax.random.key(seed), 10)
    return {
        "x_a": draw_x_a(jax.random.fold_in(arg_keys[9], 71), 0),
        "x_b": draw_x_b(jax.random.fold_in(arg_keys[9], 71), 0),
        "w_first": bell_draw(arg_keys[2], (3, 3, 3, C, C), (27 * C) ** -0.5, 0.21875),
        "w_second": bell_draw(arg_keys[3], (3, 3, 3, C, C), (27 * C) ** -0.5, 0.21875),
        "gain_first": jnp.clip(1.0 + 0.18 * jax.random.normal(arg_keys[4], (C,), jnp.float32), 0.1, 1.9),
        "bias_first": bell_draw(arg_keys[5], (C,), 0.5, 2.0, (), jnp.float32),
        "gain_second": jnp.clip(1.0 + 0.18 * jax.random.normal(arg_keys[6], (C,), jnp.float32), 0.1, 1.9),
        "bias_second": bell_draw(arg_keys[7], (C,), 0.5, 2.0, (), jnp.float32),
        "grad_out": bell_draw(arg_keys[8], (C, NX, NY, NZ), 1.0, 6.0, ((1, 4), (2, 4), (3, 8))),
    }


EPSILON = 1e-05

def spread(values):
    return values[:, None, None, None]

def silu_slope(value):
    sigma = jax.nn.sigmoid(value)
    return sigma * (1.0 + value * (1.0 - sigma))

def pad_volume(volume):
    return jnp.pad(volume, ((0, 0), (1, 1), (1, 1), (1, 1)))

def convolve(padded, weight):
    in_chan = padded.shape[0]
    out_chan = weight.shape[3]
    span_x = padded.shape[1] - 2
    span_y = padded.shape[2] - 2
    span_z = padded.shape[3] - 2
    total = jnp.zeros((out_chan, span_x * span_y * span_z), jnp.float32)
    for shift_x in range(3):
        for shift_y in range(3):
            pieces = [padded[:, shift_x:shift_x + span_x, shift_y:shift_y + span_y, shift_z:shift_z + span_z] for shift_z in range(3)]
            stacked = jnp.concatenate(pieces, axis=0).reshape(3 * in_chan, -1)
            matrix = weight[shift_x, shift_y].transpose(1, 0, 2).reshape(out_chan, 3 * in_chan)
            total = total + jnp.dot(matrix, stacked, preferred_element_type=jnp.float32)
    return total.reshape(out_chan, span_x, span_y, span_z)

def kernel_grad(padded, upstream):
    in_chan = padded.shape[0]
    out_chan = upstream.shape[0]
    span_x, span_y, span_z = (upstream.shape[1], upstream.shape[2], upstream.shape[3])
    flat = upstream.reshape(out_chan, -1)
    rows = []
    for shift_x in range(3):
        for shift_y in range(3):
            pieces = [padded[:, shift_x:shift_x + span_x, shift_y:shift_y + span_y, shift_z:shift_z + span_z] for shift_z in range(3)]
            stacked = jnp.concatenate(pieces, axis=0).reshape(3 * in_chan, -1)
            product = lax.dot_general(flat, stacked, (((1,), (1,)), ((), ())), preferred_element_type=jnp.float32)
            rows.append(product.reshape(out_chan, 3, in_chan).transpose(1, 0, 2))
    return jnp.stack(rows).reshape(3, 3, 3, out_chan, in_chan)

def flipped(weight):
    return jnp.flip(weight, (0, 1, 2)).transpose(0, 1, 2, 4, 3)

def forward_layer(features, weight, gain, bias):
    conv_out = convolve(pad_volume(features), weight)
    means = lax.optimization_barrier(jnp.sum(conv_out, axis=(1, 2, 3))) / VOXELS
    variance = lax.optimization_barrier(jnp.sum(jnp.square(conv_out - spread(means)), axis=(1, 2, 3))) / VOXELS
    scales = lax.rsqrt(variance + EPSILON)
    normed = (conv_out - spread(means)) * spread(scales)
    preact = spread(gain) * normed + spread(bias)
    output = (preact * jax.nn.sigmoid(preact)).astype(jnp.bfloat16)
    return (output, preact, normed, scales)

def backward_layer(upstream, preact, normed, scales, gain):
    slope = upstream * silu_slope(preact)
    sum_d = lax.optimization_barrier(jnp.sum(slope, axis=(1, 2, 3)))
    sum_dx = lax.optimization_barrier(jnp.sum(slope * normed, axis=(1, 2, 3)))
    delta = spread(gain * scales) * (slope - spread(sum_d / VOXELS) - normed * spread(sum_dx / VOXELS))
    return (delta.astype(jnp.bfloat16), sum_d, sum_dx)

def reference(x_a, x_b, w_first, w_second, gain_first, bias_first, gain_second, bias_second, grad_out):
    hidden_a = forward_layer(x_a, w_first, gain_first, bias_first)[0]
    y_a = forward_layer(hidden_a, w_second, gain_second, bias_second)[0]
    hidden_b, pre_one, norm_one, scale_one = forward_layer(x_b, w_first, gain_first, bias_first)
    unused, pre_two, norm_two, scale_two = forward_layer(hidden_b, w_second, gain_second, bias_second)
    factor = 1.0 / math.sqrt(VOXELS)
    delta_two, sum_d2, sum_x2 = backward_layer(grad_out.astype(jnp.float32), pre_two, norm_two, scale_two, gain_second)
    grad_w_second = kernel_grad(pad_volume(hidden_b), delta_two) * factor
    upstream_one = convolve(pad_volume(delta_two), flipped(w_second))
    delta_one, sum_d1, sum_x1 = backward_layer(upstream_one, pre_one, norm_one, scale_one, gain_first)
    grad_w_first = kernel_grad(pad_volume(x_b), delta_one) * factor
    dx_b = convolve(pad_volume(delta_one), flipped(w_first)).astype(jnp.bfloat16)
    grad_norm = jnp.stack([sum_x1, sum_d1, sum_x2, sum_d2]) * factor
    return (y_a, dx_b, grad_w_first, grad_w_second, grad_norm)
```

```python
import functools
import math

import jax
import jax.numpy as jnp
from jax import lax
from jax.experimental import pallas as pl
from jax.experimental.pallas import tpu as pltpu
from jax.sharding import PartitionSpec as P

F32 = jnp.float32
BF16 = jnp.bfloat16
EPSILON = 1e-05
C = 32
LANES = 128
SPAN_X, SPAN_Y = 2, 16
PAD_X, PAD_Y = SPAN_X + 2, SPAN_Y + 2
TAPS = 3 * C
DEPTH = PAD_X * 3 * TAPS
FLAT = 9 * TAPS
GROUP = 4
AXES = ("gx", "gy", "gz")
MESH = pl.DeviceIdType.MESH


def sigmoid(value):
    return 0.5 + 0.5 * jnp.tanh(0.5 * value)


class Halo:
    def __init__(self, rows, near, far_y, turn, far_x, edge, send, recv, place, volumes):
        self.rows, self.near, self.far_y, self.turn, self.far_x = rows, near, far_y, turn, far_x
        self.edge, self.send, self.recv, self.place, self.volumes = edge, send, recv, place, volumes
        self.count = 0
        self.sent = []

    def has(self, axis, step):
        me, size = self.place[axis]
        return me > 0 if step < 0 else me < size - 1

    def push(self, source, target, axis, step):
        me, size = self.place[axis]
        index = self.count
        self.count += 1
        copy = pltpu.make_async_remote_copy(
            src_ref=source,
            dst_ref=target,
            send_sem=self.send.at[index],
            recv_sem=self.recv.at[index],
            device_id={axis: lax.rem(me + step + size, size)},
            device_id_type=MESH,
        )

        @pl.when(self.has(axis, step))
        def _():
            copy.start()

        self.sent.append((copy, self.has(axis, step)))
        return copy, self.has(axis, -step)

    def faces_x(self, volume):
        rows = self.rows
        inner = pl.ds(1, SPAN_Y)
        down = self.push(
            rows.at[volume, 1, inner], rows.at[volume, PAD_X - 1, inner], "gx", -1
        )
        up = self.push(rows.at[volume, SPAN_X, inner], rows.at[volume, 0, inner], "gx", 1)
        return [down, up]

    def faces_y(self):
        rows, inner, every = self.rows, pl.ds(1, SPAN_X), pl.ds(0, self.volumes)
        down = self.push(
            rows.at[every, inner, 1], rows.at[every, inner, PAD_Y - 1], "gy", -1
        )
        up = self.push(rows.at[every, inner, SPAN_Y], rows.at[every, inner, 0], "gy", 1)
        return [down, up]

    def columns_z(self):
        down = self.push(self.edge.at[0], self.near.at[1], "gz", -1)
        up = self.push(self.edge.at[1], self.near.at[0], "gz", 1)
        return [down, up]

    def columns_y(self):
        down = self.push(self.near, self.far_y.at[1], "gy", -1)
        up = self.push(self.near, self.far_y.at[0], "gy", 1)
        return [down, up]

    def columns_x(self, lane):
        inside = lax.rem(lane, 32)
        for side in range(2):
            for volume in range(self.volumes):
                own = self.near[side, volume].astype(F32)
                low = pltpu.roll(self.far_y[0, side, volume].astype(F32), LANES - 16, 1)
                high = pltpu.roll(self.far_y[1, side, volume].astype(F32), 16, 1)
                own = jnp.where(inside == 0, low, jnp.where(inside == PAD_Y - 1, high, own))
                self.turn[side, volume] = own.astype(BF16)
        down = self.push(self.turn, self.far_x.at[1], "gx", -1)
        up = self.push(self.turn, self.far_x.at[0], "gx", 1)
        return [down, up]

    def corners_x(self):
        rows, every = self.rows, pl.ds(0, self.volumes)
        result = []
        for at in (0, PAD_Y - 1):
            result.append(
                self.push(rows.at[every, 1, at], rows.at[every, PAD_X - 1, at], "gx", -1)
            )
            result.append(
                self.push(rows.at[every, SPAN_X, at], rows.at[every, 0, at], "gx", 1)
            )
        return result

    def merged(self, side, volume, lane):
        own = self.turn[side, volume].astype(F32)
        low = pltpu.roll(self.far_x[0, side, volume].astype(F32), LANES - 64, 1)
        high = pltpu.roll(self.far_x[1, side, volume].astype(F32), 64, 1)
        return jnp.where(lane < 32, low, jnp.where(lane >= 96, high, own))

    @staticmethod
    def arrive(pushes):
        for copy, present in pushes:

            @pl.when(present)
            def _(copy=copy):
                copy.wait_recv()

    def drain(self):
        for copy, present in self.sent:

            @pl.when(present)
            def _(copy=copy):
                copy.wait_send()


class Fan:
    def __init__(self, place, axis, send, recv, first):
        self.me, self.size = place[axis]
        self.axis, self.send, self.recv, self.first = axis, send, recv, first
        self.copies = []

    def start(self, source_of, target):
        for step in range(1, self.size):
            to = lax.rem(self.me + step, self.size)
            copy = pltpu.make_async_remote_copy(
                src_ref=source_of(to),
                dst_ref=target,
                send_sem=self.send.at[self.first + step - 1],
                recv_sem=self.recv.at[self.first + step - 1],
                device_id={self.axis: to},
                device_id_type=MESH,
            )
            copy.start()
            self.copies.append(copy)

    def arrive(self):
        for copy in self.copies:
            copy.wait_recv()

    def drain(self):
        for copy in self.copies:
            copy.wait_send()


def kernel(
    voxels,
    x_a, x_b, grad, weights, params,
    y_out, dx_out, gw_out, norm_out,
    taps_x, taps_h, taps_d2, taps_d1,
    rows_x, rows_1, rows_2, rows_e,
    near_x, near_1, near_2, near_e,
    fary_x, fary_1, fary_2, fary_e,
    turn_x, turn_1, turn_2, turn_e,
    farx_x, farx_1, farx_2, farx_e,
    edge_x, edge_1, edge_2, edge_e,
    side_x, side_1, side_2, side_e,
    conv_1, conv_2, back_1,
    sums_x, sums_z, sums_y,
    gw_local, gw_a, gw_sa, gw_b, gw_sb, gw_c, gw_sc, gw_d, gw_e,
    halo_send, halo_recv, sums_send, sums_recv, gw_send, gw_recv,
):
    place = {axis: (lax.axis_index(axis), lax.axis_size(axis)) for axis in AXES}
    for near in (near_x, near_1, near_2, near_e):
        near[...] = jnp.zeros_like(near)
    barrier = pltpu.get_barrier_semaphore()
    partners = 0
    for axis in AXES:
        me, size = place[axis]
        for step in range(1, size):
            pl.semaphore_signal(
                barrier, inc=1, device_id={axis: lax.rem(me + step, size)}, device_id_type=MESH
            )
            partners += 1

    lane = lax.broadcasted_iota(jnp.int32, (C, LANES), 1)
    halos = []
    for index, (rows, near, fary, turn, farx, edge, volumes) in enumerate((
        (rows_x, near_x, fary_x, turn_x, farx_x, edge_x, 3),
        (rows_1, near_1, fary_1, turn_1, farx_1, edge_1, 2),
        (rows_2, near_2, fary_2, turn_2, farx_2, edge_2, 1),
        (rows_e, near_e, fary_e, turn_e, farx_e, edge_e, 1),
    )):
        halos.append(
            Halo(rows, near, fary, turn, farx, edge, halo_send.at[index], halo_recv.at[index],
                 place, volumes)
        )
    halo_x, halo_1, halo_2, halo_e = halos

    low_x, high_x = place["gx"][0] > 0, place["gx"][0] < place["gx"][1] - 1
    low_y, high_y = place["gy"][0] > 0, place["gy"][0] < place["gy"][1] - 1
    low_z, high_z = place["gz"][0] > 0, place["gz"][0] < place["gz"][1] - 1

    def keep(at_x, at_y):
        held_x = low_x if at_x == 0 else high_x if at_x == PAD_X - 1 else None
        if isinstance(at_y, int):
            held_y = low_y if at_y == 0 else high_y if at_y == PAD_Y - 1 else None
        else:
            held_y = jnp.logical_and(
                jnp.logical_or(at_y > 0, low_y), jnp.logical_or(at_y < PAD_Y - 1, high_y)
            )
        if held_x is None:
            return held_y
        return held_x if held_y is None else jnp.logical_and(held_x, held_y)

    def lane_keep(side):
        spot_x, spot_y = lane // 32, lax.rem(lane, 32)
        bad = jnp.zeros((C, LANES), jnp.int32)
        for hit, present in (
            (spot_x == 0, low_x), (spot_x == PAD_X - 1, high_x),
            (spot_y == 0, low_y), (spot_y == PAD_Y - 1, high_y),
        ):
            missing = jnp.where(present, 0, 1)
            bad = bad + jnp.where(hit, missing, 0)
        bad = bad + jnp.where(low_z if side == 0 else high_z, 0, 1)
        return bad == 0

    def extract(tile, spot, carry):
        first, last = carry
        first = jnp.where(lane == spot, pltpu.roll(tile, spot, 1), first)
        last = jnp.where(lane == spot, pltpu.roll(tile, lax.rem(spot + 1, LANES), 1), last)
        return first, last

    def put_taps(taps, volume, at_x, at_y, tile, side_lo, side_hi):
        spot = at_x * 32 + at_y
        left = jnp.where(
            lane == 0,
            pltpu.roll(side_lo, lax.rem(LANES - spot, LANES), 1),
            pltpu.roll(tile, 1, 1),
        )
        right = jnp.where(
            lane == LANES - 1,
            pltpu.roll(side_hi, LANES - 1 - spot, 1),
            pltpu.roll(tile, LANES - 1, 1),
        )
        taps[volume, at_x, at_y, 0:C] = left.astype(BF16)
        taps[volume, at_x, at_y, C : 2 * C] = tile.astype(BF16)
        taps[volume, at_x, at_y, 2 * C : 3 * C] = right.astype(BF16)

    def build(taps, volume, outer, inner, sides):
        low, high = sides
        zero = jnp.zeros((C, LANES), F32)

        def held(at_x, at_y):
            tile = outer(at_x, at_y)
            return jnp.where(keep(at_x, at_y), tile, zero)

        for at_x in (1, 2):

            def step(block, carry, at_x=at_x):
                for k in range(8):
                    at_y = block * 8 + k
                    put_taps(
                        taps, volume, at_x, at_y + 1, inner(at_x - 1, at_y), low[...], high[...]
                    )
                return carry

            lax.fori_loop(0, 2, step, 0)
            for at_y in (0, PAD_Y - 1):
                put_taps(taps, volume, at_x, at_y, held(at_x, at_y), low[...], high[...])
        for at_x in (0, PAD_X - 1):

            def step(block, carry, at_x=at_x):
                for k in range(6):
                    at_y = block * 6 + k
                    put_taps(taps, volume, at_x, at_y, held(at_x, at_y), low[...], high[...])
                return carry

            lax.fori_loop(0, 3, step, 0)

    def convolve(taps, volume, weight, emit, carry):
        def step(block, carry):
            first = block * GROUP
            columns = [
                taps[volume, :, pl.ds(first + k, 3)].reshape(DEPTH, LANES) for k in range(GROUP)
            ]
            total = jnp.dot(
                weights[weight],
                jnp.concatenate(columns, axis=1),
                preferred_element_type=F32,
            )
            for k in range(GROUP):
                for at_x in range(SPAN_X):
                    tile = total[at_x * C : (at_x + 1) * C, k * LANES : (k + 1) * LANES]
                    carry = emit(at_x, first + k, tile, carry)
            return carry

        return lax.fori_loop(0, SPAN_Y // GROUP, step, carry)

    def kernel_grad(taps, volume, upstream, index):
        def step(block, total):
            first = block * GROUP
            left, right = [], []
            for k in range(GROUP):
                left.append(
                    upstream[0, pl.ds(1, SPAN_X), first + k + 1, C : 2 * C].reshape(
                        SPAN_X * C, LANES
                    )
                )
                right.append(taps[volume, :, pl.ds(first + k, 3)].reshape(DEPTH, LANES))
            return total + lax.dot_general(
                jnp.concatenate(left, axis=1),
                jnp.concatenate(right, axis=1),
                (((1,), (1,)), ((), ())),
                preferred_element_type=F32,
            )

        total = lax.fori_loop(
            0, SPAN_Y // GROUP, step, jnp.zeros((SPAN_X * C, DEPTH), F32)
        )
        both = total[0:C, 0:FLAT] + total[C : 2 * C, 3 * TAPS : 3 * TAPS + FLAT]
        both = jnp.concatenate([both, jnp.zeros((C, 1024 - FLAT), F32)], axis=1)
        for j in range(4):
            for k in range(8):
                gw_local[j, index, k] = both[8 * j : 8 * j + 8, LANES * k : LANES * (k + 1)]

    def pack(columns):
        whole = jnp.zeros((C, LANES), F32)
        for k, column in enumerate(columns):
            whole = whole + jnp.where(lane == k, column, 0.0)
        tile = whole[0:8]
        for j in range(1, 4):
            tile = tile + pltpu.roll(whole[8 * j : 8 * j + 8], 4 * j, 1)
        return tile

    def unpack(tile, count):
        parts = [tile] + [pltpu.roll(tile, LANES - 4 * j, 1) for j in range(1, 4)]
        whole = jnp.concatenate(parts, axis=0)
        return [whole[:, k : k + 1] for k in range(count)]

    class Total:
        def __init__(self, index):
            self.fans = {}
            first = 0
            for axis, slots in (("gx", sums_x), ("gz", sums_z), ("gy", sums_y)):
                fan = Fan(place, axis, sums_send.at[index], sums_recv.at[index], first)
                first += fan.size - 1
                self.fans[axis] = (fan, slots.at[index])

        def start(self, axis, tile):
            fan, slots = self.fans[axis]
            slots[fan.me] = tile
            mine = slots.at[fan.me]
            fan.start(lambda to: mine, mine)

        def finish(self, axis):
            fan, slots = self.fans[axis]
            fan.arrive()
            tile = slots[0]
            for k in range(1, fan.size):
                tile = tile + slots[k]
            return tile

        def drain(self):
            for fan, slots in self.fans.values():
                fan.drain()

    totals = [Total(index) for index in range(4)]

    def reduce_with(total, tile, halo, waits):
        total.start("gx", tile)
        phase_1 = waits + halo.faces_y() + halo.columns_z()
        tile = total.finish("gx")
        total.start("gz", tile)
        halo.arrive(phase_1[-4:])
        phase_2 = halo.columns_y()
        corners = halo.corners_x()
        tile = total.finish("gz")
        total.start("gy", tile)
        halo.arrive(phase_2)
        last = halo.columns_x(lane)
        tile = total.finish("gy")
        return tile, waits + corners + last

    gain_1, bias_1, gain_2, bias_2 = (params[:, k : k + 1] for k in range(4))

    zero = jnp.zeros((C, LANES), F32)
    for volume, source in enumerate((x_a, x_b, grad)):
        for at_x in range(SPAN_X):

            def step(block, carry, source=source, at_x=at_x, volume=volume):
                for k in range(8):
                    at_y = block * 8 + k
                    row = source[at_x, at_y]
                    rows_x[volume, at_x + 1, at_y + 1] = row
                    carry = extract(
                        row.astype(F32), (at_x + 1) * 32 + at_y + 1, carry
                    )
                return carry

            carry = lax.fori_loop(0, 2, step, (zero, zero) if at_x == 0 else carry)
        edge_x[0, volume] = carry[0].astype(BF16)
        edge_x[1, volume] = carry[1].astype(BF16)

    pl.semaphore_wait(barrier, partners)

    waits_x = [halo_x.faces_x(0), halo_x.faces_x(1)]
    phase_1 = halo_x.faces_y() + halo_x.columns_z()
    waits_g = halo_x.faces_x(2)
    halo_x.arrive(phase_1)
    phase_2 = halo_x.columns_y()
    corners = halo_x.corners_x()
    halo_x.arrive(phase_2)
    halo_x.arrive(halo_x.columns_x(lane))
    halo_x.arrive(corners)
    ok = [lane_keep(side) for side in range(2)]
    for side in range(2):
        for volume in range(3):
            tile = halo_x.merged(side, volume, lane)
            side_x[volume, side] = jnp.where(ok[side], tile, 0.0)

    def stats_emit(keep_f32, halo, volume):
        def emit(at_x, at_y, tile, carry):
            total, squares, first, last = carry
            keep_f32[volume, at_x, at_y] = tile
            halo.rows[halo_of[volume], at_x + 1, at_y + 1] = tile.astype(BF16)
            first, last = extract(tile, (at_x + 1) * 32 + at_y + 1, (first, last))
            return total + tile, squares + tile * tile, first, last

        halo_of = {0: 0, 1: 1}
        return emit

    columns = []
    waits = []
    for volume in range(2):
        halo_x.arrive(waits_x[volume])
        build(
            taps_x, volume,
            lambda at_x, at_y, volume=volume: rows_x[volume, at_x, at_y].astype(F32),
            lambda at_x, at_y, volume=volume: rows_x[volume, at_x + 1, at_y + 1].astype(F32),
            (side_x.at[volume, 0], side_x.at[volume, 1]),
        )
        total, squares, first, last = convolve(
            taps_x, volume, 0, stats_emit(conv_1, halo_1, volume), (zero,) * 4
        )
        edge_1[0, volume] = first.astype(BF16)
        edge_1[1, volume] = last.astype(BF16)
        waits += halo_1.faces_x(volume)
        columns += [
            jnp.sum(total, axis=1, keepdims=True), jnp.sum(squares, axis=1, keepdims=True)
        ]
    tile, arrivals = reduce_with(totals[0], pack(columns), halo_1, waits)
    sums = unpack(tile, 4)
    halo_1.arrive(arrivals)

    def moments(total, squares):
        mean = total / voxels
        scale = lax.rsqrt(squares / voxels - mean * mean + EPSILON)
        return mean, scale

    columns = []
    affine_1 = None
    for volume in range(2):
        mean, scale = moments(sums[2 * volume], sums[2 * volume + 1])
        slope = jnp.broadcast_to(gain_1 * scale, (C, LANES))
        shift = jnp.broadcast_to(bias_1 - mean * gain_1 * scale, (C, LANES))

        def active(value, slope=slope, shift=shift):
            pre = value * slope + shift
            return pre * sigmoid(pre)

        for side in range(2):
            tile = active(halo_1.merged(side, volume, lane))
            side_1[volume, side] = jnp.where(ok[side], tile, 0.0)
        build(
            taps_h, volume,
            lambda at_x, at_y, volume=volume: active(rows_1[volume, at_x, at_y].astype(F32)),
            lambda at_x, at_y, volume=volume: active(conv_1[volume, at_x, at_y]),
            (side_1.at[volume, 0], side_1.at[volume, 1]),
        )
        if volume == 0:

            def emit(at_x, at_y, tile, carry):
                total, squares = carry
                conv_2[0, at_x, at_y] = tile
                return total + tile, squares + tile * tile

            total, squares = convolve(taps_h, 0, 1, emit, (zero,) * 2)
        else:

            def emit(at_x, at_y, tile, carry):
                total, squares, first, last = carry
                conv_2[1, at_x, at_y] = tile
                rows_2[0, at_x + 1, at_y + 1] = tile.astype(BF16)
                first, last = extract(tile, (at_x + 1) * 32 + at_y + 1, (first, last))
                return total + tile, squares + tile * tile, first, last

            total, squares, first, last = convolve(taps_h, 1, 1, emit, (zero,) * 4)
            edge_2[0, 0] = first.astype(BF16)
            edge_2[1, 0] = last.astype(BF16)
            waits = halo_2.faces_x(0)
        columns += [
            jnp.sum(total, axis=1, keepdims=True), jnp.sum(squares, axis=1, keepdims=True)
        ]
    mean_1, scale_1 = mean, scale
    tile, arrivals = reduce_with(totals[1], pack(columns), halo_2, waits)
    sums = unpack(tile, 4)

    mean_2, scale_2 = moments(sums[2], sums[3])

    def layer_of(mean, scale, gain, bias):
        norm_slope = jnp.broadcast_to(scale, (C, LANES))
        norm_shift = jnp.broadcast_to(-mean * scale, (C, LANES))
        wide_gain = jnp.broadcast_to(gain, (C, LANES))
        wide_bias = jnp.broadcast_to(bias, (C, LANES))

        def slope_of(value, upstream):
            normed = value * norm_slope + norm_shift
            pre = wide_gain * normed + wide_bias
            sigma = sigmoid(pre)
            return upstream * (sigma * (1.0 + pre * (1.0 - sigma))), normed

        return slope_of

    def delta_of(slope_of, sum_d, sum_x, gain, scale):
        wide_d = jnp.broadcast_to(sum_d / voxels, (C, LANES))
        wide_x = jnp.broadcast_to(sum_x / voxels, (C, LANES))
        factor = jnp.broadcast_to(gain * scale, (C, LANES))

        def delta(value, upstream):
            slope, normed = slope_of(value, upstream)
            return factor * (slope - wide_d - normed * wide_x)

        return delta

    slope_2 = layer_of(mean_2, scale_2, gain_2, bias_2)

    def sum_rows(slope_of, value_of, upstream_of):
        carry = (zero, zero)
        for at_x in range(SPAN_X):

            def step(block, carry, at_x=at_x):
                total, weighted = carry
                for k in range(8):
                    at_y = block * 8 + k
                    slope, normed = slope_of(value_of(at_x, at_y), upstream_of(at_x, at_y))
                    total, weighted = total + slope, weighted + slope * normed
                return total, weighted

            carry = lax.fori_loop(0, 2, step, carry)
        return [jnp.sum(part, axis=1, keepdims=True) for part in carry]

    columns = sum_rows(
        slope_2,
        lambda at_x, at_y: conv_2[1, at_x, at_y],
        lambda at_x, at_y: rows_x[2, at_x + 1, at_y + 1].astype(F32),
    )
    totals[2].start("gx", pack(columns))

    mean_a, scale_a = moments(sums[0], sums[1])
    slope_a = jnp.broadcast_to(gain_2 * scale_a, (C, LANES))
    shift_a = jnp.broadcast_to(bias_2 - mean_a * gain_2 * scale_a, (C, LANES))
    for at_x in range(SPAN_X):

        def step(block, carry, at_x=at_x):
            for k in range(8):
                at_y = block * 8 + k
                pre = conv_2[0, at_x, at_y] * slope_a + shift_a
                y_out[at_x, at_y] = (pre * sigmoid(pre)).astype(BF16)
            return carry

        lax.fori_loop(0, 2, step, 0)

    totals[2].start("gz", totals[2].finish("gx"))
    totals[2].start("gy", totals[2].finish("gz"))
    halo_2.arrive(arrivals)
    halo_x.arrive(waits_g)
    sum_d2, sum_x2 = unpack(totals[2].finish("gy"), 2)

    delta_2 = delta_of(slope_2, sum_d2, sum_x2, gain_2, scale_2)
    for side in range(2):
        tile = delta_2(halo_2.merged(side, 0, lane), side_x[2, side])
        side_2[0, side] = jnp.where(ok[side], tile, 0.0)
    build(
        taps_d2, 0,
        lambda at_x, at_y: delta_2(
            rows_2[0, at_x, at_y].astype(F32), rows_x[2, at_x, at_y].astype(F32)
        ),
        lambda at_x, at_y: delta_2(
            conv_2[1, at_x, at_y], rows_x[2, at_x + 1, at_y + 1].astype(F32)
        ),
        (side_2.at[0, 0], side_2.at[0, 1]),
    )
    slope_1 = layer_of(mean_1, scale_1, gain_1, bias_1)

    def emit(at_x, at_y, tile, carry):
        total, weighted, first, last = carry
        back_1[at_x, at_y] = tile
        rows_e[0, at_x + 1, at_y + 1] = tile.astype(BF16)
        first, last = extract(tile, (at_x + 1) * 32 + at_y + 1, (first, last))
        slope, normed = slope_1(conv_1[1, at_x, at_y], tile)
        return total + slope, weighted + slope * normed, first, last

    total, weighted, first, last = convolve(taps_d2, 0, 2, emit, (zero,) * 4)
    edge_e[0, 0] = first.astype(BF16)
    edge_e[1, 0] = last.astype(BF16)
    waits = halo_e.faces_x(0)
    columns = [
        jnp.sum(total, axis=1, keepdims=True), jnp.sum(weighted, axis=1, keepdims=True)
    ]
    tile, arrivals = reduce_with(totals[3], pack(columns), halo_e, waits)
    kernel_grad(taps_h, 1, taps_d2, 1)
    sum_d1, sum_x1 = unpack(tile, 2)
    halo_e.arrive(arrivals)

    delta_1 = delta_of(slope_1, sum_d1, sum_x1, gain_1, scale_1)
    for side in range(2):
        tile = delta_1(halo_1.merged(side, 1, lane), halo_e.merged(side, 0, lane))
        side_e[0, side] = jnp.where(ok[side], tile, 0.0)
    build(
        taps_d1, 0,
        lambda at_x, at_y: delta_1(
            rows_1[1, at_x, at_y].astype(F32), rows_e[0, at_x, at_y].astype(F32)
        ),
        lambda at_x, at_y: delta_1(conv_1[1, at_x, at_y], back_1[at_x, at_y]),
        (side_e.at[0, 0], side_e.at[0, 1]),
    )
    kernel_grad(taps_x, 1, taps_d1, 0)

    fan_a = Fan(place, "gx", gw_send, gw_recv, 0)
    fan_b = Fan(place, "gz", gw_send, gw_recv, 3)
    fan_c = Fan(place, "gy", gw_send, gw_recv, 10)
    fan_d = Fan(place, "gz", gw_send, gw_recv, 13)
    fan_e = Fan(place, "gx", gw_send, gw_recv, 20)
    fan_a.start(lambda to: gw_local.at[to], gw_a.at[fan_a.me])

    def emit(at_x, at_y, tile, carry):
        dx_out[at_x, at_y] = tile.astype(BF16)
        return carry

    convolve(taps_d1, 0, 3, emit, 0)

    fan_a.arrive()
    gw_a[fan_a.me] = gw_local[fan_a.me]
    for index in range(2):
        for k in range(8):
            tile = gw_a[0, index, k]
            for j in range(1, 4):
                tile = tile + gw_a[j, index, k]
            gw_sa[k, index] = tile
    fan_b.start(lambda to: gw_sa.at[to], gw_b.at[fan_b.me])
    fan_b.arrive()
    gw_b[fan_b.me] = gw_sa[fan_b.me]
    for index in range(2):
        tile = gw_b[0, index]
        for j in range(1, 8):
            tile = tile + gw_b[j, index]
        gw_c[fan_c.me, index] = tile
    fan_c.start(lambda to: gw_c.at[fan_c.me], gw_c.at[fan_c.me])
    fan_c.arrive()
    for index in range(2):
        tile = gw_c[0, index]
        for j in range(1, 4):
            tile = tile + gw_c[j, index]
        gw_d[fan_d.me, index] = tile * (1.0 / math.sqrt(voxels))
    fan_d.start(lambda to: gw_d.at[fan_d.me], gw_d.at[fan_d.me])
    fan_d.arrive()
    fan_e.start(lambda to: gw_d, gw_e.at[fan_e.me])
    gw_e[fan_e.me] = gw_d[...]
    norms = [sum_x1, sum_d1, sum_x2, sum_d2]
    whole = jnp.zeros((C, LANES), F32)
    for k, column in enumerate(norms):
        whole = whole + jnp.where(lane == k, column, 0.0)
    norm_out[...] = whole * (1.0 / math.sqrt(voxels))
    fan_e.arrive()
    for j in range(4):
        for index in range(2):
            for k in range(8):
                gw_out[index, 8 * j : 8 * j + 8, LANES * k : LANES * (k + 1)] = gw_e[j, k, index]

    for halo in halos:
        halo.drain()
    for total in totals:
        total.drain()
    for fan in (fan_a, fan_b, fan_c, fan_d, fan_e):
        fan.drain()


def stacked(weight):
    flat = weight.transpose(3, 0, 1, 2, 4).reshape(C, FLAT)
    slab = 3 * TAPS
    return jnp.concatenate(
        [jnp.pad(flat, ((0, 0), (0, slab))), jnp.pad(flat, ((0, 0), (slab, 0)))], axis=0
    )


def flipped(weight):
    return jnp.flip(weight, (0, 1, 2)).transpose(0, 1, 2, 4, 3)


def body(voxels, x_a, x_b, w_first, w_second, gain_first, bias_first, gain_second, bias_second,
         grad_out):
    weights = jnp.stack(
        [stacked(w_first), stacked(w_second), stacked(flipped(w_second)), stacked(flipped(w_first))]
    )
    params = jnp.stack([gain_first, bias_first, gain_second, bias_second], axis=1)

    def by_rows(block):
        return block.transpose(1, 2, 0, 3)

    def sized(*shape, kind=BF16):
        return pltpu.VMEM(shape, kind)

    volumes = (3, 2, 1, 1)
    scratch = [sized(count, PAD_X, PAD_Y, TAPS, LANES) for count in (2, 2, 1, 1)]
    scratch += [sized(count, PAD_X, PAD_Y, C, LANES) for count in volumes]
    scratch += [sized(2, count, C, LANES) for count in volumes]
    scratch += [sized(2, 2, count, C, LANES) for count in volumes]
    scratch += [sized(2, count, C, LANES) for count in volumes]
    scratch += [sized(2, 2, count, C, LANES) for count in volumes]
    scratch += [sized(2, count, C, LANES) for count in volumes]
    scratch += [sized(count, 2, C, LANES, kind=F32) for count in volumes]
    scratch += [
        sized(2, SPAN_X, SPAN_Y, C, LANES, kind=F32),
        sized(2, SPAN_X, SPAN_Y, C, LANES, kind=F32),
        sized(SPAN_X, SPAN_Y, C, LANES, kind=F32),
        sized(4, 4, 8, LANES, kind=F32),
        sized(4, 8, 8, LANES, kind=F32),
        sized(4, 4, 8, LANES, kind=F32),
        sized(4, 2, 8, 8, LANES, kind=F32),
        sized(4, 2, 8, 8, LANES, kind=F32),
        sized(8, 2, 8, LANES, kind=F32),
        sized(8, 2, 8, LANES, kind=F32),
        sized(2, 8, LANES, kind=F32),
        sized(4, 2, 8, LANES, kind=F32),
        sized(2, 8, LANES, kind=F32),
        sized(8, 2, 8, LANES, kind=F32),
        sized(4, 8, 2, 8, LANES, kind=F32),
        pltpu.SemaphoreType.DMA((4, 24)),
        pltpu.SemaphoreType.DMA((4, 24)),
        pltpu.SemaphoreType.DMA((4, 16)),
        pltpu.SemaphoreType.DMA((4, 16)),
        pltpu.SemaphoreType.DMA((24,)),
        pltpu.SemaphoreType.DMA((24,)),
    ]
    in_vmem = pl.BlockSpec(memory_space=pltpu.VMEM)
    y_a, dx_b, kernels, norms = pl.pallas_call(
        functools.partial(kernel, voxels),
        out_shape=(
            jax.ShapeDtypeStruct((SPAN_X, SPAN_Y, C, LANES), BF16),
            jax.ShapeDtypeStruct((SPAN_X, SPAN_Y, C, LANES), BF16),
            jax.ShapeDtypeStruct((2, C, 1024), F32),
            jax.ShapeDtypeStruct((C, LANES), F32),
        ),
        in_specs=[in_vmem] * 5,
        out_specs=(in_vmem,) * 4,
        scratch_shapes=scratch,
        compiler_params=pltpu.CompilerParams(
            collective_id=0, has_side_effects=True, vmem_limit_bytes=60 * 1024 * 1024
        ),
    )(by_rows(x_a), by_rows(x_b), by_rows(grad_out), weights, params)

    def by_channels(block):
        return block.transpose(2, 0, 1, 3)

    grads = kernels[:, :, :FLAT].reshape(2, C, 3, 3, 3, C).transpose(0, 2, 3, 4, 1, 5)
    return (by_channels(y_a), by_channels(dx_b), grads[0], grads[1], norms[:, :4].T)


def solution(mesh):
    split = P(None, "gx", "gy", "gz")
    voxels = float(SPAN_X * SPAN_Y * LANES * mesh.size)
    return jax.shard_map(
        functools.partial(body, voxels),
        mesh=mesh,
        in_specs=(split, split, P(), P(), P(), P(), P(), P(), split),
        out_specs=(split, split, P(), P(), P()),
        check_vma=False,
    )
```

```python
import functools
import math

import jax
import jax.numpy as jnp
from jax import lax
from jax.experimental import pallas as pl
from jax.experimental.pallas import tpu as pltpu
from jax.sharding import PartitionSpec as P

F32 = jnp.float32
BF16 = jnp.bfloat16
EPSILON = 1e-05
C = 32
LANES = 128
SPAN_X, SPAN_Y = 2, 16
PAD_X, PAD_Y = SPAN_X + 2, SPAN_Y + 2
TAPS = 3 * C
DEPTH = PAD_X * 3 * TAPS
FLAT = 9 * TAPS
GROUP = 4
AXES = ("gx", "gy", "gz")
MESH = pl.DeviceIdType.MESH


def sigmoid(value):
    return 0.5 + 0.5 * jnp.tanh(0.5 * value)


def rolled(tile, shift):
    shift = shift % LANES
    return pltpu.roll(tile, shift, 1) if shift else tile


class Halo:
    def __init__(
        self, rows, near, far_y, turn, far_x, edge, side, send, recv, place, volumes
    ):
        self.rows, self.near, self.far_y, self.turn, self.far_x = rows, near, far_y, turn, far_x
        self.side = side
        self.edge, self.send, self.recv, self.place, self.volumes = edge, send, recv, place, volumes
        self.count = 0
        self.sent = []

    def has(self, axis, step):
        me, size = self.place[axis]
        return me > 0 if step < 0 else me < size - 1

    def push(self, source, target, axis, step):
        me, size = self.place[axis]
        index = self.count
        self.count += 1
        copy = pltpu.make_async_remote_copy(
            src_ref=source,
            dst_ref=target,
            send_sem=self.send.at[index],
            recv_sem=self.recv.at[index],
            device_id={axis: lax.rem(me + step + size, size)},
            device_id_type=MESH,
        )

        @pl.when(self.has(axis, step))
        def _():
            copy.start()

        self.sent.append((copy, self.has(axis, step)))
        return copy, self.has(axis, -step)

    def faces_x(self, volume):
        rows = self.rows
        inner = pl.ds(1, SPAN_Y)
        down = self.push(
            rows.at[volume, 1, inner], rows.at[volume, PAD_X - 1, inner], "gx", -1
        )
        up = self.push(rows.at[volume, SPAN_X, inner], rows.at[volume, 0, inner], "gx", 1)
        return [down, up]

    def faces_y(self):
        rows, inner, every = self.rows, pl.ds(1, SPAN_X), pl.ds(0, self.volumes)
        down = self.push(
            rows.at[every, inner, 1], rows.at[every, inner, PAD_Y - 1], "gy", -1
        )
        up = self.push(rows.at[every, inner, SPAN_Y], rows.at[every, inner, 0], "gy", 1)
        return [down, up]

    def columns_z(self):
        down = self.push(self.edge.at[0], self.near.at[1], "gz", -1)
        up = self.push(self.edge.at[1], self.near.at[0], "gz", 1)
        return [down, up]

    def columns_y(self):
        down = self.push(self.near, self.far_y.at[1], "gy", -1)
        up = self.push(self.near, self.far_y.at[0], "gy", 1)
        return [down, up]

    def columns_x(self, lane):
        inside = lax.rem(lane, 32)
        down = jnp.zeros((C, LANES), F32)
        up = jnp.zeros((C, LANES), F32)
        for side in range(2):
            for volume in range(self.volumes):
                own = self.near[side, volume].astype(F32)
                low = pltpu.roll(self.far_y[0, side, volume].astype(F32), LANES - 16, 1)
                high = pltpu.roll(self.far_y[1, side, volume].astype(F32), 16, 1)
                own = jnp.where(inside == 0, low, jnp.where(inside == PAD_Y - 1, high, own))
                self.side[volume, side] = own
                at = 32 * (side * self.volumes + volume)
                here = lane // 32 == at // 32
                down = jnp.where(here, rolled(own, at - 32), down)
                up = jnp.where(here, rolled(own, at - 64), up)
        self.turn[0] = down.astype(BF16)
        self.turn[1] = up.astype(BF16)
        down = self.push(self.turn.at[0], self.far_x.at[1], "gx", -1)
        up = self.push(self.turn.at[1], self.far_x.at[0], "gx", 1)
        return [down, up]

    def corners_x(self):
        rows, every = self.rows, pl.ds(0, self.volumes)
        result = []
        for at in (0, PAD_Y - 1):
            result.append(
                self.push(rows.at[every, 1, at], rows.at[every, PAD_X - 1, at], "gx", -1)
            )
            result.append(
                self.push(rows.at[every, SPAN_X, at], rows.at[every, 0, at], "gx", 1)
            )
        return result

    def merged(self, side, volume, lane):
        at = 32 * (side * self.volumes + volume)
        low = rolled(self.far_x[0].astype(F32), -at)
        high = rolled(self.far_x[1].astype(F32), 96 - at)
        return jnp.where(lane < 32, low, jnp.where(lane >= 96, high, self.side[volume, side]))

    @staticmethod
    def arrive(pushes):
        for copy, present in pushes:

            @pl.when(present)
            def _(copy=copy):
                copy.wait_recv()

    def drain(self):
        for copy, present in self.sent:

            @pl.when(present)
            def _(copy=copy):
                copy.wait_send()


class Fan:
    def __init__(self, place, axis, send, recv, first):
        self.me, self.size = place[axis]
        self.axis, self.send, self.recv, self.first = axis, send, recv, first
        self.copies = []

    def start(self, source_of, target):
        for step in range(1, self.size):
            to = lax.rem(self.me + step, self.size)
            copy = pltpu.make_async_remote_copy(
                src_ref=source_of(to),
                dst_ref=target,
                send_sem=self.send.at[self.first + step - 1],
                recv_sem=self.recv.at[self.first + step - 1],
                device_id={self.axis: to},
                device_id_type=MESH,
            )
            copy.start()
            self.copies.append(copy)

    def arrive(self):
        for copy in self.copies:
            copy.wait_recv()

    def drain(self):
        for copy in self.copies:
            copy.wait_send()


def kernel(
    voxels,
    x_a, x_b, grad, weights, params,
    y_out, dx_out, gw_out, norm_out,
    taps_x, taps_h, taps_d2, taps_d1,
    rows_x, rows_g, rows_1, rows_2, rows_e,
    near_x, near_g, near_1, near_2, near_e,
    fary_x, fary_g, fary_1, fary_2, fary_e,
    turn_x, turn_g, turn_1, turn_2, turn_e,
    farx_x, farx_g, farx_1, farx_2, farx_e,
    edge_x, edge_g, edge_1, edge_2, edge_e,
    side_x, side_g, side_1, side_2, side_e,
    side_h,
    conv_1, conv_2, back_1,
    sums,
    gw_local, gw_a, gw_sa, gw_b, gw_sb, gw_c, gw_sc, gw_d, gw_e,
    halo_send, halo_recv, sums_send, sums_recv, gw_send, gw_recv,
):
    place = {axis: (lax.axis_index(axis), lax.axis_size(axis)) for axis in AXES}
    for near in (near_x, near_g, near_1, near_2, near_e):
        near[...] = jnp.zeros_like(near)
    barrier = pltpu.get_barrier_semaphore()
    count = place["gx"][1] * place["gy"][1] * place["gz"][1]
    flat = (place["gx"][0] * place["gy"][1] + place["gy"][0]) * place["gz"][1] + place["gz"][0]

    def other(step):
        return lax.rem(flat + step, count)

    def greet(step, carry):
        pl.semaphore_signal(
            barrier, inc=1, device_id=other(step), device_id_type=pl.DeviceIdType.LOGICAL
        )
        return carry

    lax.fori_loop(1, count, greet, 0)

    lane = lax.broadcasted_iota(jnp.int32, (C, LANES), 1)
    halos = []
    for index, (rows, near, fary, turn, farx, edge, side, volumes) in enumerate((
        (rows_x, near_x, fary_x, turn_x, farx_x, edge_x, side_x, 2),
        (rows_g, near_g, fary_g, turn_g, farx_g, edge_g, side_g, 1),
        (rows_1, near_1, fary_1, turn_1, farx_1, edge_1, side_1, 2),
        (rows_2, near_2, fary_2, turn_2, farx_2, edge_2, side_2, 1),
        (rows_e, near_e, fary_e, turn_e, farx_e, edge_e, side_e, 1),
    )):
        halos.append(
            Halo(rows, near, fary, turn, farx, edge, side, halo_send.at[index],
                 halo_recv.at[index], place, volumes)
        )
    halo_x, halo_g, halo_1, halo_2, halo_e = halos

    low_x, high_x = place["gx"][0] > 0, place["gx"][0] < place["gx"][1] - 1
    low_y, high_y = place["gy"][0] > 0, place["gy"][0] < place["gy"][1] - 1
    low_z, high_z = place["gz"][0] > 0, place["gz"][0] < place["gz"][1] - 1

    def keep(at_x, at_y):
        held_x = low_x if at_x == 0 else high_x if at_x == PAD_X - 1 else None
        if isinstance(at_y, int):
            held_y = low_y if at_y == 0 else high_y if at_y == PAD_Y - 1 else None
        else:
            held_y = jnp.logical_and(
                jnp.logical_or(at_y > 0, low_y), jnp.logical_or(at_y < PAD_Y - 1, high_y)
            )
        if held_x is None:
            return held_y
        return held_x if held_y is None else jnp.logical_and(held_x, held_y)

    def lane_keep(side):
        spot_x, spot_y = lane // 32, lax.rem(lane, 32)
        bad = jnp.zeros((C, LANES), jnp.int32)
        for hit, present in (
            (spot_x == 0, low_x), (spot_x == PAD_X - 1, high_x),
            (spot_y == 0, low_y), (spot_y == PAD_Y - 1, high_y),
        ):
            missing = jnp.where(present, 0, 1)
            bad = bad + jnp.where(hit, missing, 0)
        bad = bad + jnp.where(low_z if side == 0 else high_z, 0, 1)
        return bad == 0

    def extract(tile, spot, carry):
        first, last = carry
        first = jnp.where(lane == spot, pltpu.roll(tile, spot, 1), first)
        last = jnp.where(lane == spot, pltpu.roll(tile, lax.rem(spot + 1, LANES), 1), last)
        return first, last

    def put_taps(taps, volume, at_x, at_y, tile, side_lo, side_hi):
        spot = at_x * 32 + at_y
        left = jnp.where(
            lane == 0,
            pltpu.roll(side_lo, lax.rem(LANES - spot, LANES), 1),
            pltpu.roll(tile, 1, 1),
        )
        right = jnp.where(
            lane == LANES - 1,
            pltpu.roll(side_hi, LANES - 1 - spot, 1),
            pltpu.roll(tile, LANES - 1, 1),
        )
        taps[volume, at_x, at_y, 0:C] = left.astype(BF16)
        taps[volume, at_x, at_y, C : 2 * C] = tile.astype(BF16)
        taps[volume, at_x, at_y, 2 * C : 3 * C] = right.astype(BF16)

    def build(taps, volume, outer, inner, sides):
        low, high = sides
        zero = jnp.zeros((C, LANES), F32)

        def held(at_x, at_y):
            tile = outer(at_x, at_y)
            return jnp.where(keep(at_x, at_y), tile, zero)

        for at_x in (1, 2):

            def step(block, carry, at_x=at_x):
                for k in range(8):
                    at_y = block * 8 + k
                    put_taps(
                        taps, volume, at_x, at_y + 1, inner(at_x - 1, at_y), low[...], high[...]
                    )
                return carry

            lax.fori_loop(0, 2, step, 0)
            for at_y in (0, PAD_Y - 1):
                put_taps(taps, volume, at_x, at_y, held(at_x, at_y), low[...], high[...])
        for at_x in (0, PAD_X - 1):

            def step(block, carry, at_x=at_x):
                for k in range(6):
                    at_y = block * 6 + k
                    put_taps(taps, volume, at_x, at_y, held(at_x, at_y), low[...], high[...])
                return carry

            lax.fori_loop(0, 3, step, 0)

    def convolve(taps, volume, weight, emit, carry):
        def step(block, carry):
            first = block * GROUP
            columns = [
                taps[volume, :, pl.ds(first + k, 3)].reshape(DEPTH, LANES) for k in range(GROUP)
            ]
            total = jnp.dot(
                weights[weight],
                jnp.concatenate(columns, axis=1),
                preferred_element_type=F32,
            )
            for k in range(GROUP):
                for at_x in range(SPAN_X):
                    tile = total[at_x * C : (at_x + 1) * C, k * LANES : (k + 1) * LANES]
                    carry = emit(at_x, first + k, tile, carry)
            return carry

        return lax.fori_loop(0, SPAN_Y // GROUP, step, carry)

    def kernel_grad(taps, volume, upstream, index):
        def step(block, total):
            first = block * GROUP
            left, right = [], []
            for k in range(GROUP):
                left.append(
                    upstream[0, pl.ds(1, SPAN_X), first + k + 1, C : 2 * C].reshape(
                        SPAN_X * C, LANES
                    )
                )
                right.append(taps[volume, :, pl.ds(first + k, 3)].reshape(DEPTH, LANES))
            return total + lax.dot_general(
                jnp.concatenate(left, axis=1),
                jnp.concatenate(right, axis=1),
                (((1,), (1,)), ((), ())),
                preferred_element_type=F32,
            )

        total = lax.fori_loop(
            0, SPAN_Y // GROUP, step, jnp.zeros((SPAN_X * C, DEPTH), F32)
        )
        both = total[0:C, 0:FLAT] + total[C : 2 * C, 3 * TAPS : 3 * TAPS + FLAT]
        both = jnp.concatenate([both, jnp.zeros((C, 1024 - FLAT), F32)], axis=1)
        for j in range(4):
            for k in range(8):
                gw_local[j, index, k] = both[8 * j : 8 * j + 8, LANES * k : LANES * (k + 1)]

    channel = lax.broadcasted_iota(jnp.int32, (C, LANES), 0)

    def pack(columns):
        whole = jnp.zeros((C, LANES), F32)
        for k, column in enumerate(columns):
            whole = whole + jnp.where(lane == channel + 32 * k, column, 0.0)
        return jnp.sum(whole, axis=0, keepdims=True)

    def unpack(row, number):
        return [
            jnp.sum(jnp.where(lane == channel + 32 * k, row, 0.0), axis=1, keepdims=True)
            for k in range(number)
        ]

    class Total:
        def __init__(self, index):
            self.slots, self.index = sums.at[index], index

        def start(self, row):
            mine = self.slots.at[flat]
            mine[...] = row

            def send(step, carry):
                pltpu.make_async_remote_copy(
                    src_ref=mine,
                    dst_ref=mine,
                    send_sem=sums_send.at[self.index],
                    recv_sem=sums_recv.at[self.index],
                    device_id=other(step),
                    device_id_type=pl.DeviceIdType.LOGICAL,
                ).start()
                return carry

            lax.fori_loop(1, count, send, 0)

        def others(self, semaphore):
            part = self.slots.at[pl.ds(0, count - 1)]
            pltpu.make_async_copy(part, part, semaphore.at[self.index]).wait()

        def finish(self):
            self.others(sums_recv)
            return jnp.sum(self.slots[...], axis=0)

        def drain(self):
            self.others(sums_send)

    totals = [Total(index) for index in range(4)]

    def second(halo, phase):
        halo.arrive(phase)
        return halo.columns_y(), halo.corners_x()

    def third(halo, phase):
        halo.arrive(phase)
        return halo.columns_x(lane)

    gain_1, bias_1, gain_2, bias_2 = (params[:, k : k + 1] for k in range(4))

    zero = jnp.zeros((C, LANES), F32)
    for source, rows, edge, at in (
        (x_a, rows_x, edge_x, 0), (x_b, rows_x, edge_x, 1), (grad, rows_g, edge_g, 0)
    ):
        for at_x in range(SPAN_X):

            def step(block, carry, source=source, rows=rows, at_x=at_x, at=at):
                for k in range(8):
                    at_y = block * 8 + k
                    row = source[at_x, at_y]
                    rows[at, at_x + 1, at_y + 1] = row
                    carry = extract(
                        row.astype(F32), (at_x + 1) * 32 + at_y + 1, carry
                    )
                return carry

            carry = lax.fori_loop(0, 2, step, (zero, zero) if at_x == 0 else carry)
        edge[0, at] = carry[0].astype(BF16)
        edge[1, at] = carry[1].astype(BF16)

    pl.semaphore_wait(barrier, count - 1)

    phase = halo_x.columns_z() + halo_x.faces_y()
    waits_x = [halo_x.faces_x(0)]
    phase, corners = second(halo_x, phase)
    last = third(halo_x, phase)
    waits_x.append(halo_x.faces_x(1))
    halo_x.arrive(corners)
    halo_x.arrive(last)
    ok = [lane_keep(side) for side in range(2)]
    for side in range(2):
        for volume in range(2):
            tile = halo_x.merged(side, volume, lane)
            side_x[volume, side] = jnp.where(ok[side], tile, 0.0)

    def stats_emit(keep_f32, halo, volume):
        def emit(at_x, at_y, tile, carry):
            total, squares, first, last = carry
            keep_f32[volume, at_x, at_y] = tile
            halo.rows[halo_of[volume], at_x + 1, at_y + 1] = tile.astype(BF16)
            first, last = extract(tile, (at_x + 1) * 32 + at_y + 1, (first, last))
            return total + tile, squares + tile * tile, first, last

        halo_of = {0: 0, 1: 1}
        return emit

    columns = []
    waits = []
    for volume in range(2):
        halo_x.arrive(waits_x[volume])
        build(
            taps_x, volume,
            lambda at_x, at_y, volume=volume: rows_x[volume, at_x, at_y].astype(F32),
            lambda at_x, at_y, volume=volume: rows_x[volume, at_x + 1, at_y + 1].astype(F32),
            (side_x.at[volume, 0], side_x.at[volume, 1]),
        )
        total, squares, first, last = convolve(
            taps_x, volume, 0, stats_emit(conv_1, halo_1, volume), (zero,) * 4
        )
        edge_1[0, volume] = first.astype(BF16)
        edge_1[1, volume] = last.astype(BF16)
        if volume == 0:
            waits += halo_1.faces_x(volume)
        columns += [
            jnp.sum(total, axis=1, keepdims=True), jnp.sum(squares, axis=1, keepdims=True)
        ]
    totals[0].start(pack(columns))
    phase = halo_1.columns_z() + halo_1.faces_y()
    waits += halo_1.faces_x(1)
    phase, corners = second(halo_1, phase)
    last = third(halo_1, phase)
    row = totals[0].finish()
    halo_1.arrive(waits + corners + last)
    phase_g = halo_g.columns_z() + halo_g.faces_y()
    waits_g = halo_g.faces_x(0)
    stats = unpack(row, 4)

    def moments(total, squares):
        mean = total / voxels
        scale = lax.rsqrt(squares / voxels - mean * mean + EPSILON)
        return mean, scale

    columns = []
    affine_1 = None
    for volume in range(2):
        mean, scale = moments(stats[2 * volume], stats[2 * volume + 1])
        slope = jnp.broadcast_to(gain_1 * scale, (C, LANES))
        shift = jnp.broadcast_to(bias_1 - mean * gain_1 * scale, (C, LANES))

        def active(value, slope=slope, shift=shift):
            pre = value * slope + shift
            return pre * sigmoid(pre)

        for side in range(2):
            tile = halo_1.merged(side, volume, lane)
            side_1[volume, side] = tile
            side_h[volume, side] = jnp.where(ok[side], active(tile), 0.0)
        build(
            taps_h, volume,
            lambda at_x, at_y, volume=volume: active(rows_1[volume, at_x, at_y].astype(F32)),
            lambda at_x, at_y, volume=volume: active(conv_1[volume, at_x, at_y]),
            (side_h.at[volume, 0], side_h.at[volume, 1]),
        )
        if volume == 0:

            def emit(at_x, at_y, tile, carry):
                total, squares = carry
                conv_2[0, at_x, at_y] = tile
                return total + tile, squares + tile * tile

            total, squares = convolve(taps_h, 0, 1, emit, (zero,) * 2)
            phase_g, corners_g = second(halo_g, phase_g)
        else:

            def emit(at_x, at_y, tile, carry):
                total, squares, first, last = carry
                conv_2[1, at_x, at_y] = tile
                rows_2[0, at_x + 1, at_y + 1] = tile.astype(BF16)
                first, last = extract(tile, (at_x + 1) * 32 + at_y + 1, (first, last))
                return total + tile, squares + tile * tile, first, last

            total, squares, first, last = convolve(taps_h, 1, 1, emit, (zero,) * 4)
            edge_2[0, 0] = first.astype(BF16)
            edge_2[1, 0] = last.astype(BF16)
        columns += [
            jnp.sum(total, axis=1, keepdims=True), jnp.sum(squares, axis=1, keepdims=True)
        ]
    mean_1, scale_1 = mean, scale
    totals[1].start(pack(columns))
    phase = halo_2.columns_z() + halo_2.faces_y()
    waits = halo_2.faces_x(0)
    last_g = third(halo_g, phase_g)
    stats = unpack(totals[1].finish(), 4)

    mean_2, scale_2 = moments(stats[2], stats[3])

    def layer_of(mean, scale, gain, bias):
        norm_slope = jnp.broadcast_to(scale, (C, LANES))
        norm_shift = jnp.broadcast_to(-mean * scale, (C, LANES))
        wide_gain = jnp.broadcast_to(gain, (C, LANES))
        wide_bias = jnp.broadcast_to(bias, (C, LANES))

        def slope_of(value, upstream):
            normed = value * norm_slope + norm_shift
            pre = wide_gain * normed + wide_bias
            sigma = sigmoid(pre)
            return upstream * (sigma * (1.0 + pre * (1.0 - sigma))), normed

        return slope_of

    def delta_of(slope_of, sum_d, sum_x, gain, scale):
        wide_d = jnp.broadcast_to(sum_d / voxels, (C, LANES))
        wide_x = jnp.broadcast_to(sum_x / voxels, (C, LANES))
        factor = jnp.broadcast_to(gain * scale, (C, LANES))

        def delta(value, upstream):
            slope, normed = slope_of(value, upstream)
            return factor * (slope - wide_d - normed * wide_x)

        return delta

    slope_2 = layer_of(mean_2, scale_2, gain_2, bias_2)

    def sum_rows(slope_of, value_of, upstream_of):
        carry = (zero, zero)
        for at_x in range(SPAN_X):

            def step(block, carry, at_x=at_x):
                total, weighted = carry
                for k in range(8):
                    at_y = block * 8 + k
                    slope, normed = slope_of(value_of(at_x, at_y), upstream_of(at_x, at_y))
                    total, weighted = total + slope, weighted + slope * normed
                return total, weighted

            carry = lax.fori_loop(0, 2, step, carry)
        return [jnp.sum(part, axis=1, keepdims=True) for part in carry]

    columns = sum_rows(
        slope_2,
        lambda at_x, at_y: conv_2[1, at_x, at_y],
        lambda at_x, at_y: rows_g[0, at_x + 1, at_y + 1].astype(F32),
    )
    totals[2].start(pack(columns))
    phase, corners = second(halo_2, phase)

    mean_a, scale_a = moments(stats[0], stats[1])
    slope_a = jnp.broadcast_to(gain_2 * scale_a, (C, LANES))
    shift_a = jnp.broadcast_to(bias_2 - mean_a * gain_2 * scale_a, (C, LANES))
    for at_x in range(SPAN_X):

        def step(block, carry, at_x=at_x):
            for k in range(8):
                at_y = block * 8 + k
                pre = conv_2[0, at_x, at_y] * slope_a + shift_a
                y_out[at_x, at_y] = (pre * sigmoid(pre)).astype(BF16)
            return carry

        lax.fori_loop(0, 2, step, 0)

    last = third(halo_2, phase)
    halo_g.arrive(waits_g + corners_g + last_g)
    halo_2.arrive(waits + corners + last)
    sum_d2, sum_x2 = unpack(totals[2].finish(), 2)

    delta_2 = delta_of(slope_2, sum_d2, sum_x2, gain_2, scale_2)
    for side in range(2):
        tile = delta_2(halo_2.merged(side, 0, lane), halo_g.merged(side, 0, lane))
        side_2[0, side] = jnp.where(ok[side], tile, 0.0)
    build(
        taps_d2, 0,
        lambda at_x, at_y: delta_2(
            rows_2[0, at_x, at_y].astype(F32), rows_g[0, at_x, at_y].astype(F32)
        ),
        lambda at_x, at_y: delta_2(
            conv_2[1, at_x, at_y], rows_g[0, at_x + 1, at_y + 1].astype(F32)
        ),
        (side_2.at[0, 0], side_2.at[0, 1]),
    )
    slope_1 = layer_of(mean_1, scale_1, gain_1, bias_1)

    def emit(at_x, at_y, tile, carry):
        total, weighted, first, last = carry
        back_1[at_x, at_y] = tile
        rows_e[0, at_x + 1, at_y + 1] = tile.astype(BF16)
        first, last = extract(tile, (at_x + 1) * 32 + at_y + 1, (first, last))
        slope, normed = slope_1(conv_1[1, at_x, at_y], tile)
        return total + slope, weighted + slope * normed, first, last

    total, weighted, first, last = convolve(taps_d2, 0, 2, emit, (zero,) * 4)
    edge_e[0, 0] = first.astype(BF16)
    edge_e[1, 0] = last.astype(BF16)
    columns = [
        jnp.sum(total, axis=1, keepdims=True), jnp.sum(weighted, axis=1, keepdims=True)
    ]
    totals[3].start(pack(columns))
    phase = halo_e.columns_z() + halo_e.faces_y()
    waits = halo_e.faces_x(0)
    kernel_grad(taps_h, 1, taps_d2, 1)
    phase, corners = second(halo_e, phase)
    last = third(halo_e, phase)
    sum_d1, sum_x1 = unpack(totals[3].finish(), 2)
    halo_e.arrive(waits + corners + last)

    delta_1 = delta_of(slope_1, sum_d1, sum_x1, gain_1, scale_1)
    for side in range(2):
        tile = delta_1(side_1[1, side], halo_e.merged(side, 0, lane))
        side_e[0, side] = jnp.where(ok[side], tile, 0.0)
    build(
        taps_d1, 0,
        lambda at_x, at_y: delta_1(
            rows_1[1, at_x, at_y].astype(F32), rows_e[0, at_x, at_y].astype(F32)
        ),
        lambda at_x, at_y: delta_1(conv_1[1, at_x, at_y], back_1[at_x, at_y]),
        (side_e.at[0, 0], side_e.at[0, 1]),
    )
    kernel_grad(taps_x, 1, taps_d1, 0)

    fan_a = Fan(place, "gx", gw_send, gw_recv, 0)
    fan_b = Fan(place, "gz", gw_send, gw_recv, 3)
    fan_c = Fan(place, "gy", gw_send, gw_recv, 10)
    fan_d = Fan(place, "gz", gw_send, gw_recv, 13)
    fan_e = Fan(place, "gx", gw_send, gw_recv, 20)
    fan_a.start(lambda to: gw_local.at[to], gw_a.at[fan_a.me])

    def emit(at_x, at_y, tile, carry):
        dx_out[at_x, at_y] = tile.astype(BF16)
        return carry

    convolve(taps_d1, 0, 3, emit, 0)

    fan_a.arrive()
    gw_a[fan_a.me] = gw_local[fan_a.me]
    for index in range(2):
        for k in range(8):
            tile = gw_a[0, index, k]
            for j in range(1, 4):
                tile = tile + gw_a[j, index, k]
            gw_sa[k, index] = tile
    fan_b.start(lambda to: gw_sa.at[to], gw_b.at[fan_b.me])
    fan_b.arrive()
    gw_b[fan_b.me] = gw_sa[fan_b.me]
    for index in range(2):
        tile = gw_b[0, index]
        for j in range(1, 8):
            tile = tile + gw_b[j, index]
        gw_c[fan_c.me, index] = tile
    fan_c.start(lambda to: gw_c.at[fan_c.me], gw_c.at[fan_c.me])
    fan_c.arrive()
    for index in range(2):
        tile = gw_c[0, index]
        for j in range(1, 4):
            tile = tile + gw_c[j, index]
        gw_d[fan_d.me, index] = tile * (1.0 / math.sqrt(voxels))
    fan_d.start(lambda to: gw_d.at[fan_d.me], gw_d.at[fan_d.me])
    fan_d.arrive()
    fan_e.start(lambda to: gw_d, gw_e.at[fan_e.me])
    gw_e[fan_e.me] = gw_d[...]
    norms = [sum_x1, sum_d1, sum_x2, sum_d2]
    whole = jnp.zeros((C, LANES), F32)
    for k, column in enumerate(norms):
        whole = whole + jnp.where(lane == k, column, 0.0)
    norm_out[...] = whole * (1.0 / math.sqrt(voxels))
    fan_e.arrive()
    for j in range(4):
        for index in range(2):
            for k in range(8):
                gw_out[index, 8 * j : 8 * j + 8, LANES * k : LANES * (k + 1)] = gw_e[j, k, index]

    for halo in halos:
        halo.drain()
    for total in totals:
        total.drain()
    for fan in (fan_a, fan_b, fan_c, fan_d, fan_e):
        fan.drain()


def stacked(weight):
    flat = weight.transpose(3, 0, 1, 2, 4).reshape(C, FLAT)
    slab = 3 * TAPS
    return jnp.concatenate(
        [jnp.pad(flat, ((0, 0), (0, slab))), jnp.pad(flat, ((0, 0), (slab, 0)))], axis=0
    )


def flipped(weight):
    return jnp.flip(weight, (0, 1, 2)).transpose(0, 1, 2, 4, 3)


def body(voxels, x_a, x_b, w_first, w_second, gain_first, bias_first, gain_second, bias_second,
         grad_out):
    weights = jnp.stack(
        [stacked(w_first), stacked(w_second), stacked(flipped(w_second)), stacked(flipped(w_first))]
    )
    params = jnp.stack([gain_first, bias_first, gain_second, bias_second], axis=1)

    def by_rows(block):
        return block.transpose(1, 2, 0, 3)

    def sized(*shape, kind=BF16):
        return pltpu.VMEM(shape, kind)

    volumes = (2, 1, 2, 1, 1)
    devices = math.prod(lax.axis_size(axis) for axis in AXES)
    scratch = [sized(count, PAD_X, PAD_Y, TAPS, LANES) for count in (2, 2, 1, 1)]
    scratch += [sized(count, PAD_X, PAD_Y, C, LANES) for count in volumes]
    scratch += [sized(2, count, C, LANES) for count in volumes]
    scratch += [sized(2, 2, count, C, LANES) for count in volumes]
    scratch += [sized(2, C, LANES) for count in volumes]
    scratch += [sized(2, C, LANES) for count in volumes]
    scratch += [sized(2, count, C, LANES) for count in volumes]
    scratch += [sized(count, 2, C, LANES, kind=F32) for count in volumes]
    scratch += [sized(2, 2, C, LANES, kind=F32)]
    scratch += [
        sized(2, SPAN_X, SPAN_Y, C, LANES, kind=F32),
        sized(2, SPAN_X, SPAN_Y, C, LANES, kind=F32),
        sized(SPAN_X, SPAN_Y, C, LANES, kind=F32),
        sized(4, devices, 1, LANES, kind=F32),
        sized(4, 2, 8, 8, LANES, kind=F32),
        sized(4, 2, 8, 8, LANES, kind=F32),
        sized(8, 2, 8, LANES, kind=F32),
        sized(8, 2, 8, LANES, kind=F32),
        sized(2, 8, LANES, kind=F32),
        sized(4, 2, 8, LANES, kind=F32),
        sized(2, 8, LANES, kind=F32),
        sized(8, 2, 8, LANES, kind=F32),
        sized(4, 8, 2, 8, LANES, kind=F32),
        pltpu.SemaphoreType.DMA((5, 24)),
        pltpu.SemaphoreType.DMA((5, 24)),
        pltpu.SemaphoreType.DMA((4,)),
        pltpu.SemaphoreType.DMA((4,)),
        pltpu.SemaphoreType.DMA((24,)),
        pltpu.SemaphoreType.DMA((24,)),
    ]
    in_vmem = pl.BlockSpec(memory_space=pltpu.VMEM)
    y_a, dx_b, kernels, norms = pl.pallas_call(
        functools.partial(kernel, voxels),
        out_shape=(
            jax.ShapeDtypeStruct((SPAN_X, SPAN_Y, C, LANES), BF16),
            jax.ShapeDtypeStruct((SPAN_X, SPAN_Y, C, LANES), BF16),
            jax.ShapeDtypeStruct((2, C, 1024), F32),
            jax.ShapeDtypeStruct((C, LANES), F32),
        ),
        in_specs=[in_vmem] * 5,
        out_specs=(in_vmem,) * 4,
        scratch_shapes=scratch,
        compiler_params=pltpu.CompilerParams(
            collective_id=0, has_side_effects=True, vmem_limit_bytes=60 * 1024 * 1024
        ),
    )(by_rows(x_a), by_rows(x_b), by_rows(grad_out), weights, params)

    def by_channels(block):
        return block.transpose(2, 0, 1, 3)

    grads = kernels[:, :, :FLAT].reshape(2, C, 3, 3, 3, C).transpose(0, 2, 3, 4, 1, 5)
    return (by_channels(y_a), by_channels(dx_b), grads[0], grads[1], norms[:, :4].T)


def solution(mesh):
    split = P(None, "gx", "gy", "gz")
    voxels = float(SPAN_X * SPAN_Y * LANES * mesh.size)
    return jax.shard_map(
        functools.partial(body, voxels),
        mesh=mesh,
        in_specs=(split, split, P(), P(), P(), P(), P(), P(), split),
        out_specs=(split, split, P(), P(), P()),
        check_vma=False,
    )
```

```python
import functools
import math

import jax
import jax.numpy as jnp
from jax import lax
from jax.experimental import pallas as pl
from jax.experimental.pallas import tpu as pltpu
from jax.sharding import PartitionSpec as P

F32 = jnp.float32
BF16 = jnp.bfloat16
EPSILON = 1e-05
C = 32
LANES = 128
SPAN_X, SPAN_Y = 2, 16
PAD_X, PAD_Y = SPAN_X + 2, SPAN_Y + 2
TAPS = 3 * C
DEPTH = PAD_X * 3 * TAPS
FLAT = 9 * TAPS
GROUP = 4
AXES = ("gx", "gy", "gz")
MESH = pl.DeviceIdType.MESH


def sigmoid(value):
    return 0.5 + 0.5 * jnp.tanh(0.5 * value)


def rolled(tile, shift):
    shift = shift % LANES
    return pltpu.roll(tile, shift, 1) if shift else tile


class Halo:
    def __init__(
        self, rows, near, far_y, turn, far_x, edge, side, send, recv, place, volumes
    ):
        self.rows, self.near, self.far_y, self.turn, self.far_x = rows, near, far_y, turn, far_x
        self.side = side
        self.edge, self.send, self.recv, self.place, self.volumes = edge, send, recv, place, volumes
        self.count = 0
        self.sent = []

    def has(self, axis, step):
        me, size = self.place[axis]
        return me > 0 if step < 0 else me < size - 1

    def push(self, source, target, axis, step):
        me, size = self.place[axis]
        index = self.count
        self.count += 1
        copy = pltpu.make_async_remote_copy(
            src_ref=source,
            dst_ref=target,
            send_sem=self.send.at[index],
            recv_sem=self.recv.at[index],
            device_id={axis: lax.rem(me + step + size, size)},
            device_id_type=MESH,
        )

        @pl.when(self.has(axis, step))
        def _():
            copy.start()

        self.sent.append((copy, self.has(axis, step)))
        return copy, self.has(axis, -step)

    def faces_x(self, volume):
        rows = self.rows
        inner = pl.ds(1, SPAN_Y)
        down = self.push(
            rows.at[volume, 1, inner], rows.at[volume, PAD_X - 1, inner], "gx", -1
        )
        up = self.push(rows.at[volume, SPAN_X, inner], rows.at[volume, 0, inner], "gx", 1)
        return [down, up]

    def faces_y(self):
        rows, inner, every = self.rows, pl.ds(1, SPAN_X), pl.ds(0, self.volumes)
        down = self.push(
            rows.at[every, inner, 1], rows.at[every, inner, PAD_Y - 1], "gy", -1
        )
        up = self.push(rows.at[every, inner, SPAN_Y], rows.at[every, inner, 0], "gy", 1)
        return [down, up]

    def columns_z(self):
        down = self.push(self.edge.at[0], self.near.at[1], "gz", -1)
        up = self.push(self.edge.at[1], self.near.at[0], "gz", 1)
        return [down, up]

    def columns_y(self):
        down = self.push(self.near, self.far_y.at[1], "gy", -1)
        up = self.push(self.near, self.far_y.at[0], "gy", 1)
        return [down, up]

    def columns_x(self, lane):
        inside = lax.rem(lane, 32)
        down = jnp.zeros((C, LANES), F32)
        up = jnp.zeros((C, LANES), F32)
        for side in range(2):
            for volume in range(self.volumes):
                own = self.near[side, volume].astype(F32)
                low = pltpu.roll(self.far_y[0, side, volume].astype(F32), LANES - 16, 1)
                high = pltpu.roll(self.far_y[1, side, volume].astype(F32), 16, 1)
                own = jnp.where(inside == 0, low, jnp.where(inside == PAD_Y - 1, high, own))
                self.side[volume, side] = own
                at = 32 * (side * self.volumes + volume)
                here = lane // 32 == at // 32
                down = jnp.where(here, rolled(own, at - 32), down)
                up = jnp.where(here, rolled(own, at - 64), up)
        self.turn[0] = down.astype(BF16)
        self.turn[1] = up.astype(BF16)
        down = self.push(self.turn.at[0], self.far_x.at[1], "gx", -1)
        up = self.push(self.turn.at[1], self.far_x.at[0], "gx", 1)
        return [down, up]

    def corners_x(self):
        rows, every = self.rows, pl.ds(0, self.volumes)
        result = []
        for at in (0, PAD_Y - 1):
            result.append(
                self.push(rows.at[every, 1, at], rows.at[every, PAD_X - 1, at], "gx", -1)
            )
            result.append(
                self.push(rows.at[every, SPAN_X, at], rows.at[every, 0, at], "gx", 1)
            )
        return result

    def merged(self, side, volume, lane):
        at = 32 * (side * self.volumes + volume)
        low = rolled(self.far_x[0].astype(F32), -at)
        high = rolled(self.far_x[1].astype(F32), 96 - at)
        return jnp.where(lane < 32, low, jnp.where(lane >= 96, high, self.side[volume, side]))

    @staticmethod
    def arrive(pushes):
        for copy, present in pushes:

            @pl.when(present)
            def _(copy=copy):
                copy.wait_recv()

    def drain(self):
        for copy, present in self.sent:

            @pl.when(present)
            def _(copy=copy):
                copy.wait_send()


def kernel(
    voxels,
    x_a, x_b, grad, weights, params,
    y_out, dx_out, gw_out, norm_out,
    taps_x, taps_h, taps_d2, taps_d1,
    rows_x, rows_g, rows_1, rows_2, rows_e,
    near_x, near_g, near_1, near_2, near_e,
    fary_x, fary_g, fary_1, fary_2, fary_e,
    turn_x, turn_g, turn_1, turn_2, turn_e,
    farx_x, farx_g, farx_1, farx_2, farx_e,
    edge_x, edge_g, edge_1, edge_2, edge_e,
    side_x, side_g, side_1, side_2, side_e,
    side_h,
    conv_1, conv_2, back_1,
    sums,
    norms, slopes, early_out, early_in, late_out, late_in, gathered, pairs,
    halo_send, halo_recv, sums_send, sums_recv, gw_send, gw_recv,
):
    place = {axis: (lax.axis_index(axis), lax.axis_size(axis)) for axis in AXES}
    for near in (near_x, near_g, near_1, near_2, near_e):
        near[...] = jnp.zeros_like(near)
    for chunks in (early_out, late_out):
        for j in range(4):
            chunks[32 * j + 28 : 32 * j + 32] = jnp.zeros((4, 4, LANES), F32)
    barrier = pltpu.get_barrier_semaphore()
    count = place["gx"][1] * place["gy"][1] * place["gz"][1]
    flat = (place["gx"][0] * place["gy"][1] + place["gy"][0]) * place["gz"][1] + place["gz"][0]

    chip_x, chip_y = place["gy"][0], place["gz"][0] // 2
    chip_z = place["gx"][0] // 2 * 2 + lax.rem(place["gz"][0], 2)
    core = lax.rem(place["gx"][0], 2)

    def other(step):
        return lax.rem(flat + step, count)

    def fan_out(source_of, target, send, recv):
        spots = []
        for step_z, step_core in ((2, 1), (2, 0), (1, 1), (3, 1), (1, 0), (3, 0), (0, 1), (0, 0)):
            to_z, to_core = lax.rem(chip_z + step_z, 4), lax.rem(core + step_core, 2)
            spots.append(to_z // 2 * 64 + to_core * 32 + lax.rem(to_z, 2))

        def copies(plane, chosen):
            to_x = lax.rem(chip_x + plane // 4 + 1, 4)
            to_y = lax.rem(chip_y + lax.rem(plane, 4) + 1, 4)
            for spot in chosen:
                to = spot + to_x * 8 + to_y * 2
                pltpu.make_async_remote_copy(
                    src_ref=source_of(to), dst_ref=target, send_sem=send, recv_sem=recv,
                    device_id=to, device_id_type=pl.DeviceIdType.LOGICAL,
                ).start()

        def most(plane, carry):
            copies(plane, spots[:-1])
            return carry

        def rest(plane, carry):
            copies(plane, spots[-1:])
            return carry

        lax.fori_loop(0, 16, most, 0)
        lax.fori_loop(0, 15, rest, 0)

    def fan_in(slots, semaphore):
        part = slots.at[pl.ds(0, count - 1)]
        pltpu.make_async_copy(part, part, semaphore).wait()

    def greet(step, carry):
        pl.semaphore_signal(
            barrier, inc=1, device_id=other(step), device_id_type=pl.DeviceIdType.LOGICAL
        )
        return carry

    lax.fori_loop(1, count, greet, 0)

    lane = lax.broadcasted_iota(jnp.int32, (C, LANES), 1)
    halos = []
    for index, (rows, near, fary, turn, farx, edge, side, volumes) in enumerate((
        (rows_x, near_x, fary_x, turn_x, farx_x, edge_x, side_x, 2),
        (rows_g, near_g, fary_g, turn_g, farx_g, edge_g, side_g, 1),
        (rows_1, near_1, fary_1, turn_1, farx_1, edge_1, side_1, 2),
        (rows_2, near_2, fary_2, turn_2, farx_2, edge_2, side_2, 1),
        (rows_e, near_e, fary_e, turn_e, farx_e, edge_e, side_e, 1),
    )):
        halos.append(
            Halo(rows, near, fary, turn, farx, edge, side, halo_send.at[index],
                 halo_recv.at[index], place, volumes)
        )
    halo_x, halo_g, halo_1, halo_2, halo_e = halos

    low_x, high_x = place["gx"][0] > 0, place["gx"][0] < place["gx"][1] - 1
    low_y, high_y = place["gy"][0] > 0, place["gy"][0] < place["gy"][1] - 1
    low_z, high_z = place["gz"][0] > 0, place["gz"][0] < place["gz"][1] - 1

    def keep(at_x, at_y):
        held_x = low_x if at_x == 0 else high_x if at_x == PAD_X - 1 else None
        if isinstance(at_y, int):
            held_y = low_y if at_y == 0 else high_y if at_y == PAD_Y - 1 else None
        else:
            held_y = jnp.logical_and(
                jnp.logical_or(at_y > 0, low_y), jnp.logical_or(at_y < PAD_Y - 1, high_y)
            )
        if held_x is None:
            return held_y
        return held_x if held_y is None else jnp.logical_and(held_x, held_y)

    def lane_keep(side):
        spot_x, spot_y = lane // 32, lax.rem(lane, 32)
        bad = jnp.zeros((C, LANES), jnp.int32)
        for hit, present in (
            (spot_x == 0, low_x), (spot_x == PAD_X - 1, high_x),
            (spot_y == 0, low_y), (spot_y == PAD_Y - 1, high_y),
        ):
            missing = jnp.where(present, 0, 1)
            bad = bad + jnp.where(hit, missing, 0)
        bad = bad + jnp.where(low_z if side == 0 else high_z, 0, 1)
        return bad == 0

    def extract(tile, spot, carry):
        first, last = carry
        first = jnp.where(lane == spot, pltpu.roll(tile, spot, 1), first)
        last = jnp.where(lane == spot, pltpu.roll(tile, lax.rem(spot + 1, LANES), 1), last)
        return first, last

    def put_taps(taps, volume, at_x, at_y, tile, side_lo, side_hi):
        spot = at_x * 32 + at_y
        left = jnp.where(
            lane == 0,
            pltpu.roll(side_lo, lax.rem(LANES - spot, LANES), 1),
            pltpu.roll(tile, 1, 1),
        )
        right = jnp.where(
            lane == LANES - 1,
            pltpu.roll(side_hi, LANES - 1 - spot, 1),
            pltpu.roll(tile, LANES - 1, 1),
        )
        taps[volume, at_x, at_y, 0:C] = left.astype(BF16)
        taps[volume, at_x, at_y, C : 2 * C] = tile.astype(BF16)
        taps[volume, at_x, at_y, 2 * C : 3 * C] = right.astype(BF16)

    def build(taps, volume, outer, inner, sides):
        low, high = sides
        zero = jnp.zeros((C, LANES), F32)

        def held(at_x, at_y):
            tile = outer(at_x, at_y)
            return jnp.where(keep(at_x, at_y), tile, zero)

        for at_x in (1, 2):

            def step(block, carry, at_x=at_x):
                for k in range(8):
                    at_y = block * 8 + k
                    put_taps(
                        taps, volume, at_x, at_y + 1, inner(at_x - 1, at_y), low[...], high[...]
                    )
                return carry

            lax.fori_loop(0, 2, step, 0)
            for at_y in (0, PAD_Y - 1):
                put_taps(taps, volume, at_x, at_y, held(at_x, at_y), low[...], high[...])
        for at_x in (0, PAD_X - 1):

            def step(block, carry, at_x=at_x):
                for k in range(6):
                    at_y = block * 6 + k
                    put_taps(taps, volume, at_x, at_y, held(at_x, at_y), low[...], high[...])
                return carry

            lax.fori_loop(0, 3, step, 0)

    def convolve(taps, volume, weight, emit, carry):
        def step(block, carry):
            first = block * GROUP
            columns = [
                taps[volume, :, pl.ds(first + k, 3)].reshape(DEPTH, LANES) for k in range(GROUP)
            ]
            total = jnp.dot(
                weights[weight],
                jnp.concatenate(columns, axis=1),
                preferred_element_type=F32,
            )
            for k in range(GROUP):
                for at_x in range(SPAN_X):
                    tile = total[at_x * C : (at_x + 1) * C, k * LANES : (k + 1) * LANES]
                    carry = emit(at_x, first + k, tile, carry)
            return carry

        return lax.fori_loop(0, SPAN_Y // GROUP, step, carry)

    def kernel_grad(taps, volume, row_of, out, first_row, plain=False):
        high = SPAN_X * C + (16 if plain else 0)

        def step(block, total):
            first = block * GROUP
            left, right = [], []
            for k in range(GROUP):
                rows = [row_of(at_x, first + k) for at_x in range(SPAN_X)]
                if plain:
                    rows.append(jnp.ones((16, LANES), BF16))
                left.append(jnp.concatenate(rows, axis=0))
                right.append(taps[volume, :, pl.ds(first + k, 3)].reshape(DEPTH, LANES))
            return total + lax.dot_general(
                jnp.concatenate(left, axis=1),
                jnp.concatenate(right, axis=1),
                (((1,), (1,)), ((), ())),
                preferred_element_type=F32,
            )

        total = lax.fori_loop(0, SPAN_Y // GROUP, step, jnp.zeros((high, DEPTH), F32))
        slab = 3 * TAPS

        def wide(value):
            return jnp.concatenate(
                [value, jnp.zeros((value.shape[0], 7 * LANES - FLAT), F32)], axis=1
            )

        both = wide(total[0:C, 0:FLAT] + total[C : 2 * C, slab : slab + FLAT])
        if plain:
            alone = total[2 * C : 2 * C + 1]
            alone = wide(alone[:, 0:FLAT] + alone[:, slab : slab + FLAT])
        for k in range(7):
            lanes = slice(LANES * k, LANES * (k + 1))
            for pair in range(16):
                spot = (pair // 4 * 8 + k) * 4 + pair % 4
                out[spot, first_row : first_row + 2] = both[2 * pair : 2 * pair + 2, lanes]
                if plain:
                    out[spot, 2:3] = alone[:, lanes]

    channel = lax.broadcasted_iota(jnp.int32, (C, LANES), 0)

    def pack(columns):
        whole = jnp.zeros((C, LANES), F32)
        for k, column in enumerate(columns):
            whole = whole + jnp.where(lane == channel + 32 * k, column, 0.0)
        return jnp.sum(whole, axis=0, keepdims=True)

    def unpack(row, number):
        return [
            jnp.sum(jnp.where(lane == channel + 32 * k, row, 0.0), axis=1, keepdims=True)
            for k in range(number)
        ]

    class Total:
        def __init__(self, index):
            self.slots, self.index = sums.at[index], index

        def start(self, row):
            mine = self.slots.at[flat]
            mine[...] = row

            fan_out(
                lambda to: mine, mine, sums_send.at[self.index], sums_recv.at[self.index]
            )

        def finish(self):
            fan_in(self.slots, sums_recv.at[self.index])
            return jnp.sum(self.slots[...], axis=0)

        def drain(self):
            fan_in(self.slots, sums_send.at[self.index])

    totals = [Total(index) for index in range(4)]

    def second(halo, phase):
        halo.arrive(phase)
        return halo.columns_y(), halo.corners_x()

    def third(halo, phase):
        halo.arrive(phase)
        return halo.columns_x(lane)

    gain_1, bias_1, gain_2, bias_2 = (params[:, k : k + 1] for k in range(4))

    zero = jnp.zeros((C, LANES), F32)
    for source, rows, edge, at in (
        (x_a, rows_x, edge_x, 0), (x_b, rows_x, edge_x, 1), (grad, rows_g, edge_g, 0)
    ):
        for at_x in range(SPAN_X):

            def step(block, carry, source=source, rows=rows, at_x=at_x, at=at):
                for k in range(8):
                    at_y = block * 8 + k
                    row = source[at_x, at_y]
                    rows[at, at_x + 1, at_y + 1] = row
                    carry = extract(
                        row.astype(F32), (at_x + 1) * 32 + at_y + 1, carry
                    )
                return carry

            carry = lax.fori_loop(0, 2, step, (zero, zero) if at_x == 0 else carry)
        edge[0, at] = carry[0].astype(BF16)
        edge[1, at] = carry[1].astype(BF16)

    pl.semaphore_wait(barrier, count - 1)

    phase = halo_x.columns_z() + halo_x.faces_y()
    waits_x = [halo_x.faces_x(0)]
    phase, corners = second(halo_x, phase)
    last = third(halo_x, phase)
    waits_x.append(halo_x.faces_x(1))
    halo_x.arrive(corners)
    halo_x.arrive(last)
    ok = [lane_keep(side) for side in range(2)]
    for side in range(2):
        for volume in range(2):
            tile = halo_x.merged(side, volume, lane)
            side_x[volume, side] = jnp.where(ok[side], tile, 0.0)

    def stats_emit(keep_f32, halo, volume):
        def emit(at_x, at_y, tile, carry):
            total, squares, first, last = carry
            keep_f32[volume, at_x, at_y] = tile
            halo.rows[halo_of[volume], at_x + 1, at_y + 1] = tile.astype(BF16)
            first, last = extract(tile, (at_x + 1) * 32 + at_y + 1, (first, last))
            return total + tile, squares + tile * tile, first, last

        halo_of = {0: 0, 1: 1}
        return emit

    columns = []
    waits = []
    for volume in range(2):
        halo_x.arrive(waits_x[volume])
        build(
            taps_x, volume,
            lambda at_x, at_y, volume=volume: rows_x[volume, at_x, at_y].astype(F32),
            lambda at_x, at_y, volume=volume: rows_x[volume, at_x + 1, at_y + 1].astype(F32),
            (side_x.at[volume, 0], side_x.at[volume, 1]),
        )
        total, squares, first, last = convolve(
            taps_x, volume, 0, stats_emit(conv_1, halo_1, volume), (zero,) * 4
        )
        edge_1[0, volume] = first.astype(BF16)
        edge_1[1, volume] = last.astype(BF16)
        if volume == 0:
            waits += halo_1.faces_x(volume)
        columns += [
            jnp.sum(total, axis=1, keepdims=True), jnp.sum(squares, axis=1, keepdims=True)
        ]
    totals[0].start(pack(columns))
    phase = halo_1.columns_z() + halo_1.faces_y()
    waits += halo_1.faces_x(1)
    phase, corners = second(halo_1, phase)
    last = third(halo_1, phase)
    row = totals[0].finish()
    halo_1.arrive(waits + corners + last)
    phase_g = halo_g.columns_z() + halo_g.faces_y()
    waits_g = halo_g.faces_x(0)
    stats = unpack(row, 4)

    def moments(total, squares):
        mean = total / voxels
        scale = lax.rsqrt(squares / voxels - mean * mean + EPSILON)
        return mean, scale

    columns = []
    affine_1 = None
    for volume in range(2):
        mean, scale = moments(stats[2 * volume], stats[2 * volume + 1])
        slope = jnp.broadcast_to(gain_1 * scale, (C, LANES))
        shift = jnp.broadcast_to(bias_1 - mean * gain_1 * scale, (C, LANES))

        def active(value, slope=slope, shift=shift):
            pre = value * slope + shift
            return pre * sigmoid(pre)

        norm_slope = jnp.broadcast_to(scale, (C, LANES))
        norm_shift = jnp.broadcast_to(-mean * scale, (C, LANES))

        def own_row(at_x, at_y, volume, active, norm_slope=norm_slope, norm_shift=norm_shift):
            value = conv_1[volume, at_x, at_y]
            if volume == 1:
                norms[at_x, at_y] = (value * norm_slope + norm_shift).astype(BF16)
            return active(value)

        for side in range(2):
            tile = halo_1.merged(side, volume, lane)
            side_1[volume, side] = tile
            side_h[volume, side] = jnp.where(ok[side], active(tile), 0.0)
        build(
            taps_h, volume,
            lambda at_x, at_y, volume=volume: active(rows_1[volume, at_x, at_y].astype(F32)),
            functools.partial(own_row, volume=volume, active=active),
            (side_h.at[volume, 0], side_h.at[volume, 1]),
        )
        if volume == 0:

            def emit(at_x, at_y, tile, carry):
                total, squares = carry
                conv_2[0, at_x, at_y] = tile
                return total + tile, squares + tile * tile

            total, squares = convolve(taps_h, 0, 1, emit, (zero,) * 2)
            phase_g, corners_g = second(halo_g, phase_g)
        else:

            def emit(at_x, at_y, tile, carry):
                total, squares, first, last = carry
                conv_2[1, at_x, at_y] = tile
                rows_2[0, at_x + 1, at_y + 1] = tile.astype(BF16)
                first, last = extract(tile, (at_x + 1) * 32 + at_y + 1, (first, last))
                return total + tile, squares + tile * tile, first, last

            total, squares, first, last = convolve(taps_h, 1, 1, emit, (zero,) * 4)
            edge_2[0, 0] = first.astype(BF16)
            edge_2[1, 0] = last.astype(BF16)
        columns += [
            jnp.sum(total, axis=1, keepdims=True), jnp.sum(squares, axis=1, keepdims=True)
        ]
    mean_1, scale_1 = mean, scale
    totals[1].start(pack(columns))
    phase = halo_2.columns_z() + halo_2.faces_y()
    waits = halo_2.faces_x(0)
    last_g = third(halo_g, phase_g)
    kernel_grad(taps_x, 1, lambda at_x, at_y: norms[at_x, at_y], early_out, 0, plain=True)
    fan_out(
        lambda to: early_out.at[to], early_in.at[flat], gw_send.at[0], gw_recv.at[0]
    )
    early_in[flat] = early_out[flat]
    stats = unpack(totals[1].finish(), 4)

    mean_2, scale_2 = moments(stats[2], stats[3])

    def layer_of(mean, scale, gain, bias):
        norm_slope = jnp.broadcast_to(scale, (C, LANES))
        norm_shift = jnp.broadcast_to(-mean * scale, (C, LANES))
        wide_gain = jnp.broadcast_to(gain, (C, LANES))
        wide_bias = jnp.broadcast_to(bias, (C, LANES))

        def slope_of(value, upstream):
            normed = value * norm_slope + norm_shift
            pre = wide_gain * normed + wide_bias
            sigma = sigmoid(pre)
            return upstream * (sigma * (1.0 + pre * (1.0 - sigma))), normed

        return slope_of

    def delta_of(slope_of, sum_d, sum_x, gain, scale):
        wide_d = jnp.broadcast_to(sum_d / voxels, (C, LANES))
        wide_x = jnp.broadcast_to(sum_x / voxels, (C, LANES))
        factor = jnp.broadcast_to(gain * scale, (C, LANES))

        def delta(value, upstream):
            slope, normed = slope_of(value, upstream)
            return factor * (slope - wide_d - normed * wide_x)

        return delta

    slope_2 = layer_of(mean_2, scale_2, gain_2, bias_2)

    def sum_rows(slope_of, value_of, upstream_of):
        carry = (zero, zero)
        for at_x in range(SPAN_X):

            def step(block, carry, at_x=at_x):
                total, weighted = carry
                for k in range(8):
                    at_y = block * 8 + k
                    slope, normed = slope_of(value_of(at_x, at_y), upstream_of(at_x, at_y))
                    total, weighted = total + slope, weighted + slope * normed
                return total, weighted

            carry = lax.fori_loop(0, 2, step, carry)
        return [jnp.sum(part, axis=1, keepdims=True) for part in carry]

    columns = sum_rows(
        slope_2,
        lambda at_x, at_y: conv_2[1, at_x, at_y],
        lambda at_x, at_y: rows_g[0, at_x + 1, at_y + 1].astype(F32),
    )
    totals[2].start(pack(columns))
    phase, corners = second(halo_2, phase)

    mean_a, scale_a = moments(stats[0], stats[1])
    slope_a = jnp.broadcast_to(gain_2 * scale_a, (C, LANES))
    shift_a = jnp.broadcast_to(bias_2 - mean_a * gain_2 * scale_a, (C, LANES))
    for at_x in range(SPAN_X):

        def step(block, carry, at_x=at_x):
            for k in range(8):
                at_y = block * 8 + k
                pre = conv_2[0, at_x, at_y] * slope_a + shift_a
                y_out[at_x, at_y] = (pre * sigmoid(pre)).astype(BF16)
            return carry

        lax.fori_loop(0, 2, step, 0)

    last = third(halo_2, phase)
    halo_g.arrive(waits_g + corners_g + last_g)
    halo_2.arrive(waits + corners + last)
    sum_d2, sum_x2 = unpack(totals[2].finish(), 2)

    delta_2 = delta_of(slope_2, sum_d2, sum_x2, gain_2, scale_2)
    for side in range(2):
        tile = delta_2(halo_2.merged(side, 0, lane), halo_g.merged(side, 0, lane))
        side_2[0, side] = jnp.where(ok[side], tile, 0.0)
    build(
        taps_d2, 0,
        lambda at_x, at_y: delta_2(
            rows_2[0, at_x, at_y].astype(F32), rows_g[0, at_x, at_y].astype(F32)
        ),
        lambda at_x, at_y: delta_2(
            conv_2[1, at_x, at_y], rows_g[0, at_x + 1, at_y + 1].astype(F32)
        ),
        (side_2.at[0, 0], side_2.at[0, 1]),
    )
    slope_1 = layer_of(mean_1, scale_1, gain_1, bias_1)

    def emit(at_x, at_y, tile, carry):
        total, weighted, first, last = carry
        back_1[at_x, at_y] = tile
        rows_e[0, at_x + 1, at_y + 1] = tile.astype(BF16)
        first, last = extract(tile, (at_x + 1) * 32 + at_y + 1, (first, last))
        slope, normed = slope_1(conv_1[1, at_x, at_y], tile)
        slopes[at_x, at_y] = slope.astype(BF16)
        return total + slope, weighted + slope * normed, first, last

    total, weighted, first, last = convolve(taps_d2, 0, 2, emit, (zero,) * 4)
    edge_e[0, 0] = first.astype(BF16)
    edge_e[1, 0] = last.astype(BF16)
    columns = [
        jnp.sum(total, axis=1, keepdims=True), jnp.sum(weighted, axis=1, keepdims=True)
    ]
    totals[3].start(pack(columns))
    phase = halo_e.columns_z() + halo_e.faces_y()
    waits = halo_e.faces_x(0)
    kernel_grad(taps_x, 1, lambda at_x, at_y: slopes[at_x, at_y], late_out, 0)
    phase, corners = second(halo_e, phase)
    kernel_grad(
        taps_h, 1, lambda at_x, at_y: taps_d2[0, at_x + 1, at_y + 1, C : 2 * C], late_out, 2
    )
    last = third(halo_e, phase)
    fan_out(lambda to: late_out.at[to], late_in.at[flat], gw_send.at[1], gw_recv.at[1])
    late_in[flat] = late_out[flat]
    sum_d1, sum_x1 = unpack(totals[3].finish(), 2)
    halo_e.arrive(waits + corners + last)

    delta_1 = delta_of(slope_1, sum_d1, sum_x1, gain_1, scale_1)
    for side in range(2):
        tile = delta_1(side_1[1, side], halo_e.merged(side, 0, lane))
        side_e[0, side] = jnp.where(ok[side], tile, 0.0)
    build(
        taps_d1, 0,
        lambda at_x, at_y: delta_1(
            rows_1[1, at_x, at_y].astype(F32), rows_e[0, at_x, at_y].astype(F32)
        ),
        lambda at_x, at_y: delta_1(conv_1[1, at_x, at_y], back_1[at_x, at_y]),
        (side_e.at[0, 0], side_e.at[0, 1]),
    )
    whole = 1.0 / math.sqrt(voxels)
    for k, column in enumerate(
        (gain_1 * scale_1 * whole, sum_d1 / voxels, sum_x1 / voxels)
    ):
        tile = jnp.broadcast_to(column, (C, LANES))
        for pair in range(16):
            pairs[k, pair] = tile[2 * pair : 2 * pair + 2]
    fan_in(early_in, gw_recv.at[0])
    early = jnp.sum(early_in[...], axis=0)
    at = flat // 32 * 4 + lax.rem(flat, 4)
    fan_in(late_in, gw_recv.at[1])
    late = jnp.sum(late_in[...], axis=0)
    gathered[flat, 0:2] = pairs[0, at] * (
        late[0:2] - pairs[1, at] * early[2:3] - pairs[2, at] * early[0:2]
    )
    gathered[flat, 2:4] = late[2:4] * whole
    mine = gathered.at[flat]
    fan_out(lambda to: mine, mine, gw_send.at[2], gw_recv.at[2])

    def emit(at_x, at_y, tile, carry):
        dx_out[at_x, at_y] = tile.astype(BF16)
        return carry

    convolve(taps_d1, 0, 3, emit, 0)

    tile = jnp.zeros((C, LANES), F32)
    for k, column in enumerate((sum_x1, sum_d1, sum_x2, sum_d2)):
        tile = tile + jnp.where(lane == k, column, 0.0)
    norm_out[...] = tile * whole
    fan_in(gathered, gw_recv.at[2])
    gw_out[...] = gathered[...]

    for halo in halos:
        halo.drain()
    for total in totals:
        total.drain()
    for k, chunks in enumerate((early_out, late_out, gathered)):
        fan_in(chunks, gw_send.at[k])


def stacked(weight):
    flat = weight.transpose(3, 0, 1, 2, 4).reshape(C, FLAT)
    slab = 3 * TAPS
    return jnp.concatenate(
        [jnp.pad(flat, ((0, 0), (0, slab))), jnp.pad(flat, ((0, 0), (slab, 0)))], axis=0
    )


def flipped(weight):
    return jnp.flip(weight, (0, 1, 2)).transpose(0, 1, 2, 4, 3)


def body(voxels, x_a, x_b, w_first, w_second, gain_first, bias_first, gain_second, bias_second,
         grad_out):
    weights = jnp.stack(
        [stacked(w_first), stacked(w_second), stacked(flipped(w_second)), stacked(flipped(w_first))]
    )
    params = jnp.stack([gain_first, bias_first, gain_second, bias_second], axis=1)

    def by_rows(block):
        return block.transpose(1, 2, 0, 3)

    def sized(*shape, kind=BF16):
        return pltpu.VMEM(shape, kind)

    volumes = (2, 1, 2, 1, 1)
    devices = math.prod(lax.axis_size(axis) for axis in AXES)
    scratch = [sized(count, PAD_X, PAD_Y, TAPS, LANES) for count in (2, 2, 1, 1)]
    scratch += [sized(count, PAD_X, PAD_Y, C, LANES) for count in volumes]
    scratch += [sized(2, count, C, LANES) for count in volumes]
    scratch += [sized(2, 2, count, C, LANES) for count in volumes]
    scratch += [sized(2, C, LANES) for count in volumes]
    scratch += [sized(2, C, LANES) for count in volumes]
    scratch += [sized(2, count, C, LANES) for count in volumes]
    scratch += [sized(count, 2, C, LANES, kind=F32) for count in volumes]
    scratch += [sized(2, 2, C, LANES, kind=F32)]
    scratch += [
        sized(2, SPAN_X, SPAN_Y, C, LANES, kind=F32),
        sized(2, SPAN_X, SPAN_Y, C, LANES, kind=F32),
        sized(SPAN_X, SPAN_Y, C, LANES, kind=F32),
        sized(4, devices, 1, LANES, kind=F32),
        sized(SPAN_X, SPAN_Y, C, LANES),
        sized(SPAN_X, SPAN_Y, C, LANES),
        sized(devices, 4, LANES, kind=F32),
        sized(devices, 4, LANES, kind=F32),
        sized(devices, 4, LANES, kind=F32),
        sized(devices, 4, LANES, kind=F32),
        sized(devices, 4, LANES, kind=F32),
        sized(3, 16, 2, LANES, kind=F32),
        pltpu.SemaphoreType.DMA((5, 24)),
        pltpu.SemaphoreType.DMA((5, 24)),
        pltpu.SemaphoreType.DMA((4,)),
        pltpu.SemaphoreType.DMA((4,)),
        pltpu.SemaphoreType.DMA((3,)),
        pltpu.SemaphoreType.DMA((3,)),
    ]
    in_vmem = pl.BlockSpec(memory_space=pltpu.VMEM)
    y_a, dx_b, kernels, norms = pl.pallas_call(
        functools.partial(kernel, voxels),
        out_shape=(
            jax.ShapeDtypeStruct((SPAN_X, SPAN_Y, C, LANES), BF16),
            jax.ShapeDtypeStruct((SPAN_X, SPAN_Y, C, LANES), BF16),
            jax.ShapeDtypeStruct((devices, 4, LANES), F32),
            jax.ShapeDtypeStruct((C, LANES), F32),
        ),
        in_specs=[in_vmem] * 5,
        out_specs=(in_vmem,) * 4,
        scratch_shapes=scratch,
        compiler_params=pltpu.CompilerParams(
            collective_id=0, has_side_effects=True, vmem_limit_bytes=60 * 1024 * 1024
        ),
    )(by_rows(x_a), by_rows(x_b), by_rows(grad_out), weights, params)

    def by_channels(block):
        return block.transpose(2, 0, 1, 3)

    kernels = kernels.reshape(4, 8, 4, 2, 2, LANES).transpose(3, 0, 2, 4, 1, 5)
    grads = kernels.reshape(2, C, 8 * LANES)[:, :, :FLAT].reshape(2, C, 3, 3, 3, C).transpose(0, 2, 3, 4, 1, 5)
    return (by_channels(y_a), by_channels(dx_b), grads[0], grads[1], norms[:, :4].T)


def solution(mesh):
    split = P(None, "gx", "gy", "gz")
    voxels = float(SPAN_X * SPAN_Y * LANES * mesh.size)
    return jax.shard_map(
        functools.partial(body, voxels),
        mesh=mesh,
        in_specs=(split, split, P(), P(), P(), P(), P(), P(), split),
        out_specs=(split, split, P(), P(), P()),
        check_vma=False,
    )
```

```python
import functools
import math

import jax
import jax.numpy as jnp
from jax import lax
from jax.experimental import pallas as pl
from jax.experimental.pallas import tpu as pltpu
from jax.sharding import PartitionSpec as P

F32 = jnp.float32
BF16 = jnp.bfloat16
EPSILON = 1e-05
C = 32
LANES = 128
SPAN_X, SPAN_Y = 2, 16
PAD_X, PAD_Y = SPAN_X + 2, SPAN_Y + 2
TAPS = 3 * C
DEPTH = PAD_X * 3 * TAPS
FLAT = 9 * TAPS
GROUP = 4
AXES = ("gx", "gy", "gz")
MESH = pl.DeviceIdType.MESH


def sigmoid(value):
    return 0.5 + 0.5 * jnp.tanh(0.5 * value)


def rolled(tile, shift):
    shift = shift % LANES
    return pltpu.roll(tile, shift, 1) if shift else tile


class Halo:
    def __init__(
        self, rows, near, far_y, turn, far_x, edge, side, send, recv, place, volumes
    ):
        self.rows, self.near, self.far_y, self.turn, self.far_x = rows, near, far_y, turn, far_x
        self.side = side
        self.edge, self.send, self.recv, self.place, self.volumes = edge, send, recv, place, volumes
        self.count = 0
        self.sent = []

    def has(self, axis, step):
        me, size = self.place[axis]
        return me > 0 if step < 0 else me < size - 1

    def push(self, source, target, axis, step):
        me, size = self.place[axis]
        index = self.count
        self.count += 1
        copy = pltpu.make_async_remote_copy(
            src_ref=source,
            dst_ref=target,
            send_sem=self.send.at[index],
            recv_sem=self.recv.at[index],
            device_id={axis: lax.rem(me + step + size, size)},
            device_id_type=MESH,
        )

        @pl.when(self.has(axis, step))
        def _():
            copy.start()

        self.sent.append((copy, self.has(axis, step)))
        return copy, self.has(axis, -step)

    def faces_x(self, volume):
        rows = self.rows
        inner = pl.ds(1, SPAN_Y)
        down = self.push(
            rows.at[volume, 1, inner], rows.at[volume, PAD_X - 1, inner], "gx", -1
        )
        up = self.push(rows.at[volume, SPAN_X, inner], rows.at[volume, 0, inner], "gx", 1)
        return [down, up]

    def faces_y(self):
        rows, inner, every = self.rows, pl.ds(1, SPAN_X), pl.ds(0, self.volumes)
        down = self.push(
            rows.at[every, inner, 1], rows.at[every, inner, PAD_Y - 1], "gy", -1
        )
        up = self.push(rows.at[every, inner, SPAN_Y], rows.at[every, inner, 0], "gy", 1)
        return [down, up]

    def columns_z(self):
        down = self.push(self.edge.at[0], self.near.at[1], "gz", -1)
        up = self.push(self.edge.at[1], self.near.at[0], "gz", 1)
        return [down, up]

    def columns_y(self):
        down = self.push(self.near, self.far_y.at[1], "gy", -1)
        up = self.push(self.near, self.far_y.at[0], "gy", 1)
        return [down, up]

    def columns_x(self, lane):
        inside = lax.rem(lane, 32)
        down = jnp.zeros((C, LANES), F32)
        up = jnp.zeros((C, LANES), F32)
        for side in range(2):
            for volume in range(self.volumes):
                own = self.near[side, volume].astype(F32)
                low = pltpu.roll(self.far_y[0, side, volume].astype(F32), LANES - 16, 1)
                high = pltpu.roll(self.far_y[1, side, volume].astype(F32), 16, 1)
                own = jnp.where(inside == 0, low, jnp.where(inside == PAD_Y - 1, high, own))
                self.side[volume, side] = own
                at = 32 * (side * self.volumes + volume)
                here = lane // 32 == at // 32
                down = jnp.where(here, rolled(own, at - 32), down)
                up = jnp.where(here, rolled(own, at - 64), up)
        self.turn[0] = down.astype(BF16)
        self.turn[1] = up.astype(BF16)
        down = self.push(self.turn.at[0], self.far_x.at[1], "gx", -1)
        up = self.push(self.turn.at[1], self.far_x.at[0], "gx", 1)
        return [down, up]

    def corners_x(self):
        rows, every = self.rows, pl.ds(0, self.volumes)
        result = []
        for at in (0, PAD_Y - 1):
            result.append(
                self.push(rows.at[every, 1, at], rows.at[every, PAD_X - 1, at], "gx", -1)
            )
            result.append(
                self.push(rows.at[every, SPAN_X, at], rows.at[every, 0, at], "gx", 1)
            )
        return result

    def merged(self, side, volume, lane):
        at = 32 * (side * self.volumes + volume)
        low = rolled(self.far_x[0].astype(F32), -at)
        high = rolled(self.far_x[1].astype(F32), 96 - at)
        return jnp.where(lane < 32, low, jnp.where(lane >= 96, high, self.side[volume, side]))

    @staticmethod
    def arrive(pushes):
        for copy, present in pushes:

            @pl.when(present)
            def _(copy=copy):
                copy.wait_recv()

    def drain(self):
        for copy, present in self.sent:

            @pl.when(present)
            def _(copy=copy):
                copy.wait_send()


def kernel(
    voxels,
    x_a, x_b, grad, w_first, w_second, gain_first, bias_first, gain_second, bias_second,
    y_out, dx_out, gw_first, gw_second, norm_out,
    block_a, block_b, block_g, block_y, block_dx, kernel_1, kernel_2, weights, stage,
    taps_x, taps_h, taps_d2, taps_d1,
    rows_x, rows_g, rows_1, rows_2, rows_e,
    near_x, near_g, near_1, near_2, near_e,
    fary_x, fary_g, fary_1, fary_2, fary_e,
    turn_x, turn_g, turn_1, turn_2, turn_e,
    farx_x, farx_g, farx_1, farx_2, farx_e,
    edge_x, edge_g, edge_1, edge_2, edge_e,
    side_x, side_g, side_1, side_2, side_e,
    side_h,
    conv_1, conv_2, back_1,
    sums,
    norms, slopes, early_out, early_in, late_out, late_in, gathered, pairs,
    halo_send, halo_recv, sums_send, sums_recv, gw_send, gw_recv, local,
):
    loads = [
        pltpu.make_async_copy(source, target, local.at[index])
        for index, (source, target) in enumerate((
            (x_a, block_a), (x_b, block_b), (grad, block_g), (w_first, kernel_1),
            (w_second, kernel_2),
        ))
    ]
    for load in loads:
        load.start()
    place = {axis: (lax.axis_index(axis), lax.axis_size(axis)) for axis in AXES}
    for near in (near_x, near_g, near_1, near_2, near_e):
        near[...] = jnp.zeros_like(near)
    for chunks in (early_out, late_out):
        for j in range(4):
            chunks[32 * j + 28 : 32 * j + 32] = jnp.zeros((4, 4, LANES), F32)
    barrier = pltpu.get_barrier_semaphore()
    count = place["gx"][1] * place["gy"][1] * place["gz"][1]
    flat = (place["gx"][0] * place["gy"][1] + place["gy"][0]) * place["gz"][1] + place["gz"][0]

    chip_x, chip_y = place["gy"][0], place["gz"][0] // 2
    chip_z = place["gx"][0] // 2 * 2 + lax.rem(place["gz"][0], 2)
    core = lax.rem(place["gx"][0], 2)

    def other(step):
        return lax.rem(flat + step, count)

    def fan_out(source_of, target, send, recv):
        spots = []
        for step_z, step_core in ((2, 1), (2, 0), (1, 1), (3, 1), (1, 0), (3, 0), (0, 1), (0, 0)):
            to_z, to_core = lax.rem(chip_z + step_z, 4), lax.rem(core + step_core, 2)
            spots.append(to_z // 2 * 64 + to_core * 32 + lax.rem(to_z, 2))

        def copies(plane, chosen):
            to_x = lax.rem(chip_x + plane // 4 + 1, 4)
            to_y = lax.rem(chip_y + lax.rem(plane, 4) + 1, 4)
            for spot in chosen:
                to = spot + to_x * 8 + to_y * 2
                pltpu.make_async_remote_copy(
                    src_ref=source_of(to), dst_ref=target, send_sem=send, recv_sem=recv,
                    device_id=to, device_id_type=pl.DeviceIdType.LOGICAL,
                ).start()

        def most(plane, carry):
            copies(plane, spots[:-1])
            return carry

        def rest(plane, carry):
            copies(plane, spots[-1:])
            return carry

        lax.fori_loop(0, 16, most, 0)
        lax.fori_loop(0, 15, rest, 0)

    def fan_in(slots, semaphore):
        part = slots.at[pl.ds(0, count - 1)]
        pltpu.make_async_copy(part, part, semaphore).wait()

    def greet(step, carry):
        pl.semaphore_signal(
            barrier, inc=1, device_id=other(step), device_id_type=pl.DeviceIdType.LOGICAL
        )
        return carry

    lax.fori_loop(1, count, greet, 0)

    lane = lax.broadcasted_iota(jnp.int32, (C, LANES), 1)
    halos = []
    for index, (rows, near, fary, turn, farx, edge, side, volumes) in enumerate((
        (rows_x, near_x, fary_x, turn_x, farx_x, edge_x, side_x, 2),
        (rows_g, near_g, fary_g, turn_g, farx_g, edge_g, side_g, 1),
        (rows_1, near_1, fary_1, turn_1, farx_1, edge_1, side_1, 2),
        (rows_2, near_2, fary_2, turn_2, farx_2, edge_2, side_2, 1),
        (rows_e, near_e, fary_e, turn_e, farx_e, edge_e, side_e, 1),
    )):
        halos.append(
            Halo(rows, near, fary, turn, farx, edge, side, halo_send.at[index],
                 halo_recv.at[index], place, volumes)
        )
    halo_x, halo_g, halo_1, halo_2, halo_e = halos

    low_x, high_x = place["gx"][0] > 0, place["gx"][0] < place["gx"][1] - 1
    low_y, high_y = place["gy"][0] > 0, place["gy"][0] < place["gy"][1] - 1
    low_z, high_z = place["gz"][0] > 0, place["gz"][0] < place["gz"][1] - 1

    def keep(at_x, at_y):
        held_x = low_x if at_x == 0 else high_x if at_x == PAD_X - 1 else None
        if isinstance(at_y, int):
            held_y = low_y if at_y == 0 else high_y if at_y == PAD_Y - 1 else None
        else:
            held_y = jnp.logical_and(
                jnp.logical_or(at_y > 0, low_y), jnp.logical_or(at_y < PAD_Y - 1, high_y)
            )
        if held_x is None:
            return held_y
        return held_x if held_y is None else jnp.logical_and(held_x, held_y)

    def lane_keep(side):
        spot_x, spot_y = lane // 32, lax.rem(lane, 32)
        bad = jnp.zeros((C, LANES), jnp.int32)
        for hit, present in (
            (spot_x == 0, low_x), (spot_x == PAD_X - 1, high_x),
            (spot_y == 0, low_y), (spot_y == PAD_Y - 1, high_y),
        ):
            missing = jnp.where(present, 0, 1)
            bad = bad + jnp.where(hit, missing, 0)
        bad = bad + jnp.where(low_z if side == 0 else high_z, 0, 1)
        return bad == 0

    def extract(tile, spot, carry):
        first, last = carry
        first = jnp.where(lane == spot, pltpu.roll(tile, spot, 1), first)
        last = jnp.where(lane == spot, pltpu.roll(tile, lax.rem(spot + 1, LANES), 1), last)
        return first, last

    def put_taps(taps, volume, at_x, at_y, tile, side_lo, side_hi):
        spot = at_x * 32 + at_y
        left = jnp.where(
            lane == 0,
            pltpu.roll(side_lo, lax.rem(LANES - spot, LANES), 1),
            pltpu.roll(tile, 1, 1),
        )
        right = jnp.where(
            lane == LANES - 1,
            pltpu.roll(side_hi, LANES - 1 - spot, 1),
            pltpu.roll(tile, LANES - 1, 1),
        )
        taps[volume, at_x, at_y, 0:C] = left.astype(BF16)
        taps[volume, at_x, at_y, C : 2 * C] = tile.astype(BF16)
        taps[volume, at_x, at_y, 2 * C : 3 * C] = right.astype(BF16)

    def build(taps, volume, outer, inner, sides):
        low, high = sides
        zero = jnp.zeros((C, LANES), F32)

        def held(at_x, at_y):
            tile = outer(at_x, at_y)
            return jnp.where(keep(at_x, at_y), tile, zero)

        for at_x in (1, 2):

            def step(block, carry, at_x=at_x):
                for k in range(8):
                    at_y = block * 8 + k
                    put_taps(
                        taps, volume, at_x, at_y + 1, inner(at_x - 1, at_y), low[...], high[...]
                    )
                return carry

            lax.fori_loop(0, 2, step, 0)
            for at_y in (0, PAD_Y - 1):
                put_taps(taps, volume, at_x, at_y, held(at_x, at_y), low[...], high[...])
        for at_x in (0, PAD_X - 1):

            def step(block, carry, at_x=at_x):
                for k in range(6):
                    at_y = block * 6 + k
                    put_taps(taps, volume, at_x, at_y, held(at_x, at_y), low[...], high[...])
                return carry

            lax.fori_loop(0, 3, step, 0)

    def convolve(taps, volume, weight, emit, carry):
        def step(block, carry):
            first = block * GROUP
            columns = [
                taps[volume, :, pl.ds(first + k, 3)].reshape(DEPTH, LANES) for k in range(GROUP)
            ]
            total = jnp.dot(
                weights[weight],
                jnp.concatenate(columns, axis=1),
                preferred_element_type=F32,
            )
            for k in range(GROUP):
                for at_x in range(SPAN_X):
                    tile = total[at_x * C : (at_x + 1) * C, k * LANES : (k + 1) * LANES]
                    carry = emit(at_x, first + k, tile, carry)
            return carry

        return lax.fori_loop(0, SPAN_Y // GROUP, step, carry)

    def kernel_grad(taps, volume, row_of, out, first_row, plain=False):
        high = SPAN_X * C + (16 if plain else 0)

        def step(block, total):
            first = block * GROUP
            left, right = [], []
            for k in range(GROUP):
                rows = [row_of(at_x, first + k) for at_x in range(SPAN_X)]
                if plain:
                    rows.append(jnp.ones((16, LANES), BF16))
                left.append(jnp.concatenate(rows, axis=0))
                right.append(taps[volume, :, pl.ds(first + k, 3)].reshape(DEPTH, LANES))
            return total + lax.dot_general(
                jnp.concatenate(left, axis=1),
                jnp.concatenate(right, axis=1),
                (((1,), (1,)), ((), ())),
                preferred_element_type=F32,
            )

        total = lax.fori_loop(0, SPAN_Y // GROUP, step, jnp.zeros((high, DEPTH), F32))
        slab = 3 * TAPS

        def wide(value):
            return jnp.concatenate(
                [value, jnp.zeros((value.shape[0], 7 * LANES - FLAT), F32)], axis=1
            )

        both = wide(total[0:C, 0:FLAT] + total[C : 2 * C, slab : slab + FLAT])
        if plain:
            alone = total[2 * C : 2 * C + 1]
            alone = wide(alone[:, 0:FLAT] + alone[:, slab : slab + FLAT])
        for k in range(7):
            lanes = slice(LANES * k, LANES * (k + 1))
            for pair in range(16):
                spot = (pair // 4 * 8 + k) * 4 + pair % 4
                out[spot, first_row : first_row + 2] = both[2 * pair : 2 * pair + 2, lanes]
                if plain:
                    out[spot, 2:3] = alone[:, lanes]

    channel = lax.broadcasted_iota(jnp.int32, (C, LANES), 0)

    def pack(columns):
        whole = jnp.zeros((C, LANES), F32)
        for k, column in enumerate(columns):
            whole = whole + jnp.where(lane == channel + 32 * k, column, 0.0)
        return jnp.sum(whole, axis=0, keepdims=True)

    def unpack(row, number):
        return [
            jnp.sum(jnp.where(lane == channel + 32 * k, row, 0.0), axis=1, keepdims=True)
            for k in range(number)
        ]

    class Total:
        def __init__(self, index):
            self.slots, self.index = sums.at[index], index

        def start(self, row):
            mine = self.slots.at[flat]
            mine[...] = row

            fan_out(
                lambda to: mine, mine, sums_send.at[self.index], sums_recv.at[self.index]
            )

        def finish(self):
            fan_in(self.slots, sums_recv.at[self.index])
            return jnp.sum(self.slots[...], axis=0)

        def drain(self):
            fan_in(self.slots, sums_send.at[self.index])

    totals = [Total(index) for index in range(4)]

    def second(halo, phase):
        halo.arrive(phase)
        return halo.columns_y(), halo.corners_x()

    def third(halo, phase):
        halo.arrive(phase)
        return halo.columns_x(lane)

    small_lane = lax.broadcasted_iota(jnp.int32, (C, C), 1)
    small_row = lax.broadcasted_iota(jnp.int32, (C, C), 0)

    def column(row):
        return jnp.sum(jnp.where(small_lane == small_row, row[...], 0.0), axis=1, keepdims=True)

    gain_1, bias_1, gain_2, bias_2 = (
        column(row) for row in (gain_first, bias_first, gain_second, bias_second)
    )

    def stack_weights(source, forward, backward):
        tiles = [
            jnp.concatenate(
                [source[tap].astype(F32) for tap in range(4 * k, min(4 * k + 4, 27))]
                + ([jnp.zeros((C, C), F32)] if k == 6 else []),
                axis=1,
            )
            for k in range(7)
        ]
        turned = [tile.T for tile in tiles]
        pieces = [turned[tap // 4][C * (tap % 4) : C * (tap % 4) + C] for tap in range(26, -1, -1)]
        back = [jnp.concatenate((pieces + pieces[:1])[4 * k : 4 * k + 4], axis=1) for k in range(7)]
        for index, parts in ((forward, tiles), (backward, back)):
            last = jnp.where(lane < 96, parts[6], 0.0)
            empty = jnp.zeros((C, LANES), F32)
            top = parts[:6] + [last, empty, empty]
            moved = [pltpu.roll(part, 32, 1) for part in parts[:6] + [last]]
            low = [empty, empty]
            for k in range(7):
                low.append(jnp.where(lane < 32, moved[k - 1] if k else empty, moved[k]))
            for k in range(9):
                weights[index, 0:C, LANES * k : LANES * (k + 1)] = top[k].astype(BF16)
                weights[index, C : 2 * C, LANES * k : LANES * (k + 1)] = low[k].astype(BF16)

    zero = jnp.zeros((C, LANES), F32)

    def take(load, source, rows, edge, at):
        load.wait()
        for at_x in range(SPAN_X):
            rows[at, at_x + 1, 1 : SPAN_Y + 1] = jnp.swapaxes(
                source[:, at_x].astype(F32), 0, 1
            ).astype(BF16)
        for at_x in range(SPAN_X):

            def step(block, carry, at_x=at_x):
                for k in range(8):
                    at_y = block * 8 + k
                    carry = extract(
                        rows[at, at_x + 1, at_y + 1].astype(F32),
                        (at_x + 1) * 32 + at_y + 1,
                        carry,
                    )
                return carry

            carry = lax.fori_loop(0, 2, step, (zero, zero) if at_x == 0 else carry)
        edge[0, at] = carry[0].astype(BF16)
        edge[1, at] = carry[1].astype(BF16)

    take(loads[0], block_a, rows_x, edge_x, 0)
    take(loads[1], block_b, rows_x, edge_x, 1)

    pl.semaphore_wait(barrier, count - 1)

    phase = halo_x.columns_z() + halo_x.faces_y()
    waits_x = [halo_x.faces_x(0)]
    loads[3].wait()
    loads[4].wait()
    stack_weights(kernel_1, 0, 3)
    stack_weights(kernel_2, 1, 2)
    phase, corners = second(halo_x, phase)
    take(loads[2], block_g, rows_g, edge_g, 0)
    last = third(halo_x, phase)
    waits_x.append(halo_x.faces_x(1))
    halo_x.arrive(corners)
    halo_x.arrive(last)
    ok = [lane_keep(side) for side in range(2)]
    for side in range(2):
        for volume in range(2):
            tile = halo_x.merged(side, volume, lane)
            side_x[volume, side] = jnp.where(ok[side], tile, 0.0)

    def stats_emit(keep_f32, halo, volume):
        def emit(at_x, at_y, tile, carry):
            total, squares, first, last = carry
            keep_f32[volume, at_x, at_y] = tile
            halo.rows[halo_of[volume], at_x + 1, at_y + 1] = tile.astype(BF16)
            first, last = extract(tile, (at_x + 1) * 32 + at_y + 1, (first, last))
            return total + tile, squares + tile * tile, first, last

        halo_of = {0: 0, 1: 1}
        return emit

    columns = []
    waits = []
    for volume in range(2):
        halo_x.arrive(waits_x[volume])
        build(
            taps_x, volume,
            lambda at_x, at_y, volume=volume: rows_x[volume, at_x, at_y].astype(F32),
            lambda at_x, at_y, volume=volume: rows_x[volume, at_x + 1, at_y + 1].astype(F32),
            (side_x.at[volume, 0], side_x.at[volume, 1]),
        )
        total, squares, first, last = convolve(
            taps_x, volume, 0, stats_emit(conv_1, halo_1, volume), (zero,) * 4
        )
        edge_1[0, volume] = first.astype(BF16)
        edge_1[1, volume] = last.astype(BF16)
        if volume == 0:
            waits += halo_1.faces_x(volume)
        columns += [
            jnp.sum(total, axis=1, keepdims=True), jnp.sum(squares, axis=1, keepdims=True)
        ]
    totals[0].start(pack(columns))
    phase = halo_1.columns_z() + halo_1.faces_y()
    waits += halo_1.faces_x(1)
    phase, corners = second(halo_1, phase)
    last = third(halo_1, phase)
    row = totals[0].finish()
    halo_1.arrive(waits + corners + last)
    phase_g = halo_g.columns_z() + halo_g.faces_y()
    waits_g = halo_g.faces_x(0)
    stats = unpack(row, 4)

    def moments(total, squares):
        mean = total / voxels
        scale = lax.rsqrt(squares / voxels - mean * mean + EPSILON)
        return mean, scale

    columns = []
    affine_1 = None
    for volume in range(2):
        mean, scale = moments(stats[2 * volume], stats[2 * volume + 1])
        slope = jnp.broadcast_to(gain_1 * scale, (C, LANES))
        shift = jnp.broadcast_to(bias_1 - mean * gain_1 * scale, (C, LANES))

        def active(value, slope=slope, shift=shift):
            pre = value * slope + shift
            return pre * sigmoid(pre)

        norm_slope = jnp.broadcast_to(scale, (C, LANES))
        norm_shift = jnp.broadcast_to(-mean * scale, (C, LANES))

        def own_row(at_x, at_y, volume, active, norm_slope=norm_slope, norm_shift=norm_shift):
            value = conv_1[volume, at_x, at_y]
            if volume == 1:
                norms[at_x, at_y] = (value * norm_slope + norm_shift).astype(BF16)
            return active(value)

        for side in range(2):
            tile = halo_1.merged(side, volume, lane)
            side_1[volume, side] = tile
            side_h[volume, side] = jnp.where(ok[side], active(tile), 0.0)
        build(
            taps_h, volume,
            lambda at_x, at_y, volume=volume: active(rows_1[volume, at_x, at_y].astype(F32)),
            functools.partial(own_row, volume=volume, active=active),
            (side_h.at[volume, 0], side_h.at[volume, 1]),
        )
        if volume == 0:

            def emit(at_x, at_y, tile, carry):
                total, squares = carry
                conv_2[0, at_x, at_y] = tile
                return total + tile, squares + tile * tile

            total, squares = convolve(taps_h, 0, 1, emit, (zero,) * 2)
            phase_g, corners_g = second(halo_g, phase_g)
        else:

            def emit(at_x, at_y, tile, carry):
                total, squares, first, last = carry
                conv_2[1, at_x, at_y] = tile
                rows_2[0, at_x + 1, at_y + 1] = tile.astype(BF16)
                first, last = extract(tile, (at_x + 1) * 32 + at_y + 1, (first, last))
                return total + tile, squares + tile * tile, first, last

            total, squares, first, last = convolve(taps_h, 1, 1, emit, (zero,) * 4)
            edge_2[0, 0] = first.astype(BF16)
            edge_2[1, 0] = last.astype(BF16)
        columns += [
            jnp.sum(total, axis=1, keepdims=True), jnp.sum(squares, axis=1, keepdims=True)
        ]
    mean_1, scale_1 = mean, scale
    totals[1].start(pack(columns))
    phase = halo_2.columns_z() + halo_2.faces_y()
    waits = halo_2.faces_x(0)
    last_g = third(halo_g, phase_g)
    kernel_grad(taps_x, 1, lambda at_x, at_y: norms[at_x, at_y], early_out, 0, plain=True)
    fan_out(
        lambda to: early_out.at[to], early_in.at[flat], gw_send.at[0], gw_recv.at[0]
    )
    early_in[flat] = early_out[flat]
    stats = unpack(totals[1].finish(), 4)

    mean_2, scale_2 = moments(stats[2], stats[3])

    def layer_of(mean, scale, gain, bias):
        norm_slope = jnp.broadcast_to(scale, (C, LANES))
        norm_shift = jnp.broadcast_to(-mean * scale, (C, LANES))
        wide_gain = jnp.broadcast_to(gain, (C, LANES))
        wide_bias = jnp.broadcast_to(bias, (C, LANES))

        def slope_of(value, upstream):
            normed = value * norm_slope + norm_shift
            pre = wide_gain * normed + wide_bias
            sigma = sigmoid(pre)
            return upstream * (sigma * (1.0 + pre * (1.0 - sigma))), normed

        return slope_of

    def delta_of(slope_of, sum_d, sum_x, gain, scale):
        wide_d = jnp.broadcast_to(sum_d / voxels, (C, LANES))
        wide_x = jnp.broadcast_to(sum_x / voxels, (C, LANES))
        factor = jnp.broadcast_to(gain * scale, (C, LANES))

        def delta(value, upstream):
            slope, normed = slope_of(value, upstream)
            return factor * (slope - wide_d - normed * wide_x)

        return delta

    slope_2 = layer_of(mean_2, scale_2, gain_2, bias_2)

    def sum_rows(slope_of, value_of, upstream_of):
        carry = (zero, zero)
        for at_x in range(SPAN_X):

            def step(block, carry, at_x=at_x):
                total, weighted = carry
                for k in range(8):
                    at_y = block * 8 + k
                    slope, normed = slope_of(value_of(at_x, at_y), upstream_of(at_x, at_y))
                    total, weighted = total + slope, weighted + slope * normed
                return total, weighted

            carry = lax.fori_loop(0, 2, step, carry)
        return [jnp.sum(part, axis=1, keepdims=True) for part in carry]

    columns = sum_rows(
        slope_2,
        lambda at_x, at_y: conv_2[1, at_x, at_y],
        lambda at_x, at_y: rows_g[0, at_x + 1, at_y + 1].astype(F32),
    )
    totals[2].start(pack(columns))
    phase, corners = second(halo_2, phase)

    mean_a, scale_a = moments(stats[0], stats[1])
    slope_a = jnp.broadcast_to(gain_2 * scale_a, (C, LANES))
    shift_a = jnp.broadcast_to(bias_2 - mean_a * gain_2 * scale_a, (C, LANES))
    for at_x in range(SPAN_X):

        def step(block, carry, at_x=at_x):
            for k in range(8):
                at_y = block * 8 + k
                pre = conv_2[0, at_x, at_y] * slope_a + shift_a
                stage[at_x, at_y] = pre * sigmoid(pre)
            return carry

        lax.fori_loop(0, 2, step, 0)
        block_y[:, at_x] = jnp.swapaxes(stage[at_x], 0, 1).astype(BF16)
    store_y = pltpu.make_async_copy(block_y, y_out, local.at[5])
    store_y.start()

    last = third(halo_2, phase)
    halo_g.arrive(waits_g + corners_g + last_g)
    halo_2.arrive(waits + corners + last)
    sum_d2, sum_x2 = unpack(totals[2].finish(), 2)

    delta_2 = delta_of(slope_2, sum_d2, sum_x2, gain_2, scale_2)
    for side in range(2):
        tile = delta_2(halo_2.merged(side, 0, lane), halo_g.merged(side, 0, lane))
        side_2[0, side] = jnp.where(ok[side], tile, 0.0)
    build(
        taps_d2, 0,
        lambda at_x, at_y: delta_2(
            rows_2[0, at_x, at_y].astype(F32), rows_g[0, at_x, at_y].astype(F32)
        ),
        lambda at_x, at_y: delta_2(
            conv_2[1, at_x, at_y], rows_g[0, at_x + 1, at_y + 1].astype(F32)
        ),
        (side_2.at[0, 0], side_2.at[0, 1]),
    )
    slope_1 = layer_of(mean_1, scale_1, gain_1, bias_1)

    def emit(at_x, at_y, tile, carry):
        total, weighted, first, last = carry
        back_1[at_x, at_y] = tile
        rows_e[0, at_x + 1, at_y + 1] = tile.astype(BF16)
        first, last = extract(tile, (at_x + 1) * 32 + at_y + 1, (first, last))
        slope, normed = slope_1(conv_1[1, at_x, at_y], tile)
        slopes[at_x, at_y] = slope.astype(BF16)
        return total + slope, weighted + slope * normed, first, last

    total, weighted, first, last = convolve(taps_d2, 0, 2, emit, (zero,) * 4)
    edge_e[0, 0] = first.astype(BF16)
    edge_e[1, 0] = last.astype(BF16)
    columns = [
        jnp.sum(total, axis=1, keepdims=True), jnp.sum(weighted, axis=1, keepdims=True)
    ]
    totals[3].start(pack(columns))
    phase = halo_e.columns_z() + halo_e.faces_y()
    waits = halo_e.faces_x(0)
    kernel_grad(taps_x, 1, lambda at_x, at_y: slopes[at_x, at_y], late_out, 0)
    phase, corners = second(halo_e, phase)
    kernel_grad(
        taps_h, 1, lambda at_x, at_y: taps_d2[0, at_x + 1, at_y + 1, C : 2 * C], late_out, 2
    )
    last = third(halo_e, phase)
    fan_out(lambda to: late_out.at[to], late_in.at[flat], gw_send.at[1], gw_recv.at[1])
    late_in[flat] = late_out[flat]
    sum_d1, sum_x1 = unpack(totals[3].finish(), 2)
    halo_e.arrive(waits + corners + last)

    delta_1 = delta_of(slope_1, sum_d1, sum_x1, gain_1, scale_1)
    for side in range(2):
        tile = delta_1(side_1[1, side], halo_e.merged(side, 0, lane))
        side_e[0, side] = jnp.where(ok[side], tile, 0.0)
    build(
        taps_d1, 0,
        lambda at_x, at_y: delta_1(
            rows_1[1, at_x, at_y].astype(F32), rows_e[0, at_x, at_y].astype(F32)
        ),
        lambda at_x, at_y: delta_1(conv_1[1, at_x, at_y], back_1[at_x, at_y]),
        (side_e.at[0, 0], side_e.at[0, 1]),
    )
    whole = 1.0 / math.sqrt(voxels)
    for k, factor in enumerate(
        (gain_1 * scale_1 * whole, sum_d1 / voxels, sum_x1 / voxels)
    ):
        tile = jnp.broadcast_to(factor, (C, LANES))
        for pair in range(16):
            pairs[k, pair] = tile[2 * pair : 2 * pair + 2]
    fan_in(early_in, gw_recv.at[0])
    early = jnp.sum(early_in[...], axis=0)
    at = flat // 32 * 4 + lax.rem(flat, 4)
    fan_in(late_in, gw_recv.at[1])
    late = jnp.sum(late_in[...], axis=0)
    gathered[flat, 0:2] = pairs[0, at] * (
        late[0:2] - pairs[1, at] * early[2:3] - pairs[2, at] * early[0:2]
    )
    gathered[flat, 2:4] = late[2:4] * whole
    mine = gathered.at[flat]
    fan_out(lambda to: mine, mine, gw_send.at[2], gw_recv.at[2])

    def emit(at_x, at_y, tile, carry):
        stage[at_x, at_y] = tile
        return carry

    convolve(taps_d1, 0, 3, emit, 0)
    for at_x in range(SPAN_X):
        block_dx[:, at_x] = jnp.swapaxes(stage[at_x], 0, 1).astype(BF16)
    store_dx = pltpu.make_async_copy(block_dx, dx_out, local.at[6])
    store_dx.start()

    for k, total in enumerate((sum_x1, sum_d1, sum_x2, sum_d2)):
        norm_out[k : k + 1] = whole * jnp.sum(
            jnp.where(small_lane == small_row, total, 0.0), axis=0, keepdims=True
        )
    fan_in(gathered, gw_recv.at[2])
    for member, out in ((0, gw_first), (1, gw_second)):
        for k in range(7):
            tile = jnp.concatenate(
                [
                    gathered[(pair // 4 * 8 + k) * 4 + pair % 4, 2 * member : 2 * member + 2]
                    for pair in range(16)
                ],
                axis=0,
            )
            for tap in range(4 * k, min(4 * k + 4, 27)):
                out[tap] = tile[:, C * (tap % 4) : C * (tap % 4) + C]

    store_y.wait()
    store_dx.wait()
    for halo in halos:
        halo.drain()
    for total in totals:
        total.drain()
    for k, chunks in enumerate((early_out, late_out, gathered)):
        fan_in(chunks, gw_send.at[k])


def body(voxels, x_a, x_b, w_first, w_second, gain_first, bias_first, gain_second, bias_second,
         grad_out):
    def sized(*shape, kind=BF16):
        return pltpu.VMEM(shape, kind)

    volumes = (2, 1, 2, 1, 1)
    devices = math.prod(lax.axis_size(axis) for axis in AXES)
    block = (C, SPAN_X, SPAN_Y, LANES)
    scratch = [sized(*block)] * 5 + [sized(27, C, C)] * 2
    scratch += [
        sized(4, SPAN_X * C, DEPTH), sized(SPAN_X, SPAN_Y, C, LANES, kind=F32)
    ]
    scratch += [sized(count, PAD_X, PAD_Y, TAPS, LANES) for count in (2, 2, 1, 1)]
    scratch += [sized(count, PAD_X, PAD_Y, C, LANES) for count in volumes]
    scratch += [sized(2, count, C, LANES) for count in volumes]
    scratch += [sized(2, 2, count, C, LANES) for count in volumes]
    scratch += [sized(2, C, LANES) for count in volumes]
    scratch += [sized(2, C, LANES) for count in volumes]
    scratch += [sized(2, count, C, LANES) for count in volumes]
    scratch += [sized(count, 2, C, LANES, kind=F32) for count in volumes]
    scratch += [sized(2, 2, C, LANES, kind=F32)]
    scratch += [
        sized(2, SPAN_X, SPAN_Y, C, LANES, kind=F32),
        sized(2, SPAN_X, SPAN_Y, C, LANES, kind=F32),
        sized(SPAN_X, SPAN_Y, C, LANES, kind=F32),
        sized(4, devices, 1, LANES, kind=F32),
        sized(SPAN_X, SPAN_Y, C, LANES),
        sized(SPAN_X, SPAN_Y, C, LANES),
        sized(devices, 4, LANES, kind=F32),
        sized(devices, 4, LANES, kind=F32),
        sized(devices, 4, LANES, kind=F32),
        sized(devices, 4, LANES, kind=F32),
        sized(devices, 4, LANES, kind=F32),
        sized(3, 16, 2, LANES, kind=F32),
        pltpu.SemaphoreType.DMA((5, 24)),
        pltpu.SemaphoreType.DMA((5, 24)),
        pltpu.SemaphoreType.DMA((4,)),
        pltpu.SemaphoreType.DMA((4,)),
        pltpu.SemaphoreType.DMA((3,)),
        pltpu.SemaphoreType.DMA((3,)),
        pltpu.SemaphoreType.DMA((7,)),
    ]
    in_vmem = pl.BlockSpec(memory_space=pltpu.VMEM)
    anywhere = pl.BlockSpec(memory_space=pl.ANY)
    taps = jax.ShapeDtypeStruct((27, C, C), F32)
    y_a, dx_b, grad_first, grad_second, norms = pl.pallas_call(
        functools.partial(kernel, voxels),
        out_shape=(
            jax.ShapeDtypeStruct(block, BF16),
            jax.ShapeDtypeStruct(block, BF16),
            taps,
            taps,
            jax.ShapeDtypeStruct((4, C), F32),
        ),
        in_specs=[anywhere] * 5 + [in_vmem] * 4,
        out_specs=(anywhere,) * 2 + (in_vmem,) * 3,
        scratch_shapes=scratch,
        compiler_params=pltpu.CompilerParams(
            collective_id=0, has_side_effects=True, vmem_limit_bytes=60 * 1024 * 1024
        ),
    )(
        x_a, x_b, grad_out, w_first.reshape(27, C, C), w_second.reshape(27, C, C),
        *(row.reshape(1, C) for row in (gain_first, bias_first, gain_second, bias_second)),
    )
    return (
        y_a, dx_b, grad_first.reshape(3, 3, 3, C, C), grad_second.reshape(3, 3, 3, C, C), norms
    )


def solution(mesh):
    split = P(None, "gx", "gy", "gz")
    voxels = float(SPAN_X * SPAN_Y * LANES * mesh.size)
    return jax.shard_map(
        functools.partial(body, voxels),
        mesh=mesh,
        in_specs=(split, split, P(), P(), P(), P(), P(), P(), split),
        out_specs=(split, split, P(), P(), P()),
        check_vma=False,
    )
```

```python
import functools
import math

import jax
import jax.numpy as jnp
from jax import lax
from jax.experimental import pallas as pl
from jax.experimental.pallas import tpu as pltpu
from jax.sharding import PartitionSpec as P

F32 = jnp.float32
BF16 = jnp.bfloat16
EPSILON = 1e-05
C = 32
LANES = 128
SPAN_X, SPAN_Y = 2, 16
PAD_X, PAD_Y = SPAN_X + 2, SPAN_Y + 2
TAPS = 3 * C
DEPTH = PAD_X * 3 * TAPS
FLAT = 9 * TAPS
GROUP = 4
AXES = ("gx", "gy", "gz")
MESH = pl.DeviceIdType.MESH


def sigmoid(value):
    return 0.5 + 0.5 * jnp.tanh(0.5 * value)


def rolled(tile, shift):
    shift = shift % LANES
    return pltpu.roll(tile, shift, 1) if shift else tile


class Halo:
    def __init__(
        self, rows, near, far_y, turn, far_x, edge, side, send, recv, place, volumes
    ):
        self.rows, self.near, self.far_y, self.turn, self.far_x = rows, near, far_y, turn, far_x
        self.side = side
        self.edge, self.send, self.recv, self.place, self.volumes = edge, send, recv, place, volumes
        self.count = 0
        self.sent = []

    def has(self, axis, step):
        me, size = self.place[axis]
        return me > 0 if step < 0 else me < size - 1

    def push(self, source, target, axis, step):
        me, size = self.place[axis]
        index = self.count
        self.count += 1
        copy = pltpu.make_async_remote_copy(
            src_ref=source,
            dst_ref=target,
            send_sem=self.send.at[index],
            recv_sem=self.recv.at[index],
            device_id={axis: lax.rem(me + step + size, size)},
            device_id_type=MESH,
        )

        @pl.when(self.has(axis, step))
        def _():
            copy.start()

        self.sent.append((copy, self.has(axis, step)))
        return copy, self.has(axis, -step)

    def faces_x(self, volume):
        rows = self.rows
        inner = pl.ds(1, SPAN_Y)
        down = self.push(
            rows.at[volume, 1, inner], rows.at[volume, PAD_X - 1, inner], "gx", -1
        )
        up = self.push(rows.at[volume, SPAN_X, inner], rows.at[volume, 0, inner], "gx", 1)
        return [down, up]

    def faces_y(self):
        rows, inner, every = self.rows, pl.ds(1, SPAN_X), pl.ds(0, self.volumes)
        down = self.push(
            rows.at[every, inner, 1], rows.at[every, inner, PAD_Y - 1], "gy", -1
        )
        up = self.push(rows.at[every, inner, SPAN_Y], rows.at[every, inner, 0], "gy", 1)
        return [down, up]

    def columns_z(self):
        down = self.push(self.edge.at[0], self.near.at[1], "gz", -1)
        up = self.push(self.edge.at[1], self.near.at[0], "gz", 1)
        return [down, up]

    def columns_y(self):
        down = self.push(self.near, self.far_y.at[1], "gy", -1)
        up = self.push(self.near, self.far_y.at[0], "gy", 1)
        return [down, up]

    def columns_x(self, lane):
        inside = lax.rem(lane, 32)
        down = jnp.zeros((C, LANES), F32)
        up = jnp.zeros((C, LANES), F32)
        for side in range(2):
            for volume in range(self.volumes):
                own = self.near[side, volume].astype(F32)
                low = pltpu.roll(self.far_y[0, side, volume].astype(F32), LANES - 16, 1)
                high = pltpu.roll(self.far_y[1, side, volume].astype(F32), 16, 1)
                own = jnp.where(inside == 0, low, jnp.where(inside == PAD_Y - 1, high, own))
                self.side[volume, side] = own
                at = 32 * (side * self.volumes + volume)
                here = lane // 32 == at // 32
                down = jnp.where(here, rolled(own, at - 32), down)
                up = jnp.where(here, rolled(own, at - 64), up)
        self.turn[0] = down.astype(BF16)
        self.turn[1] = up.astype(BF16)
        down = self.push(self.turn.at[0], self.far_x.at[1], "gx", -1)
        up = self.push(self.turn.at[1], self.far_x.at[0], "gx", 1)
        return [down, up]

    def corners_x(self):
        rows, every = self.rows, pl.ds(0, self.volumes)
        result = []
        for at in (0, PAD_Y - 1):
            result.append(
                self.push(rows.at[every, 1, at], rows.at[every, PAD_X - 1, at], "gx", -1)
            )
            result.append(
                self.push(rows.at[every, SPAN_X, at], rows.at[every, 0, at], "gx", 1)
            )
        return result

    def merged(self, side, volume, lane):
        at = 32 * (side * self.volumes + volume)
        low = rolled(self.far_x[0].astype(F32), -at)
        high = rolled(self.far_x[1].astype(F32), 96 - at)
        return jnp.where(lane < 32, low, jnp.where(lane >= 96, high, self.side[volume, side]))

    @staticmethod
    def arrive(pushes):
        for copy, present in pushes:

            @pl.when(present)
            def _(copy=copy):
                copy.wait_recv()

    def drain(self):
        for copy, present in self.sent:

            @pl.when(present)
            def _(copy=copy):
                copy.wait_send()


def kernel(
    voxels,
    x_a, x_b, grad, w_first, w_second, gain_first, bias_first, gain_second, bias_second,
    y_out, dx_out, gw_first, gw_second, norm_out,
    block_a, block_b, block_g, kernel_1, kernel_2, row_1, row_2, row_3, row_4, weights, stage,
    taps_x, taps_h, taps_d2, taps_d1,
    rows_x, rows_g, rows_1, rows_2, rows_e,
    near_x, near_g, near_1, near_2, near_e,
    fary_x, fary_g, fary_1, fary_2, fary_e,
    turn_x, turn_g, turn_1, turn_2, turn_e,
    farx_x, farx_g, farx_1, farx_2, farx_e,
    edge_x, edge_g, edge_1, edge_2, edge_e,
    side_x, side_g, side_1, side_2, side_e,
    side_h,
    conv_1, conv_2, back_1,
    sums,
    norms, slopes, early_out, early_in, late_out, late_in, gathered, pairs,
    halo_send, halo_recv, sums_send, sums_recv, gw_send, gw_recv, local,
):
    loads = [
        pltpu.make_async_copy(source, target, local.at[index])
        for index, (source, target) in enumerate((
            (x_a, block_a), (x_b, block_b), (grad, block_g), (w_first, kernel_1),
            (w_second, kernel_2), (gain_first, row_1), (bias_first, row_2), (gain_second, row_3),
            (bias_second, row_4),
        ))
    ]
    for load in loads:
        load.start()
    place = {axis: (lax.axis_index(axis), lax.axis_size(axis)) for axis in AXES}
    for near in (near_x, near_g, near_1, near_2, near_e):
        near[...] = jnp.zeros_like(near)
    for chunks in (early_out, late_out):
        for j in range(4):
            chunks[32 * j + 28 : 32 * j + 32] = jnp.zeros((4, 4, LANES), F32)
    barrier = pltpu.get_barrier_semaphore()
    count = place["gx"][1] * place["gy"][1] * place["gz"][1]
    flat = (place["gx"][0] * place["gy"][1] + place["gy"][0]) * place["gz"][1] + place["gz"][0]

    chip_x, chip_y = place["gy"][0], place["gz"][0] // 2
    chip_z = place["gx"][0] // 2 * 2 + lax.rem(place["gz"][0], 2)
    core = lax.rem(place["gx"][0], 2)

    def other(step):
        return lax.rem(flat + step, count)

    def fan_out(source_of, target, send, recv):
        spots = []
        for step_z, step_core in ((2, 1), (2, 0), (1, 1), (3, 1), (1, 0), (3, 0), (0, 1), (0, 0)):
            to_z, to_core = lax.rem(chip_z + step_z, 4), lax.rem(core + step_core, 2)
            spots.append(to_z // 2 * 64 + to_core * 32 + lax.rem(to_z, 2))

        def copies(plane, chosen):
            to_x = lax.rem(chip_x + plane // 4 + 1, 4)
            to_y = lax.rem(chip_y + lax.rem(plane, 4) + 1, 4)
            for spot in chosen:
                to = spot + to_x * 8 + to_y * 2
                pltpu.make_async_remote_copy(
                    src_ref=source_of(to), dst_ref=target, send_sem=send, recv_sem=recv,
                    device_id=to, device_id_type=pl.DeviceIdType.LOGICAL,
                ).start()

        def most(plane, carry):
            copies(plane, spots[:-1])
            return carry

        def rest(plane, carry):
            copies(plane, spots[-1:])
            return carry

        lax.fori_loop(0, 16, most, 0)
        lax.fori_loop(0, 15, rest, 0)

    def fan_in(slots, semaphore):
        part = slots.at[pl.ds(0, count - 1)]
        pltpu.make_async_copy(part, part, semaphore).wait()

    def greet(step, carry):
        pl.semaphore_signal(
            barrier, inc=1, device_id=other(step), device_id_type=pl.DeviceIdType.LOGICAL
        )
        return carry

    lax.fori_loop(1, count, greet, 0)

    lane = lax.broadcasted_iota(jnp.int32, (C, LANES), 1)
    halos = []
    for index, (rows, near, fary, turn, farx, edge, side, volumes) in enumerate((
        (rows_x, near_x, fary_x, turn_x, farx_x, edge_x, side_x, 2),
        (rows_g, near_g, fary_g, turn_g, farx_g, edge_g, side_g, 1),
        (rows_1, near_1, fary_1, turn_1, farx_1, edge_1, side_1, 2),
        (rows_2, near_2, fary_2, turn_2, farx_2, edge_2, side_2, 1),
        (rows_e, near_e, fary_e, turn_e, farx_e, edge_e, side_e, 1),
    )):
        halos.append(
            Halo(rows, near, fary, turn, farx, edge, side, halo_send.at[index],
                 halo_recv.at[index], place, volumes)
        )
    halo_x, halo_g, halo_1, halo_2, halo_e = halos

    low_x, high_x = place["gx"][0] > 0, place["gx"][0] < place["gx"][1] - 1
    low_y, high_y = place["gy"][0] > 0, place["gy"][0] < place["gy"][1] - 1
    low_z, high_z = place["gz"][0] > 0, place["gz"][0] < place["gz"][1] - 1

    def keep(at_x, at_y):
        held_x = low_x if at_x == 0 else high_x if at_x == PAD_X - 1 else None
        if isinstance(at_y, int):
            held_y = low_y if at_y == 0 else high_y if at_y == PAD_Y - 1 else None
        else:
            held_y = jnp.logical_and(
                jnp.logical_or(at_y > 0, low_y), jnp.logical_or(at_y < PAD_Y - 1, high_y)
            )
        if held_x is None:
            return held_y
        return held_x if held_y is None else jnp.logical_and(held_x, held_y)

    def lane_keep(side):
        spot_x, spot_y = lane // 32, lax.rem(lane, 32)
        bad = jnp.zeros((C, LANES), jnp.int32)
        for hit, present in (
            (spot_x == 0, low_x), (spot_x == PAD_X - 1, high_x),
            (spot_y == 0, low_y), (spot_y == PAD_Y - 1, high_y),
        ):
            missing = jnp.where(present, 0, 1)
            bad = bad + jnp.where(hit, missing, 0)
        bad = bad + jnp.where(low_z if side == 0 else high_z, 0, 1)
        return bad == 0

    def extract(tile, spot, carry):
        first, last = carry
        first = jnp.where(lane == spot, pltpu.roll(tile, spot, 1), first)
        last = jnp.where(lane == spot, pltpu.roll(tile, lax.rem(spot + 1, LANES), 1), last)
        return first, last

    def put_taps(taps, volume, at_x, at_y, tile, side_lo, side_hi):
        spot = at_x * 32 + at_y
        left = jnp.where(
            lane == 0,
            pltpu.roll(side_lo, lax.rem(LANES - spot, LANES), 1),
            pltpu.roll(tile, 1, 1),
        )
        right = jnp.where(
            lane == LANES - 1,
            pltpu.roll(side_hi, LANES - 1 - spot, 1),
            pltpu.roll(tile, LANES - 1, 1),
        )
        taps[volume, at_x, at_y, 0:C] = left.astype(BF16)
        taps[volume, at_x, at_y, C : 2 * C] = tile.astype(BF16)
        taps[volume, at_x, at_y, 2 * C : 3 * C] = right.astype(BF16)

    def build(taps, volume, outer, inner, sides):
        low, high = sides
        zero = jnp.zeros((C, LANES), F32)

        def held(at_x, at_y):
            tile = outer(at_x, at_y)
            return jnp.where(keep(at_x, at_y), tile, zero)

        for at_x in (1, 2):

            def step(block, carry, at_x=at_x):
                for k in range(8):
                    at_y = block * 8 + k
                    put_taps(
                        taps, volume, at_x, at_y + 1, inner(at_x - 1, at_y), low[...], high[...]
                    )
                return carry

            lax.fori_loop(0, 2, step, 0)
            for at_y in (0, PAD_Y - 1):
                put_taps(taps, volume, at_x, at_y, held(at_x, at_y), low[...], high[...])
        for at_x in (0, PAD_X - 1):

            def step(block, carry, at_x=at_x):
                for k in range(6):
                    at_y = block * 6 + k
                    put_taps(taps, volume, at_x, at_y, held(at_x, at_y), low[...], high[...])
                return carry

            lax.fori_loop(0, 3, step, 0)

    def convolve(taps, volume, weight, emit, carry):
        def step(block, carry):
            first = block * GROUP
            columns = [
                taps[volume, :, pl.ds(first + k, 3)].reshape(DEPTH, LANES) for k in range(GROUP)
            ]
            total = jnp.dot(
                weights[weight],
                jnp.concatenate(columns, axis=1),
                preferred_element_type=F32,
            )
            for k in range(GROUP):
                for at_x in range(SPAN_X):
                    tile = total[at_x * C : (at_x + 1) * C, k * LANES : (k + 1) * LANES]
                    carry = emit(at_x, first + k, tile, carry)
            return carry

        return lax.fori_loop(0, SPAN_Y // GROUP, step, carry)

    def kernel_grad(taps, volume, row_of, out, first_row, plain=False):
        high = SPAN_X * C + (16 if plain else 0)

        def step(block, total):
            first = block * GROUP
            left, right = [], []
            for k in range(GROUP):
                rows = [row_of(at_x, first + k) for at_x in range(SPAN_X)]
                if plain:
                    rows.append(jnp.ones((16, LANES), BF16))
                left.append(jnp.concatenate(rows, axis=0))
                right.append(taps[volume, :, pl.ds(first + k, 3)].reshape(DEPTH, LANES))
            return total + lax.dot_general(
                jnp.concatenate(left, axis=1),
                jnp.concatenate(right, axis=1),
                (((1,), (1,)), ((), ())),
                preferred_element_type=F32,
            )

        total = lax.fori_loop(0, SPAN_Y // GROUP, step, jnp.zeros((high, DEPTH), F32))
        slab = 3 * TAPS

        def wide(value):
            return jnp.concatenate(
                [value, jnp.zeros((value.shape[0], 7 * LANES - FLAT), F32)], axis=1
            )

        both = wide(total[0:C, 0:FLAT] + total[C : 2 * C, slab : slab + FLAT])
        if plain:
            alone = total[2 * C : 2 * C + 1]
            alone = wide(alone[:, 0:FLAT] + alone[:, slab : slab + FLAT])
        for k in range(7):
            lanes = slice(LANES * k, LANES * (k + 1))
            for pair in range(16):
                spot = (pair // 4 * 8 + k) * 4 + pair % 4
                out[spot, first_row : first_row + 2] = both[2 * pair : 2 * pair + 2, lanes]
                if plain:
                    out[spot, 2:3] = alone[:, lanes]

    channel = lax.broadcasted_iota(jnp.int32, (C, LANES), 0)

    def pack(columns):
        whole = jnp.zeros((C, LANES), F32)
        for k, column in enumerate(columns):
            whole = whole + jnp.where(lane == channel + 32 * k, column, 0.0)
        return jnp.sum(whole, axis=0, keepdims=True)

    def unpack(row, number):
        return [
            jnp.sum(jnp.where(lane == channel + 32 * k, row, 0.0), axis=1, keepdims=True)
            for k in range(number)
        ]

    class Total:
        def __init__(self, index):
            self.slots, self.index = sums.at[index], index

        def start(self, row):
            mine = self.slots.at[flat]
            mine[...] = row

            fan_out(
                lambda to: mine, mine, sums_send.at[self.index], sums_recv.at[self.index]
            )

        def finish(self):
            fan_in(self.slots, sums_recv.at[self.index])
            return jnp.sum(self.slots[...], axis=0)

        def drain(self):
            fan_in(self.slots, sums_send.at[self.index])

    totals = [Total(index) for index in range(4)]

    def second(halo, phase):
        halo.arrive(phase)
        return halo.columns_y(), halo.corners_x()

    def third(halo, phase):
        halo.arrive(phase)
        return halo.columns_x(lane)

    small_lane = lax.broadcasted_iota(jnp.int32, (C, C), 1)
    small_row = lax.broadcasted_iota(jnp.int32, (C, C), 0)

    def column(row):
        return jnp.sum(jnp.where(small_lane == small_row, row[...], 0.0), axis=1, keepdims=True)

    for load in loads[5:]:
        load.wait()
    gain_1, bias_1, gain_2, bias_2 = (column(row) for row in (row_1, row_2, row_3, row_4))

    def stack_weights(source, forward, backward):
        tiles = [
            jnp.concatenate(
                [source[tap].astype(F32) for tap in range(4 * k, min(4 * k + 4, 27))]
                + ([jnp.zeros((C, C), F32)] if k == 6 else []),
                axis=1,
            )
            for k in range(7)
        ]
        turned = [tile.T for tile in tiles]
        pieces = [turned[tap // 4][C * (tap % 4) : C * (tap % 4) + C] for tap in range(26, -1, -1)]
        back = [jnp.concatenate((pieces + pieces[:1])[4 * k : 4 * k + 4], axis=1) for k in range(7)]
        for index, parts in ((forward, tiles), (backward, back)):
            last = jnp.where(lane < 96, parts[6], 0.0)
            empty = jnp.zeros((C, LANES), F32)
            top = parts[:6] + [last, empty, empty]
            moved = [pltpu.roll(part, 32, 1) for part in parts[:6] + [last]]
            low = [empty, empty]
            for k in range(7):
                low.append(jnp.where(lane < 32, moved[k - 1] if k else empty, moved[k]))
            for k in range(9):
                weights[index, 0:C, LANES * k : LANES * (k + 1)] = top[k].astype(BF16)
                weights[index, C : 2 * C, LANES * k : LANES * (k + 1)] = low[k].astype(BF16)

    zero = jnp.zeros((C, LANES), F32)

    def take(load, source, rows, edge, at):
        load.wait()
        for at_x in range(SPAN_X):
            rows[at, at_x + 1, 1 : SPAN_Y + 1] = jnp.swapaxes(
                source[:, at_x].astype(F32), 0, 1
            ).astype(BF16)
        for at_x in range(SPAN_X):

            def step(block, carry, at_x=at_x):
                for k in range(8):
                    at_y = block * 8 + k
                    carry = extract(
                        rows[at, at_x + 1, at_y + 1].astype(F32),
                        (at_x + 1) * 32 + at_y + 1,
                        carry,
                    )
                return carry

            carry = lax.fori_loop(0, 2, step, (zero, zero) if at_x == 0 else carry)
        edge[0, at] = carry[0].astype(BF16)
        edge[1, at] = carry[1].astype(BF16)

    take(loads[0], block_a, rows_x, edge_x, 0)
    take(loads[1], block_b, rows_x, edge_x, 1)

    pl.semaphore_wait(barrier, count - 1)

    phase = halo_x.columns_z() + halo_x.faces_y()
    waits_x = [halo_x.faces_x(0)]
    loads[3].wait()
    loads[4].wait()
    stack_weights(kernel_1, 0, 3)
    stack_weights(kernel_2, 1, 2)
    phase, corners = second(halo_x, phase)
    take(loads[2], block_g, rows_g, edge_g, 0)
    last = third(halo_x, phase)
    waits_x.append(halo_x.faces_x(1))
    halo_x.arrive(corners)
    halo_x.arrive(last)
    ok = [lane_keep(side) for side in range(2)]
    for side in range(2):
        for volume in range(2):
            tile = halo_x.merged(side, volume, lane)
            side_x[volume, side] = jnp.where(ok[side], tile, 0.0)

    def stats_emit(keep_f32, halo, volume):
        def emit(at_x, at_y, tile, carry):
            total, squares, first, last = carry
            keep_f32[volume, at_x, at_y] = tile
            halo.rows[halo_of[volume], at_x + 1, at_y + 1] = tile.astype(BF16)
            first, last = extract(tile, (at_x + 1) * 32 + at_y + 1, (first, last))
            return total + tile, squares + tile * tile, first, last

        halo_of = {0: 0, 1: 1}
        return emit

    columns = []
    waits = []
    for volume in range(2):
        halo_x.arrive(waits_x[volume])
        build(
            taps_x, volume,
            lambda at_x, at_y, volume=volume: rows_x[volume, at_x, at_y].astype(F32),
            lambda at_x, at_y, volume=volume: rows_x[volume, at_x + 1, at_y + 1].astype(F32),
            (side_x.at[volume, 0], side_x.at[volume, 1]),
        )
        total, squares, first, last = convolve(
            taps_x, volume, 0, stats_emit(conv_1, halo_1, volume), (zero,) * 4
        )
        edge_1[0, volume] = first.astype(BF16)
        edge_1[1, volume] = last.astype(BF16)
        if volume == 0:
            waits += halo_1.faces_x(volume)
        columns += [
            jnp.sum(total, axis=1, keepdims=True), jnp.sum(squares, axis=1, keepdims=True)
        ]
    totals[0].start(pack(columns))
    phase = halo_1.columns_z() + halo_1.faces_y()
    waits += halo_1.faces_x(1)
    phase, corners = second(halo_1, phase)
    last = third(halo_1, phase)
    row = totals[0].finish()
    halo_1.arrive(waits + corners + last)
    phase_g = halo_g.columns_z() + halo_g.faces_y()
    waits_g = halo_g.faces_x(0)
    stats = unpack(row, 4)

    def moments(total, squares):
        mean = total / voxels
        scale = lax.rsqrt(squares / voxels - mean * mean + EPSILON)
        return mean, scale

    columns = []
    affine_1 = None
    for volume in range(2):
        mean, scale = moments(stats[2 * volume], stats[2 * volume + 1])
        slope = jnp.broadcast_to(gain_1 * scale, (C, LANES))
        shift = jnp.broadcast_to(bias_1 - mean * gain_1 * scale, (C, LANES))

        def active(value, slope=slope, shift=shift):
            pre = value * slope + shift
            return pre * sigmoid(pre)

        norm_slope = jnp.broadcast_to(scale, (C, LANES))
        norm_shift = jnp.broadcast_to(-mean * scale, (C, LANES))

        def own_row(at_x, at_y, volume, active, norm_slope=norm_slope, norm_shift=norm_shift):
            value = conv_1[volume, at_x, at_y]
            if volume == 1:
                norms[at_x, at_y] = (value * norm_slope + norm_shift).astype(BF16)
            return active(value)

        for side in range(2):
            tile = halo_1.merged(side, volume, lane)
            side_1[volume, side] = tile
            side_h[volume, side] = jnp.where(ok[side], active(tile), 0.0)
        build(
            taps_h, volume,
            lambda at_x, at_y, volume=volume: active(rows_1[volume, at_x, at_y].astype(F32)),
            functools.partial(own_row, volume=volume, active=active),
            (side_h.at[volume, 0], side_h.at[volume, 1]),
        )
        if volume == 0:

            def emit(at_x, at_y, tile, carry):
                total, squares = carry
                conv_2[0, at_x, at_y] = tile
                return total + tile, squares + tile * tile

            total, squares = convolve(taps_h, 0, 1, emit, (zero,) * 2)
            phase_g, corners_g = second(halo_g, phase_g)
        else:

            def emit(at_x, at_y, tile, carry):
                total, squares, first, last = carry
                conv_2[1, at_x, at_y] = tile
                rows_2[0, at_x + 1, at_y + 1] = tile.astype(BF16)
                first, last = extract(tile, (at_x + 1) * 32 + at_y + 1, (first, last))
                return total + tile, squares + tile * tile, first, last

            total, squares, first, last = convolve(taps_h, 1, 1, emit, (zero,) * 4)
            edge_2[0, 0] = first.astype(BF16)
            edge_2[1, 0] = last.astype(BF16)
        columns += [
            jnp.sum(total, axis=1, keepdims=True), jnp.sum(squares, axis=1, keepdims=True)
        ]
    mean_1, scale_1 = mean, scale
    totals[1].start(pack(columns))
    phase = halo_2.columns_z() + halo_2.faces_y()
    waits = halo_2.faces_x(0)
    last_g = third(halo_g, phase_g)
    kernel_grad(taps_x, 1, lambda at_x, at_y: norms[at_x, at_y], early_out, 0, plain=True)
    fan_out(
        lambda to: early_out.at[to], early_in.at[flat], gw_send.at[0], gw_recv.at[0]
    )
    early_in[flat] = early_out[flat]
    stats = unpack(totals[1].finish(), 4)

    mean_2, scale_2 = moments(stats[2], stats[3])

    def layer_of(mean, scale, gain, bias):
        norm_slope = jnp.broadcast_to(scale, (C, LANES))
        norm_shift = jnp.broadcast_to(-mean * scale, (C, LANES))
        wide_gain = jnp.broadcast_to(gain, (C, LANES))
        wide_bias = jnp.broadcast_to(bias, (C, LANES))

        def slope_of(value, upstream):
            normed = value * norm_slope + norm_shift
            pre = wide_gain * normed + wide_bias
            sigma = sigmoid(pre)
            return upstream * (sigma * (1.0 + pre * (1.0 - sigma))), normed

        return slope_of

    def delta_of(slope_of, sum_d, sum_x, gain, scale):
        wide_d = jnp.broadcast_to(sum_d / voxels, (C, LANES))
        wide_x = jnp.broadcast_to(sum_x / voxels, (C, LANES))
        factor = jnp.broadcast_to(gain * scale, (C, LANES))

        def delta(value, upstream):
            slope, normed = slope_of(value, upstream)
            return factor * (slope - wide_d - normed * wide_x)

        return delta

    slope_2 = layer_of(mean_2, scale_2, gain_2, bias_2)

    def sum_rows(slope_of, value_of, upstream_of):
        carry = (zero, zero)
        for at_x in range(SPAN_X):

            def step(block, carry, at_x=at_x):
                total, weighted = carry
                for k in range(8):
                    at_y = block * 8 + k
                    slope, normed = slope_of(value_of(at_x, at_y), upstream_of(at_x, at_y))
                    total, weighted = total + slope, weighted + slope * normed
                return total, weighted

            carry = lax.fori_loop(0, 2, step, carry)
        return [jnp.sum(part, axis=1, keepdims=True) for part in carry]

    columns = sum_rows(
        slope_2,
        lambda at_x, at_y: conv_2[1, at_x, at_y],
        lambda at_x, at_y: rows_g[0, at_x + 1, at_y + 1].astype(F32),
    )
    totals[2].start(pack(columns))
    phase, corners = second(halo_2, phase)

    mean_a, scale_a = moments(stats[0], stats[1])
    slope_a = jnp.broadcast_to(gain_2 * scale_a, (C, LANES))
    shift_a = jnp.broadcast_to(bias_2 - mean_a * gain_2 * scale_a, (C, LANES))
    for at_x in range(SPAN_X):

        def step(block, carry, at_x=at_x):
            for k in range(8):
                at_y = block * 8 + k
                pre = conv_2[0, at_x, at_y] * slope_a + shift_a
                stage[at_x, at_y] = pre * sigmoid(pre)
            return carry

        lax.fori_loop(0, 2, step, 0)
        y_out[:, at_x] = jnp.swapaxes(stage[at_x], 0, 1).astype(BF16)

    last = third(halo_2, phase)
    halo_g.arrive(waits_g + corners_g + last_g)
    halo_2.arrive(waits + corners + last)
    sum_d2, sum_x2 = unpack(totals[2].finish(), 2)

    delta_2 = delta_of(slope_2, sum_d2, sum_x2, gain_2, scale_2)
    for side in range(2):
        tile = delta_2(halo_2.merged(side, 0, lane), halo_g.merged(side, 0, lane))
        side_2[0, side] = jnp.where(ok[side], tile, 0.0)
    build(
        taps_d2, 0,
        lambda at_x, at_y: delta_2(
            rows_2[0, at_x, at_y].astype(F32), rows_g[0, at_x, at_y].astype(F32)
        ),
        lambda at_x, at_y: delta_2(
            conv_2[1, at_x, at_y], rows_g[0, at_x + 1, at_y + 1].astype(F32)
        ),
        (side_2.at[0, 0], side_2.at[0, 1]),
    )
    slope_1 = layer_of(mean_1, scale_1, gain_1, bias_1)

    def emit(at_x, at_y, tile, carry):
        total, weighted, first, last = carry
        back_1[at_x, at_y] = tile
        rows_e[0, at_x + 1, at_y + 1] = tile.astype(BF16)
        first, last = extract(tile, (at_x + 1) * 32 + at_y + 1, (first, last))
        slope, normed = slope_1(conv_1[1, at_x, at_y], tile)
        slopes[at_x, at_y] = slope.astype(BF16)
        return total + slope, weighted + slope * normed, first, last

    total, weighted, first, last = convolve(taps_d2, 0, 2, emit, (zero,) * 4)
    edge_e[0, 0] = first.astype(BF16)
    edge_e[1, 0] = last.astype(BF16)
    columns = [
        jnp.sum(total, axis=1, keepdims=True), jnp.sum(weighted, axis=1, keepdims=True)
    ]
    totals[3].start(pack(columns))
    phase = halo_e.columns_z() + halo_e.faces_y()
    waits = halo_e.faces_x(0)
    kernel_grad(taps_x, 1, lambda at_x, at_y: slopes[at_x, at_y], late_out, 0)
    phase, corners = second(halo_e, phase)
    kernel_grad(
        taps_h, 1, lambda at_x, at_y: taps_d2[0, at_x + 1, at_y + 1, C : 2 * C], late_out, 2
    )
    last = third(halo_e, phase)
    fan_out(lambda to: late_out.at[to], late_in.at[flat], gw_send.at[1], gw_recv.at[1])
    late_in[flat] = late_out[flat]
    sum_d1, sum_x1 = unpack(totals[3].finish(), 2)
    halo_e.arrive(waits + corners + last)

    delta_1 = delta_of(slope_1, sum_d1, sum_x1, gain_1, scale_1)
    for side in range(2):
        tile = delta_1(side_1[1, side], halo_e.merged(side, 0, lane))
        side_e[0, side] = jnp.where(ok[side], tile, 0.0)
    build(
        taps_d1, 0,
        lambda at_x, at_y: delta_1(
            rows_1[1, at_x, at_y].astype(F32), rows_e[0, at_x, at_y].astype(F32)
        ),
        lambda at_x, at_y: delta_1(conv_1[1, at_x, at_y], back_1[at_x, at_y]),
        (side_e.at[0, 0], side_e.at[0, 1]),
    )
    whole = 1.0 / math.sqrt(voxels)
    for k, factor in enumerate(
        (gain_1 * scale_1 * whole, sum_d1 / voxels, sum_x1 / voxels)
    ):
        tile = jnp.broadcast_to(factor, (C, LANES))
        for pair in range(16):
            pairs[k, pair] = tile[2 * pair : 2 * pair + 2]
    fan_in(early_in, gw_recv.at[0])
    early = jnp.sum(early_in[...], axis=0)
    at = flat // 32 * 4 + lax.rem(flat, 4)
    fan_in(late_in, gw_recv.at[1])
    late = jnp.sum(late_in[...], axis=0)
    gathered[flat, 0:2] = pairs[0, at] * (
        late[0:2] - pairs[1, at] * early[2:3] - pairs[2, at] * early[0:2]
    )
    gathered[flat, 2:4] = late[2:4] * whole
    mine = gathered.at[flat]
    fan_out(lambda to: mine, mine, gw_send.at[2], gw_recv.at[2])

    def emit(at_x, at_y, tile, carry):
        stage[at_x, at_y] = tile
        return carry

    convolve(taps_d1, 0, 3, emit, 0)
    for at_x in range(SPAN_X):
        dx_out[:, at_x] = jnp.swapaxes(stage[at_x], 0, 1).astype(BF16)

    for k, total in enumerate((sum_x1, sum_d1, sum_x2, sum_d2)):
        norm_out[k : k + 1] = whole * jnp.sum(
            jnp.where(small_lane == small_row, total, 0.0), axis=0, keepdims=True
        )
    fan_in(gathered, gw_recv.at[2])
    for member, out in ((0, gw_first), (1, gw_second)):
        for k in range(7):
            tile = jnp.concatenate(
                [
                    gathered[(pair // 4 * 8 + k) * 4 + pair % 4, 2 * member : 2 * member + 2]
                    for pair in range(16)
                ],
                axis=0,
            )
            for tap in range(4 * k, min(4 * k + 4, 27)):
                out[tap] = tile[:, C * (tap % 4) : C * (tap % 4) + C]

    for halo in halos:
        halo.drain()
    for total in totals:
        total.drain()
    for k, chunks in enumerate((early_out, late_out, gathered)):
        fan_in(chunks, gw_send.at[k])


def write_out(*refs):
    sources, targets, semaphores = refs[:5], refs[5:10], refs[10]
    copies = [
        pltpu.make_async_copy(source, target, semaphores.at[index])
        for index, (source, target) in enumerate(zip(sources, targets))
    ]
    for copy in copies:
        copy.start()
    for copy in copies:
        copy.wait()


def body(voxels, x_a, x_b, w_first, w_second, gain_first, bias_first, gain_second, bias_second,
         grad_out):
    def sized(*shape, kind=BF16):
        return pltpu.VMEM(shape, kind)

    volumes = (2, 1, 2, 1, 1)
    devices = math.prod(lax.axis_size(axis) for axis in AXES)
    block = (C, SPAN_X, SPAN_Y, LANES)
    scratch = [sized(*block)] * 3 + [sized(27, C, C)] * 2 + [sized(1, C, kind=F32)] * 4
    scratch += [
        sized(4, SPAN_X * C, DEPTH), sized(SPAN_X, SPAN_Y, C, LANES, kind=F32)
    ]
    scratch += [sized(count, PAD_X, PAD_Y, TAPS, LANES) for count in (2, 2, 1, 1)]
    scratch += [sized(count, PAD_X, PAD_Y, C, LANES) for count in volumes]
    scratch += [sized(2, count, C, LANES) for count in volumes]
    scratch += [sized(2, 2, count, C, LANES) for count in volumes]
    scratch += [sized(2, C, LANES) for count in volumes]
    scratch += [sized(2, C, LANES) for count in volumes]
    scratch += [sized(2, count, C, LANES) for count in volumes]
    scratch += [sized(count, 2, C, LANES, kind=F32) for count in volumes]
    scratch += [sized(2, 2, C, LANES, kind=F32)]
    scratch += [
        sized(2, SPAN_X, SPAN_Y, C, LANES, kind=F32),
        sized(2, SPAN_X, SPAN_Y, C, LANES, kind=F32),
        sized(SPAN_X, SPAN_Y, C, LANES, kind=F32),
        sized(4, devices, 1, LANES, kind=F32),
        sized(SPAN_X, SPAN_Y, C, LANES),
        sized(SPAN_X, SPAN_Y, C, LANES),
        sized(devices, 4, LANES, kind=F32),
        sized(devices, 4, LANES, kind=F32),
        sized(devices, 4, LANES, kind=F32),
        sized(devices, 4, LANES, kind=F32),
        sized(devices, 4, LANES, kind=F32),
        sized(3, 16, 2, LANES, kind=F32),
        pltpu.SemaphoreType.DMA((5, 24)),
        pltpu.SemaphoreType.DMA((5, 24)),
        pltpu.SemaphoreType.DMA((4,)),
        pltpu.SemaphoreType.DMA((4,)),
        pltpu.SemaphoreType.DMA((3,)),
        pltpu.SemaphoreType.DMA((3,)),
        pltpu.SemaphoreType.DMA((9,)),
    ]
    in_vmem = pl.BlockSpec(memory_space=pltpu.VMEM)
    in_hbm = pl.BlockSpec(memory_space=pltpu.HBM)
    taps = jax.ShapeDtypeStruct((27, C, C), F32)
    out_shape = (
        jax.ShapeDtypeStruct(block, BF16),
        jax.ShapeDtypeStruct(block, BF16),
        taps,
        taps,
        jax.ShapeDtypeStruct((4, C), F32),
    )
    results = pl.pallas_call(
        functools.partial(kernel, voxels),
        out_shape=out_shape,
        in_specs=[in_hbm] * 9,
        out_specs=(in_vmem,) * 5,
        scratch_shapes=scratch,
        compiler_params=pltpu.CompilerParams(
            collective_id=0, has_side_effects=True, vmem_limit_bytes=28 * 1024 * 1024
        ),
    )(
        *(pltpu.with_memory_space_constraint(value, pltpu.HBM) for value in (
            x_a, x_b, grad_out, w_first.reshape(27, C, C), w_second.reshape(27, C, C),
            *(row.reshape(1, C) for row in (gain_first, bias_first, gain_second, bias_second)),
        )),
    )
    y_a, dx_b, grad_first, grad_second, norms = pl.pallas_call(
        write_out,
        out_shape=out_shape,
        in_specs=[in_vmem] * 5,
        out_specs=(in_hbm,) * 5,
        scratch_shapes=[pltpu.SemaphoreType.DMA((5,))],
        compiler_params=pltpu.CompilerParams(vmem_limit_bytes=8 * 1024 * 1024),
    )(*results)
    return (
        y_a, dx_b, grad_first.reshape(3, 3, 3, C, C), grad_second.reshape(3, 3, 3, C, C), norms
    )


def solution(mesh):
    split = P(None, "gx", "gy", "gz")
    voxels = float(SPAN_X * SPAN_Y * LANES * mesh.size)
    return jax.shard_map(
        functools.partial(body, voxels),
        mesh=mesh,
        in_specs=(split, split, P(), P(), P(), P(), P(), P(), split),
        out_specs=(split, split, P(), P(), P()),
        check_vma=False,
    )
```

```python
import functools
import math

import jax
import jax.numpy as jnp
from jax import lax
from jax.experimental import pallas as pl
from jax.experimental.pallas import tpu as pltpu
from jax.sharding import PartitionSpec as P

F32 = jnp.float32
BF16 = jnp.bfloat16
EPSILON = 1e-05
C = 32
LANES = 128
SPAN_X, SPAN_Y = 2, 16
PAD_X, PAD_Y = SPAN_X + 2, SPAN_Y + 2
TAPS = 3 * C
DEPTH = PAD_X * 3 * TAPS
FLAT = 9 * TAPS
GROUP = 4
AXES = ("gx", "gy", "gz")
MESH = pl.DeviceIdType.MESH


def sigmoid(value):
    return 0.5 + 0.5 * jnp.tanh(0.5 * value)


def rolled(tile, shift):
    shift = shift % LANES
    return pltpu.roll(tile, shift, 1) if shift else tile


class Halo:
    def __init__(self, rows, cols, edge, side, send, recv, place, volumes):
        self.rows, self.cols, self.edge, self.side = rows, cols, edge, side
        self.send, self.recv, self.place, self.volumes = send, recv, place, volumes
        self.count = 0
        self.sent = []

    def has(self, steps):
        present = None
        for axis, step in zip(AXES, steps):
            if step:
                me, size = self.place[axis]
                inside = me > 0 if step < 0 else me < size - 1
                present = inside if present is None else jnp.logical_and(present, inside)
        return present

    def push(self, source, target, *steps):
        index = self.count
        self.count += 1
        to = {}
        for axis, step in zip(AXES, steps):
            if step:
                me, size = self.place[axis]
                to[axis] = lax.rem(me + step + size, size)
        copy = pltpu.make_async_remote_copy(
            src_ref=source,
            dst_ref=target,
            send_sem=self.send.at[index],
            recv_sem=self.recv.at[index],
            device_id=to,
            device_id_type=MESH,
        )
        present = self.has(steps)

        @pl.when(present)
        def _():
            copy.start()

        self.sent.append((copy, present))
        return copy, self.has([-step for step in steps])

    def faces_x(self, volume):
        rows, inner = self.rows, pl.ds(1, SPAN_Y)
        return [
            self.push(
                rows.at[volume, 1 if step < 0 else SPAN_X, inner],
                rows.at[volume, PAD_X - 1 if step < 0 else 0, inner],
                step, 0, 0,
            )
            for step in (-1, 1)
        ]

    def columns(self, step_x, step_y):
        return [
            self.push(
                self.edge.at[0 if step < 0 else 1],
                self.cols.at[1 if step < 0 else 0, 1 - step_x, 1 - step_y],
                step_x, step_y, step,
            )
            for step in (-1, 1)
        ]

    def small(self):
        rows, every = self.rows, pl.ds(0, self.volumes)
        near = self.columns(0, 0)
        rest = []
        for step_x in (-1, 0, 1):
            at_x = (1 if step_x < 0 else SPAN_X) if step_x else pl.ds(1, SPAN_X)
            to_x = (PAD_X - 1 if step_x < 0 else 0) if step_x else pl.ds(1, SPAN_X)
            for step_y in (-1, 1):
                rest.append(
                    self.push(
                        rows.at[every, at_x, 1 if step_y < 0 else SPAN_Y],
                        rows.at[every, to_x, PAD_Y - 1 if step_y < 0 else 0],
                        step_x, step_y, 0,
                    )
                )
        for step_x, step_y in (
            (-1, -1), (-1, 1), (1, -1), (1, 1), (-1, 0), (1, 0), (0, -1), (0, 1)
        ):
            rest += self.columns(step_x, step_y)
        return near, rest

    def own(self, side, volume, lane):
        tile = self.cols[side, 1, 1].astype(F32)
        at = 32 * volume
        return jnp.where(lane < 64, rolled(tile, 33 - at), rolled(tile, 49 - at))

    def merged(self, side, volume, lane):
        at = 32 * volume
        inside = lax.rem(lane, 32)

        def strip(index, low, middle, high):
            low, middle, high = (
                rolled(self.cols[side, index, k].astype(F32), shift - at)
                for k, shift in enumerate((low, middle, high))
            )
            return jnp.where(inside == 0, low, jnp.where(inside == PAD_Y - 1, high, middle))

        return jnp.where(
            lane < 64,
            jnp.where(lane < 32, strip(0, -31, -15, 1), strip(1, 17, 33, 49)),
            jnp.where(lane < 96, strip(1, 33, 49, 65), strip(2, 81, 97, 113)),
        )

    @staticmethod
    def arrive(pushes):
        for copy, present in pushes:

            @pl.when(present)
            def _(copy=copy):
                copy.wait_recv()

    def drain(self):
        for copy, present in self.sent:

            @pl.when(present)
            def _(copy=copy):
                copy.wait_send()


def kernel(
    voxels,
    x_a, x_b, grad, w_first, w_second, gain_first, bias_first, gain_second, bias_second,
    y_out, dx_out, gw_first, gw_second, norm_out,
    block_a, block_b, block_g, kernel_1, kernel_2, row_1, row_2, row_3, row_4, weights, stage,
    taps_x, taps_h, taps_d2, taps_d1,
    rows_x, rows_1, rows_2, rows_e,
    cols_x, cols_1, cols_2, cols_e,
    edge_x, edge_1, edge_2, edge_e,
    side_x, side_1, side_2, side_e,
    side_h,
    conv_1, conv_2, back_1,
    sums,
    norms, slopes, early_out, early_in, late_out, late_in, gathered, pairs,
    halo_send, halo_recv, sums_send, sums_recv, gw_send, gw_recv, local,
):
    loads = [
        pltpu.make_async_copy(source, target, local.at[index])
        for index, (source, target) in enumerate((
            (x_a, block_a), (x_b, block_b), (grad, block_g), (w_first, kernel_1),
            (w_second, kernel_2), (gain_first, row_1), (bias_first, row_2), (gain_second, row_3),
            (bias_second, row_4),
        ))
    ]
    for load in loads:
        load.start()
    place = {axis: (lax.axis_index(axis), lax.axis_size(axis)) for axis in AXES}
    for chunks in (early_out, late_out):
        for j in range(4):
            chunks[32 * j + 28 : 32 * j + 32] = jnp.zeros((4, 4, LANES), F32)
    barrier = pltpu.get_barrier_semaphore()
    count = place["gx"][1] * place["gy"][1] * place["gz"][1]
    flat = (place["gx"][0] * place["gy"][1] + place["gy"][0]) * place["gz"][1] + place["gz"][0]

    chip_x, chip_y = place["gy"][0], place["gz"][0] // 2
    chip_z = place["gx"][0] // 2 * 2 + lax.rem(place["gz"][0], 2)
    core = lax.rem(place["gx"][0], 2)

    def other(step):
        return lax.rem(flat + step, count)

    def fan_out(source_of, target, send, recv):
        spots = []
        for step_z, step_core in ((2, 1), (2, 0), (1, 1), (3, 1), (1, 0), (3, 0), (0, 1), (0, 0)):
            to_z, to_core = lax.rem(chip_z + step_z, 4), lax.rem(core + step_core, 2)
            spots.append(to_z // 2 * 64 + to_core * 32 + lax.rem(to_z, 2))

        def copies(plane, chosen):
            to_x = lax.rem(chip_x + plane // 4 + 1, 4)
            to_y = lax.rem(chip_y + lax.rem(plane, 4) + 1, 4)
            for spot in chosen:
                to = spot + to_x * 8 + to_y * 2
                pltpu.make_async_remote_copy(
                    src_ref=source_of(to), dst_ref=target, send_sem=send, recv_sem=recv,
                    device_id=to, device_id_type=pl.DeviceIdType.LOGICAL,
                ).start()

        def most(plane, carry):
            copies(plane, spots[:-1])
            return carry

        def rest(plane, carry):
            copies(plane, spots[-1:])
            return carry

        lax.fori_loop(0, 16, most, 0)
        lax.fori_loop(0, 15, rest, 0)

    def fan_in(slots, semaphore):
        part = slots.at[pl.ds(0, count - 1)]
        pltpu.make_async_copy(part, part, semaphore).wait()

    def greet(step, carry):
        pl.semaphore_signal(
            barrier, inc=1, device_id=other(step), device_id_type=pl.DeviceIdType.LOGICAL
        )
        return carry

    lax.fori_loop(1, count, greet, 0)

    lane = lax.broadcasted_iota(jnp.int32, (C, LANES), 1)
    halos = []
    for index, (rows, cols, edge, side, volumes) in enumerate((
        (rows_x, cols_x, edge_x, side_x, 3),
        (rows_1, cols_1, edge_1, side_1, 2),
        (rows_2, cols_2, edge_2, side_2, 1),
        (rows_e, cols_e, edge_e, side_e, 1),
    )):
        halos.append(
            Halo(rows, cols, edge, side, halo_send.at[index], halo_recv.at[index], place, volumes)
        )
    halo_x, halo_1, halo_2, halo_e = halos

    low_x, high_x = place["gx"][0] > 0, place["gx"][0] < place["gx"][1] - 1
    low_y, high_y = place["gy"][0] > 0, place["gy"][0] < place["gy"][1] - 1
    low_z, high_z = place["gz"][0] > 0, place["gz"][0] < place["gz"][1] - 1

    def keep(at_x, at_y):
        held_x = low_x if at_x == 0 else high_x if at_x == PAD_X - 1 else None
        if isinstance(at_y, int):
            held_y = low_y if at_y == 0 else high_y if at_y == PAD_Y - 1 else None
        else:
            held_y = jnp.logical_and(
                jnp.logical_or(at_y > 0, low_y), jnp.logical_or(at_y < PAD_Y - 1, high_y)
            )
        if held_x is None:
            return held_y
        return held_x if held_y is None else jnp.logical_and(held_x, held_y)

    def lane_keep(side):
        spot_x, spot_y = lane // 32, lax.rem(lane, 32)
        bad = jnp.zeros((C, LANES), jnp.int32)
        for hit, present in (
            (spot_x == 0, low_x), (spot_x == PAD_X - 1, high_x),
            (spot_y == 0, low_y), (spot_y == PAD_Y - 1, high_y),
        ):
            missing = jnp.where(present, 0, 1)
            bad = bad + jnp.where(hit, missing, 0)
        bad = bad + jnp.where(low_z if side == 0 else high_z, 0, 1)
        return bad == 0

    def extract(tile, spot, carry):
        first, last = carry
        first = jnp.where(lane == spot, pltpu.roll(tile, spot, 1), first)
        last = jnp.where(lane == spot, pltpu.roll(tile, lax.rem(spot + 1, LANES), 1), last)
        return first, last

    def put_taps(taps, volume, at_x, at_y, tile, side_lo, side_hi):
        spot = at_x * 32 + at_y
        left = jnp.where(
            lane == 0,
            pltpu.roll(side_lo, lax.rem(LANES - spot, LANES), 1),
            pltpu.roll(tile, 1, 1),
        )
        right = jnp.where(
            lane == LANES - 1,
            pltpu.roll(side_hi, LANES - 1 - spot, 1),
            pltpu.roll(tile, LANES - 1, 1),
        )
        taps[volume, at_x, at_y, 0:C] = left.astype(BF16)
        taps[volume, at_x, at_y, C : 2 * C] = tile.astype(BF16)
        taps[volume, at_x, at_y, 2 * C : 3 * C] = right.astype(BF16)

    def build_inner(taps, volume, inner, sides):
        low, high = sides
        for at_x in (1, 2):

            def step(block, carry, at_x=at_x):
                for k in range(8):
                    at_y = block * 8 + k
                    put_taps(
                        taps, volume, at_x, at_y + 1, inner(at_x - 1, at_y), low[...], high[...]
                    )
                return carry

            lax.fori_loop(0, 2, step, 0)

    def build_outer(taps, volume, outer, sides):
        low, high = sides
        zero = jnp.zeros((C, LANES), F32)

        def put(at_x, at_y):
            tile = jnp.where(keep(at_x, at_y), outer(at_x, at_y), zero)
            put_taps(taps, volume, at_x, at_y, tile, low[...], high[...])

        for at_x in (1, 2):
            for at_y in (0, PAD_Y - 1):
                put(at_x, at_y)
        for at_x in (0, PAD_X - 1):

            def step(block, carry, at_x=at_x):
                for k in range(6):
                    put(at_x, block * 6 + k)
                return carry

            lax.fori_loop(0, 3, step, 0)

    def build(taps, volume, outer, inner, sides):
        build_inner(taps, volume, inner, sides)
        build_outer(taps, volume, outer, sides)

    def convolve(taps, volume, weight, emit, carry):
        def step(block, carry):
            first = block * GROUP
            columns = [
                taps[volume, :, pl.ds(first + k, 3)].reshape(DEPTH, LANES) for k in range(GROUP)
            ]
            total = jnp.dot(
                weights[weight],
                jnp.concatenate(columns, axis=1),
                preferred_element_type=F32,
            )
            for k in range(GROUP):
                for at_x in range(SPAN_X):
                    tile = total[at_x * C : (at_x + 1) * C, k * LANES : (k + 1) * LANES]
                    carry = emit(at_x, first + k, tile, carry)
            return carry

        return lax.fori_loop(0, SPAN_Y // GROUP, step, carry)

    def kernel_grad(taps, volume, row_of, out, first_row, plain=False):
        high = SPAN_X * C + (16 if plain else 0)

        def step(block, total):
            first = block * GROUP
            left, right = [], []
            for k in range(GROUP):
                rows = [row_of(at_x, first + k) for at_x in range(SPAN_X)]
                if plain:
                    rows.append(jnp.ones((16, LANES), BF16))
                left.append(jnp.concatenate(rows, axis=0))
                right.append(taps[volume, :, pl.ds(first + k, 3)].reshape(DEPTH, LANES))
            return total + lax.dot_general(
                jnp.concatenate(left, axis=1),
                jnp.concatenate(right, axis=1),
                (((1,), (1,)), ((), ())),
                preferred_element_type=F32,
            )

        total = lax.fori_loop(0, SPAN_Y // GROUP, step, jnp.zeros((high, DEPTH), F32))
        slab = 3 * TAPS

        def wide(value):
            return jnp.concatenate(
                [value, jnp.zeros((value.shape[0], 7 * LANES - FLAT), F32)], axis=1
            )

        both = wide(total[0:C, 0:FLAT] + total[C : 2 * C, slab : slab + FLAT])
        if plain:
            alone = total[2 * C : 2 * C + 1]
            alone = wide(alone[:, 0:FLAT] + alone[:, slab : slab + FLAT])
        for k in range(7):
            lanes = slice(LANES * k, LANES * (k + 1))
            for pair in range(16):
                spot = (pair // 4 * 8 + k) * 4 + pair % 4
                out[spot, first_row : first_row + 2] = both[2 * pair : 2 * pair + 2, lanes]
                if plain:
                    out[spot, 2:3] = alone[:, lanes]

    channel = lax.broadcasted_iota(jnp.int32, (C, LANES), 0)

    def pack(columns):
        whole = jnp.zeros((C, LANES), F32)
        for k, column in enumerate(columns):
            whole = whole + jnp.where(lane == channel + 32 * k, column, 0.0)
        return jnp.sum(whole, axis=0, keepdims=True)

    def unpack(row, number):
        return [
            jnp.sum(jnp.where(lane == channel + 32 * k, row, 0.0), axis=1, keepdims=True)
            for k in range(number)
        ]

    class Total:
        def __init__(self, index):
            self.slots, self.index = sums.at[index], index

        def start(self, row):
            mine = self.slots.at[flat]
            mine[...] = row

            fan_out(
                lambda to: mine, mine, sums_send.at[self.index], sums_recv.at[self.index]
            )

        def finish(self):
            fan_in(self.slots, sums_recv.at[self.index])
            return jnp.sum(self.slots[...], axis=0)

        def drain(self):
            fan_in(self.slots, sums_send.at[self.index])

    totals = [Total(index) for index in range(4)]

    small_lane = lax.broadcasted_iota(jnp.int32, (C, C), 1)
    small_row = lax.broadcasted_iota(jnp.int32, (C, C), 0)

    def column(row):
        return jnp.sum(jnp.where(small_lane == small_row, row[...], 0.0), axis=1, keepdims=True)

    for load in loads[5:]:
        load.wait()
    gain_1, bias_1, gain_2, bias_2 = (column(row) for row in (row_1, row_2, row_3, row_4))

    def stack_weights(source, forward, backward):
        tiles = [
            jnp.concatenate(
                [source[tap].astype(F32) for tap in range(4 * k, min(4 * k + 4, 27))]
                + ([jnp.zeros((C, C), F32)] if k == 6 else []),
                axis=1,
            )
            for k in range(7)
        ]
        turned = [tile.T for tile in tiles]
        pieces = [turned[tap // 4][C * (tap % 4) : C * (tap % 4) + C] for tap in range(26, -1, -1)]
        back = [jnp.concatenate((pieces + pieces[:1])[4 * k : 4 * k + 4], axis=1) for k in range(7)]
        for index, parts in ((forward, tiles), (backward, back)):
            last = jnp.where(lane < 96, parts[6], 0.0)
            empty = jnp.zeros((C, LANES), F32)
            top = parts[:6] + [last, empty, empty]
            moved = [pltpu.roll(part, 32, 1) for part in parts[:6] + [last]]
            low = [empty, empty]
            for k in range(7):
                low.append(jnp.where(lane < 32, moved[k - 1] if k else empty, moved[k]))
            for k in range(9):
                weights[index, 0:C, LANES * k : LANES * (k + 1)] = top[k].astype(BF16)
                weights[index, C : 2 * C, LANES * k : LANES * (k + 1)] = low[k].astype(BF16)

    zero = jnp.zeros((C, LANES), F32)

    def take(load, source, at, carry):
        load.wait()
        for at_x in range(SPAN_X):
            rows_x[at, at_x + 1, 1 : SPAN_Y + 1] = jnp.swapaxes(
                source[:, at_x].astype(F32), 0, 1
            ).astype(BF16)
        for at_x in range(SPAN_X):

            def step(block, carry, at_x=at_x):
                for k in range(8):
                    at_y = block * 8 + k
                    carry = extract(
                        rows_x[at, at_x + 1, at_y + 1].astype(F32),
                        32 * at + 16 * at_x + at_y,
                        carry,
                    )
                return carry

            carry = lax.fori_loop(0, 2, step, carry)
        return carry

    carry = (zero, zero)
    for at, source in enumerate((block_a, block_b, block_g)):
        carry = take(loads[at], source, at, carry)
    edge_x[0] = carry[0].astype(BF16)
    edge_x[1] = carry[1].astype(BF16)

    pl.semaphore_wait(barrier, count - 1)

    near, rest = halo_x.small()
    waits_x = [halo_x.faces_x(0), halo_x.faces_x(1)]
    loads[3].wait()
    loads[4].wait()
    stack_weights(kernel_1, 0, 3)
    stack_weights(kernel_2, 1, 2)
    ok = [lane_keep(side) for side in range(2)]
    halo_x.arrive(near)
    for volume in range(2):
        for side in range(2):
            side_x[volume, side] = jnp.where(ok[side], halo_x.own(side, volume, lane), 0.0)
        build_inner(
            taps_x, volume,
            lambda at_x, at_y, volume=volume: rows_x[volume, at_x + 1, at_y + 1].astype(F32),
            (side_x.at[volume, 0], side_x.at[volume, 1]),
        )
    halo_x.arrive(rest)
    for side in range(2):
        for volume in range(3):
            tile = halo_x.merged(side, volume, lane)
            side_x[volume, side] = jnp.where(ok[side], tile, 0.0)

    columns = []
    waits_1 = []
    carry = (zero,) * 2
    for volume in range(2):
        halo_x.arrive(waits_x[volume])
        build_outer(
            taps_x, volume,
            lambda at_x, at_y, volume=volume: rows_x[volume, at_x, at_y].astype(F32),
            (side_x.at[volume, 0], side_x.at[volume, 1]),
        )

        def emit(at_x, at_y, tile, carry, volume=volume):
            total, squares, first, last = carry
            conv_1[volume, at_x, at_y] = tile
            rows_1[volume, at_x + 1, at_y + 1] = tile.astype(BF16)
            first, last = extract(tile, 32 * volume + 16 * at_x + at_y, (first, last))
            return total + tile, squares + tile * tile, first, last

        total, squares, *carry = convolve(taps_x, volume, 0, emit, (zero, zero, *carry))
        if volume == 0:
            waits_1.append(halo_1.faces_x(0))
        columns += [
            jnp.sum(total, axis=1, keepdims=True), jnp.sum(squares, axis=1, keepdims=True)
        ]
    edge_1[0] = carry[0].astype(BF16)
    edge_1[1] = carry[1].astype(BF16)
    totals[0].start(pack(columns))
    near, rest = halo_1.small()
    waits_1.append(halo_1.faces_x(1))
    row = totals[0].finish()
    halo_1.arrive(near + rest)
    waits_g = halo_x.faces_x(2)
    stats = unpack(row, 4)

    def moments(total, squares):
        mean = total / voxels
        scale = lax.rsqrt(squares / voxels - mean * mean + EPSILON)
        return mean, scale

    columns = []
    for volume in range(2):
        mean, scale = moments(stats[2 * volume], stats[2 * volume + 1])
        slope = jnp.broadcast_to(gain_1 * scale, (C, LANES))
        shift = jnp.broadcast_to(bias_1 - mean * gain_1 * scale, (C, LANES))

        def active(value, slope=slope, shift=shift):
            pre = value * slope + shift
            return pre * sigmoid(pre)

        norm_slope = jnp.broadcast_to(scale, (C, LANES))
        norm_shift = jnp.broadcast_to(-mean * scale, (C, LANES))

        def own_row(at_x, at_y, volume, active, norm_slope=norm_slope, norm_shift=norm_shift):
            value = conv_1[volume, at_x, at_y]
            if volume == 1:
                norms[at_x, at_y] = (value * norm_slope + norm_shift).astype(BF16)
            return active(value)

        for side in range(2):
            tile = halo_1.merged(side, volume, lane)
            side_1[volume, side] = tile
            side_h[volume, side] = jnp.where(ok[side], active(tile), 0.0)
        sides = (side_h.at[volume, 0], side_h.at[volume, 1])
        build_inner(
            taps_h, volume, functools.partial(own_row, volume=volume, active=active), sides
        )
        halo_1.arrive(waits_1[volume])
        build_outer(
            taps_h, volume,
            lambda at_x, at_y, volume=volume: active(rows_1[volume, at_x, at_y].astype(F32)),
            sides,
        )
        if volume == 0:

            def emit(at_x, at_y, tile, carry):
                total, squares = carry
                conv_2[0, at_x, at_y] = tile
                return total + tile, squares + tile * tile

            total, squares = convolve(taps_h, 0, 1, emit, (zero,) * 2)
        else:

            def emit(at_x, at_y, tile, carry):
                total, squares, first, last = carry
                conv_2[1, at_x, at_y] = tile
                rows_2[0, at_x + 1, at_y + 1] = tile.astype(BF16)
                first, last = extract(tile, 16 * at_x + at_y, (first, last))
                return total + tile, squares + tile * tile, first, last

            total, squares, first, last = convolve(taps_h, 1, 1, emit, (zero,) * 4)
            edge_2[0] = first.astype(BF16)
            edge_2[1] = last.astype(BF16)
        columns += [
            jnp.sum(total, axis=1, keepdims=True), jnp.sum(squares, axis=1, keepdims=True)
        ]
    mean_1, scale_1 = mean, scale
    totals[1].start(pack(columns))
    near, rest = halo_2.small()
    waits = near + rest + halo_2.faces_x(0)
    kernel_grad(taps_x, 1, lambda at_x, at_y: norms[at_x, at_y], early_out, 0, plain=True)
    fan_out(
        lambda to: early_out.at[to], early_in.at[flat], gw_send.at[0], gw_recv.at[0]
    )
    early_in[flat] = early_out[flat]
    stats = unpack(totals[1].finish(), 4)

    mean_2, scale_2 = moments(stats[2], stats[3])

    def layer_of(mean, scale, gain, bias):
        norm_slope = jnp.broadcast_to(scale, (C, LANES))
        norm_shift = jnp.broadcast_to(-mean * scale, (C, LANES))
        wide_gain = jnp.broadcast_to(gain, (C, LANES))
        wide_bias = jnp.broadcast_to(bias, (C, LANES))

        def slope_of(value, upstream):
            normed = value * norm_slope + norm_shift
            pre = wide_gain * normed + wide_bias
            sigma = sigmoid(pre)
            return upstream * (sigma * (1.0 + pre * (1.0 - sigma))), normed

        return slope_of

    def delta_of(slope_of, sum_d, sum_x, gain, scale):
        wide_d = jnp.broadcast_to(sum_d / voxels, (C, LANES))
        wide_x = jnp.broadcast_to(sum_x / voxels, (C, LANES))
        factor = jnp.broadcast_to(gain * scale, (C, LANES))

        def delta(value, upstream):
            slope, normed = slope_of(value, upstream)
            return factor * (slope - wide_d - normed * wide_x)

        return delta

    slope_2 = layer_of(mean_2, scale_2, gain_2, bias_2)

    def sum_rows(slope_of, value_of, upstream_of):
        carry = (zero, zero)
        for at_x in range(SPAN_X):

            def step(block, carry, at_x=at_x):
                total, weighted = carry
                for k in range(8):
                    at_y = block * 8 + k
                    slope, normed = slope_of(value_of(at_x, at_y), upstream_of(at_x, at_y))
                    total, weighted = total + slope, weighted + slope * normed
                return total, weighted

            carry = lax.fori_loop(0, 2, step, carry)
        return [jnp.sum(part, axis=1, keepdims=True) for part in carry]

    columns = sum_rows(
        slope_2,
        lambda at_x, at_y: conv_2[1, at_x, at_y],
        lambda at_x, at_y: rows_x[2, at_x + 1, at_y + 1].astype(F32),
    )
    totals[2].start(pack(columns))

    mean_a, scale_a = moments(stats[0], stats[1])
    slope_a = jnp.broadcast_to(gain_2 * scale_a, (C, LANES))
    shift_a = jnp.broadcast_to(bias_2 - mean_a * gain_2 * scale_a, (C, LANES))
    for at_x in range(SPAN_X):

        def step(block, carry, at_x=at_x):
            for k in range(8):
                at_y = block * 8 + k
                pre = conv_2[0, at_x, at_y] * slope_a + shift_a
                stage[at_x, at_y] = pre * sigmoid(pre)
            return carry

        lax.fori_loop(0, 2, step, 0)
        y_out[:, at_x] = jnp.swapaxes(stage[at_x], 0, 1).astype(BF16)

    halo_x.arrive(waits_g)
    halo_2.arrive(waits)
    sum_d2, sum_x2 = unpack(totals[2].finish(), 2)

    delta_2 = delta_of(slope_2, sum_d2, sum_x2, gain_2, scale_2)
    for side in range(2):
        tile = delta_2(halo_2.merged(side, 0, lane), side_x[2, side])
        side_2[0, side] = jnp.where(ok[side], tile, 0.0)
    build(
        taps_d2, 0,
        lambda at_x, at_y: delta_2(
            rows_2[0, at_x, at_y].astype(F32), rows_x[2, at_x, at_y].astype(F32)
        ),
        lambda at_x, at_y: delta_2(
            conv_2[1, at_x, at_y], rows_x[2, at_x + 1, at_y + 1].astype(F32)
        ),
        (side_2.at[0, 0], side_2.at[0, 1]),
    )
    slope_1 = layer_of(mean_1, scale_1, gain_1, bias_1)

    def emit(at_x, at_y, tile, carry):
        total, weighted, first, last = carry
        back_1[at_x, at_y] = tile
        rows_e[0, at_x + 1, at_y + 1] = tile.astype(BF16)
        first, last = extract(tile, 16 * at_x + at_y, (first, last))
        slope, normed = slope_1(conv_1[1, at_x, at_y], tile)
        slopes[at_x, at_y] = slope.astype(BF16)
        return total + slope, weighted + slope * normed, first, last

    total, weighted, first, last = convolve(taps_d2, 0, 2, emit, (zero,) * 4)
    edge_e[0] = first.astype(BF16)
    edge_e[1] = last.astype(BF16)
    columns = [
        jnp.sum(total, axis=1, keepdims=True), jnp.sum(weighted, axis=1, keepdims=True)
    ]
    totals[3].start(pack(columns))
    near, rest = halo_e.small()
    waits = near + rest + halo_e.faces_x(0)
    kernel_grad(taps_x, 1, lambda at_x, at_y: slopes[at_x, at_y], late_out, 0)
    kernel_grad(
        taps_h, 1, lambda at_x, at_y: taps_d2[0, at_x + 1, at_y + 1, C : 2 * C], late_out, 2
    )
    fan_out(lambda to: late_out.at[to], late_in.at[flat], gw_send.at[1], gw_recv.at[1])
    late_in[flat] = late_out[flat]
    sum_d1, sum_x1 = unpack(totals[3].finish(), 2)
    halo_e.arrive(waits)

    delta_1 = delta_of(slope_1, sum_d1, sum_x1, gain_1, scale_1)
    for side in range(2):
        tile = delta_1(side_1[1, side], halo_e.merged(side, 0, lane))
        side_e[0, side] = jnp.where(ok[side], tile, 0.0)
    build(
        taps_d1, 0,
        lambda at_x, at_y: delta_1(
            rows_1[1, at_x, at_y].astype(F32), rows_e[0, at_x, at_y].astype(F32)
        ),
        lambda at_x, at_y: delta_1(conv_1[1, at_x, at_y], back_1[at_x, at_y]),
        (side_e.at[0, 0], side_e.at[0, 1]),
    )
    whole = 1.0 / math.sqrt(voxels)
    for k, factor in enumerate(
        (gain_1 * scale_1 * whole, sum_d1 / voxels, sum_x1 / voxels)
    ):
        tile = jnp.broadcast_to(factor, (C, LANES))
        for pair in range(16):
            pairs[k, pair] = tile[2 * pair : 2 * pair + 2]
    fan_in(early_in, gw_recv.at[0])
    early = jnp.sum(early_in[...], axis=0)
    at = flat // 32 * 4 + lax.rem(flat, 4)
    fan_in(late_in, gw_recv.at[1])
    late = jnp.sum(late_in[...], axis=0)
    gathered[flat, 0:2] = pairs[0, at] * (
        late[0:2] - pairs[1, at] * early[2:3] - pairs[2, at] * early[0:2]
    )
    gathered[flat, 2:4] = late[2:4] * whole
    mine = gathered.at[flat]
    fan_out(lambda to: mine, mine, gw_send.at[2], gw_recv.at[2])

    def emit(at_x, at_y, tile, carry):
        stage[at_x, at_y] = tile
        return carry

    convolve(taps_d1, 0, 3, emit, 0)
    for at_x in range(SPAN_X):
        dx_out[:, at_x] = jnp.swapaxes(stage[at_x], 0, 1).astype(BF16)

    for k, total in enumerate((sum_x1, sum_d1, sum_x2, sum_d2)):
        norm_out[k : k + 1] = whole * jnp.sum(
            jnp.where(small_lane == small_row, total, 0.0), axis=0, keepdims=True
        )
    fan_in(gathered, gw_recv.at[2])
    for member, out in ((0, gw_first), (1, gw_second)):
        for k in range(7):
            tile = jnp.concatenate(
                [
                    gathered[(pair // 4 * 8 + k) * 4 + pair % 4, 2 * member : 2 * member + 2]
                    for pair in range(16)
                ],
                axis=0,
            )
            for tap in range(4 * k, min(4 * k + 4, 27)):
                out[tap] = tile[:, C * (tap % 4) : C * (tap % 4) + C]

    for halo in halos:
        halo.drain()
    for total in totals:
        total.drain()
    for k, chunks in enumerate((early_out, late_out, gathered)):
        fan_in(chunks, gw_send.at[k])


def write_out(*refs):
    sources, targets, semaphores = refs[:5], refs[5:10], refs[10]
    copies = [
        pltpu.make_async_copy(source, target, semaphores.at[index])
        for index, (source, target) in enumerate(zip(sources, targets))
    ]
    for copy in copies:
        copy.start()
    for copy in copies:
        copy.wait()


def body(voxels, x_a, x_b, w_first, w_second, gain_first, bias_first, gain_second, bias_second,
         grad_out):
    def sized(*shape, kind=BF16):
        return pltpu.VMEM(shape, kind)

    volumes = (3, 2, 1, 1)
    devices = math.prod(lax.axis_size(axis) for axis in AXES)
    block = (C, SPAN_X, SPAN_Y, LANES)
    scratch = [sized(*block)] * 3 + [sized(27, C, C)] * 2 + [sized(1, C, kind=F32)] * 4
    scratch += [
        sized(4, SPAN_X * C, DEPTH), sized(SPAN_X, SPAN_Y, C, LANES, kind=F32)
    ]
    scratch += [sized(count, PAD_X, PAD_Y, TAPS, LANES) for count in (2, 2, 1, 1)]
    scratch += [sized(count, PAD_X, PAD_Y, C, LANES) for count in volumes]
    scratch += [sized(2, 3, 3, C, LANES) for count in volumes]
    scratch += [sized(2, C, LANES) for count in volumes]
    scratch += [sized(count, 2, C, LANES, kind=F32) for count in volumes]
    scratch += [sized(2, 2, C, LANES, kind=F32)]
    scratch += [
        sized(2, SPAN_X, SPAN_Y, C, LANES, kind=F32),
        sized(2, SPAN_X, SPAN_Y, C, LANES, kind=F32),
        sized(SPAN_X, SPAN_Y, C, LANES, kind=F32),
        sized(4, devices, 1, LANES, kind=F32),
        sized(SPAN_X, SPAN_Y, C, LANES),
        sized(SPAN_X, SPAN_Y, C, LANES),
        sized(devices, 4, LANES, kind=F32),
        sized(devices, 4, LANES, kind=F32),
        sized(devices, 4, LANES, kind=F32),
        sized(devices, 4, LANES, kind=F32),
        sized(devices, 4, LANES, kind=F32),
        sized(3, 16, 2, LANES, kind=F32),
        pltpu.SemaphoreType.DMA((4, 32)),
        pltpu.SemaphoreType.DMA((4, 32)),
        pltpu.SemaphoreType.DMA((4,)),
        pltpu.SemaphoreType.DMA((4,)),
        pltpu.SemaphoreType.DMA((3,)),
        pltpu.SemaphoreType.DMA((3,)),
        pltpu.SemaphoreType.DMA((9,)),
    ]
    in_vmem = pl.BlockSpec(memory_space=pltpu.VMEM)
    in_hbm = pl.BlockSpec(memory_space=pltpu.HBM)
    taps = jax.ShapeDtypeStruct((27, C, C), F32)
    out_shape = (
        jax.ShapeDtypeStruct(block, BF16),
        jax.ShapeDtypeStruct(block, BF16),
        taps,
        taps,
        jax.ShapeDtypeStruct((4, C), F32),
    )
    results = pl.pallas_call(
        functools.partial(kernel, voxels),
        out_shape=out_shape,
        in_specs=[in_hbm] * 9,
        out_specs=(in_vmem,) * 5,
        scratch_shapes=scratch,
        compiler_params=pltpu.CompilerParams(
            collective_id=0, has_side_effects=True, vmem_limit_bytes=28 * 1024 * 1024
        ),
    )(
        *(pltpu.with_memory_space_constraint(value, pltpu.HBM) for value in (
            x_a, x_b, grad_out, w_first.reshape(27, C, C), w_second.reshape(27, C, C),
            *(row.reshape(1, C) for row in (gain_first, bias_first, gain_second, bias_second)),
        )),
    )
    y_a, dx_b, grad_first, grad_second, norms = pl.pallas_call(
        write_out,
        out_shape=out_shape,
        in_specs=[in_vmem] * 5,
        out_specs=(in_hbm,) * 5,
        scratch_shapes=[pltpu.SemaphoreType.DMA((5,))],
        compiler_params=pltpu.CompilerParams(vmem_limit_bytes=8 * 1024 * 1024),
    )(*results)
    return (
        y_a, dx_b, grad_first.reshape(3, 3, 3, C, C), grad_second.reshape(3, 3, 3, C, C), norms
    )


def solution(mesh):
    split = P(None, "gx", "gy", "gz")
    voxels = float(SPAN_X * SPAN_Y * LANES * mesh.size)
    return jax.shard_map(
        functools.partial(body, voxels),
        mesh=mesh,
        in_specs=(split, split, P(), P(), P(), P(), P(), P(), split),
        out_specs=(split, split, P(), P(), P()),
        check_vma=False,
    )
```

```python
import functools
import math

import jax
import jax.numpy as jnp
from jax import lax
from jax.experimental import pallas as pl
from jax.experimental.pallas import tpu as pltpu
from jax.sharding import PartitionSpec as P

F32 = jnp.float32
BF16 = jnp.bfloat16
EPSILON = 1e-05
C = 32
LANES = 128
SPAN_X, SPAN_Y = 2, 16
PAD_X, PAD_Y = SPAN_X + 2, SPAN_Y + 2
TAPS = 3 * C
DEPTH = PAD_X * 3 * TAPS
FLAT = 9 * TAPS
GROUP = 4
INNER = 16
OUTER = 18
AXES = ("gx", "gy", "gz")
MESH = pl.DeviceIdType.MESH


def sigmoid(value):
    return 0.5 + 0.5 * jnp.tanh(0.5 * value)


def unrolled(first, last, step, carry):
    for index in range(first, last):
        carry = step(index, carry)
    return carry


def rolled(tile, shift):
    shift = shift % LANES
    return pltpu.roll(tile, shift, 1) if shift else tile


class Halo:
    def __init__(self, rows, cols, edge, side, send, recv, place, volumes):
        self.rows, self.cols, self.edge, self.side = rows, cols, edge, side
        self.send, self.recv, self.place, self.volumes = send, recv, place, volumes
        self.count = 0
        self.sent = []

    def has(self, steps):
        present = None
        for axis, step in zip(AXES, steps):
            if step:
                me, size = self.place[axis]
                inside = me > 0 if step < 0 else me < size - 1
                present = inside if present is None else jnp.logical_and(present, inside)
        return present

    def push(self, source, target, *steps):
        index = self.count
        self.count += 1
        to = {}
        for axis, step in zip(AXES, steps):
            if step:
                me, size = self.place[axis]
                to[axis] = lax.rem(me + step + size, size)
        copy = pltpu.make_async_remote_copy(
            src_ref=source,
            dst_ref=target,
            send_sem=self.send.at[index],
            recv_sem=self.recv.at[index],
            device_id=to,
            device_id_type=MESH,
        )
        present = self.has(steps)

        @pl.when(present)
        def _():
            copy.start()

        self.sent.append((copy, present))
        return copy, self.has([-step for step in steps])

    def faces_x(self, volume):
        rows, inner = self.rows, pl.ds(1, SPAN_Y)
        return [
            self.push(
                rows.at[volume, 1 if step < 0 else SPAN_X, inner],
                rows.at[volume, PAD_X - 1 if step < 0 else 0, inner],
                step, 0, 0,
            )
            for step in (-1, 1)
        ]

    def columns(self, step_x, step_y):
        return [
            self.push(
                self.edge.at[0 if step < 0 else 1],
                self.cols.at[1 if step < 0 else 0, 1 - step_x, 1 - step_y],
                step_x, step_y, step,
            )
            for step in (-1, 1)
        ]

    def small(self):
        rows, every = self.rows, pl.ds(0, self.volumes)
        near = self.columns(0, 0)
        rest = []
        for step_x in (-1, 0, 1):
            at_x = (1 if step_x < 0 else SPAN_X) if step_x else pl.ds(1, SPAN_X)
            to_x = (PAD_X - 1 if step_x < 0 else 0) if step_x else pl.ds(1, SPAN_X)
            for step_y in (-1, 1):
                rest.append(
                    self.push(
                        rows.at[every, at_x, 1 if step_y < 0 else SPAN_Y],
                        rows.at[every, to_x, PAD_Y - 1 if step_y < 0 else 0],
                        step_x, step_y, 0,
                    )
                )
        for step_x, step_y in (
            (-1, -1), (-1, 1), (1, -1), (1, 1), (-1, 0), (1, 0), (0, -1), (0, 1)
        ):
            rest += self.columns(step_x, step_y)
        return near, rest

    def own(self, side, volume, lane):
        tile = self.cols[side, 1, 1]
        at = 32 * volume
        return jnp.where(lane < 64, rolled(tile, 33 - at), rolled(tile, 49 - at))

    def merged(self, side, volume, lane):
        at = 32 * volume
        inside = lax.rem(lane, 32)

        def strip(index, low, middle, high):
            low, middle, high = (
                rolled(self.cols[side, index, k], shift - at)
                for k, shift in enumerate((low, middle, high))
            )
            return jnp.where(inside == 0, low, jnp.where(inside == PAD_Y - 1, high, middle))

        return jnp.where(
            lane < 64,
            jnp.where(lane < 32, strip(0, -31, -15, 1), strip(1, 17, 33, 49)),
            jnp.where(lane < 96, strip(1, 33, 49, 65), strip(2, 81, 97, 113)),
        )

    @staticmethod
    def arrive(pushes):
        for copy, present in pushes:

            @pl.when(present)
            def _(copy=copy):
                copy.wait_recv()

    def drain(self):
        for copy, present in self.sent:

            @pl.when(present)
            def _(copy=copy):
                copy.wait_send()


def kernel(
    voxels,
    x_a, x_b, grad, w_first, w_second, gain_first, bias_first, gain_second, bias_second,
    y_out, dx_out, gw_first, gw_second, norm_out,
    block_a, block_b, block_g, kernel_1, kernel_2, row_1, row_2, row_3, row_4, weights, stage,
    taps_x, taps_h, taps_d2, taps_d1,
    rows_x, rows_1, rows_2, rows_e,
    cols_x, cols_1, cols_2, cols_e,
    edge_x, edge_1, edge_2, edge_e,
    side_x, side_1, side_2, side_e,
    side_h,
    conv_1, conv_2, back_1,
    sums,
    norms, slopes, early_out, early_in, late_out, late_in, gathered, pairs,
    halo_send, halo_recv, sums_send, sums_recv, gw_send, gw_recv, local,
):
    loads = [
        pltpu.make_async_copy(source, target, local.at[index])
        for index, (source, target) in enumerate((
            (x_a, block_a), (x_b, block_b), (grad, block_g), (w_first, kernel_1),
            (w_second, kernel_2), (gain_first, row_1), (bias_first, row_2), (gain_second, row_3),
            (bias_second, row_4),
        ))
    ]
    for load in loads:
        load.start()
    place = {axis: (lax.axis_index(axis), lax.axis_size(axis)) for axis in AXES}
    for chunks in (early_out, late_out):
        for j in range(4):
            chunks[32 * j + 28 : 32 * j + 32] = jnp.zeros((4, 4, LANES), F32)
    barrier = pltpu.get_barrier_semaphore()
    count = place["gx"][1] * place["gy"][1] * place["gz"][1]
    flat = (place["gx"][0] * place["gy"][1] + place["gy"][0]) * place["gz"][1] + place["gz"][0]

    chip_x, chip_y = place["gy"][0], place["gz"][0] // 2
    chip_z = place["gx"][0] // 2 * 2 + lax.rem(place["gz"][0], 2)
    core = lax.rem(place["gx"][0], 2)

    def other(step):
        return lax.rem(flat + step, count)

    def fan_out(source_of, target, send, recv):
        spots = []
        for step_z, step_core in ((2, 1), (2, 0), (1, 1), (3, 1), (1, 0), (3, 0), (0, 1), (0, 0)):
            to_z, to_core = lax.rem(chip_z + step_z, 4), lax.rem(core + step_core, 2)
            spots.append(to_z // 2 * 64 + to_core * 32 + lax.rem(to_z, 2))

        def copies(plane, chosen):
            to_x = lax.rem(chip_x + plane // 4 + 1, 4)
            to_y = lax.rem(chip_y + lax.rem(plane, 4) + 1, 4)
            for spot in chosen:
                to = spot + to_x * 8 + to_y * 2
                pltpu.make_async_remote_copy(
                    src_ref=source_of(to), dst_ref=target, send_sem=send, recv_sem=recv,
                    device_id=to, device_id_type=pl.DeviceIdType.LOGICAL,
                ).start()

        def most(block, carry):
            for k in range(4):
                copies(block * 4 + k, spots[:-1])
            return carry

        def rest(block, carry):
            for k in range(5):
                copies(block * 5 + k, spots[-1:])
            return carry

        lax.fori_loop(0, 4, most, 0)
        lax.fori_loop(0, 3, rest, 0)

    def fan_in(slots, semaphore):
        part = slots.at[pl.ds(0, count - 1)]
        pltpu.make_async_copy(part, part, semaphore).wait()

    def greet(step, carry):
        pl.semaphore_signal(
            barrier, inc=1, device_id=other(step), device_id_type=pl.DeviceIdType.LOGICAL
        )
        return carry

    lax.fori_loop(1, count, greet, 0)

    lane = lax.broadcasted_iota(jnp.int32, (C, LANES), 1)
    halos = []
    for index, (rows, cols, edge, side, volumes) in enumerate((
        (rows_x, cols_x, edge_x, side_x, 3),
        (rows_1, cols_1, edge_1, side_1, 2),
        (rows_2, cols_2, edge_2, side_2, 1),
        (rows_e, cols_e, edge_e, side_e, 1),
    )):
        halos.append(
            Halo(rows, cols, edge, side, halo_send.at[index], halo_recv.at[index], place, volumes)
        )
    halo_x, halo_1, halo_2, halo_e = halos

    low_x, high_x = place["gx"][0] > 0, place["gx"][0] < place["gx"][1] - 1
    low_y, high_y = place["gy"][0] > 0, place["gy"][0] < place["gy"][1] - 1
    low_z, high_z = place["gz"][0] > 0, place["gz"][0] < place["gz"][1] - 1

    def keep(at_x, at_y):
        held_x = low_x if at_x == 0 else high_x if at_x == PAD_X - 1 else None
        if isinstance(at_y, int):
            held_y = low_y if at_y == 0 else high_y if at_y == PAD_Y - 1 else None
        else:
            held_y = jnp.logical_and(
                jnp.logical_or(at_y > 0, low_y), jnp.logical_or(at_y < PAD_Y - 1, high_y)
            )
        if held_x is None:
            return held_y
        return held_x if held_y is None else jnp.logical_and(held_x, held_y)

    def lane_keep(side):
        spot_x, spot_y = lane // 32, lax.rem(lane, 32)
        bad = jnp.zeros((C, LANES), jnp.int32)
        for hit, present in (
            (spot_x == 0, low_x), (spot_x == PAD_X - 1, high_x),
            (spot_y == 0, low_y), (spot_y == PAD_Y - 1, high_y),
        ):
            missing = jnp.where(present, 0, 1)
            bad = bad + jnp.where(hit, missing, 0)
        bad = bad + jnp.where(low_z if side == 0 else high_z, 0, 1)
        return bad == 0

    def extract(tile, spot, carry):
        first, last = carry
        tile = tile.astype(BF16)
        first = jnp.where(lane == spot, pltpu.roll(tile, spot, 1), first)
        last = jnp.where(lane == spot, pltpu.roll(tile, lax.rem(spot + 1, LANES), 1), last)
        return first, last

    def put_taps(taps, volume, spots, tiles, sides):
        low, high = sides[0][...], sides[1][...]
        shifted = []
        for (at_x, at_y), tile in zip(spots, tiles):
            spot = at_x * 32 + at_y
            left = jnp.where(
                lane == 0,
                pltpu.roll(low, lax.rem(LANES - spot, LANES), 1),
                pltpu.roll(tile, 1, 1),
            )
            right = jnp.where(
                lane == LANES - 1,
                pltpu.roll(high, LANES - 1 - spot, 1),
                pltpu.roll(tile, LANES - 1, 1),
            )
            shifted.append((left, tile, right))
        for (at_x, at_y), rows in zip(spots, shifted):
            for k, row in enumerate(rows):
                taps[volume, at_x, at_y, k * C : (k + 1) * C] = row

    def build_inner(taps, volume, inner, sides):
        for at_x in range(SPAN_X):

            def step(block, carry, at_x=at_x):
                rows = [block * INNER + k for k in range(INNER)]
                tiles = [inner(at_x, at_y).astype(BF16) for at_y in rows]
                put_taps(taps, volume, [(at_x + 1, at_y + 1) for at_y in rows], tiles, sides)
                return carry

            unrolled(0, SPAN_Y // INNER, step, 0)

    def build_outer(taps, volume, outer, sides):
        def put(spots):
            tiles = [
                jnp.where(keep(at_x, at_y), outer(at_x, at_y).astype(BF16), none)
                for at_x, at_y in spots
            ]
            put_taps(taps, volume, spots, tiles, sides)

        put([(at_x, at_y) for at_x in (1, 2) for at_y in (0, PAD_Y - 1)])
        for at_x in (0, PAD_X - 1):

            def step(block, carry, at_x=at_x):
                put([(at_x, block * OUTER + k) for k in range(OUTER)])
                return carry

            unrolled(0, PAD_Y // OUTER, step, 0)

    def build(taps, volume, outer, inner, sides):
        build_inner(taps, volume, inner, sides)
        build_outer(taps, volume, outer, sides)

    def convolve(taps, volume, weight, emit, carry):
        def step(block, carry):
            first = block * GROUP
            columns = [
                taps[volume, :, pl.ds(first + k, 3)].reshape(DEPTH, LANES) for k in range(GROUP)
            ]
            total = jnp.dot(
                weights[weight],
                jnp.concatenate(columns, axis=1),
                preferred_element_type=F32,
            )
            for k in range(GROUP):
                for at_x in range(SPAN_X):
                    tile = total[at_x * C : (at_x + 1) * C, k * LANES : (k + 1) * LANES]
                    carry = emit(at_x, first + k, tile, carry)
            return carry

        return unrolled(0, SPAN_Y // GROUP, step, carry)

    def kernel_grad(taps, volume, row_of, out, first_row, plain=False):
        high = SPAN_X * C + (16 if plain else 0)

        def step(block, total):
            first = block * GROUP
            left, right = [], []
            for k in range(GROUP):
                rows = [row_of(at_x, first + k) for at_x in range(SPAN_X)]
                if plain:
                    rows.append(jnp.ones((16, LANES), BF16))
                left.append(jnp.concatenate(rows, axis=0))
                right.append(taps[volume, :, pl.ds(first + k, 3)].reshape(DEPTH, LANES))
            return total + lax.dot_general(
                jnp.concatenate(left, axis=1),
                jnp.concatenate(right, axis=1),
                (((1,), (1,)), ((), ())),
                preferred_element_type=F32,
            )

        total = unrolled(0, SPAN_Y // GROUP, step, 0.0)
        slab = 3 * TAPS

        def wide(value):
            return jnp.concatenate(
                [value, jnp.zeros((value.shape[0], 7 * LANES - FLAT), F32)], axis=1
            )

        both = wide(total[0:C, 0:FLAT] + total[C : 2 * C, slab : slab + FLAT])
        if plain:
            alone = total[2 * C : 2 * C + 1]
            alone = wide(alone[:, 0:FLAT] + alone[:, slab : slab + FLAT])
        for k in range(7):
            lanes = slice(LANES * k, LANES * (k + 1))
            for pair in range(16):
                spot = (pair // 4 * 8 + k) * 4 + pair % 4
                out[spot, first_row : first_row + 2] = both[2 * pair : 2 * pair + 2, lanes]
                if plain:
                    out[spot, 2:3] = alone[:, lanes]

    channel = lax.broadcasted_iota(jnp.int32, (C, LANES), 0)

    def pack(columns):
        whole = jnp.zeros((C, LANES), F32)
        for k, column in enumerate(columns):
            whole = whole + jnp.where(lane == channel + 32 * k, column, 0.0)
        return jnp.sum(whole, axis=0, keepdims=True)

    def unpack(row, number):
        return [
            jnp.sum(jnp.where(lane == channel + 32 * k, row, 0.0), axis=1, keepdims=True)
            for k in range(number)
        ]

    class Total:
        def __init__(self, index):
            self.slots, self.index = sums.at[index], index

        def start(self, row):
            mine = self.slots.at[flat]
            mine[...] = row

            fan_out(
                lambda to: mine, mine, sums_send.at[self.index], sums_recv.at[self.index]
            )

        def finish(self):
            fan_in(self.slots, sums_recv.at[self.index])
            return jnp.sum(self.slots[...], axis=0)

        def drain(self):
            fan_in(self.slots, sums_send.at[self.index])

    totals = [Total(index) for index in range(4)]

    small_lane = lax.broadcasted_iota(jnp.int32, (C, C), 1)
    small_row = lax.broadcasted_iota(jnp.int32, (C, C), 0)

    def column(row):
        return jnp.sum(jnp.where(small_lane == small_row, row[...], 0.0), axis=1, keepdims=True)

    for load in loads[5:]:
        load.wait()
    gain_1, bias_1, gain_2, bias_2 = (column(row) for row in (row_1, row_2, row_3, row_4))

    def stack_weights(source, forward, backward):
        tiles = [
            jnp.concatenate(
                [source[tap].astype(F32) for tap in range(4 * k, min(4 * k + 4, 27))]
                + ([jnp.zeros((C, C), F32)] if k == 6 else []),
                axis=1,
            )
            for k in range(7)
        ]
        turned = [tile.T for tile in tiles]
        pieces = [turned[tap // 4][C * (tap % 4) : C * (tap % 4) + C] for tap in range(26, -1, -1)]
        back = [jnp.concatenate((pieces + pieces[:1])[4 * k : 4 * k + 4], axis=1) for k in range(7)]
        for index, parts in ((forward, tiles), (backward, back)):
            last = jnp.where(lane < 96, parts[6], 0.0)
            empty = jnp.zeros((C, LANES), F32)
            top = parts[:6] + [last, empty, empty]
            moved = [pltpu.roll(part, 32, 1) for part in parts[:6] + [last]]
            low = [empty, empty]
            for k in range(7):
                low.append(jnp.where(lane < 32, moved[k - 1] if k else empty, moved[k]))
            for k in range(9):
                weights[index, 0:C, LANES * k : LANES * (k + 1)] = top[k].astype(BF16)
                weights[index, C : 2 * C, LANES * k : LANES * (k + 1)] = low[k].astype(BF16)

    zero = jnp.zeros((C, LANES), F32)
    none = jnp.zeros((C, LANES), BF16)

    def take(load, source, at, carry):
        load.wait()
        for at_x in range(SPAN_X):
            rows_x[at, at_x + 1, 1 : SPAN_Y + 1] = jnp.swapaxes(
                source[:, at_x].astype(F32), 0, 1
            ).astype(BF16)
        for at_x in range(SPAN_X):

            def step(block, carry, at_x=at_x):
                for k in range(8):
                    at_y = block * 8 + k
                    carry = extract(
                        rows_x[at, at_x + 1, at_y + 1],
                        32 * at + 16 * at_x + at_y,
                        carry,
                    )
                return carry

            carry = unrolled(0, 2, step, carry)
        return carry

    carry = (none, none)
    for at, source in enumerate((block_a, block_b, block_g)):
        carry = take(loads[at], source, at, carry)
    edge_x[0] = carry[0]
    edge_x[1] = carry[1]

    pl.semaphore_wait(barrier, count - 1)

    near, rest = halo_x.small()
    waits_x = [halo_x.faces_x(0), halo_x.faces_x(1)]
    loads[3].wait()
    loads[4].wait()
    stack_weights(kernel_1, 0, 3)
    stack_weights(kernel_2, 1, 2)
    ok = [lane_keep(side) for side in range(2)]
    halo_x.arrive(near)
    for volume in range(2):
        for side in range(2):
            side_x[volume, side] = jnp.where(ok[side], halo_x.own(side, volume, lane), none)
        build_inner(
            taps_x, volume,
            lambda at_x, at_y, volume=volume: rows_x[volume, at_x + 1, at_y + 1],
            (side_x.at[volume, 0], side_x.at[volume, 1]),
        )
    halo_x.arrive(rest)
    for side in range(2):
        for volume in range(3):
            tile = halo_x.merged(side, volume, lane)
            side_x[volume, side] = jnp.where(ok[side], tile, none)

    columns = []
    waits_1 = []
    carry = (none,) * 2
    for volume in range(2):
        halo_x.arrive(waits_x[volume])
        build_outer(
            taps_x, volume,
            lambda at_x, at_y, volume=volume: rows_x[volume, at_x, at_y],
            (side_x.at[volume, 0], side_x.at[volume, 1]),
        )

        def emit(at_x, at_y, tile, carry, volume=volume):
            total, squares, first, last = carry
            conv_1[volume, at_x, at_y] = tile
            rows_1[volume, at_x + 1, at_y + 1] = tile.astype(BF16)
            first, last = extract(tile, 32 * volume + 16 * at_x + at_y, (first, last))
            return total + tile, squares + tile * tile, first, last

        total, squares, *carry = convolve(taps_x, volume, 0, emit, (zero, zero, *carry))
        if volume == 0:
            waits_1.append(halo_1.faces_x(0))
        columns += [
            jnp.sum(total, axis=1, keepdims=True), jnp.sum(squares, axis=1, keepdims=True)
        ]
    edge_1[0] = carry[0]
    edge_1[1] = carry[1]
    totals[0].start(pack(columns))
    near, rest = halo_1.small()
    waits_1.append(halo_1.faces_x(1))
    row = totals[0].finish()
    halo_1.arrive(near + rest)
    waits_g = halo_x.faces_x(2)
    stats = unpack(row, 4)

    def moments(total, squares):
        mean = total / voxels
        scale = lax.rsqrt(squares / voxels - mean * mean + EPSILON)
        return mean, scale

    columns = []
    for volume in range(2):
        mean, scale = moments(stats[2 * volume], stats[2 * volume + 1])
        slope = jnp.broadcast_to(gain_1 * scale, (C, LANES))
        shift = jnp.broadcast_to(bias_1 - mean * gain_1 * scale, (C, LANES))

        def active(value, slope=slope, shift=shift):
            pre = value * slope + shift
            return pre * sigmoid(pre)

        norm_slope = jnp.broadcast_to(scale, (C, LANES))
        norm_shift = jnp.broadcast_to(-mean * scale, (C, LANES))

        def own_row(at_x, at_y, volume, active, norm_slope=norm_slope, norm_shift=norm_shift):
            value = conv_1[volume, at_x, at_y]
            if volume == 1:
                norms[at_x, at_y] = (value * norm_slope + norm_shift).astype(BF16)
            return active(value)

        for side in range(2):
            tile = halo_1.merged(side, volume, lane)
            side_1[volume, side] = tile
            side_h[volume, side] = jnp.where(
                ok[side], active(tile.astype(F32)), 0.0
            ).astype(BF16)
        sides = (side_h.at[volume, 0], side_h.at[volume, 1])
        build_inner(
            taps_h, volume, functools.partial(own_row, volume=volume, active=active), sides
        )
        halo_1.arrive(waits_1[volume])
        build_outer(
            taps_h, volume,
            lambda at_x, at_y, volume=volume: active(rows_1[volume, at_x, at_y].astype(F32)),
            sides,
        )
        if volume == 0:

            def emit(at_x, at_y, tile, carry):
                total, squares = carry
                conv_2[0, at_x, at_y] = tile
                return total + tile, squares + tile * tile

            total, squares = convolve(taps_h, 0, 1, emit, (zero,) * 2)
        else:

            def emit(at_x, at_y, tile, carry):
                total, squares, first, last = carry
                conv_2[1, at_x, at_y] = tile
                rows_2[0, at_x + 1, at_y + 1] = tile.astype(BF16)
                first, last = extract(tile, 16 * at_x + at_y, (first, last))
                return total + tile, squares + tile * tile, first, last

            total, squares, first, last = convolve(taps_h, 1, 1, emit, (zero, zero, none, none))
            edge_2[0] = first
            edge_2[1] = last
        columns += [
            jnp.sum(total, axis=1, keepdims=True), jnp.sum(squares, axis=1, keepdims=True)
        ]
    mean_1, scale_1 = mean, scale
    totals[1].start(pack(columns))
    near, rest = halo_2.small()
    waits = near + rest + halo_2.faces_x(0)
    kernel_grad(taps_x, 1, lambda at_x, at_y: norms[at_x, at_y], early_out, 0, plain=True)
    fan_out(
        lambda to: early_out.at[to], early_in.at[flat], gw_send.at[0], gw_recv.at[0]
    )
    early_in[flat] = early_out[flat]
    stats = unpack(totals[1].finish(), 4)

    mean_2, scale_2 = moments(stats[2], stats[3])

    def layer_of(mean, scale, gain, bias):
        norm_slope = jnp.broadcast_to(scale, (C, LANES))
        norm_shift = jnp.broadcast_to(-mean * scale, (C, LANES))
        wide_gain = jnp.broadcast_to(gain, (C, LANES))
        wide_bias = jnp.broadcast_to(bias, (C, LANES))

        def slope_of(value, upstream):
            normed = value * norm_slope + norm_shift
            pre = wide_gain * normed + wide_bias
            sigma = sigmoid(pre)
            return upstream * (sigma * (1.0 + pre * (1.0 - sigma))), normed

        return slope_of

    def delta_of(slope_of, sum_d, sum_x, gain, scale):
        wide_d = jnp.broadcast_to(sum_d / voxels, (C, LANES))
        wide_x = jnp.broadcast_to(sum_x / voxels, (C, LANES))
        factor = jnp.broadcast_to(gain * scale, (C, LANES))

        def delta(value, upstream):
            slope, normed = slope_of(value, upstream)
            return factor * (slope - wide_d - normed * wide_x)

        return delta

    slope_2 = layer_of(mean_2, scale_2, gain_2, bias_2)

    def sum_rows(slope_of, value_of, upstream_of):
        carry = (zero, zero)
        for at_x in range(SPAN_X):

            def step(block, carry, at_x=at_x):
                total, weighted = carry
                for k in range(8):
                    at_y = block * 8 + k
                    slope, normed = slope_of(value_of(at_x, at_y), upstream_of(at_x, at_y))
                    total, weighted = total + slope, weighted + slope * normed
                return total, weighted

            carry = unrolled(0, 2, step, carry)
        return [jnp.sum(part, axis=1, keepdims=True) for part in carry]

    columns = sum_rows(
        slope_2,
        lambda at_x, at_y: conv_2[1, at_x, at_y],
        lambda at_x, at_y: rows_x[2, at_x + 1, at_y + 1].astype(F32),
    )
    totals[2].start(pack(columns))

    mean_a, scale_a = moments(stats[0], stats[1])
    slope_a = jnp.broadcast_to(gain_2 * scale_a, (C, LANES))
    shift_a = jnp.broadcast_to(bias_2 - mean_a * gain_2 * scale_a, (C, LANES))
    for at_x in range(SPAN_X):

        def step(block, carry, at_x=at_x):
            for k in range(8):
                at_y = block * 8 + k
                pre = conv_2[0, at_x, at_y] * slope_a + shift_a
                stage[at_x, at_y] = pre * sigmoid(pre)
            return carry

        unrolled(0, 2, step, 0)
        y_out[:, at_x] = jnp.swapaxes(stage[at_x], 0, 1).astype(BF16)

    halo_x.arrive(waits_g)
    halo_2.arrive(waits)
    sum_d2, sum_x2 = unpack(totals[2].finish(), 2)

    delta_2 = delta_of(slope_2, sum_d2, sum_x2, gain_2, scale_2)
    for side in range(2):
        tile = delta_2(
            halo_2.merged(side, 0, lane).astype(F32), side_x[2, side].astype(F32)
        )
        side_2[0, side] = jnp.where(ok[side], tile, 0.0).astype(BF16)
    build(
        taps_d2, 0,
        lambda at_x, at_y: delta_2(
            rows_2[0, at_x, at_y].astype(F32), rows_x[2, at_x, at_y].astype(F32)
        ),
        lambda at_x, at_y: delta_2(
            conv_2[1, at_x, at_y], rows_x[2, at_x + 1, at_y + 1].astype(F32)
        ),
        (side_2.at[0, 0], side_2.at[0, 1]),
    )
    slope_1 = layer_of(mean_1, scale_1, gain_1, bias_1)

    def emit(at_x, at_y, tile, carry):
        total, weighted, first, last = carry
        back_1[at_x, at_y] = tile
        rows_e[0, at_x + 1, at_y + 1] = tile.astype(BF16)
        first, last = extract(tile, 16 * at_x + at_y, (first, last))
        slope, normed = slope_1(conv_1[1, at_x, at_y], tile)
        slopes[at_x, at_y] = slope.astype(BF16)
        return total + slope, weighted + slope * normed, first, last

    total, weighted, first, last = convolve(taps_d2, 0, 2, emit, (zero, zero, none, none))
    edge_e[0] = first
    edge_e[1] = last
    columns = [
        jnp.sum(total, axis=1, keepdims=True), jnp.sum(weighted, axis=1, keepdims=True)
    ]
    totals[3].start(pack(columns))
    near, rest = halo_e.small()
    waits = near + rest + halo_e.faces_x(0)
    kernel_grad(taps_x, 1, lambda at_x, at_y: slopes[at_x, at_y], late_out, 0)
    kernel_grad(
        taps_h, 1, lambda at_x, at_y: taps_d2[0, at_x + 1, at_y + 1, C : 2 * C], late_out, 2
    )
    fan_out(lambda to: late_out.at[to], late_in.at[flat], gw_send.at[1], gw_recv.at[1])
    late_in[flat] = late_out[flat]
    sum_d1, sum_x1 = unpack(totals[3].finish(), 2)
    halo_e.arrive(waits)

    delta_1 = delta_of(slope_1, sum_d1, sum_x1, gain_1, scale_1)
    for side in range(2):
        tile = delta_1(
            side_1[1, side].astype(F32), halo_e.merged(side, 0, lane).astype(F32)
        )
        side_e[0, side] = jnp.where(ok[side], tile, 0.0).astype(BF16)
    build(
        taps_d1, 0,
        lambda at_x, at_y: delta_1(
            rows_1[1, at_x, at_y].astype(F32), rows_e[0, at_x, at_y].astype(F32)
        ),
        lambda at_x, at_y: delta_1(conv_1[1, at_x, at_y], back_1[at_x, at_y]),
        (side_e.at[0, 0], side_e.at[0, 1]),
    )
    whole = 1.0 / math.sqrt(voxels)
    for k, factor in enumerate(
        (gain_1 * scale_1 * whole, sum_d1 / voxels, sum_x1 / voxels)
    ):
        tile = jnp.broadcast_to(factor, (C, LANES))
        for pair in range(16):
            pairs[k, pair] = tile[2 * pair : 2 * pair + 2]
    fan_in(early_in, gw_recv.at[0])
    early = jnp.sum(early_in[...], axis=0)
    at = flat // 32 * 4 + lax.rem(flat, 4)
    fan_in(late_in, gw_recv.at[1])
    late = jnp.sum(late_in[...], axis=0)
    gathered[flat, 0:2] = pairs[0, at] * (
        late[0:2] - pairs[1, at] * early[2:3] - pairs[2, at] * early[0:2]
    )
    gathered[flat, 2:4] = late[2:4] * whole
    mine = gathered.at[flat]
    fan_out(lambda to: mine, mine, gw_send.at[2], gw_recv.at[2])

    def emit(at_x, at_y, tile, carry):
        stage[at_x, at_y] = tile
        return carry

    convolve(taps_d1, 0, 3, emit, 0)
    for at_x in range(SPAN_X):
        dx_out[:, at_x] = jnp.swapaxes(stage[at_x], 0, 1).astype(BF16)

    for k, total in enumerate((sum_x1, sum_d1, sum_x2, sum_d2)):
        norm_out[k : k + 1] = whole * jnp.sum(
            jnp.where(small_lane == small_row, total, 0.0), axis=0, keepdims=True
        )
    fan_in(gathered, gw_recv.at[2])
    for member, out in ((0, gw_first), (1, gw_second)):
        for k in range(7):
            tile = jnp.concatenate(
                [
                    gathered[(pair // 4 * 8 + k) * 4 + pair % 4, 2 * member : 2 * member + 2]
                    for pair in range(16)
                ],
                axis=0,
            )
            for tap in range(4 * k, min(4 * k + 4, 27)):
                out[tap] = tile[:, C * (tap % 4) : C * (tap % 4) + C]

    for halo in halos:
        halo.drain()
    for total in totals:
        total.drain()
    for k, chunks in enumerate((early_out, late_out, gathered)):
        fan_in(chunks, gw_send.at[k])


def write_out(*refs):
    sources, targets, semaphores = refs[:5], refs[5:10], refs[10]
    copies = [
        pltpu.make_async_copy(source, target, semaphores.at[index])
        for index, (source, target) in enumerate(zip(sources, targets))
    ]
    for copy in copies:
        copy.start()
    for copy in copies:
        copy.wait()


def body(voxels, x_a, x_b, w_first, w_second, gain_first, bias_first, gain_second, bias_second,
         grad_out):
    def sized(*shape, kind=BF16):
        return pltpu.VMEM(shape, kind)

    volumes = (3, 2, 1, 1)
    devices = math.prod(lax.axis_size(axis) for axis in AXES)
    block = (C, SPAN_X, SPAN_Y, LANES)
    scratch = [sized(*block)] * 3 + [sized(27, C, C)] * 2 + [sized(1, C, kind=F32)] * 4
    scratch += [
        sized(4, SPAN_X * C, DEPTH), sized(SPAN_X, SPAN_Y, C, LANES, kind=F32)
    ]
    scratch += [sized(count, PAD_X, PAD_Y, TAPS, LANES) for count in (2, 2, 1, 1)]
    scratch += [sized(count, PAD_X, PAD_Y, C, LANES) for count in volumes]
    scratch += [sized(2, 3, 3, C, LANES) for count in volumes]
    scratch += [sized(2, C, LANES) for count in volumes]
    scratch += [sized(count, 2, C, LANES) for count in volumes] + [sized(2, 2, C, LANES)]
    scratch += [
        sized(2, SPAN_X, SPAN_Y, C, LANES, kind=F32),
        sized(2, SPAN_X, SPAN_Y, C, LANES, kind=F32),
        sized(SPAN_X, SPAN_Y, C, LANES, kind=F32),
        sized(4, devices, 1, LANES, kind=F32),
        sized(SPAN_X, SPAN_Y, C, LANES),
        sized(SPAN_X, SPAN_Y, C, LANES),
        sized(devices, 4, LANES, kind=F32),
        sized(devices, 4, LANES, kind=F32),
        sized(devices, 4, LANES, kind=F32),
        sized(devices, 4, LANES, kind=F32),
        sized(devices, 4, LANES, kind=F32),
        sized(3, 16, 2, LANES, kind=F32),
        pltpu.SemaphoreType.DMA((4, 32)),
        pltpu.SemaphoreType.DMA((4, 32)),
        pltpu.SemaphoreType.DMA((4,)),
        pltpu.SemaphoreType.DMA((4,)),
        pltpu.SemaphoreType.DMA((3,)),
        pltpu.SemaphoreType.DMA((3,)),
        pltpu.SemaphoreType.DMA((9,)),
    ]
    in_vmem = pl.BlockSpec(memory_space=pltpu.VMEM)
    in_hbm = pl.BlockSpec(memory_space=pltpu.HBM)
    taps = jax.ShapeDtypeStruct((27, C, C), F32)
    out_shape = (
        jax.ShapeDtypeStruct(block, BF16),
        jax.ShapeDtypeStruct(block, BF16),
        taps,
        taps,
        jax.ShapeDtypeStruct((4, C), F32),
    )
    results = pl.pallas_call(
        functools.partial(kernel, voxels),
        out_shape=out_shape,
        in_specs=[in_hbm] * 9,
        out_specs=(in_vmem,) * 5,
        scratch_shapes=scratch,
        compiler_params=pltpu.CompilerParams(
            collective_id=0, has_side_effects=True, vmem_limit_bytes=28 * 1024 * 1024
        ),
    )(
        *(pltpu.with_memory_space_constraint(value, pltpu.HBM) for value in (
            x_a, x_b, grad_out, w_first.reshape(27, C, C), w_second.reshape(27, C, C),
            *(row.reshape(1, C) for row in (gain_first, bias_first, gain_second, bias_second)),
        )),
    )
    y_a, dx_b, grad_first, grad_second, norms = pl.pallas_call(
        write_out,
        out_shape=out_shape,
        in_specs=[in_vmem] * 5,
        out_specs=(in_hbm,) * 5,
        scratch_shapes=[pltpu.SemaphoreType.DMA((5,))],
        compiler_params=pltpu.CompilerParams(vmem_limit_bytes=8 * 1024 * 1024),
    )(*results)
    return (
        y_a, dx_b, grad_first.reshape(3, 3, 3, C, C), grad_second.reshape(3, 3, 3, C, C), norms
    )


def solution(mesh):
    split = P(None, "gx", "gy", "gz")
    voxels = float(SPAN_X * SPAN_Y * LANES * mesh.size)
    return jax.shard_map(
        functools.partial(body, voxels),
        mesh=mesh,
        in_specs=(split, split, P(), P(), P(), P(), P(), P(), split),
        out_specs=(split, split, P(), P(), P()),
        check_vma=False,
    )
```

```python
import functools
import math

import jax
import jax.numpy as jnp
from jax import lax
from jax.experimental import pallas as pl
from jax.experimental.pallas import tpu as pltpu
from jax.sharding import PartitionSpec as P

F32 = jnp.float32
BF16 = jnp.bfloat16
EPSILON = 1e-05
C = 32
LANES = 128
SPAN_X, SPAN_Y = 2, 16
PAD_X, PAD_Y = SPAN_X + 2, SPAN_Y + 2
TAPS = 3 * C
DEPTH = PAD_X * 3 * TAPS
FLAT = 9 * TAPS
GROUP = 4
INNER = 16
OUTER = 18
AXES = ("gx", "gy", "gz")
MESH = pl.DeviceIdType.MESH


def sigmoid(value):
    return 0.5 + 0.5 * jnp.tanh(0.5 * value)


def unrolled(first, last, step, carry):
    for index in range(first, last):
        carry = step(index, carry)
    return carry


def rolled(tile, shift):
    shift = shift % LANES
    return pltpu.roll(tile, shift, 1) if shift else tile


class Halo:
    def __init__(self, rows, cols, edge, side, send, recv, place, volumes):
        self.rows, self.cols, self.edge, self.side = rows, cols, edge, side
        self.send, self.recv, self.place, self.volumes = send, recv, place, volumes
        self.count = 0
        self.sent = []

    def has(self, steps):
        present = None
        for axis, step in zip(AXES, steps):
            if step:
                me, size = self.place[axis]
                inside = me > 0 if step < 0 else me < size - 1
                present = inside if present is None else jnp.logical_and(present, inside)
        return present

    def push(self, source, target, *steps):
        index = self.count
        self.count += 1
        to = {}
        for axis, step in zip(AXES, steps):
            if step:
                me, size = self.place[axis]
                to[axis] = lax.rem(me + step + size, size)
        copy = pltpu.make_async_remote_copy(
            src_ref=source,
            dst_ref=target,
            send_sem=self.send.at[index],
            recv_sem=self.recv.at[index],
            device_id=to,
            device_id_type=MESH,
        )
        present = self.has(steps)

        @pl.when(present)
        def _():
            copy.start()

        self.sent.append((copy, present))
        return copy, self.has([-step for step in steps])

    def faces_x(self, volume):
        rows, inner = self.rows, pl.ds(1, SPAN_Y)
        return [
            self.push(
                rows.at[volume, 1 if step < 0 else SPAN_X, inner],
                rows.at[volume, PAD_X - 1 if step < 0 else 0, inner],
                step, 0, 0,
            )
            for step in (-1, 1)
        ]

    def columns(self, step_x, step_y):
        return [
            self.push(
                self.edge.at[0 if step < 0 else 1],
                self.cols.at[1 if step < 0 else 0, 1 - step_x, 1 - step_y],
                step_x, step_y, step,
            )
            for step in (-1, 1)
        ]

    def small(self):
        rows, every = self.rows, pl.ds(0, self.volumes)
        near = self.columns(0, 0)
        rest = []
        for step_x in (-1, 0, 1):
            at_x = (1 if step_x < 0 else SPAN_X) if step_x else pl.ds(1, SPAN_X)
            to_x = (PAD_X - 1 if step_x < 0 else 0) if step_x else pl.ds(1, SPAN_X)
            for step_y in (-1, 1):
                rest.append(
                    self.push(
                        rows.at[every, at_x, 1 if step_y < 0 else SPAN_Y],
                        rows.at[every, to_x, PAD_Y - 1 if step_y < 0 else 0],
                        step_x, step_y, 0,
                    )
                )
        for step_x, step_y in (
            (-1, -1), (-1, 1), (1, -1), (1, 1), (-1, 0), (1, 0), (0, -1), (0, 1)
        ):
            rest += self.columns(step_x, step_y)
        return near, rest

    def own(self, side, volume, lane):
        tile = self.cols[side, 1, 1]
        at = 32 * volume
        return jnp.where(lane < 64, rolled(tile, 33 - at), rolled(tile, 49 - at))

    def merged(self, side, volume, lane):
        at = 32 * volume
        inside = lax.rem(lane, 32)

        def strip(index, low, middle, high):
            low, middle, high = (
                rolled(self.cols[side, index, k], shift - at)
                for k, shift in enumerate((low, middle, high))
            )
            return jnp.where(inside == 0, low, jnp.where(inside == PAD_Y - 1, high, middle))

        return jnp.where(
            lane < 64,
            jnp.where(lane < 32, strip(0, -31, -15, 1), strip(1, 17, 33, 49)),
            jnp.where(lane < 96, strip(1, 33, 49, 65), strip(2, 81, 97, 113)),
        )

    @staticmethod
    def arrive(pushes):
        for copy, present in pushes:

            @pl.when(present)
            def _(copy=copy):
                copy.wait_recv()

    def drain(self):
        for copy, present in self.sent:

            @pl.when(present)
            def _(copy=copy):
                copy.wait_send()


def kernel(
    voxels,
    x_a, x_b, grad, w_first, w_second, gain_first, bias_first, gain_second, bias_second,
    y_out, dx_out, gw_first, gw_second, norm_out,
    block_a, block_b, block_g, kernel_1, kernel_2, row_1, row_2, row_3, row_4, weights, stage,
    taps_x, taps_h, taps_d2, taps_d1,
    rows_x, rows_1, rows_2, rows_e,
    cols_x, cols_1, cols_2, cols_e,
    edge_x, edge_1, edge_2, edge_e,
    side_x, side_1, side_2, side_e,
    side_h,
    conv_1, conv_2, back_1,
    sums,
    norms, slopes, norms_2, slopes_2,
    early_out, early_in, mid_out, mid_in, late_out, late_in, gathered, pairs,
    halo_send, halo_recv, sums_send, sums_recv, gw_send, gw_recv, local,
):
    loads = [
        pltpu.make_async_copy(source, target, local.at[index])
        for index, (source, target) in enumerate((
            (x_a, block_a), (x_b, block_b), (grad, block_g), (w_first, kernel_1),
            (w_second, kernel_2), (gain_first, row_1), (bias_first, row_2), (gain_second, row_3),
            (bias_second, row_4),
        ))
    ]
    for load in loads:
        load.start()
    place = {axis: (lax.axis_index(axis), lax.axis_size(axis)) for axis in AXES}
    for chunks in (early_out, mid_out, late_out):
        for j in range(4):
            at = slice(32 * j + 28, 32 * j + 32)
            chunks[at] = jnp.zeros((4, chunks.shape[1], LANES), F32)
    for rows in (norms, slopes, norms_2, slopes_2):
        for at in (0, SPAN_Y + 2):
            rows[:, at : at + 2] = jnp.zeros((SPAN_X, 2, C, LANES), BF16)
    barrier = pltpu.get_barrier_semaphore()
    count = place["gx"][1] * place["gy"][1] * place["gz"][1]
    flat = (place["gx"][0] * place["gy"][1] + place["gy"][0]) * place["gz"][1] + place["gz"][0]

    chip_x, chip_y = place["gy"][0], place["gz"][0] // 2
    chip_z = place["gx"][0] // 2 * 2 + lax.rem(place["gz"][0], 2)
    core = lax.rem(place["gx"][0], 2)

    def other(step):
        return lax.rem(flat + step, count)

    def fan_out(source_of, target, send, recv):
        spots = []
        for step_z, step_core in ((2, 1), (2, 0), (1, 1), (3, 1), (1, 0), (3, 0), (0, 1), (0, 0)):
            to_z, to_core = lax.rem(chip_z + step_z, 4), lax.rem(core + step_core, 2)
            spots.append(to_z // 2 * 64 + to_core * 32 + lax.rem(to_z, 2))

        def copies(plane, chosen):
            to_x = lax.rem(chip_x + plane // 4 + 1, 4)
            to_y = lax.rem(chip_y + lax.rem(plane, 4) + 1, 4)
            for spot in chosen:
                to = spot + to_x * 8 + to_y * 2
                pltpu.make_async_remote_copy(
                    src_ref=source_of(to), dst_ref=target, send_sem=send, recv_sem=recv,
                    device_id=to, device_id_type=pl.DeviceIdType.LOGICAL,
                ).start()

        def most(block, carry):
            for k in range(4):
                copies(block * 4 + k, spots[:-1])
            return carry

        def rest(block, carry):
            for k in range(5):
                copies(block * 5 + k, spots[-1:])
            return carry

        lax.fori_loop(0, 4, most, 0)
        lax.fori_loop(0, 3, rest, 0)

    def fan_in(slots, semaphore):
        part = slots.at[pl.ds(0, count - 1)]
        pltpu.make_async_copy(part, part, semaphore).wait()

    def greet(step, carry):
        pl.semaphore_signal(
            barrier, inc=1, device_id=other(step), device_id_type=pl.DeviceIdType.LOGICAL
        )
        return carry

    lax.fori_loop(1, count, greet, 0)

    lane = lax.broadcasted_iota(jnp.int32, (C, LANES), 1)
    halos = []
    for index, (rows, cols, edge, side, volumes) in enumerate((
        (rows_x, cols_x, edge_x, side_x, 3),
        (rows_1, cols_1, edge_1, side_1, 2),
        (rows_2, cols_2, edge_2, side_2, 1),
        (rows_e, cols_e, edge_e, side_e, 1),
    )):
        halos.append(
            Halo(rows, cols, edge, side, halo_send.at[index], halo_recv.at[index], place, volumes)
        )
    halo_x, halo_1, halo_2, halo_e = halos

    low_x, high_x = place["gx"][0] > 0, place["gx"][0] < place["gx"][1] - 1
    low_y, high_y = place["gy"][0] > 0, place["gy"][0] < place["gy"][1] - 1
    low_z, high_z = place["gz"][0] > 0, place["gz"][0] < place["gz"][1] - 1

    def keep(at_x, at_y):
        held_x = low_x if at_x == 0 else high_x if at_x == PAD_X - 1 else None
        if isinstance(at_y, int):
            held_y = low_y if at_y == 0 else high_y if at_y == PAD_Y - 1 else None
        else:
            held_y = jnp.logical_and(
                jnp.logical_or(at_y > 0, low_y), jnp.logical_or(at_y < PAD_Y - 1, high_y)
            )
        if held_x is None:
            return held_y
        return held_x if held_y is None else jnp.logical_and(held_x, held_y)

    def lane_keep(side):
        spot_x, spot_y = lane // 32, lax.rem(lane, 32)
        bad = jnp.zeros((C, LANES), jnp.int32)
        for hit, present in (
            (spot_x == 0, low_x), (spot_x == PAD_X - 1, high_x),
            (spot_y == 0, low_y), (spot_y == PAD_Y - 1, high_y),
        ):
            missing = jnp.where(present, 0, 1)
            bad = bad + jnp.where(hit, missing, 0)
        bad = bad + jnp.where(low_z if side == 0 else high_z, 0, 1)
        return bad == 0

    def extract(tile, spot, carry):
        first, last = carry
        tile = tile.astype(BF16)
        first = jnp.where(lane == spot, pltpu.roll(tile, spot, 1), first)
        last = jnp.where(lane == spot, pltpu.roll(tile, lax.rem(spot + 1, LANES), 1), last)
        return first, last

    def put_taps(taps, volume, spots, tiles, sides):
        low, high = sides[0][...], sides[1][...]
        shifted = []
        for (at_x, at_y), tile in zip(spots, tiles):
            spot = at_x * 32 + at_y
            left = jnp.where(
                lane == 0,
                pltpu.roll(low, lax.rem(LANES - spot, LANES), 1),
                pltpu.roll(tile, 1, 1),
            )
            right = jnp.where(
                lane == LANES - 1,
                pltpu.roll(high, LANES - 1 - spot, 1),
                pltpu.roll(tile, LANES - 1, 1),
            )
            shifted.append((left, tile, right))
        for (at_x, at_y), rows in zip(spots, shifted):
            for k, row in enumerate(rows):
                taps[volume, at_x, at_y, k * C : (k + 1) * C] = row

    def build_inner(taps, volume, inner, sides):
        for at_x in range(SPAN_X):

            def step(block, carry, at_x=at_x):
                rows = [block * INNER + k for k in range(INNER)]
                tiles = [inner(at_x, at_y).astype(BF16) for at_y in rows]
                put_taps(taps, volume, [(at_x + 1, at_y + 1) for at_y in rows], tiles, sides)
                return carry

            unrolled(0, SPAN_Y // INNER, step, 0)

    def build_outer(taps, volume, outer, sides):
        def put(spots):
            tiles = [
                jnp.where(keep(at_x, at_y), outer(at_x, at_y).astype(BF16), none)
                for at_x, at_y in spots
            ]
            put_taps(taps, volume, spots, tiles, sides)

        put([(at_x, at_y) for at_x in (1, 2) for at_y in (0, PAD_Y - 1)])
        for at_x in (0, PAD_X - 1):

            def step(block, carry, at_x=at_x):
                put([(at_x, block * OUTER + k) for k in range(OUTER)])
                return carry

            unrolled(0, PAD_Y // OUTER, step, 0)

    def build(taps, volume, outer, inner, sides):
        build_inner(taps, volume, inner, sides)
        build_outer(taps, volume, outer, sides)

    def convolve(taps, volume, weight, emit, carry):
        def step(block, carry):
            first = block * GROUP
            columns = [
                taps[volume, :, pl.ds(first + k, 3)].reshape(DEPTH, LANES) for k in range(GROUP)
            ]
            total = jnp.dot(
                weights[weight],
                jnp.concatenate(columns, axis=1),
                preferred_element_type=F32,
            )
            for k in range(GROUP):
                for at_x in range(SPAN_X):
                    tile = total[at_x * C : (at_x + 1) * C, k * LANES : (k + 1) * LANES]
                    carry = emit(at_x, first + k, tile, carry)
            return carry

        return unrolled(0, SPAN_Y // GROUP, step, carry)

    def kernel_grad(taps, volume, buffers, out, plain):
        tap_row = lax.broadcasted_iota(jnp.int32, (16, LANES), 0)
        left, right = [], []
        for at_y in range(PAD_Y):
            parts = [
                rows[at_x, at_y - tap + 2]
                for rows in buffers for tap in range(3) for at_x in range(SPAN_X)
            ]
            if plain:
                inside = [0 <= at_y - tap < SPAN_Y for tap in range(3)]
                first = inside.index(True)
                mine = jnp.logical_and(tap_row >= first, tap_row < first + sum(inside))
                parts.append(jnp.where(mine, 1.0, 0.0).astype(BF16))
            left.append(jnp.concatenate(parts, axis=0))
            right.append(taps[volume, :, at_y].reshape(PAD_X * TAPS, LANES))
        total = lax.dot_general(
            jnp.concatenate(left, axis=1),
            jnp.concatenate(right, axis=1),
            (((1,), (1,)), ((), ())),
            preferred_element_type=F32,
        )

        def wide(pieces):
            height = pieces[0].shape[0]
            return jnp.concatenate(
                pieces + [jnp.zeros((height, 7 * LANES - FLAT), F32)], axis=1
            )

        def slab(row, height, at_x):
            return total[row : row + height, TAPS * at_x : TAPS * (at_x + 1)]

        blocks = []
        for index in range(len(buffers)):
            first = 6 * C * index
            pieces = []
            for tap_x in range(3):
                for tap_y in range(3):
                    row = first + 2 * C * tap_y
                    pieces.append(slab(row, C, tap_x) + slab(row + C, C, tap_x + 1))
            blocks.append(wide(pieces))
        if plain:
            first = 6 * C * len(buffers)
            alone = wide([
                slab(first + tap_y, 1, tap_x) + slab(first + tap_y, 1, tap_x + 1)
                for tap_x in range(3) for tap_y in range(3)
            ])
        for k in range(7):
            lanes = slice(LANES * k, LANES * (k + 1))
            for pair in range(16):
                spot = (pair // 4 * 8 + k) * 4 + pair % 4
                for index, block in enumerate(blocks):
                    out[spot, 2 * index : 2 * index + 2] = block[2 * pair : 2 * pair + 2, lanes]
                if plain:
                    last = 2 * len(blocks)
                    out[spot, last : last + 1] = alone[:, lanes]

    channel = lax.broadcasted_iota(jnp.int32, (C, LANES), 0)

    def pack(columns):
        whole = jnp.zeros((C, LANES), F32)
        for k, column in enumerate(columns):
            whole = whole + jnp.where(lane == channel + 32 * k, column, 0.0)
        return jnp.sum(whole, axis=0, keepdims=True)

    def unpack(row, number):
        return [
            jnp.sum(jnp.where(lane == channel + 32 * k, row, 0.0), axis=1, keepdims=True)
            for k in range(number)
        ]

    class Total:
        def __init__(self, index):
            self.slots, self.index = sums.at[index], index

        def start(self, row):
            mine = self.slots.at[flat]
            mine[...] = row

            fan_out(
                lambda to: mine, mine, sums_send.at[self.index], sums_recv.at[self.index]
            )

        def finish(self):
            fan_in(self.slots, sums_recv.at[self.index])
            return jnp.sum(self.slots[...], axis=0)

        def drain(self):
            fan_in(self.slots, sums_send.at[self.index])

    totals = [Total(index) for index in range(4)]

    small_lane = lax.broadcasted_iota(jnp.int32, (C, C), 1)
    small_row = lax.broadcasted_iota(jnp.int32, (C, C), 0)

    def column(row):
        return jnp.sum(jnp.where(small_lane == small_row, row[...], 0.0), axis=1, keepdims=True)

    for load in loads[5:]:
        load.wait()
    gain_1, bias_1, gain_2, bias_2 = (column(row) for row in (row_1, row_2, row_3, row_4))

    def stack_weights(source, forward, backward):
        tiles = [
            jnp.concatenate(
                [source[tap].astype(F32) for tap in range(4 * k, min(4 * k + 4, 27))]
                + ([jnp.zeros((C, C), F32)] if k == 6 else []),
                axis=1,
            )
            for k in range(7)
        ]
        turned = [tile.T for tile in tiles]
        pieces = [turned[tap // 4][C * (tap % 4) : C * (tap % 4) + C] for tap in range(26, -1, -1)]
        back = [jnp.concatenate((pieces + pieces[:1])[4 * k : 4 * k + 4], axis=1) for k in range(7)]
        for index, parts in ((forward, tiles), (backward, back)):
            last = jnp.where(lane < 96, parts[6], 0.0)
            empty = jnp.zeros((C, LANES), F32)
            top = parts[:6] + [last, empty, empty]
            moved = [pltpu.roll(part, 32, 1) for part in parts[:6] + [last]]
            low = [empty, empty]
            for k in range(7):
                low.append(jnp.where(lane < 32, moved[k - 1] if k else empty, moved[k]))
            for k in range(9):
                weights[index, 0:C, LANES * k : LANES * (k + 1)] = top[k].astype(BF16)
                weights[index, C : 2 * C, LANES * k : LANES * (k + 1)] = low[k].astype(BF16)

    zero = jnp.zeros((C, LANES), F32)
    none = jnp.zeros((C, LANES), BF16)

    def take(load, source, at, carry):
        load.wait()
        for at_x in range(SPAN_X):
            rows_x[at, at_x + 1, 1 : SPAN_Y + 1] = jnp.swapaxes(
                source[:, at_x].astype(F32), 0, 1
            ).astype(BF16)
        for at_x in range(SPAN_X):

            def step(block, carry, at_x=at_x):
                for k in range(8):
                    at_y = block * 8 + k
                    carry = extract(
                        rows_x[at, at_x + 1, at_y + 1],
                        32 * at + 16 * at_x + at_y,
                        carry,
                    )
                return carry

            carry = unrolled(0, 2, step, carry)
        return carry

    carry = (none, none)
    for at, source in enumerate((block_a, block_b, block_g)):
        carry = take(loads[at], source, at, carry)
    edge_x[0] = carry[0]
    edge_x[1] = carry[1]

    pl.semaphore_wait(barrier, count - 1)

    near, rest = halo_x.small()
    waits_x = [halo_x.faces_x(0), halo_x.faces_x(1)]
    loads[3].wait()
    loads[4].wait()
    stack_weights(kernel_1, 0, 3)
    stack_weights(kernel_2, 1, 2)
    ok = [lane_keep(side) for side in range(2)]
    halo_x.arrive(near)
    for volume in range(2):
        for side in range(2):
            side_x[volume, side] = jnp.where(ok[side], halo_x.own(side, volume, lane), none)
        build_inner(
            taps_x, volume,
            lambda at_x, at_y, volume=volume: rows_x[volume, at_x + 1, at_y + 1],
            (side_x.at[volume, 0], side_x.at[volume, 1]),
        )
    halo_x.arrive(rest)
    for side in range(2):
        for volume in range(3):
            tile = halo_x.merged(side, volume, lane)
            side_x[volume, side] = jnp.where(ok[side], tile, none)

    columns = []
    waits_1 = []
    carry = (none,) * 2
    for volume in range(2):
        halo_x.arrive(waits_x[volume])
        build_outer(
            taps_x, volume,
            lambda at_x, at_y, volume=volume: rows_x[volume, at_x, at_y],
            (side_x.at[volume, 0], side_x.at[volume, 1]),
        )

        def emit(at_x, at_y, tile, carry, volume=volume):
            total, squares, first, last = carry
            conv_1[volume, at_x, at_y] = tile
            rows_1[volume, at_x + 1, at_y + 1] = tile.astype(BF16)
            first, last = extract(tile, 32 * volume + 16 * at_x + at_y, (first, last))
            return total + tile, squares + tile * tile, first, last

        total, squares, *carry = convolve(taps_x, volume, 0, emit, (zero, zero, *carry))
        if volume == 0:
            waits_1.append(halo_1.faces_x(0))
        columns += [
            jnp.sum(total, axis=1, keepdims=True), jnp.sum(squares, axis=1, keepdims=True)
        ]
    edge_1[0] = carry[0]
    edge_1[1] = carry[1]
    totals[0].start(pack(columns))
    near, rest = halo_1.small()
    waits_1.append(halo_1.faces_x(1))
    row = totals[0].finish()
    halo_1.arrive(near + rest)
    waits_g = halo_x.faces_x(2)
    stats = unpack(row, 4)

    def moments(total, squares):
        mean = total / voxels
        scale = lax.rsqrt(squares / voxels - mean * mean + EPSILON)
        return mean, scale

    columns = []
    for volume in range(2):
        mean, scale = moments(stats[2 * volume], stats[2 * volume + 1])
        slope = jnp.broadcast_to(gain_1 * scale, (C, LANES))
        shift = jnp.broadcast_to(bias_1 - mean * gain_1 * scale, (C, LANES))

        def active(value, slope=slope, shift=shift):
            pre = value * slope + shift
            return pre * sigmoid(pre)

        norm_slope = jnp.broadcast_to(scale, (C, LANES))
        norm_shift = jnp.broadcast_to(-mean * scale, (C, LANES))

        def own_row(at_x, at_y, volume, active, norm_slope=norm_slope, norm_shift=norm_shift):
            value = conv_1[volume, at_x, at_y]
            if volume == 1:
                norms[at_x, at_y + 2] = (value * norm_slope + norm_shift).astype(BF16)
            return active(value)

        for side in range(2):
            tile = halo_1.merged(side, volume, lane)
            side_1[volume, side] = tile
            side_h[volume, side] = jnp.where(
                ok[side], active(tile.astype(F32)), 0.0
            ).astype(BF16)
        sides = (side_h.at[volume, 0], side_h.at[volume, 1])
        build_inner(
            taps_h, volume, functools.partial(own_row, volume=volume, active=active), sides
        )
        halo_1.arrive(waits_1[volume])
        build_outer(
            taps_h, volume,
            lambda at_x, at_y, volume=volume: active(rows_1[volume, at_x, at_y].astype(F32)),
            sides,
        )
        if volume == 0:

            def emit(at_x, at_y, tile, carry):
                total, squares = carry
                conv_2[0, at_x, at_y] = tile
                return total + tile, squares + tile * tile

            total, squares = convolve(taps_h, 0, 1, emit, (zero,) * 2)
        else:

            def emit(at_x, at_y, tile, carry):
                total, squares, first, last = carry
                conv_2[1, at_x, at_y] = tile
                rows_2[0, at_x + 1, at_y + 1] = tile.astype(BF16)
                first, last = extract(tile, 16 * at_x + at_y, (first, last))
                return total + tile, squares + tile * tile, first, last

            total, squares, first, last = convolve(taps_h, 1, 1, emit, (zero, zero, none, none))
            edge_2[0] = first
            edge_2[1] = last
        columns += [
            jnp.sum(total, axis=1, keepdims=True), jnp.sum(squares, axis=1, keepdims=True)
        ]
    mean_1, scale_1 = mean, scale
    totals[1].start(pack(columns))
    near, rest = halo_2.small()
    waits = near + rest + halo_2.faces_x(0)
    kernel_grad(taps_x, 1, [norms], early_out, True)
    fan_out(
        lambda to: early_out.at[to], early_in.at[flat], gw_send.at[0], gw_recv.at[0]
    )
    early_in[flat] = early_out[flat]
    stats = unpack(totals[1].finish(), 4)

    mean_2, scale_2 = moments(stats[2], stats[3])

    def layer_of(mean, scale, gain, bias):
        norm_slope = jnp.broadcast_to(scale, (C, LANES))
        norm_shift = jnp.broadcast_to(-mean * scale, (C, LANES))
        wide_gain = jnp.broadcast_to(gain, (C, LANES))
        wide_bias = jnp.broadcast_to(bias, (C, LANES))

        def slope_of(value, upstream):
            normed = value * norm_slope + norm_shift
            pre = wide_gain * normed + wide_bias
            sigma = sigmoid(pre)
            return upstream * (sigma * (1.0 + pre * (1.0 - sigma))), normed

        return slope_of

    def delta_of(slope_of, sum_d, sum_x, gain, scale):
        wide_d = jnp.broadcast_to(sum_d / voxels, (C, LANES))
        wide_x = jnp.broadcast_to(sum_x / voxels, (C, LANES))
        factor = jnp.broadcast_to(gain * scale, (C, LANES))

        def delta(value, upstream):
            slope, normed = slope_of(value, upstream)
            return factor * (slope - wide_d - normed * wide_x)

        return delta

    slope_2 = layer_of(mean_2, scale_2, gain_2, bias_2)

    def sum_rows(slope_of, value_of, upstream_of):
        carry = (zero, zero)
        for at_x in range(SPAN_X):

            def step(block, carry, at_x=at_x):
                total, weighted = carry
                for k in range(8):
                    at_y = block * 8 + k
                    slope, normed = slope_of(value_of(at_x, at_y), upstream_of(at_x, at_y))
                    slopes_2[at_x, at_y + 2] = slope.astype(BF16)
                    norms_2[at_x, at_y + 2] = normed.astype(BF16)
                    total, weighted = total + slope, weighted + slope * normed
                return total, weighted

            carry = unrolled(0, 2, step, carry)
        return [jnp.sum(part, axis=1, keepdims=True) for part in carry]

    columns = sum_rows(
        slope_2,
        lambda at_x, at_y: conv_2[1, at_x, at_y],
        lambda at_x, at_y: rows_x[2, at_x + 1, at_y + 1].astype(F32),
    )
    totals[2].start(pack(columns))

    mean_a, scale_a = moments(stats[0], stats[1])
    slope_a = jnp.broadcast_to(gain_2 * scale_a, (C, LANES))
    shift_a = jnp.broadcast_to(bias_2 - mean_a * gain_2 * scale_a, (C, LANES))
    for at_x in range(SPAN_X):

        def step(block, carry, at_x=at_x):
            for k in range(8):
                at_y = block * 8 + k
                pre = conv_2[0, at_x, at_y] * slope_a + shift_a
                stage[at_x, at_y] = pre * sigmoid(pre)
            return carry

        unrolled(0, 2, step, 0)
        y_out[:, at_x] = jnp.swapaxes(stage[at_x], 0, 1).astype(BF16)

    kernel_grad(taps_h, 1, [slopes_2, norms_2], mid_out, True)
    fan_out(lambda to: mid_out.at[to], mid_in.at[flat], gw_send.at[1], gw_recv.at[1])
    mid_in[flat] = mid_out[flat]
    halo_x.arrive(waits_g)
    halo_2.arrive(waits)
    sum_d2, sum_x2 = unpack(totals[2].finish(), 2)

    delta_2 = delta_of(slope_2, sum_d2, sum_x2, gain_2, scale_2)
    for side in range(2):
        tile = delta_2(
            halo_2.merged(side, 0, lane).astype(F32), side_x[2, side].astype(F32)
        )
        side_2[0, side] = jnp.where(ok[side], tile, 0.0).astype(BF16)
    build(
        taps_d2, 0,
        lambda at_x, at_y: delta_2(
            rows_2[0, at_x, at_y].astype(F32), rows_x[2, at_x, at_y].astype(F32)
        ),
        lambda at_x, at_y: delta_2(
            conv_2[1, at_x, at_y], rows_x[2, at_x + 1, at_y + 1].astype(F32)
        ),
        (side_2.at[0, 0], side_2.at[0, 1]),
    )
    slope_1 = layer_of(mean_1, scale_1, gain_1, bias_1)

    def emit(at_x, at_y, tile, carry):
        total, weighted, first, last = carry
        back_1[at_x, at_y] = tile
        rows_e[0, at_x + 1, at_y + 1] = tile.astype(BF16)
        first, last = extract(tile, 16 * at_x + at_y, (first, last))
        slope, normed = slope_1(conv_1[1, at_x, at_y], tile)
        slopes[at_x, at_y + 2] = slope.astype(BF16)
        return total + slope, weighted + slope * normed, first, last

    total, weighted, first, last = convolve(taps_d2, 0, 2, emit, (zero, zero, none, none))
    edge_e[0] = first
    edge_e[1] = last
    columns = [
        jnp.sum(total, axis=1, keepdims=True), jnp.sum(weighted, axis=1, keepdims=True)
    ]
    totals[3].start(pack(columns))
    near, rest = halo_e.small()
    waits = near + rest + halo_e.faces_x(0)
    kernel_grad(taps_x, 1, [slopes], late_out, False)
    fan_out(lambda to: late_out.at[to], late_in.at[flat], gw_send.at[2], gw_recv.at[2])
    late_in[flat] = late_out[flat]
    sum_d1, sum_x1 = unpack(totals[3].finish(), 2)

    whole = 1.0 / math.sqrt(voxels)
    for k, factor in enumerate(
        (
            gain_1 * scale_1 * whole, sum_d1 / voxels, sum_x1 / voxels,
            gain_2 * scale_2 * whole, sum_d2 / voxels, sum_x2 / voxels,
        )
    ):
        tile = jnp.broadcast_to(factor, (C, LANES))
        for pair in range(16):
            pairs[k, pair] = tile[2 * pair : 2 * pair + 2]
    fan_in(early_in, gw_recv.at[0])
    early = jnp.sum(early_in[...], axis=0)
    fan_in(mid_in, gw_recv.at[1])
    mid = jnp.sum(mid_in[...], axis=0)
    at = flat // 32 * 4 + lax.rem(flat, 4)
    fan_in(late_in, gw_recv.at[2])
    late = jnp.sum(late_in[...], axis=0)
    gathered[flat, 0:2] = pairs[0, at] * (
        late[0:2] - pairs[1, at] * early[2:3] - pairs[2, at] * early[0:2]
    )
    gathered[flat, 2:4] = pairs[3, at] * (
        mid[0:2] - pairs[4, at] * mid[4:5] - pairs[5, at] * mid[2:4]
    )
    mine = gathered.at[flat]
    fan_out(lambda to: mine, mine, gw_send.at[3], gw_recv.at[3])

    halo_e.arrive(waits)
    delta_1 = delta_of(slope_1, sum_d1, sum_x1, gain_1, scale_1)
    for side in range(2):
        tile = delta_1(
            side_1[1, side].astype(F32), halo_e.merged(side, 0, lane).astype(F32)
        )
        side_e[0, side] = jnp.where(ok[side], tile, 0.0).astype(BF16)
    build(
        taps_d1, 0,
        lambda at_x, at_y: delta_1(
            rows_1[1, at_x, at_y].astype(F32), rows_e[0, at_x, at_y].astype(F32)
        ),
        lambda at_x, at_y: delta_1(conv_1[1, at_x, at_y], back_1[at_x, at_y]),
        (side_e.at[0, 0], side_e.at[0, 1]),
    )
    def emit(at_x, at_y, tile, carry):
        stage[at_x, at_y] = tile
        return carry

    convolve(taps_d1, 0, 3, emit, 0)
    for at_x in range(SPAN_X):
        dx_out[:, at_x] = jnp.swapaxes(stage[at_x], 0, 1).astype(BF16)

    for k, total in enumerate((sum_x1, sum_d1, sum_x2, sum_d2)):
        norm_out[k : k + 1] = whole * jnp.sum(
            jnp.where(small_lane == small_row, total, 0.0), axis=0, keepdims=True
        )
    fan_in(gathered, gw_recv.at[3])
    for member, out in ((0, gw_first), (1, gw_second)):
        for k in range(7):
            tile = jnp.concatenate(
                [
                    gathered[(pair // 4 * 8 + k) * 4 + pair % 4, 2 * member : 2 * member + 2]
                    for pair in range(16)
                ],
                axis=0,
            )
            for tap in range(4 * k, min(4 * k + 4, 27)):
                out[tap] = tile[:, C * (tap % 4) : C * (tap % 4) + C]

    for halo in halos:
        halo.drain()
    for total in totals:
        total.drain()
    for k, chunks in enumerate((early_out, mid_out, late_out, gathered)):
        fan_in(chunks, gw_send.at[k])


def write_out(*refs):
    sources, targets, semaphores = refs[:5], refs[5:10], refs[10]
    copies = [
        pltpu.make_async_copy(source, target, semaphores.at[index])
        for index, (source, target) in enumerate(zip(sources, targets))
    ]
    for copy in copies:
        copy.start()
    for copy in copies:
        copy.wait()


def body(voxels, x_a, x_b, w_first, w_second, gain_first, bias_first, gain_second, bias_second,
         grad_out):
    def sized(*shape, kind=BF16):
        return pltpu.VMEM(shape, kind)

    volumes = (3, 2, 1, 1)
    devices = math.prod(lax.axis_size(axis) for axis in AXES)
    block = (C, SPAN_X, SPAN_Y, LANES)
    scratch = [sized(*block)] * 3 + [sized(27, C, C)] * 2 + [sized(1, C, kind=F32)] * 4
    scratch += [
        sized(4, SPAN_X * C, DEPTH), sized(SPAN_X, SPAN_Y, C, LANES, kind=F32)
    ]
    scratch += [sized(count, PAD_X, PAD_Y, TAPS, LANES) for count in (2, 2, 1, 1)]
    scratch += [sized(count, PAD_X, PAD_Y, C, LANES) for count in volumes]
    scratch += [sized(2, 3, 3, C, LANES) for count in volumes]
    scratch += [sized(2, C, LANES) for count in volumes]
    scratch += [sized(count, 2, C, LANES) for count in volumes] + [sized(2, 2, C, LANES)]
    scratch += [
        sized(2, SPAN_X, SPAN_Y, C, LANES, kind=F32),
        sized(2, SPAN_X, SPAN_Y, C, LANES, kind=F32),
        sized(SPAN_X, SPAN_Y, C, LANES, kind=F32),
        sized(4, devices, 1, LANES, kind=F32),
        *[sized(SPAN_X, SPAN_Y + 4, C, LANES)] * 4,
        *[sized(devices, 3, LANES, kind=F32)] * 2,
        *[sized(devices, 5, LANES, kind=F32)] * 2,
        *[sized(devices, 2, LANES, kind=F32)] * 2,
        sized(devices, 4, LANES, kind=F32),
        sized(6, 16, 2, LANES, kind=F32),
        pltpu.SemaphoreType.DMA((4, 32)),
        pltpu.SemaphoreType.DMA((4, 32)),
        pltpu.SemaphoreType.DMA((4,)),
        pltpu.SemaphoreType.DMA((4,)),
        pltpu.SemaphoreType.DMA((4,)),
        pltpu.SemaphoreType.DMA((4,)),
        pltpu.SemaphoreType.DMA((9,)),
    ]
    in_vmem = pl.BlockSpec(memory_space=pltpu.VMEM)
    in_hbm = pl.BlockSpec(memory_space=pltpu.HBM)
    taps = jax.ShapeDtypeStruct((27, C, C), F32)
    out_shape = (
        jax.ShapeDtypeStruct(block, BF16),
        jax.ShapeDtypeStruct(block, BF16),
        taps,
        taps,
        jax.ShapeDtypeStruct((4, C), F32),
    )
    results = pl.pallas_call(
        functools.partial(kernel, voxels),
        out_shape=out_shape,
        in_specs=[in_hbm] * 9,
        out_specs=(in_vmem,) * 5,
        scratch_shapes=scratch,
        compiler_params=pltpu.CompilerParams(
            collective_id=0, has_side_effects=True, vmem_limit_bytes=28 * 1024 * 1024
        ),
    )(
        *(pltpu.with_memory_space_constraint(value, pltpu.HBM) for value in (
            x_a, x_b, grad_out, w_first.reshape(27, C, C), w_second.reshape(27, C, C),
            *(row.reshape(1, C) for row in (gain_first, bias_first, gain_second, bias_second)),
        )),
    )
    y_a, dx_b, grad_first, grad_second, norms = pl.pallas_call(
        write_out,
        out_shape=out_shape,
        in_specs=[in_vmem] * 5,
        out_specs=(in_hbm,) * 5,
        scratch_shapes=[pltpu.SemaphoreType.DMA((5,))],
        compiler_params=pltpu.CompilerParams(vmem_limit_bytes=8 * 1024 * 1024),
    )(*results)
    return (
        y_a, dx_b, grad_first.reshape(3, 3, 3, C, C), grad_second.reshape(3, 3, 3, C, C), norms
    )


def solution(mesh):
    split = P(None, "gx", "gy", "gz")
    voxels = float(SPAN_X * SPAN_Y * LANES * mesh.size)
    return jax.shard_map(
        functools.partial(body, voxels),
        mesh=mesh,
        in_specs=(split, split, P(), P(), P(), P(), P(), P(), split),
        out_specs=(split, split, P(), P(), P()),
        check_vma=False,
    )
```

```python
import functools
import math

import jax
import jax.numpy as jnp
from jax import lax
from jax.experimental import pallas as pl
from jax.experimental.pallas import tpu as pltpu
from jax.sharding import PartitionSpec as P

F32 = jnp.float32
BF16 = jnp.bfloat16
EPSILON = 1e-05
C = 32
LANES = 128
SPAN_X, SPAN_Y = 2, 16
PAD_X, PAD_Y = SPAN_X + 2, SPAN_Y + 2
TAPS = 3 * C
DEPTH = PAD_X * TAPS
HEIGHT = 3 * SPAN_X * C
FLAT = 9 * TAPS
GROUP = 2
INNER = 16
OUTER = 18
AXES = ("gx", "gy", "gz")
MESH = pl.DeviceIdType.MESH


def sigmoid(value):
    return 0.5 + 0.5 * jnp.tanh(0.5 * value)


def unrolled(first, last, step, carry):
    for index in range(first, last):
        carry = step(index, carry)
    return carry


def rolled(tile, shift):
    shift = shift % LANES
    return pltpu.roll(tile, shift, 1) if shift else tile


class Halo:
    def __init__(self, rows, cols, edge, side, send, recv, place, volumes):
        self.rows, self.cols, self.edge, self.side = rows, cols, edge, side
        self.send, self.recv, self.place, self.volumes = send, recv, place, volumes
        self.count = 0
        self.sent = []

    def has(self, steps):
        present = None
        for axis, step in zip(AXES, steps):
            if step:
                me, size = self.place[axis]
                inside = me > 0 if step < 0 else me < size - 1
                present = inside if present is None else jnp.logical_and(present, inside)
        return present

    def push(self, source, target, *steps):
        index = self.count
        self.count += 1
        to = {}
        for axis, step in zip(AXES, steps):
            if step:
                me, size = self.place[axis]
                to[axis] = lax.rem(me + step + size, size)
        copy = pltpu.make_async_remote_copy(
            src_ref=source,
            dst_ref=target,
            send_sem=self.send.at[index],
            recv_sem=self.recv.at[index],
            device_id=to,
            device_id_type=MESH,
        )
        present = self.has(steps)

        @pl.when(present)
        def _():
            copy.start()

        self.sent.append((copy, present))
        return copy, self.has([-step for step in steps])

    def faces_x(self, volume):
        rows, inner = self.rows, pl.ds(1, SPAN_Y)
        return [
            self.push(
                rows.at[volume, 1 if step < 0 else SPAN_X, inner],
                rows.at[volume, PAD_X - 1 if step < 0 else 0, inner],
                step, 0, 0,
            )
            for step in (-1, 1)
        ]

    def columns(self, step_x, step_y):
        return [
            self.push(
                self.edge.at[0 if step < 0 else 1],
                self.cols.at[1 if step < 0 else 0, 1 - step_x, 1 - step_y],
                step_x, step_y, step,
            )
            for step in (-1, 1)
        ]

    def small(self):
        rows, every = self.rows, pl.ds(0, self.volumes)
        near = self.columns(0, 0)
        rest = []
        for step_x in (-1, 0, 1):
            at_x = (1 if step_x < 0 else SPAN_X) if step_x else pl.ds(1, SPAN_X)
            to_x = (PAD_X - 1 if step_x < 0 else 0) if step_x else pl.ds(1, SPAN_X)
            for step_y in (-1, 1):
                rest.append(
                    self.push(
                        rows.at[every, at_x, 1 if step_y < 0 else SPAN_Y],
                        rows.at[every, to_x, PAD_Y - 1 if step_y < 0 else 0],
                        step_x, step_y, 0,
                    )
                )
        for step_x, step_y in (
            (-1, -1), (-1, 1), (1, -1), (1, 1), (-1, 0), (1, 0), (0, -1), (0, 1)
        ):
            rest += self.columns(step_x, step_y)
        return near, rest

    def put_edge(self, first, last, lane):
        for index, tile in enumerate((first, last)):
            if self.volumes < 3:
                tile = jnp.where(lane[:16] < 64, tile[:16], pltpu.roll(tile[16:], 64, 1))
            self.edge[index] = tile

    def tile(self, side, index_x, index_y):
        tile = self.cols[side, index_x, index_y]
        if self.volumes < 3:
            tile = jnp.concatenate([tile, pltpu.roll(tile, 64, 1)], axis=0)
        return tile

    def own(self, side, volume, lane):
        tile = self.tile(side, 1, 1)
        at = 32 * volume
        return jnp.where(lane < 64, rolled(tile, 33 - at), rolled(tile, 49 - at))

    def merged(self, side, volume, lane):
        at = 32 * volume
        inside = lax.rem(lane, 32)

        def strip(index, low, middle, high):
            low, middle, high = (
                rolled(self.tile(side, index, k), shift - at)
                for k, shift in enumerate((low, middle, high))
            )
            return jnp.where(inside == 0, low, jnp.where(inside == PAD_Y - 1, high, middle))

        return jnp.where(
            lane < 64,
            jnp.where(lane < 32, strip(0, -31, -15, 1), strip(1, 17, 33, 49)),
            jnp.where(lane < 96, strip(1, 33, 49, 65), strip(2, 81, 97, 113)),
        )

    @staticmethod
    def arrive(pushes):
        for copy, present in pushes:

            @pl.when(present)
            def _(copy=copy):
                copy.wait_recv()

    def drain(self):
        for copy, present in self.sent:

            @pl.when(present)
            def _(copy=copy):
                copy.wait_send()


def kernel(
    voxels,
    x_a, x_b, grad, w_first, w_second, gain_first, bias_first, gain_second, bias_second,
    y_out, dx_out, gw_first, gw_second, norm_out,
    block_a, block_b, block_g, kernel_1, kernel_2, row_1, row_2, row_3, row_4, weights, stage,
    taps_x, taps_h, taps_d2, taps_d1,
    rows_x, rows_1, rows_2, rows_e,
    cols_x, cols_1, cols_2, cols_e,
    edge_x, edge_1, edge_2, edge_e,
    side_x, side_1, side_2, side_e,
    side_h,
    conv_1, conv_2, back_1,
    sums,
    norms, slopes, norms_2, slopes_2,
    early_out, early_in, mid_out, mid_in, late_out, late_in, gathered, pairs,
    halo_send, halo_recv, sums_send, sums_recv, gw_send, gw_recv, local,
):
    loads = [
        pltpu.make_async_copy(source, target, local.at[index])
        for index, (source, target) in enumerate((
            (x_a, block_a), (x_b, block_b), (grad, block_g), (w_first, kernel_1),
            (w_second, kernel_2), (gain_first, row_1), (bias_first, row_2), (gain_second, row_3),
            (bias_second, row_4),
        ))
    ]
    for load in loads:
        load.start()
    place = {axis: (lax.axis_index(axis), lax.axis_size(axis)) for axis in AXES}
    for chunks in (early_out, mid_out, late_out):
        for j in range(4):
            at = slice(32 * j + 28, 32 * j + 32)
            chunks[at] = jnp.zeros((4, chunks.shape[1], LANES), F32)
    for rows in (norms, slopes, norms_2, slopes_2):
        for at in (0, SPAN_Y + 2):
            rows[:, at : at + 2] = jnp.zeros((SPAN_X, 2, C, LANES), BF16)
    barrier = pltpu.get_barrier_semaphore()
    count = place["gx"][1] * place["gy"][1] * place["gz"][1]
    flat = (place["gx"][0] * place["gy"][1] + place["gy"][0]) * place["gz"][1] + place["gz"][0]

    chip_x, chip_y = place["gy"][0], place["gz"][0] // 2
    chip_z = place["gx"][0] // 2 * 2 + lax.rem(place["gz"][0], 2)
    core = lax.rem(place["gx"][0], 2)

    def other(step):
        return lax.rem(flat + step, count)

    def fan_out(source_of, target, send, recv):
        spots = []
        for step_z, step_core in ((2, 1), (2, 0), (1, 1), (3, 1), (1, 0), (3, 0), (0, 1), (0, 0)):
            to_z, to_core = lax.rem(chip_z + step_z, 4), lax.rem(core + step_core, 2)
            spots.append(to_z // 2 * 64 + to_core * 32 + lax.rem(to_z, 2))

        def copies(plane, chosen):
            to_x = lax.rem(chip_x + plane // 4 + 1, 4)
            to_y = lax.rem(chip_y + lax.rem(plane, 4) + 1, 4)
            for spot in chosen:
                to = spot + to_x * 8 + to_y * 2
                pltpu.make_async_remote_copy(
                    src_ref=source_of(to), dst_ref=target, send_sem=send, recv_sem=recv,
                    device_id=to, device_id_type=pl.DeviceIdType.LOGICAL,
                ).start()

        def most(block, carry):
            for k in range(8):
                copies(block * 8 + k, spots[:-1])
            return carry

        def rest(block, carry):
            for k in range(15):
                copies(block * 15 + k, spots[-1:])
            return carry

        lax.fori_loop(0, 2, most, 0)
        rest(0, 0)

    def fan_in(slots, semaphore):
        part = slots.at[pl.ds(0, count - 1)]
        pltpu.make_async_copy(part, part, semaphore).wait()

    def greet(step, carry):
        pl.semaphore_signal(
            barrier, inc=1, device_id=other(step), device_id_type=pl.DeviceIdType.LOGICAL
        )
        return carry

    lax.fori_loop(1, count, greet, 0)

    lane = lax.broadcasted_iota(jnp.int32, (C, LANES), 1)
    halos = []
    for index, (rows, cols, edge, side, volumes) in enumerate((
        (rows_x, cols_x, edge_x, side_x, 3),
        (rows_1, cols_1, edge_1, side_1, 2),
        (rows_2, cols_2, edge_2, side_2, 1),
        (rows_e, cols_e, edge_e, side_e, 1),
    )):
        halos.append(
            Halo(rows, cols, edge, side, halo_send.at[index], halo_recv.at[index], place, volumes)
        )
    halo_x, halo_1, halo_2, halo_e = halos

    low_x, high_x = place["gx"][0] > 0, place["gx"][0] < place["gx"][1] - 1
    low_y, high_y = place["gy"][0] > 0, place["gy"][0] < place["gy"][1] - 1
    low_z, high_z = place["gz"][0] > 0, place["gz"][0] < place["gz"][1] - 1

    def keep(at_x, at_y):
        held_x = low_x if at_x == 0 else high_x if at_x == PAD_X - 1 else None
        if isinstance(at_y, int):
            held_y = low_y if at_y == 0 else high_y if at_y == PAD_Y - 1 else None
        else:
            held_y = jnp.logical_and(
                jnp.logical_or(at_y > 0, low_y), jnp.logical_or(at_y < PAD_Y - 1, high_y)
            )
        if held_x is None:
            return held_y
        return held_x if held_y is None else jnp.logical_and(held_x, held_y)

    def lane_keep(side):
        spot_x, spot_y = lane // 32, lax.rem(lane, 32)
        bad = jnp.zeros((C, LANES), jnp.int32)
        for hit, present in (
            (spot_x == 0, low_x), (spot_x == PAD_X - 1, high_x),
            (spot_y == 0, low_y), (spot_y == PAD_Y - 1, high_y),
        ):
            missing = jnp.where(present, 0, 1)
            bad = bad + jnp.where(hit, missing, 0)
        bad = bad + jnp.where(low_z if side == 0 else high_z, 0, 1)
        return bad == 0

    def extract(tile, spot, carry):
        first, last = carry
        tile = tile.astype(BF16)
        first = jnp.where(lane == spot, pltpu.roll(tile, spot, 1), first)
        last = jnp.where(lane == spot, pltpu.roll(tile, lax.rem(spot + 1, LANES), 1), last)
        return first, last

    def put_taps(taps, volume, spots, tiles, sides):
        low, high = sides[0][...], sides[1][...]
        shifted = []
        for (at_x, at_y), tile in zip(spots, tiles):
            spot = at_x * 32 + at_y
            left = jnp.where(
                lane == 0,
                pltpu.roll(low, lax.rem(LANES - spot, LANES), 1),
                pltpu.roll(tile, 1, 1),
            )
            right = jnp.where(
                lane == LANES - 1,
                pltpu.roll(high, LANES - 1 - spot, 1),
                pltpu.roll(tile, LANES - 1, 1),
            )
            shifted.append((left, tile, right))
        for (at_x, at_y), rows in zip(spots, shifted):
            for k, row in enumerate(rows):
                taps[volume, at_x, at_y, k * C : (k + 1) * C] = row

    def build_inner(taps, volume, inner, sides):
        for at_x in range(SPAN_X):

            def step(block, carry, at_x=at_x):
                rows = [block * INNER + k for k in range(INNER)]
                tiles = [inner(at_x, at_y).astype(BF16) for at_y in rows]
                put_taps(taps, volume, [(at_x + 1, at_y + 1) for at_y in rows], tiles, sides)
                return carry

            unrolled(0, SPAN_Y // INNER, step, 0)

    def build_outer(taps, volume, outer, sides):
        def put(spots):
            tiles = [
                jnp.where(keep(at_x, at_y), outer(at_x, at_y).astype(BF16), none)
                for at_x, at_y in spots
            ]
            put_taps(taps, volume, spots, tiles, sides)

        put([(at_x, at_y) for at_x in (1, 2) for at_y in (0, PAD_Y - 1)])
        for at_x in (0, PAD_X - 1):

            def step(block, carry, at_x=at_x):
                put([(at_x, block * OUTER + k) for k in range(OUTER)])
                return carry

            unrolled(0, PAD_Y // OUTER, step, 0)

    def build(taps, volume, outer, inner, sides):
        build_inner(taps, volume, inner, sides)
        build_outer(taps, volume, outer, sides)

    def convolve(taps, volume, weight, emit, carry):
        parts = {}
        for block in range(PAD_Y // GROUP):
            columns = [
                taps[volume, :, block * GROUP + k].reshape(DEPTH, LANES) for k in range(GROUP)
            ]
            total = jnp.dot(
                weights[weight], jnp.concatenate(columns, axis=1), preferred_element_type=F32
            )
            for k in range(GROUP):
                parts[block * GROUP + k] = total[:, k * LANES : (k + 1) * LANES]
            for at_y in range((block - 1) * GROUP, block * GROUP):
                if at_y < 0 or at_y + 2 not in parts:
                    continue
                for at_x in range(SPAN_X):
                    low = at_x * C
                    tile = parts[at_y][low : low + C]
                    for tap in (1, 2):
                        first = tap * SPAN_X * C + low
                        tile = tile + parts[at_y + tap][first : first + C]
                    carry = emit(at_x, at_y, tile, carry)
        return carry

    def kernel_grad(taps, volume, buffers, out, plain):
        tap_row = lax.broadcasted_iota(jnp.int32, (16, LANES), 0)
        left, right = [], []
        for at_y in range(PAD_Y):
            parts = [
                rows[at_x, at_y - tap + 2]
                for rows in buffers for tap in range(3) for at_x in range(SPAN_X)
            ]
            if plain:
                inside = [0 <= at_y - tap < SPAN_Y for tap in range(3)]
                first = inside.index(True)
                mine = jnp.logical_and(tap_row >= first, tap_row < first + sum(inside))
                parts.append(jnp.where(mine, 1.0, 0.0).astype(BF16))
            left.append(jnp.concatenate(parts, axis=0))
            right.append(taps[volume, :, at_y].reshape(DEPTH, LANES))
        total = lax.dot_general(
            jnp.concatenate(left, axis=1),
            jnp.concatenate(right, axis=1),
            (((1,), (1,)), ((), ())),
            preferred_element_type=F32,
        )

        def wide(pieces):
            height = pieces[0].shape[0]
            return jnp.concatenate(
                pieces + [jnp.zeros((height, 7 * LANES - FLAT), F32)], axis=1
            )

        def slab(row, height, at_x):
            return total[row : row + height, TAPS * at_x : TAPS * (at_x + 1)]

        blocks = []
        for index in range(len(buffers)):
            first = 6 * C * index
            pieces = []
            for tap_x in range(3):
                for tap_y in range(3):
                    row = first + 2 * C * tap_y
                    pieces.append(slab(row, C, tap_x) + slab(row + C, C, tap_x + 1))
            blocks.append(wide(pieces))
        if plain:
            first = 6 * C * len(buffers)
            alone = wide([
                slab(first + tap_y, 1, tap_x) + slab(first + tap_y, 1, tap_x + 1)
                for tap_x in range(3) for tap_y in range(3)
            ])
        for k in range(7):
            lanes = slice(LANES * k, LANES * (k + 1))
            for pair in range(16):
                spot = (pair // 4 * 8 + k) * 4 + pair % 4
                for index, block in enumerate(blocks):
                    out[spot, 2 * index : 2 * index + 2] = block[2 * pair : 2 * pair + 2, lanes]
                if plain:
                    last = 2 * len(blocks)
                    out[spot, last : last + 1] = alone[:, lanes]

    channel = lax.broadcasted_iota(jnp.int32, (C, LANES), 0)

    def pack(columns):
        whole = jnp.zeros((C, LANES), F32)
        for k, column in enumerate(columns):
            whole = whole + jnp.where(lane == channel + 32 * k, column, 0.0)
        return jnp.sum(whole, axis=0, keepdims=True)

    def unpack(row, number):
        return [
            jnp.sum(jnp.where(lane == channel + 32 * k, row, 0.0), axis=1, keepdims=True)
            for k in range(number)
        ]

    class Total:
        def __init__(self, index):
            self.slots, self.index = sums.at[index], index

        def start(self, row):
            mine = self.slots.at[flat]
            mine[...] = row

            fan_out(
                lambda to: mine, mine, sums_send.at[self.index], sums_recv.at[self.index]
            )

        def finish(self):
            fan_in(self.slots, sums_recv.at[self.index])
            return jnp.sum(self.slots[...], axis=0)

        def drain(self):
            fan_in(self.slots, sums_send.at[self.index])

    totals = [Total(index) for index in range(4)]

    small_lane = lax.broadcasted_iota(jnp.int32, (C, C), 1)
    small_row = lax.broadcasted_iota(jnp.int32, (C, C), 0)

    def column(row):
        return jnp.sum(jnp.where(small_lane == small_row, row[...], 0.0), axis=1, keepdims=True)

    for load in loads[5:]:
        load.wait()
    gain_1, bias_1, gain_2, bias_2 = (column(row) for row in (row_1, row_2, row_3, row_4))

    def stack_weights(source, forward, backward):
        tiles = [
            jnp.concatenate(
                [source[tap].astype(F32) for tap in range(4 * k, min(4 * k + 4, 27))]
                + ([jnp.zeros((C, C), F32)] if k == 6 else []),
                axis=1,
            )
            for k in range(7)
        ]
        turned = [tile.T for tile in tiles]
        empty = jnp.zeros((C, C), F32)
        ahead = [source[tap].astype(F32) for tap in range(27)]
        back = [turned[tap // 4][C * (tap % 4) : C * (tap % 4) + C] for tap in range(26, -1, -1)]
        for index, pieces in ((forward, ahead), (backward, back)):
            for tap_y in range(3):
                line = [
                    pieces[(tap_x * 3 + tap_y) * 3 + tap_z]
                    for tap_x in range(3) for tap_z in range(3)
                ]
                for at_x, row in ((0, line + [empty] * 3), (1, [empty] * 3 + line)):
                    first = (tap_y * SPAN_X + at_x) * C
                    for k in range(3):
                        weights[index, first : first + C, LANES * k : LANES * (k + 1)] = (
                            jnp.concatenate(row[4 * k : 4 * k + 4], axis=1).astype(BF16)
                        )

    zero = jnp.zeros((C, LANES), F32)
    none = jnp.zeros((C, LANES), BF16)

    def take(load, source, at, carry):
        load.wait()
        for at_x in range(SPAN_X):
            rows_x[at, at_x + 1, 1 : SPAN_Y + 1] = jnp.swapaxes(
                source[:, at_x].astype(F32), 0, 1
            ).astype(BF16)
        for at_x in range(SPAN_X):

            def step(block, carry, at_x=at_x):
                for k in range(8):
                    at_y = block * 8 + k
                    carry = extract(
                        rows_x[at, at_x + 1, at_y + 1],
                        32 * at + 16 * at_x + at_y,
                        carry,
                    )
                return carry

            carry = unrolled(0, 2, step, carry)
        return carry

    carry = (none, none)
    for at, source in enumerate((block_a, block_b, block_g)):
        carry = take(loads[at], source, at, carry)
    halo_x.put_edge(*carry, lane)

    pl.semaphore_wait(barrier, count - 1)

    near, rest = halo_x.small()
    waits_x = [halo_x.faces_x(0), halo_x.faces_x(1)]
    loads[3].wait()
    loads[4].wait()
    stack_weights(kernel_1, 0, 3)
    stack_weights(kernel_2, 1, 2)
    ok = [lane_keep(side) for side in range(2)]
    halo_x.arrive(near)
    for volume in range(2):
        for side in range(2):
            side_x[volume, side] = jnp.where(ok[side], halo_x.own(side, volume, lane), none)
        build_inner(
            taps_x, volume,
            lambda at_x, at_y, volume=volume: rows_x[volume, at_x + 1, at_y + 1],
            (side_x.at[volume, 0], side_x.at[volume, 1]),
        )
    halo_x.arrive(rest)
    for side in range(2):
        for volume in range(3):
            tile = halo_x.merged(side, volume, lane)
            side_x[volume, side] = jnp.where(ok[side], tile, none)

    columns = []
    waits_1 = []
    carry = (none,) * 2
    for volume in range(2):
        halo_x.arrive(waits_x[volume])
        build_outer(
            taps_x, volume,
            lambda at_x, at_y, volume=volume: rows_x[volume, at_x, at_y],
            (side_x.at[volume, 0], side_x.at[volume, 1]),
        )

        def emit(at_x, at_y, tile, carry, volume=volume):
            total, squares, first, last = carry
            conv_1[volume, at_x, at_y] = tile
            rows_1[volume, at_x + 1, at_y + 1] = tile.astype(BF16)
            first, last = extract(tile, 32 * volume + 16 * at_x + at_y, (first, last))
            return total + tile, squares + tile * tile, first, last

        total, squares, *carry = convolve(taps_x, volume, 0, emit, (zero, zero, *carry))
        if volume == 0:
            waits_1.append(halo_1.faces_x(0))
        columns += [
            jnp.sum(total, axis=1, keepdims=True), jnp.sum(squares, axis=1, keepdims=True)
        ]
    halo_1.put_edge(*carry, lane)
    totals[0].start(pack(columns))
    near, rest = halo_1.small()
    waits_1.append(halo_1.faces_x(1))
    row = totals[0].finish()
    halo_1.arrive(near + rest)
    waits_g = halo_x.faces_x(2)
    stats = unpack(row, 4)

    def moments(total, squares):
        mean = total / voxels
        scale = lax.rsqrt(squares / voxels - mean * mean + EPSILON)
        return mean, scale

    columns = []
    for volume in range(2):
        mean, scale = moments(stats[2 * volume], stats[2 * volume + 1])
        slope = jnp.broadcast_to(gain_1 * scale, (C, LANES))
        shift = jnp.broadcast_to(bias_1 - mean * gain_1 * scale, (C, LANES))

        def active(value, slope=slope, shift=shift):
            pre = value * slope + shift
            return pre * sigmoid(pre)

        norm_slope = jnp.broadcast_to(scale, (C, LANES))
        norm_shift = jnp.broadcast_to(-mean * scale, (C, LANES))

        def own_row(at_x, at_y, volume, active, norm_slope=norm_slope, norm_shift=norm_shift):
            value = conv_1[volume, at_x, at_y]
            if volume == 1:
                norms[at_x, at_y + 2] = (value * norm_slope + norm_shift).astype(BF16)
            return active(value)

        for side in range(2):
            tile = halo_1.merged(side, volume, lane)
            side_1[volume, side] = tile
            side_h[volume, side] = jnp.where(
                ok[side], active(tile.astype(F32)), 0.0
            ).astype(BF16)
        sides = (side_h.at[volume, 0], side_h.at[volume, 1])
        build_inner(
            taps_h, volume, functools.partial(own_row, volume=volume, active=active), sides
        )
        halo_1.arrive(waits_1[volume])
        build_outer(
            taps_h, volume,
            lambda at_x, at_y, volume=volume: active(rows_1[volume, at_x, at_y].astype(F32)),
            sides,
        )
        if volume == 0:

            def emit(at_x, at_y, tile, carry):
                total, squares = carry
                conv_2[0, at_x, at_y] = tile
                return total + tile, squares + tile * tile

            total, squares = convolve(taps_h, 0, 1, emit, (zero,) * 2)
        else:

            def emit(at_x, at_y, tile, carry):
                total, squares, first, last = carry
                conv_2[1, at_x, at_y] = tile
                rows_2[0, at_x + 1, at_y + 1] = tile.astype(BF16)
                first, last = extract(tile, 16 * at_x + at_y, (first, last))
                return total + tile, squares + tile * tile, first, last

            total, squares, first, last = convolve(taps_h, 1, 1, emit, (zero, zero, none, none))
            halo_2.put_edge(first, last, lane)
        columns += [
            jnp.sum(total, axis=1, keepdims=True), jnp.sum(squares, axis=1, keepdims=True)
        ]
    mean_1, scale_1 = mean, scale
    totals[1].start(pack(columns))
    near, rest = halo_2.small()
    waits = near + rest + halo_2.faces_x(0)
    kernel_grad(taps_x, 1, [norms], early_out, True)
    fan_out(
        lambda to: early_out.at[to], early_in.at[flat], gw_send.at[0], gw_recv.at[0]
    )
    early_in[flat] = early_out[flat]
    stats = unpack(totals[1].finish(), 4)

    mean_2, scale_2 = moments(stats[2], stats[3])

    def layer_of(mean, scale, gain, bias):
        norm_slope = jnp.broadcast_to(scale, (C, LANES))
        norm_shift = jnp.broadcast_to(-mean * scale, (C, LANES))
        wide_gain = jnp.broadcast_to(gain, (C, LANES))
        wide_bias = jnp.broadcast_to(bias, (C, LANES))

        def slope_of(value, upstream):
            normed = value * norm_slope + norm_shift
            pre = wide_gain * normed + wide_bias
            sigma = sigmoid(pre)
            return upstream * (sigma * (1.0 + pre * (1.0 - sigma))), normed

        return slope_of

    def delta_of(slope_of, sum_d, sum_x, gain, scale):
        wide_d = jnp.broadcast_to(sum_d / voxels, (C, LANES))
        wide_x = jnp.broadcast_to(sum_x / voxels, (C, LANES))
        factor = jnp.broadcast_to(gain * scale, (C, LANES))

        def delta(value, upstream):
            slope, normed = slope_of(value, upstream)
            return factor * (slope - wide_d - normed * wide_x)

        return delta

    slope_2 = layer_of(mean_2, scale_2, gain_2, bias_2)

    def sum_rows(slope_of, value_of, upstream_of):
        carry = (zero, zero)
        for at_x in range(SPAN_X):

            def step(block, carry, at_x=at_x):
                total, weighted = carry
                for k in range(8):
                    at_y = block * 8 + k
                    slope, normed = slope_of(value_of(at_x, at_y), upstream_of(at_x, at_y))
                    slopes_2[at_x, at_y + 2] = slope.astype(BF16)
                    norms_2[at_x, at_y + 2] = normed.astype(BF16)
                    total, weighted = total + slope, weighted + slope * normed
                return total, weighted

            carry = unrolled(0, 2, step, carry)
        return [jnp.sum(part, axis=1, keepdims=True) for part in carry]

    columns = sum_rows(
        slope_2,
        lambda at_x, at_y: conv_2[1, at_x, at_y],
        lambda at_x, at_y: rows_x[2, at_x + 1, at_y + 1].astype(F32),
    )
    totals[2].start(pack(columns))

    mean_a, scale_a = moments(stats[0], stats[1])
    slope_a = jnp.broadcast_to(gain_2 * scale_a, (C, LANES))
    shift_a = jnp.broadcast_to(bias_2 - mean_a * gain_2 * scale_a, (C, LANES))
    for at_x in range(SPAN_X):

        def step(block, carry, at_x=at_x):
            for k in range(8):
                at_y = block * 8 + k
                pre = conv_2[0, at_x, at_y] * slope_a + shift_a
                stage[at_x, at_y] = pre * sigmoid(pre)
            return carry

        unrolled(0, 2, step, 0)
        y_out[:, at_x] = jnp.swapaxes(stage[at_x], 0, 1).astype(BF16)

    kernel_grad(taps_h, 1, [slopes_2, norms_2], mid_out, True)
    fan_out(lambda to: mid_out.at[to], mid_in.at[flat], gw_send.at[1], gw_recv.at[1])
    mid_in[flat] = mid_out[flat]
    halo_x.arrive(waits_g)
    halo_2.arrive(waits)
    sum_d2, sum_x2 = unpack(totals[2].finish(), 2)

    delta_2 = delta_of(slope_2, sum_d2, sum_x2, gain_2, scale_2)
    for side in range(2):
        tile = delta_2(
            halo_2.merged(side, 0, lane).astype(F32), side_x[2, side].astype(F32)
        )
        side_2[0, side] = jnp.where(ok[side], tile, 0.0).astype(BF16)
    build(
        taps_d2, 0,
        lambda at_x, at_y: delta_2(
            rows_2[0, at_x, at_y].astype(F32), rows_x[2, at_x, at_y].astype(F32)
        ),
        lambda at_x, at_y: delta_2(
            conv_2[1, at_x, at_y], rows_x[2, at_x + 1, at_y + 1].astype(F32)
        ),
        (side_2.at[0, 0], side_2.at[0, 1]),
    )
    slope_1 = layer_of(mean_1, scale_1, gain_1, bias_1)

    def emit(at_x, at_y, tile, carry):
        total, weighted, first, last = carry
        back_1[at_x, at_y] = tile
        rows_e[0, at_x + 1, at_y + 1] = tile.astype(BF16)
        first, last = extract(tile, 16 * at_x + at_y, (first, last))
        slope, normed = slope_1(conv_1[1, at_x, at_y], tile)
        slopes[at_x, at_y + 2] = slope.astype(BF16)
        return total + slope, weighted + slope * normed, first, last

    total, weighted, first, last = convolve(taps_d2, 0, 2, emit, (zero, zero, none, none))
    halo_e.put_edge(first, last, lane)
    columns = [
        jnp.sum(total, axis=1, keepdims=True), jnp.sum(weighted, axis=1, keepdims=True)
    ]
    totals[3].start(pack(columns))
    near, rest = halo_e.small()
    kernel_grad(taps_x, 1, [slopes], late_out, False)
    fan_out(lambda to: late_out.at[to], late_in.at[flat], gw_send.at[2], gw_recv.at[2])
    waits = near + rest + halo_e.faces_x(0)
    late_in[flat] = late_out[flat]
    sum_d1, sum_x1 = unpack(totals[3].finish(), 2)

    whole = 1.0 / math.sqrt(voxels)
    for k, factor in enumerate(
        (
            gain_1 * scale_1 * whole, sum_d1 / voxels, sum_x1 / voxels,
            gain_2 * scale_2 * whole, sum_d2 / voxels, sum_x2 / voxels,
        )
    ):
        tile = jnp.broadcast_to(factor, (C, LANES))
        for pair in range(16):
            pairs[k, pair] = tile[2 * pair : 2 * pair + 2]
    fan_in(early_in, gw_recv.at[0])
    early = jnp.sum(early_in[...], axis=0)
    fan_in(mid_in, gw_recv.at[1])
    mid = jnp.sum(mid_in[...], axis=0)
    at = flat // 32 * 4 + lax.rem(flat, 4)
    fan_in(late_in, gw_recv.at[2])
    late = jnp.sum(late_in[...], axis=0)
    gathered[flat, 0:2] = pairs[0, at] * (
        late[0:2] - pairs[1, at] * early[2:3] - pairs[2, at] * early[0:2]
    )
    gathered[flat, 2:4] = pairs[3, at] * (
        mid[0:2] - pairs[4, at] * mid[4:5] - pairs[5, at] * mid[2:4]
    )
    mine = gathered.at[flat]
    fan_out(lambda to: mine, mine, gw_send.at[3], gw_recv.at[3])

    halo_e.arrive(waits)
    delta_1 = delta_of(slope_1, sum_d1, sum_x1, gain_1, scale_1)
    for side in range(2):
        tile = delta_1(
            side_1[1, side].astype(F32), halo_e.merged(side, 0, lane).astype(F32)
        )
        side_e[0, side] = jnp.where(ok[side], tile, 0.0).astype(BF16)
    build(
        taps_d1, 0,
        lambda at_x, at_y: delta_1(
            rows_1[1, at_x, at_y].astype(F32), rows_e[0, at_x, at_y].astype(F32)
        ),
        lambda at_x, at_y: delta_1(conv_1[1, at_x, at_y], back_1[at_x, at_y]),
        (side_e.at[0, 0], side_e.at[0, 1]),
    )
    def emit(at_x, at_y, tile, carry):
        stage[at_x, at_y] = tile
        return carry

    convolve(taps_d1, 0, 3, emit, 0)
    for at_x in range(SPAN_X):
        dx_out[:, at_x] = jnp.swapaxes(stage[at_x], 0, 1).astype(BF16)

    for k, total in enumerate((sum_x1, sum_d1, sum_x2, sum_d2)):
        norm_out[k : k + 1] = whole * jnp.sum(
            jnp.where(small_lane == small_row, total, 0.0), axis=0, keepdims=True
        )
    fan_in(gathered, gw_recv.at[3])
    for member, out in ((0, gw_first), (1, gw_second)):
        for k in range(7):
            tile = jnp.concatenate(
                [
                    gathered[(pair // 4 * 8 + k) * 4 + pair % 4, 2 * member : 2 * member + 2]
                    for pair in range(16)
                ],
                axis=0,
            )
            for tap in range(4 * k, min(4 * k + 4, 27)):
                out[tap] = tile[:, C * (tap % 4) : C * (tap % 4) + C]

    for halo in halos:
        halo.drain()
    for total in totals:
        total.drain()
    for k, chunks in enumerate((early_out, mid_out, late_out, gathered)):
        fan_in(chunks, gw_send.at[k])


def write_out(*refs):
    sources, targets, semaphores = refs[:5], refs[5:10], refs[10]
    copies = [
        pltpu.make_async_copy(source, target, semaphores.at[index])
        for index, (source, target) in enumerate(zip(sources, targets))
    ]
    for copy in copies:
        copy.start()
    for copy in copies:
        copy.wait()


def body(voxels, x_a, x_b, w_first, w_second, gain_first, bias_first, gain_second, bias_second,
         grad_out):
    def sized(*shape, kind=BF16):
        return pltpu.VMEM(shape, kind)

    volumes = (3, 2, 1, 1)
    devices = math.prod(lax.axis_size(axis) for axis in AXES)
    block = (C, SPAN_X, SPAN_Y, LANES)
    scratch = [sized(*block)] * 3 + [sized(27, C, C)] * 2 + [sized(1, C, kind=F32)] * 4
    scratch += [
        sized(4, HEIGHT, DEPTH), sized(SPAN_X, SPAN_Y, C, LANES, kind=F32)
    ]
    scratch += [sized(count, PAD_X, PAD_Y, TAPS, LANES) for count in (2, 2, 1, 1)]
    scratch += [sized(count, PAD_X, PAD_Y, C, LANES) for count in volumes]
    heights = [C if count == 3 else C // 2 for count in volumes]
    scratch += [sized(2, 3, 3, height, LANES) for height in heights]
    scratch += [sized(2, height, LANES) for height in heights]
    scratch += [sized(count, 2, C, LANES) for count in volumes] + [sized(2, 2, C, LANES)]
    scratch += [
        sized(2, SPAN_X, SPAN_Y, C, LANES, kind=F32),
        sized(2, SPAN_X, SPAN_Y, C, LANES, kind=F32),
        sized(SPAN_X, SPAN_Y, C, LANES, kind=F32),
        sized(4, devices, 1, LANES, kind=F32),
        *[sized(SPAN_X, SPAN_Y + 4, C, LANES)] * 4,
        *[sized(devices, 3, LANES, kind=F32)] * 2,
        *[sized(devices, 5, LANES, kind=F32)] * 2,
        *[sized(devices, 2, LANES, kind=F32)] * 2,
        sized(devices, 4, LANES, kind=F32),
        sized(6, 16, 2, LANES, kind=F32),
        pltpu.SemaphoreType.DMA((4, 32)),
        pltpu.SemaphoreType.DMA((4, 32)),
        pltpu.SemaphoreType.DMA((4,)),
        pltpu.SemaphoreType.DMA((4,)),
        pltpu.SemaphoreType.DMA((4,)),
        pltpu.SemaphoreType.DMA((4,)),
        pltpu.SemaphoreType.DMA((9,)),
    ]
    in_vmem = pl.BlockSpec(memory_space=pltpu.VMEM)
    in_hbm = pl.BlockSpec(memory_space=pltpu.HBM)
    taps = jax.ShapeDtypeStruct((27, C, C), F32)
    out_shape = (
        jax.ShapeDtypeStruct(block, BF16),
        jax.ShapeDtypeStruct(block, BF16),
        taps,
        taps,
        jax.ShapeDtypeStruct((4, C), F32),
    )
    results = pl.pallas_call(
        functools.partial(kernel, voxels),
        out_shape=out_shape,
        in_specs=[in_hbm] * 9,
        out_specs=(in_vmem,) * 5,
        scratch_shapes=scratch,
        compiler_params=pltpu.CompilerParams(
            collective_id=0, has_side_effects=True, vmem_limit_bytes=28 * 1024 * 1024
        ),
    )(
        *(pltpu.with_memory_space_constraint(value, pltpu.HBM) for value in (
            x_a, x_b, grad_out, w_first.reshape(27, C, C), w_second.reshape(27, C, C),
            *(row.reshape(1, C) for row in (gain_first, bias_first, gain_second, bias_second)),
        )),
    )
    y_a, dx_b, grad_first, grad_second, norms = pl.pallas_call(
        write_out,
        out_shape=out_shape,
        in_specs=[in_vmem] * 5,
        out_specs=(in_hbm,) * 5,
        scratch_shapes=[pltpu.SemaphoreType.DMA((5,))],
        compiler_params=pltpu.CompilerParams(vmem_limit_bytes=8 * 1024 * 1024),
    )(*results)
    return (
        y_a, dx_b, grad_first.reshape(3, 3, 3, C, C), grad_second.reshape(3, 3, 3, C, C), norms
    )


def solution(mesh):
    split = P(None, "gx", "gy", "gz")
    voxels = float(SPAN_X * SPAN_Y * LANES * mesh.size)
    return jax.shard_map(
        functools.partial(body, voxels),
        mesh=mesh,
        in_specs=(split, split, P(), P(), P(), P(), P(), P(), split),
        out_specs=(split, split, P(), P(), P()),
        check_vma=False,
    )
```

```python
import functools
import math

import jax
import jax.numpy as jnp
from jax import lax
from jax.experimental import pallas as pl
from jax.experimental.pallas import tpu as pltpu
from jax.sharding import PartitionSpec as P

F32 = jnp.float32
BF16 = jnp.bfloat16
EPSILON = 1e-05
C = 32
LANES = 128
SPAN_X, SPAN_Y = 2, 16
PAD_X, PAD_Y = SPAN_X + 2, SPAN_Y + 2
TAPS = 3 * C
DEPTH = PAD_X * TAPS
HEIGHT = 3 * SPAN_X * C
FLAT = 9 * TAPS
GROUP = 2
INNER = 16
OUTER = 18
AXES = ("gx", "gy", "gz")
MESH = pl.DeviceIdType.MESH


def sigmoid(value):
    return 0.5 + 0.5 * jnp.tanh(0.5 * value)


def unrolled(first, last, step, carry):
    for index in range(first, last):
        carry = step(index, carry)
    return carry


def rolled(tile, shift):
    shift = shift % LANES
    return pltpu.roll(tile, shift, 1) if shift else tile


class Halo:
    def __init__(self, rows, cols, edge, side, send, recv, place, volumes):
        self.rows, self.cols, self.edge, self.side = rows, cols, edge, side
        self.send, self.recv, self.place, self.volumes = send, recv, place, volumes
        self.count = 0
        self.sent = []

    def has(self, steps):
        present = None
        for axis, step in zip(AXES, steps):
            if step:
                me, size = self.place[axis]
                inside = me > 0 if step < 0 else me < size - 1
                present = inside if present is None else jnp.logical_and(present, inside)
        return present

    def push(self, source, target, *steps):
        index = self.count
        self.count += 1
        to = {}
        for axis, step in zip(AXES, steps):
            if step:
                me, size = self.place[axis]
                to[axis] = lax.rem(me + step + size, size)
        copy = pltpu.make_async_remote_copy(
            src_ref=source,
            dst_ref=target,
            send_sem=self.send.at[index],
            recv_sem=self.recv.at[index],
            device_id=to,
            device_id_type=MESH,
        )
        present = self.has(steps)

        @pl.when(present)
        def _():
            copy.start()

        self.sent.append((copy, present))
        return copy, self.has([-step for step in steps])

    def faces_x(self, volume):
        rows, inner = self.rows, pl.ds(1, SPAN_Y)
        return [
            self.push(
                rows.at[volume, 1 if step < 0 else SPAN_X, inner],
                rows.at[volume, PAD_X - 1 if step < 0 else 0, inner],
                step, 0, 0,
            )
            for step in (-1, 1)
        ]

    def columns(self, step_x, step_y):
        return [
            self.push(
                self.edge.at[0 if step < 0 else 1],
                self.cols.at[1 if step < 0 else 0, 1 - step_x, 1 - step_y],
                step_x, step_y, step,
            )
            for step in (-1, 1)
        ]

    def small(self):
        rows, every = self.rows, pl.ds(0, self.volumes)
        near = self.columns(0, 0)
        rest = []
        for step_x in (-1, 0, 1):
            at_x = (1 if step_x < 0 else SPAN_X) if step_x else pl.ds(1, SPAN_X)
            to_x = (PAD_X - 1 if step_x < 0 else 0) if step_x else pl.ds(1, SPAN_X)
            for step_y in (-1, 1):
                rest.append(
                    self.push(
                        rows.at[every, at_x, 1 if step_y < 0 else SPAN_Y],
                        rows.at[every, to_x, PAD_Y - 1 if step_y < 0 else 0],
                        step_x, step_y, 0,
                    )
                )
        for step_x, step_y in (
            (-1, -1), (-1, 1), (1, -1), (1, 1), (-1, 0), (1, 0), (0, -1), (0, 1)
        ):
            rest += self.columns(step_x, step_y)
        return near, rest

    def put_edge(self, first, last, lane):
        for index, tile in enumerate((first, last)):
            if self.volumes < 3:
                tile = jnp.where(lane[:16] < 64, tile[:16], pltpu.roll(tile[16:], 64, 1))
            self.edge[index] = tile

    def tile(self, side, index_x, index_y):
        tile = self.cols[side, index_x, index_y]
        if self.volumes < 3:
            tile = jnp.concatenate([tile, pltpu.roll(tile, 64, 1)], axis=0)
        return tile

    def own(self, side, volume, lane):
        tile = self.tile(side, 1, 1)
        at = 32 * volume
        return jnp.where(lane < 64, rolled(tile, 33 - at), rolled(tile, 49 - at))

    def merged(self, side, volume, lane):
        at = 32 * volume
        inside = lax.rem(lane, 32)

        def strip(index, low, middle, high):
            low, middle, high = (
                rolled(self.tile(side, index, k), shift - at)
                for k, shift in enumerate((low, middle, high))
            )
            return jnp.where(inside == 0, low, jnp.where(inside == PAD_Y - 1, high, middle))

        return jnp.where(
            lane < 64,
            jnp.where(lane < 32, strip(0, -31, -15, 1), strip(1, 17, 33, 49)),
            jnp.where(lane < 96, strip(1, 33, 49, 65), strip(2, 81, 97, 113)),
        )

    @staticmethod
    def arrive(pushes):
        for copy, present in pushes:

            @pl.when(present)
            def _(copy=copy):
                copy.wait_recv()

    def drain(self):
        for copy, present in self.sent:

            @pl.when(present)
            def _(copy=copy):
                copy.wait_send()


def kernel(
    voxels,
    x_a, x_b, grad, w_first, w_second, gain_first, bias_first, gain_second, bias_second,
    y_out, dx_out, gw_first, gw_second, norm_out,
    block_a, block_b, block_g, kernel_1, kernel_2, row_1, row_2, row_3, row_4, weights, stage,
    taps_x, taps_h, taps_d2, taps_d1,
    rows_x, rows_1, rows_2, rows_e,
    cols_x, cols_1, cols_2, cols_e,
    edge_x, edge_1, edge_2, edge_e,
    side_x, side_1, side_2, side_e,
    side_h,
    conv_1, conv_2, back_1,
    sums,
    norms, slopes, norms_2, slopes_2,
    early_out, early_in, mid_out, mid_in, late_out, late_in, gathered, pairs,
    halo_send, halo_recv, sums_send, sums_recv, gw_send, gw_recv, local,
):
    loads = [
        pltpu.make_async_copy(source, target, local.at[index])
        for index, (source, target) in enumerate((
            (x_a, block_a), (x_b, block_b), (grad, block_g), (w_first, kernel_1),
            (w_second, kernel_2), (gain_first, row_1), (bias_first, row_2), (gain_second, row_3),
            (bias_second, row_4),
        ))
    ]
    for load in loads:
        load.start()
    place = {axis: (lax.axis_index(axis), lax.axis_size(axis)) for axis in AXES}
    for chunks in (early_out, mid_out, late_out):
        for j in range(4):
            at = slice(32 * j + 28, 32 * j + 32)
            chunks[at] = jnp.zeros((4, chunks.shape[1], LANES), F32)
    for rows in (norms, slopes, norms_2, slopes_2):
        for at in (0, SPAN_Y + 2):
            rows[:, at : at + 2] = jnp.zeros((SPAN_X, 2, C, LANES), BF16)
    barrier = pltpu.get_barrier_semaphore()
    count = place["gx"][1] * place["gy"][1] * place["gz"][1]
    flat = (place["gx"][0] * place["gy"][1] + place["gy"][0]) * place["gz"][1] + place["gz"][0]

    chip_x, chip_y = place["gy"][0], place["gz"][0] // 2
    chip_z = place["gx"][0] // 2 * 2 + lax.rem(place["gz"][0], 2)
    core = lax.rem(place["gx"][0], 2)

    def other(step):
        return lax.rem(flat + step, count)

    def fan_out(source_of, target, send, recv):
        spots = []
        for step_z, step_core in ((2, 1), (2, 0), (1, 1), (3, 1), (1, 0), (3, 0), (0, 1), (0, 0)):
            to_z, to_core = lax.rem(chip_z + step_z, 4), lax.rem(core + step_core, 2)
            spots.append(to_z // 2 * 64 + to_core * 32 + lax.rem(to_z, 2))

        def copies(plane, chosen):
            to_x = lax.rem(chip_x + plane // 4 + 1, 4)
            to_y = lax.rem(chip_y + lax.rem(plane, 4) + 1, 4)
            for spot in chosen:
                to = spot + to_x * 8 + to_y * 2
                pltpu.make_async_remote_copy(
                    src_ref=source_of(to), dst_ref=target, send_sem=send, recv_sem=recv,
                    device_id=to, device_id_type=pl.DeviceIdType.LOGICAL,
                ).start()

        def most(block, carry):
            for k in range(8):
                copies(block * 8 + k, spots[:-1])
            return carry

        def rest(block, carry):
            for k in range(15):
                copies(block * 15 + k, spots[-1:])
            return carry

        lax.fori_loop(0, 2, most, 0)
        rest(0, 0)

    def fan_in(slots, semaphore):
        part = slots.at[pl.ds(0, count - 1)]
        pltpu.make_async_copy(part, part, semaphore).wait()

    def greet(step, carry):
        pl.semaphore_signal(
            barrier, inc=1, device_id=other(step), device_id_type=pl.DeviceIdType.LOGICAL
        )
        return carry

    lax.fori_loop(1, count, greet, 0)

    lane = lax.broadcasted_iota(jnp.int32, (C, LANES), 1)
    halos = []
    def lone(refs, volume):
        return refs.at[pl.ds(volume, 1)]

    for index, (rows, cols, edge, side, volumes) in enumerate((
        (rows_x, cols_x, edge_x, side_x, 3),
        (lone(rows_1, 0), cols_1.at[0], edge_1.at[0], lone(side_1, 0), 1),
        (lone(rows_1, 1), cols_1.at[1], edge_1.at[1], lone(side_1, 1), 1),
        (rows_2, cols_2, edge_2, side_2, 1),
        (rows_e, cols_e, edge_e, side_e, 1),
    )):
        halos.append(
            Halo(rows, cols, edge, side, halo_send.at[index], halo_recv.at[index], place, volumes)
        )
    halo_x, halo_a, halo_b, halo_2, halo_e = halos
    halo_1 = (halo_a, halo_b)

    low_x, high_x = place["gx"][0] > 0, place["gx"][0] < place["gx"][1] - 1
    low_y, high_y = place["gy"][0] > 0, place["gy"][0] < place["gy"][1] - 1
    low_z, high_z = place["gz"][0] > 0, place["gz"][0] < place["gz"][1] - 1

    def keep(at_x, at_y):
        held_x = low_x if at_x == 0 else high_x if at_x == PAD_X - 1 else None
        if isinstance(at_y, int):
            held_y = low_y if at_y == 0 else high_y if at_y == PAD_Y - 1 else None
        else:
            held_y = jnp.logical_and(
                jnp.logical_or(at_y > 0, low_y), jnp.logical_or(at_y < PAD_Y - 1, high_y)
            )
        if held_x is None:
            return held_y
        return held_x if held_y is None else jnp.logical_and(held_x, held_y)

    def lane_keep(side):
        spot_x, spot_y = lane // 32, lax.rem(lane, 32)
        bad = jnp.zeros((C, LANES), jnp.int32)
        for hit, present in (
            (spot_x == 0, low_x), (spot_x == PAD_X - 1, high_x),
            (spot_y == 0, low_y), (spot_y == PAD_Y - 1, high_y),
        ):
            missing = jnp.where(present, 0, 1)
            bad = bad + jnp.where(hit, missing, 0)
        bad = bad + jnp.where(low_z if side == 0 else high_z, 0, 1)
        return bad == 0

    def extract(tile, spot, carry):
        first, last = carry
        tile = tile.astype(BF16)
        first = jnp.where(lane == spot, pltpu.roll(tile, spot, 1), first)
        last = jnp.where(lane == spot, pltpu.roll(tile, lax.rem(spot + 1, LANES), 1), last)
        return first, last

    def put_taps(taps, volume, spots, tiles, sides):
        low, high = sides[0][...], sides[1][...]
        shifted = []
        for (at_x, at_y), tile in zip(spots, tiles):
            spot = at_x * 32 + at_y
            left = jnp.where(
                lane == 0,
                pltpu.roll(low, lax.rem(LANES - spot, LANES), 1),
                pltpu.roll(tile, 1, 1),
            )
            right = jnp.where(
                lane == LANES - 1,
                pltpu.roll(high, LANES - 1 - spot, 1),
                pltpu.roll(tile, LANES - 1, 1),
            )
            shifted.append((left, tile, right))
        for (at_x, at_y), rows in zip(spots, shifted):
            for k, row in enumerate(rows):
                taps[volume, at_x, at_y, k * C : (k + 1) * C] = row

    def build_inner(taps, volume, inner, sides):
        for at_x in range(SPAN_X):

            def step(block, carry, at_x=at_x):
                rows = [block * INNER + k for k in range(INNER)]
                tiles = [inner(at_x, at_y).astype(BF16) for at_y in rows]
                put_taps(taps, volume, [(at_x + 1, at_y + 1) for at_y in rows], tiles, sides)
                return carry

            unrolled(0, SPAN_Y // INNER, step, 0)

    def build_outer(taps, volume, outer, sides):
        def put(spots):
            tiles = [
                jnp.where(keep(at_x, at_y), outer(at_x, at_y).astype(BF16), none)
                for at_x, at_y in spots
            ]
            put_taps(taps, volume, spots, tiles, sides)

        put([(at_x, at_y) for at_x in (1, 2) for at_y in (0, PAD_Y - 1)])
        for at_x in (0, PAD_X - 1):

            def step(block, carry, at_x=at_x):
                put([(at_x, block * OUTER + k) for k in range(OUTER)])
                return carry

            unrolled(0, PAD_Y // OUTER, step, 0)

    def build(taps, volume, outer, inner, sides):
        build_inner(taps, volume, inner, sides)
        build_outer(taps, volume, outer, sides)

    def convolve(taps, volume, weight, emit, carry):
        parts = {}
        for block in range(PAD_Y // GROUP):
            columns = [
                taps[volume, :, block * GROUP + k].reshape(DEPTH, LANES) for k in range(GROUP)
            ]
            total = jnp.dot(
                weights[weight], jnp.concatenate(columns, axis=1), preferred_element_type=F32
            )
            for k in range(GROUP):
                parts[block * GROUP + k] = total[:, k * LANES : (k + 1) * LANES]
            for at_y in range((block - 1) * GROUP, block * GROUP):
                if at_y < 0 or at_y + 2 not in parts:
                    continue
                for at_x in range(SPAN_X):
                    low = at_x * C
                    tile = parts[at_y][low : low + C]
                    for tap in (1, 2):
                        first = tap * SPAN_X * C + low
                        tile = tile + parts[at_y + tap][first : first + C]
                    carry = emit(at_x, at_y, tile, carry)
        return carry

    def kernel_grad(taps, volume, buffers, out, plain):
        tap_row = lax.broadcasted_iota(jnp.int32, (16, LANES), 0)
        left, right = [], []
        for at_y in range(PAD_Y):
            parts = [
                rows[at_x, at_y - tap + 2]
                for rows in buffers for tap in range(3) for at_x in range(SPAN_X)
            ]
            if plain:
                inside = [0 <= at_y - tap < SPAN_Y for tap in range(3)]
                first = inside.index(True)
                mine = jnp.logical_and(tap_row >= first, tap_row < first + sum(inside))
                parts.append(jnp.where(mine, 1.0, 0.0).astype(BF16))
            left.append(jnp.concatenate(parts, axis=0))
            right.append(taps[volume, :, at_y].reshape(DEPTH, LANES))
        total = lax.dot_general(
            jnp.concatenate(left, axis=1),
            jnp.concatenate(right, axis=1),
            (((1,), (1,)), ((), ())),
            preferred_element_type=F32,
        )

        def wide(pieces):
            height = pieces[0].shape[0]
            return jnp.concatenate(
                pieces + [jnp.zeros((height, 7 * LANES - FLAT), F32)], axis=1
            )

        def slab(row, height, at_x):
            return total[row : row + height, TAPS * at_x : TAPS * (at_x + 1)]

        blocks = []
        for index in range(len(buffers)):
            first = 6 * C * index
            pieces = []
            for tap_x in range(3):
                for tap_y in range(3):
                    row = first + 2 * C * tap_y
                    pieces.append(slab(row, C, tap_x) + slab(row + C, C, tap_x + 1))
            blocks.append(wide(pieces))
        if plain:
            first = 6 * C * len(buffers)
            alone = wide([
                slab(first + tap_y, 1, tap_x) + slab(first + tap_y, 1, tap_x + 1)
                for tap_x in range(3) for tap_y in range(3)
            ])
        for k in range(7):
            lanes = slice(LANES * k, LANES * (k + 1))
            for pair in range(16):
                spot = (pair // 4 * 8 + k) * 4 + pair % 4
                for index, block in enumerate(blocks):
                    out[spot, 2 * index : 2 * index + 2] = block[2 * pair : 2 * pair + 2, lanes]
                if plain:
                    last = 2 * len(blocks)
                    out[spot, last : last + 1] = alone[:, lanes]

    channel = lax.broadcasted_iota(jnp.int32, (C, LANES), 0)

    def pack(columns):
        whole = jnp.zeros((C, LANES), F32)
        for k, column in enumerate(columns):
            whole = whole + jnp.where(lane == channel + 32 * k, column, 0.0)
        return jnp.sum(whole, axis=0, keepdims=True)

    def unpack(row, number):
        return [
            jnp.sum(jnp.where(lane == channel + 32 * k, row, 0.0), axis=1, keepdims=True)
            for k in range(number)
        ]

    class Total:
        def __init__(self, index):
            self.slots, self.index = sums.at[index], index

        def start(self, row):
            mine = self.slots.at[flat]
            mine[...] = row

            fan_out(
                lambda to: mine, mine, sums_send.at[self.index], sums_recv.at[self.index]
            )

        def finish(self):
            fan_in(self.slots, sums_recv.at[self.index])
            return jnp.sum(self.slots[...], axis=0)

        def drain(self):
            fan_in(self.slots, sums_send.at[self.index])

    totals = [Total(index) for index in range(4)]

    small_lane = lax.broadcasted_iota(jnp.int32, (C, C), 1)
    small_row = lax.broadcasted_iota(jnp.int32, (C, C), 0)

    def column(row):
        return jnp.sum(jnp.where(small_lane == small_row, row[...], 0.0), axis=1, keepdims=True)

    for load in loads[5:]:
        load.wait()
    gain_1, bias_1, gain_2, bias_2 = (column(row) for row in (row_1, row_2, row_3, row_4))

    def stack_weights(source, forward, backward):
        tiles = [
            jnp.concatenate(
                [source[tap].astype(F32) for tap in range(4 * k, min(4 * k + 4, 27))]
                + ([jnp.zeros((C, C), F32)] if k == 6 else []),
                axis=1,
            )
            for k in range(7)
        ]
        turned = [tile.T for tile in tiles]
        empty = jnp.zeros((C, C), F32)
        ahead = [source[tap].astype(F32) for tap in range(27)]
        back = [turned[tap // 4][C * (tap % 4) : C * (tap % 4) + C] for tap in range(26, -1, -1)]
        for index, pieces in ((forward, ahead), (backward, back)):
            for tap_y in range(3):
                line = [
                    pieces[(tap_x * 3 + tap_y) * 3 + tap_z]
                    for tap_x in range(3) for tap_z in range(3)
                ]
                for at_x, row in ((0, line + [empty] * 3), (1, [empty] * 3 + line)):
                    first = (tap_y * SPAN_X + at_x) * C
                    for k in range(3):
                        weights[index, first : first + C, LANES * k : LANES * (k + 1)] = (
                            jnp.concatenate(row[4 * k : 4 * k + 4], axis=1).astype(BF16)
                        )

    zero = jnp.zeros((C, LANES), F32)
    none = jnp.zeros((C, LANES), BF16)

    def take(load, source, at, carry):
        load.wait()
        for at_x in range(SPAN_X):
            rows_x[at, at_x + 1, 1 : SPAN_Y + 1] = jnp.swapaxes(
                source[:, at_x].astype(F32), 0, 1
            ).astype(BF16)
        for at_x in range(SPAN_X):

            def step(block, carry, at_x=at_x):
                for k in range(8):
                    at_y = block * 8 + k
                    carry = extract(
                        rows_x[at, at_x + 1, at_y + 1],
                        32 * at + 16 * at_x + at_y,
                        carry,
                    )
                return carry

            carry = unrolled(0, 2, step, carry)
        return carry

    carry = (none, none)
    for at, source in enumerate((block_a, block_b, block_g)):
        carry = take(loads[at], source, at, carry)
    halo_x.put_edge(*carry, lane)

    pl.semaphore_wait(barrier, count - 1)

    near, rest = halo_x.small()
    waits_x = {volume: halo_x.faces_x(volume) for volume in (1, 0)}
    loads[3].wait()
    loads[4].wait()
    stack_weights(kernel_1, 0, 3)
    stack_weights(kernel_2, 1, 2)
    ok = [lane_keep(side) for side in range(2)]
    halo_x.arrive(near)
    for volume in (1, 0):
        for side in range(2):
            side_x[volume, side] = jnp.where(ok[side], halo_x.own(side, volume, lane), none)
        build_inner(
            taps_x, volume,
            lambda at_x, at_y, volume=volume: rows_x[volume, at_x + 1, at_y + 1],
            (side_x.at[volume, 0], side_x.at[volume, 1]),
        )
    halo_x.arrive(rest)
    for side in range(2):
        for volume in range(3):
            tile = halo_x.merged(side, volume, lane)
            side_x[volume, side] = jnp.where(ok[side], tile, none)

    def both_sums(total, squares):
        return [jnp.sum(total, axis=1, keepdims=True), jnp.sum(squares, axis=1, keepdims=True)]

    def moments(total, squares):
        mean = total / voxels
        scale = lax.rsqrt(squares / voxels - mean * mean + EPSILON)
        return mean, scale

    def first_layer(volume):
        halo_x.arrive(waits_x[volume])
        build_outer(
            taps_x, volume,
            lambda at_x, at_y: rows_x[volume, at_x, at_y],
            (side_x.at[volume, 0], side_x.at[volume, 1]),
        )

        def emit(at_x, at_y, tile, carry):
            total, squares, first, last = carry
            conv_1[volume, at_x, at_y] = tile
            rows_1[volume, at_x + 1, at_y + 1] = tile.astype(BF16)
            first, last = extract(tile, 16 * at_x + at_y, (first, last))
            return total + tile, squares + tile * tile, first, last

        total, squares, first, last = convolve(
            taps_x, volume, 0, emit, (zero, zero, none, none)
        )
        halo_1[volume].put_edge(first, last, lane)
        return both_sums(total, squares)

    def second_layer(volume, mean, scale, waits):
        halo = halo_1[volume]
        slope = jnp.broadcast_to(gain_1 * scale, (C, LANES))
        shift = jnp.broadcast_to(bias_1 - mean * gain_1 * scale, (C, LANES))
        norm_slope = jnp.broadcast_to(scale, (C, LANES))
        norm_shift = jnp.broadcast_to(-mean * scale, (C, LANES))

        def active(value):
            pre = value * slope + shift
            return pre * sigmoid(pre)

        def own_row(at_x, at_y):
            value = conv_1[volume, at_x, at_y]
            if volume == 1:
                norms[at_x, at_y + 2] = (value * norm_slope + norm_shift).astype(BF16)
            return active(value)

        for side in range(2):
            tile = halo.merged(side, 0, lane)
            side_1[volume, side] = tile
            side_h[volume, side] = jnp.where(
                ok[side], active(tile.astype(F32)), 0.0
            ).astype(BF16)
        sides = (side_h.at[volume, 0], side_h.at[volume, 1])
        build_inner(taps_h, volume, own_row, sides)
        halo.arrive(waits)
        build_outer(
            taps_h, volume,
            lambda at_x, at_y: active(rows_1[volume, at_x, at_y].astype(F32)),
            sides,
        )

        def emit(at_x, at_y, tile, carry):
            conv_2[volume, at_x, at_y] = tile
            total, squares, *columns = carry
            if volume == 1:
                rows_2[0, at_x + 1, at_y + 1] = tile.astype(BF16)
                columns = extract(tile, 16 * at_x + at_y, columns)
            return total + tile, squares + tile * tile, *columns

        start = (zero, zero) + ((none, none) if volume == 1 else ())
        total, squares, *columns = convolve(taps_h, volume, 1, emit, start)
        if volume == 1:
            halo_2.put_edge(*columns, lane)
        return both_sums(total, squares)

    sums_b = first_layer(1)
    totals[0].start(pack(sums_b))
    near, rest = halo_b.small()
    face_b = halo_b.faces_x(0)
    sums_a = first_layer(0)
    near_a, rest_a = halo_a.small()
    face_a = halo_a.faces_x(0)
    mean_1, scale_1 = moments(*unpack(totals[0].finish(), 2))
    halo_b.arrive(near + rest)
    waits_g = halo_x.faces_x(2)
    sums_b = second_layer(1, mean_1, scale_1, face_b)
    totals[1].start(pack(sums_b + sums_a))
    near, rest = halo_2.small()
    waits = near + rest + halo_2.faces_x(0)
    kernel_grad(taps_x, 1, [norms], early_out, True)
    fan_out(
        lambda to: early_out.at[to], early_in.at[flat], gw_send.at[0], gw_recv.at[0]
    )
    early_in[flat] = early_out[flat]
    stats = unpack(totals[1].finish(), 4)

    mean_2, scale_2 = moments(stats[0], stats[1])

    def layer_of(mean, scale, gain, bias):
        norm_slope = jnp.broadcast_to(scale, (C, LANES))
        norm_shift = jnp.broadcast_to(-mean * scale, (C, LANES))
        wide_gain = jnp.broadcast_to(gain, (C, LANES))
        wide_bias = jnp.broadcast_to(bias, (C, LANES))

        def slope_of(value, upstream):
            normed = value * norm_slope + norm_shift
            pre = wide_gain * normed + wide_bias
            sigma = sigmoid(pre)
            return upstream * (sigma * (1.0 + pre * (1.0 - sigma))), normed

        return slope_of

    def delta_of(slope_of, sum_d, sum_x, gain, scale):
        wide_d = jnp.broadcast_to(sum_d / voxels, (C, LANES))
        wide_x = jnp.broadcast_to(sum_x / voxels, (C, LANES))
        factor = jnp.broadcast_to(gain * scale, (C, LANES))

        def delta(value, upstream):
            slope, normed = slope_of(value, upstream)
            return factor * (slope - wide_d - normed * wide_x)

        return delta

    slope_2 = layer_of(mean_2, scale_2, gain_2, bias_2)

    def sum_rows(slope_of, value_of, upstream_of):
        carry = (zero, zero)
        for at_x in range(SPAN_X):

            def step(block, carry, at_x=at_x):
                total, weighted = carry
                for k in range(8):
                    at_y = block * 8 + k
                    slope, normed = slope_of(value_of(at_x, at_y), upstream_of(at_x, at_y))
                    slopes_2[at_x, at_y + 2] = slope.astype(BF16)
                    norms_2[at_x, at_y + 2] = normed.astype(BF16)
                    total, weighted = total + slope, weighted + slope * normed
                return total, weighted

            carry = unrolled(0, 2, step, carry)
        return [jnp.sum(part, axis=1, keepdims=True) for part in carry]

    columns = sum_rows(
        slope_2,
        lambda at_x, at_y: conv_2[1, at_x, at_y],
        lambda at_x, at_y: rows_x[2, at_x + 1, at_y + 1].astype(F32),
    )
    totals[2].start(pack(columns))

    kernel_grad(taps_h, 1, [slopes_2, norms_2], mid_out, True)
    fan_out(lambda to: mid_out.at[to], mid_in.at[flat], gw_send.at[1], gw_recv.at[1])
    mid_in[flat] = mid_out[flat]
    halo_a.arrive(near_a + rest_a)
    sums_a = second_layer(0, *moments(stats[2], stats[3]), face_a)
    halo_x.arrive(waits_g)
    halo_2.arrive(waits)
    sum_d2, sum_x2 = unpack(totals[2].finish(), 2)

    delta_2 = delta_of(slope_2, sum_d2, sum_x2, gain_2, scale_2)
    for side in range(2):
        tile = delta_2(
            halo_2.merged(side, 0, lane).astype(F32), side_x[2, side].astype(F32)
        )
        side_2[0, side] = jnp.where(ok[side], tile, 0.0).astype(BF16)
    build(
        taps_d2, 0,
        lambda at_x, at_y: delta_2(
            rows_2[0, at_x, at_y].astype(F32), rows_x[2, at_x, at_y].astype(F32)
        ),
        lambda at_x, at_y: delta_2(
            conv_2[1, at_x, at_y], rows_x[2, at_x + 1, at_y + 1].astype(F32)
        ),
        (side_2.at[0, 0], side_2.at[0, 1]),
    )
    slope_1 = layer_of(mean_1, scale_1, gain_1, bias_1)

    def emit(at_x, at_y, tile, carry):
        total, weighted, first, last = carry
        back_1[at_x, at_y] = tile
        rows_e[0, at_x + 1, at_y + 1] = tile.astype(BF16)
        first, last = extract(tile, 16 * at_x + at_y, (first, last))
        slope, normed = slope_1(conv_1[1, at_x, at_y], tile)
        slopes[at_x, at_y + 2] = slope.astype(BF16)
        return total + slope, weighted + slope * normed, first, last

    total, weighted, first, last = convolve(taps_d2, 0, 2, emit, (zero, zero, none, none))
    halo_e.put_edge(first, last, lane)
    columns = [
        jnp.sum(total, axis=1, keepdims=True), jnp.sum(weighted, axis=1, keepdims=True)
    ]
    totals[3].start(pack(columns + sums_a))
    near, rest = halo_e.small()
    kernel_grad(taps_x, 1, [slopes], late_out, False)
    fan_out(lambda to: late_out.at[to], late_in.at[flat], gw_send.at[2], gw_recv.at[2])
    waits = near + rest + halo_e.faces_x(0)
    late_in[flat] = late_out[flat]
    sum_d1, sum_x1, *sums_a = unpack(totals[3].finish(), 4)

    whole = 1.0 / math.sqrt(voxels)
    for k, factor in enumerate(
        (
            gain_1 * scale_1 * whole, sum_d1 / voxels, sum_x1 / voxels,
            gain_2 * scale_2 * whole, sum_d2 / voxels, sum_x2 / voxels,
        )
    ):
        tile = jnp.broadcast_to(factor, (C, LANES))
        for pair in range(16):
            pairs[k, pair] = tile[2 * pair : 2 * pair + 2]
    fan_in(early_in, gw_recv.at[0])
    early = jnp.sum(early_in[...], axis=0)
    fan_in(mid_in, gw_recv.at[1])
    mid = jnp.sum(mid_in[...], axis=0)
    at = flat // 32 * 4 + lax.rem(flat, 4)
    fan_in(late_in, gw_recv.at[2])
    late = jnp.sum(late_in[...], axis=0)
    gathered[flat, 0:2] = pairs[0, at] * (
        late[0:2] - pairs[1, at] * early[2:3] - pairs[2, at] * early[0:2]
    )
    gathered[flat, 2:4] = pairs[3, at] * (
        mid[0:2] - pairs[4, at] * mid[4:5] - pairs[5, at] * mid[2:4]
    )
    mine = gathered.at[flat]
    fan_out(lambda to: mine, mine, gw_send.at[3], gw_recv.at[3])

    halo_e.arrive(waits)
    delta_1 = delta_of(slope_1, sum_d1, sum_x1, gain_1, scale_1)
    for side in range(2):
        tile = delta_1(
            side_1[1, side].astype(F32), halo_e.merged(side, 0, lane).astype(F32)
        )
        side_e[0, side] = jnp.where(ok[side], tile, 0.0).astype(BF16)
    build(
        taps_d1, 0,
        lambda at_x, at_y: delta_1(
            rows_1[1, at_x, at_y].astype(F32), rows_e[0, at_x, at_y].astype(F32)
        ),
        lambda at_x, at_y: delta_1(conv_1[1, at_x, at_y], back_1[at_x, at_y]),
        (side_e.at[0, 0], side_e.at[0, 1]),
    )
    def emit(at_x, at_y, tile, carry):
        stage[at_x, at_y] = tile
        return carry

    convolve(taps_d1, 0, 3, emit, 0)
    for at_x in range(SPAN_X):
        dx_out[:, at_x] = jnp.swapaxes(stage[at_x], 0, 1).astype(BF16)

    mean_a, scale_a = moments(*sums_a)
    slope_a = jnp.broadcast_to(gain_2 * scale_a, (C, LANES))
    shift_a = jnp.broadcast_to(bias_2 - mean_a * gain_2 * scale_a, (C, LANES))
    for at_x in range(SPAN_X):

        def step(block, carry, at_x=at_x):
            for k in range(8):
                at_y = block * 8 + k
                pre = conv_2[0, at_x, at_y] * slope_a + shift_a
                stage[at_x, at_y] = pre * sigmoid(pre)
            return carry

        unrolled(0, 2, step, 0)
        y_out[:, at_x] = jnp.swapaxes(stage[at_x], 0, 1).astype(BF16)

    for k, total in enumerate((sum_x1, sum_d1, sum_x2, sum_d2)):
        norm_out[k : k + 1] = whole * jnp.sum(
            jnp.where(small_lane == small_row, total, 0.0), axis=0, keepdims=True
        )
    fan_in(gathered, gw_recv.at[3])
    for member, out in ((0, gw_first), (1, gw_second)):
        for k in range(7):
            tile = jnp.concatenate(
                [
                    gathered[(pair // 4 * 8 + k) * 4 + pair % 4, 2 * member : 2 * member + 2]
                    for pair in range(16)
                ],
                axis=0,
            )
            for tap in range(4 * k, min(4 * k + 4, 27)):
                out[tap] = tile[:, C * (tap % 4) : C * (tap % 4) + C]

    for halo in halos:
        halo.drain()
    for total in totals:
        total.drain()
    for k, chunks in enumerate((early_out, mid_out, late_out, gathered)):
        fan_in(chunks, gw_send.at[k])


def write_out(*refs):
    sources, targets, semaphores = refs[:5], refs[5:10], refs[10]
    copies = [
        pltpu.make_async_copy(source, target, semaphores.at[index])
        for index, (source, target) in enumerate(zip(sources, targets))
    ]
    for copy in copies:
        copy.start()
    for copy in copies:
        copy.wait()


def body(voxels, x_a, x_b, w_first, w_second, gain_first, bias_first, gain_second, bias_second,
         grad_out):
    def sized(*shape, kind=BF16):
        return pltpu.VMEM(shape, kind)

    volumes = (3, 2, 1, 1)
    devices = math.prod(lax.axis_size(axis) for axis in AXES)
    block = (C, SPAN_X, SPAN_Y, LANES)
    scratch = [sized(*block)] * 3 + [sized(27, C, C)] * 2 + [sized(1, C, kind=F32)] * 4
    scratch += [
        sized(4, HEIGHT, DEPTH), sized(SPAN_X, SPAN_Y, C, LANES, kind=F32)
    ]
    scratch += [sized(count, PAD_X, PAD_Y, TAPS, LANES) for count in (2, 2, 1, 1)]
    scratch += [sized(count, PAD_X, PAD_Y, C, LANES) for count in volumes]
    heights = [C if count == 3 else C // 2 for count in volumes]
    pairs = [(2,) if count == 2 else () for count in volumes]
    scratch += [
        sized(*pair, 2, 3, 3, height, LANES) for pair, height in zip(pairs, heights)
    ]
    scratch += [sized(*pair, 2, height, LANES) for pair, height in zip(pairs, heights)]
    scratch += [sized(count, 2, C, LANES) for count in volumes] + [sized(2, 2, C, LANES)]
    scratch += [
        sized(2, SPAN_X, SPAN_Y, C, LANES, kind=F32),
        sized(2, SPAN_X, SPAN_Y, C, LANES, kind=F32),
        sized(SPAN_X, SPAN_Y, C, LANES, kind=F32),
        sized(4, devices, 1, LANES, kind=F32),
        *[sized(SPAN_X, SPAN_Y + 4, C, LANES)] * 4,
        *[sized(devices, 3, LANES, kind=F32)] * 2,
        *[sized(devices, 5, LANES, kind=F32)] * 2,
        *[sized(devices, 2, LANES, kind=F32)] * 2,
        sized(devices, 4, LANES, kind=F32),
        sized(6, 16, 2, LANES, kind=F32),
        pltpu.SemaphoreType.DMA((5, 32)),
        pltpu.SemaphoreType.DMA((5, 32)),
        pltpu.SemaphoreType.DMA((4,)),
        pltpu.SemaphoreType.DMA((4,)),
        pltpu.SemaphoreType.DMA((4,)),
        pltpu.SemaphoreType.DMA((4,)),
        pltpu.SemaphoreType.DMA((9,)),
    ]
    in_vmem = pl.BlockSpec(memory_space=pltpu.VMEM)
    in_hbm = pl.BlockSpec(memory_space=pltpu.HBM)
    taps = jax.ShapeDtypeStruct((27, C, C), F32)
    out_shape = (
        jax.ShapeDtypeStruct(block, BF16),
        jax.ShapeDtypeStruct(block, BF16),
        taps,
        taps,
        jax.ShapeDtypeStruct((4, C), F32),
    )
    results = pl.pallas_call(
        functools.partial(kernel, voxels),
        out_shape=out_shape,
        in_specs=[in_hbm] * 9,
        out_specs=(in_vmem,) * 5,
        scratch_shapes=scratch,
        compiler_params=pltpu.CompilerParams(
            collective_id=0, has_side_effects=True, vmem_limit_bytes=28 * 1024 * 1024
        ),
    )(
        *(pltpu.with_memory_space_constraint(value, pltpu.HBM) for value in (
            x_a, x_b, grad_out, w_first.reshape(27, C, C), w_second.reshape(27, C, C),
            *(row.reshape(1, C) for row in (gain_first, bias_first, gain_second, bias_second)),
        )),
    )
    y_a, dx_b, grad_first, grad_second, norms = pl.pallas_call(
        write_out,
        out_shape=out_shape,
        in_specs=[in_vmem] * 5,
        out_specs=(in_hbm,) * 5,
        scratch_shapes=[pltpu.SemaphoreType.DMA((5,))],
        compiler_params=pltpu.CompilerParams(vmem_limit_bytes=8 * 1024 * 1024),
    )(*results)
    return (
        y_a, dx_b, grad_first.reshape(3, 3, 3, C, C), grad_second.reshape(3, 3, 3, C, C), norms
    )


def solution(mesh):
    split = P(None, "gx", "gy", "gz")
    voxels = float(SPAN_X * SPAN_Y * LANES * mesh.size)
    return jax.shard_map(
        functools.partial(body, voxels),
        mesh=mesh,
        in_specs=(split, split, P(), P(), P(), P(), P(), P(), split),
        out_specs=(split, split, P(), P(), P()),
        check_vma=False,
    )
```

```python
import functools
import math

import jax
import jax.numpy as jnp
from jax import lax
from jax.experimental import pallas as pl
from jax.experimental.pallas import tpu as pltpu
from jax.sharding import PartitionSpec as P

F32 = jnp.float32
BF16 = jnp.bfloat16
EPSILON = 1e-05
C = 32
LANES = 128
SPAN_X, SPAN_Y = 2, 16
PAD_X, PAD_Y = SPAN_X + 2, SPAN_Y + 2
TAPS = 3 * C
DEPTH = PAD_X * TAPS
HEIGHT = 3 * SPAN_X * C
FLAT = 9 * TAPS
GROUP = 2
INNER = 16
OUTER = 18
AXES = ("gx", "gy", "gz")
MESH = pl.DeviceIdType.MESH


def sigmoid(value):
    return 0.5 + 0.5 * jnp.tanh(0.5 * value)


def unrolled(first, last, step, carry):
    for index in range(first, last):
        carry = step(index, carry)
    return carry


def rolled(tile, shift):
    shift = shift % LANES
    return pltpu.roll(tile, shift, 1) if shift else tile


class Halo:
    def __init__(self, rows, cols, edge, side, send, recv, place, volumes):
        self.rows, self.cols, self.edge, self.side = rows, cols, edge, side
        self.send, self.recv, self.place, self.volumes = send, recv, place, volumes
        self.count = 0
        self.sent = []

    def has(self, steps):
        present = None
        for axis, step in zip(AXES, steps):
            if step:
                me, size = self.place[axis]
                inside = me > 0 if step < 0 else me < size - 1
                present = inside if present is None else jnp.logical_and(present, inside)
        return present

    def push(self, source, target, *steps):
        index = self.count
        self.count += 1
        to = {}
        for axis, step in zip(AXES, steps):
            if step:
                me, size = self.place[axis]
                to[axis] = lax.rem(me + step + size, size)
        copy = pltpu.make_async_remote_copy(
            src_ref=source,
            dst_ref=target,
            send_sem=self.send.at[index],
            recv_sem=self.recv.at[index],
            device_id=to,
            device_id_type=MESH,
        )
        present = self.has(steps)

        @pl.when(present)
        def _():
            copy.start()

        self.sent.append((copy, present))
        return copy, self.has([-step for step in steps])

    def faces_x(self, volume):
        rows, inner = self.rows, pl.ds(1, SPAN_Y)
        return [
            self.push(
                rows.at[volume, 1 if step < 0 else SPAN_X, inner],
                rows.at[volume, PAD_X - 1 if step < 0 else 0, inner],
                step, 0, 0,
            )
            for step in (-1, 1)
        ]

    def columns(self, step_x, step_y):
        return [
            self.push(
                self.edge.at[0 if step < 0 else 1],
                self.cols.at[1 if step < 0 else 0, 1 - step_x, 1 - step_y],
                step_x, step_y, step,
            )
            for step in (-1, 1)
        ]

    def small(self):
        rows, every = self.rows, pl.ds(0, self.volumes)
        near = self.columns(0, 0)
        rest = []
        for step_x in (-1, 0, 1):
            at_x = (1 if step_x < 0 else SPAN_X) if step_x else pl.ds(1, SPAN_X)
            to_x = (PAD_X - 1 if step_x < 0 else 0) if step_x else pl.ds(1, SPAN_X)
            for step_y in (-1, 1):
                rest.append(
                    self.push(
                        rows.at[every, at_x, 1 if step_y < 0 else SPAN_Y],
                        rows.at[every, to_x, PAD_Y - 1 if step_y < 0 else 0],
                        step_x, step_y, 0,
                    )
                )
        for step_x, step_y in (
            (-1, -1), (-1, 1), (1, -1), (1, 1), (-1, 0), (1, 0), (0, -1), (0, 1)
        ):
            rest += self.columns(step_x, step_y)
        return near, rest

    def put_edge(self, first, last, lane):
        for index, tile in enumerate((first, last)):
            if self.volumes < 3:
                tile = jnp.where(lane[:16] < 64, tile[:16], pltpu.roll(tile[16:], 64, 1))
            self.edge[index] = tile

    def tile(self, side, index_x, index_y):
        tile = self.cols[side, index_x, index_y]
        if self.volumes < 3:
            tile = jnp.concatenate([tile, pltpu.roll(tile, 64, 1)], axis=0)
        return tile

    def own(self, side, volume, lane):
        tile = self.tile(side, 1, 1)
        at = 32 * volume
        return jnp.where(lane < 64, rolled(tile, 33 - at), rolled(tile, 49 - at))

    def merged(self, side, volume, lane):
        at = 32 * volume
        inside = lax.rem(lane, 32)

        def strip(index, low, middle, high):
            low, middle, high = (
                rolled(self.tile(side, index, k), shift - at)
                for k, shift in enumerate((low, middle, high))
            )
            return jnp.where(inside == 0, low, jnp.where(inside == PAD_Y - 1, high, middle))

        return jnp.where(
            lane < 64,
            jnp.where(lane < 32, strip(0, -31, -15, 1), strip(1, 17, 33, 49)),
            jnp.where(lane < 96, strip(1, 33, 49, 65), strip(2, 81, 97, 113)),
        )

    @staticmethod
    def arrive(pushes):
        for copy, present in pushes:

            @pl.when(present)
            def _(copy=copy):
                copy.wait_recv()

    def drain(self):
        for copy, present in self.sent:

            @pl.when(present)
            def _(copy=copy):
                copy.wait_send()


def kernel(
    voxels,
    x_a, x_b, grad, w_first, w_second, gain_first, bias_first, gain_second, bias_second,
    y_out, dx_out, gw_first, gw_second, norm_out,
    block_a, block_b, block_g, kernel_1, kernel_2, row_1, row_2, row_3, row_4, weights, stage,
    taps_x, taps_h, taps_d2, taps_d1,
    rows_x, rows_1, rows_2, rows_e,
    cols_x, cols_1, cols_2, cols_e,
    edge_x, edge_1, edge_2, edge_e,
    side_x, side_1, side_2, side_e,
    side_h,
    conv_1, conv_2, back_1,
    sums,
    norms, slopes, norms_2, slopes_2,
    early_out, early_in, mid_out, mid_in, late_out, late_in, gathered, pairs,
    halo_send, halo_recv, sums_send, sums_recv, gw_send, gw_recv, local,
):
    loads = [
        pltpu.make_async_copy(source, target, local.at[index])
        for index, (source, target) in enumerate((
            (x_a, block_a), (x_b, block_b), (grad, block_g), (w_first, kernel_1),
            (w_second, kernel_2), (gain_first, row_1), (bias_first, row_2), (gain_second, row_3),
            (bias_second, row_4),
        ))
    ]
    for load in loads:
        load.start()
    place = {axis: (lax.axis_index(axis), lax.axis_size(axis)) for axis in AXES}
    for chunks in (early_out, mid_out, late_out):
        for j in range(4):
            at = slice(32 * j + 28, 32 * j + 32)
            chunks[at] = jnp.zeros((4, chunks.shape[1], LANES), F32)
    for rows in (norms, slopes, norms_2, slopes_2):
        for at in (0, SPAN_Y + 2):
            rows[:, at : at + 2] = jnp.zeros((SPAN_X, 2, C, LANES), BF16)
    barrier = pltpu.get_barrier_semaphore()
    count = place["gx"][1] * place["gy"][1] * place["gz"][1]
    flat = (place["gx"][0] * place["gy"][1] + place["gy"][0]) * place["gz"][1] + place["gz"][0]

    chip_x, chip_y = place["gy"][0], place["gz"][0] // 2
    chip_z = place["gx"][0] // 2 * 2 + lax.rem(place["gz"][0], 2)
    core = lax.rem(place["gx"][0], 2)

    def other(step):
        return lax.rem(flat + step, count)

    def fan_out(source_of, target, send, recv):
        spots = []
        for step_z, step_core in ((2, 1), (2, 0), (1, 1), (3, 1), (1, 0), (3, 0), (0, 1), (0, 0)):
            to_z, to_core = lax.rem(chip_z + step_z, 4), lax.rem(core + step_core, 2)
            spots.append(to_z // 2 * 64 + to_core * 32 + lax.rem(to_z, 2))

        def copies(plane, chosen):
            to_x = lax.rem(chip_x + plane // 4 + 1, 4)
            to_y = lax.rem(chip_y + lax.rem(plane, 4) + 1, 4)
            for spot in chosen:
                to = spot + to_x * 8 + to_y * 2
                pltpu.make_async_remote_copy(
                    src_ref=source_of(to), dst_ref=target, send_sem=send, recv_sem=recv,
                    device_id=to, device_id_type=pl.DeviceIdType.LOGICAL,
                ).start()

        def most(block, carry):
            for k in range(8):
                copies(block * 8 + k, spots[:-1])
            return carry

        def rest(block, carry):
            for k in range(15):
                copies(block * 15 + k, spots[-1:])
            return carry

        lax.fori_loop(0, 2, most, 0)
        rest(0, 0)

    def fan_in(slots, semaphore):
        part = slots.at[pl.ds(0, count - 1)]
        pltpu.make_async_copy(part, part, semaphore).wait()

    def greet(step, carry):
        pl.semaphore_signal(
            barrier, inc=1, device_id=other(step), device_id_type=pl.DeviceIdType.LOGICAL
        )
        return carry

    lax.fori_loop(1, count, greet, 0)

    lane = lax.broadcasted_iota(jnp.int32, (C, LANES), 1)
    halos = []
    def lone(refs, volume):
        return refs.at[pl.ds(volume, 1)]

    for index, (rows, cols, edge, side, volumes) in enumerate((
        (rows_x, cols_x, edge_x, side_x, 3),
        (lone(rows_1, 0), cols_1.at[0], edge_1.at[0], lone(side_1, 0), 1),
        (lone(rows_1, 1), cols_1.at[1], edge_1.at[1], lone(side_1, 1), 1),
        (rows_2, cols_2, edge_2, side_2, 1),
        (rows_e, cols_e, edge_e, side_e, 1),
    )):
        halos.append(
            Halo(rows, cols, edge, side, halo_send.at[index], halo_recv.at[index], place, volumes)
        )
    halo_x, halo_a, halo_b, halo_2, halo_e = halos
    halo_1 = (halo_a, halo_b)

    low_x, high_x = place["gx"][0] > 0, place["gx"][0] < place["gx"][1] - 1
    low_y, high_y = place["gy"][0] > 0, place["gy"][0] < place["gy"][1] - 1
    low_z, high_z = place["gz"][0] > 0, place["gz"][0] < place["gz"][1] - 1

    def keep(at_x, at_y):
        held_x = low_x if at_x == 0 else high_x if at_x == PAD_X - 1 else None
        if isinstance(at_y, int):
            held_y = low_y if at_y == 0 else high_y if at_y == PAD_Y - 1 else None
        else:
            held_y = jnp.logical_and(
                jnp.logical_or(at_y > 0, low_y), jnp.logical_or(at_y < PAD_Y - 1, high_y)
            )
        if held_x is None:
            return held_y
        return held_x if held_y is None else jnp.logical_and(held_x, held_y)

    def lane_keep(side):
        spot_x, spot_y = lane // 32, lax.rem(lane, 32)
        bad = jnp.zeros((C, LANES), jnp.int32)
        for hit, present in (
            (spot_x == 0, low_x), (spot_x == PAD_X - 1, high_x),
            (spot_y == 0, low_y), (spot_y == PAD_Y - 1, high_y),
        ):
            missing = jnp.where(present, 0, 1)
            bad = bad + jnp.where(hit, missing, 0)
        bad = bad + jnp.where(low_z if side == 0 else high_z, 0, 1)
        return bad == 0

    def extract(tile, spot, carry):
        first, last = carry
        tile = tile.astype(BF16)
        first = jnp.where(lane == spot, pltpu.roll(tile, spot, 1), first)
        last = jnp.where(lane == spot, pltpu.roll(tile, lax.rem(spot + 1, LANES), 1), last)
        return first, last

    def put_taps(taps, volume, spots, tiles, sides):
        low, high = sides[0][...], sides[1][...]
        shifted = []
        for (at_x, at_y), tile in zip(spots, tiles):
            spot = at_x * 32 + at_y
            left = jnp.where(
                lane == 0,
                pltpu.roll(low, lax.rem(LANES - spot, LANES), 1),
                pltpu.roll(tile, 1, 1),
            )
            right = jnp.where(
                lane == LANES - 1,
                pltpu.roll(high, LANES - 1 - spot, 1),
                pltpu.roll(tile, LANES - 1, 1),
            )
            shifted.append((left, tile, right))
        for (at_x, at_y), rows in zip(spots, shifted):
            for k, row in enumerate(rows):
                taps[volume, at_x, at_y, k * C : (k + 1) * C] = row

    def build_inner(taps, volume, inner, sides):
        for at_x in range(SPAN_X):

            def step(block, carry, at_x=at_x):
                rows = [block * INNER + k for k in range(INNER)]
                tiles = [inner(at_x, at_y).astype(BF16) for at_y in rows]
                put_taps(taps, volume, [(at_x + 1, at_y + 1) for at_y in rows], tiles, sides)
                return carry

            unrolled(0, SPAN_Y // INNER, step, 0)

    def build_outer(taps, volume, outer, sides):
        def put(spots):
            tiles = [
                jnp.where(keep(at_x, at_y), outer(at_x, at_y).astype(BF16), none)
                for at_x, at_y in spots
            ]
            put_taps(taps, volume, spots, tiles, sides)

        put([(at_x, at_y) for at_x in (1, 2) for at_y in (0, PAD_Y - 1)])
        for at_x in (0, PAD_X - 1):

            def step(block, carry, at_x=at_x):
                put([(at_x, block * OUTER + k) for k in range(OUTER)])
                return carry

            unrolled(0, PAD_Y // OUTER, step, 0)

    def build(taps, volume, outer, inner, sides):
        build_inner(taps, volume, inner, sides)
        build_outer(taps, volume, outer, sides)

    def convolve(taps, volume, weight, emit, carry):
        parts = {}
        for block in range(PAD_Y // GROUP):
            columns = [
                taps[volume, :, block * GROUP + k].reshape(DEPTH, LANES) for k in range(GROUP)
            ]
            total = jnp.dot(
                weights[weight], jnp.concatenate(columns, axis=1), preferred_element_type=F32
            )
            for k in range(GROUP):
                parts[block * GROUP + k] = total[:, k * LANES : (k + 1) * LANES]
            for at_y in range((block - 1) * GROUP, block * GROUP):
                if at_y < 0 or at_y + 2 not in parts:
                    continue
                for at_x in range(SPAN_X):
                    low = at_x * C
                    tile = parts[at_y][low : low + C]
                    for tap in (1, 2):
                        first = tap * SPAN_X * C + low
                        tile = tile + parts[at_y + tap][first : first + C]
                    carry = emit(at_x, at_y, tile, carry)
        return carry

    def kernel_grad(taps, volume, buffers, out, plain):
        tap_row = lax.broadcasted_iota(jnp.int32, (16, LANES), 0)
        left, right = [], []
        for at_y in range(PAD_Y):
            parts = [
                rows[at_x, at_y - tap + 2]
                for rows in buffers for tap in range(3) for at_x in range(SPAN_X)
            ]
            if plain:
                inside = [0 <= at_y - tap < SPAN_Y for tap in range(3)]
                first = inside.index(True)
                mine = jnp.logical_and(tap_row >= first, tap_row < first + sum(inside))
                parts.append(jnp.where(mine, 1.0, 0.0).astype(BF16))
            left.append(jnp.concatenate(parts, axis=0))
            right.append(taps[volume, :, at_y].reshape(DEPTH, LANES))
        total = lax.dot_general(
            jnp.concatenate(left, axis=1),
            jnp.concatenate(right, axis=1),
            (((1,), (1,)), ((), ())),
            preferred_element_type=F32,
        )

        def wide(pieces):
            height = pieces[0].shape[0]
            return jnp.concatenate(
                pieces + [jnp.zeros((height, 7 * LANES - FLAT), F32)], axis=1
            )

        def slab(row, height, at_x):
            return total[row : row + height, TAPS * at_x : TAPS * (at_x + 1)]

        blocks = []
        for index in range(len(buffers)):
            first = 6 * C * index
            pieces = []
            for tap_x in range(3):
                for tap_y in range(3):
                    row = first + 2 * C * tap_y
                    pieces.append(slab(row, C, tap_x) + slab(row + C, C, tap_x + 1))
            blocks.append(wide(pieces))
        if plain:
            first = 6 * C * len(buffers)
            alone = wide([
                slab(first + tap_y, 1, tap_x) + slab(first + tap_y, 1, tap_x + 1)
                for tap_x in range(3) for tap_y in range(3)
            ])
        for k in range(7):
            lanes = slice(LANES * k, LANES * (k + 1))
            for pair in range(16):
                spot = (pair // 4 * 8 + k) * 4 + pair % 4
                for index, block in enumerate(blocks):
                    out[spot, 2 * index : 2 * index + 2] = block[2 * pair : 2 * pair + 2, lanes]
                if plain:
                    last = 2 * len(blocks)
                    out[spot, last : last + 1] = alone[:, lanes]

    channel = lax.broadcasted_iota(jnp.int32, (C, LANES), 0)

    def pack(columns):
        whole = jnp.zeros((C, LANES), F32)
        for k, column in enumerate(columns):
            whole = whole + jnp.where(lane == channel + 32 * k, column, 0.0)
        return jnp.sum(whole, axis=0, keepdims=True)

    def unpack(row, number):
        return [
            jnp.sum(jnp.where(lane == channel + 32 * k, row, 0.0), axis=1, keepdims=True)
            for k in range(number)
        ]

    class Total:
        def __init__(self, index):
            self.slots, self.index = sums.at[index], index

        def start(self, row):
            mine = self.slots.at[flat]
            mine[...] = row

            fan_out(
                lambda to: mine, mine, sums_send.at[self.index], sums_recv.at[self.index]
            )

        def finish(self):
            fan_in(self.slots, sums_recv.at[self.index])
            return jnp.sum(self.slots[...], axis=0)

        def drain(self):
            fan_in(self.slots, sums_send.at[self.index])

    totals = [Total(index) for index in range(4)]

    small_lane = lax.broadcasted_iota(jnp.int32, (C, C), 1)
    small_row = lax.broadcasted_iota(jnp.int32, (C, C), 0)

    def column(row):
        return jnp.sum(jnp.where(small_lane == small_row, row[...], 0.0), axis=1, keepdims=True)

    for load in loads[5:]:
        load.wait()
    gain_1, bias_1, gain_2, bias_2 = (column(row) for row in (row_1, row_2, row_3, row_4))

    def stack_weights(source, forward, backward):
        tiles = [
            jnp.concatenate(
                [source[tap].astype(F32) for tap in range(4 * k, min(4 * k + 4, 27))]
                + ([jnp.zeros((C, C), F32)] if k == 6 else []),
                axis=1,
            )
            for k in range(7)
        ]
        turned = [tile.T for tile in tiles]
        empty = jnp.zeros((C, C), F32)
        ahead = [source[tap].astype(F32) for tap in range(27)]
        back = [turned[tap // 4][C * (tap % 4) : C * (tap % 4) + C] for tap in range(26, -1, -1)]
        for index, pieces in ((forward, ahead), (backward, back)):
            for tap_y in range(3):
                line = [
                    pieces[(tap_x * 3 + tap_y) * 3 + tap_z]
                    for tap_x in range(3) for tap_z in range(3)
                ]
                for at_x, row in ((0, line + [empty] * 3), (1, [empty] * 3 + line)):
                    first = (tap_y * SPAN_X + at_x) * C
                    for k in range(3):
                        weights[index, first : first + C, LANES * k : LANES * (k + 1)] = (
                            jnp.concatenate(row[4 * k : 4 * k + 4], axis=1).astype(BF16)
                        )

    zero = jnp.zeros((C, LANES), F32)
    none = jnp.zeros((C, LANES), BF16)

    def take(load, source, at, carry):
        load.wait()
        for at_x in range(SPAN_X):
            rows_x[at, at_x + 1, 1 : SPAN_Y + 1] = jnp.swapaxes(
                source[:, at_x].astype(F32), 0, 1
            ).astype(BF16)
        for at_x in range(SPAN_X):

            def step(block, carry, at_x=at_x):
                for k in range(8):
                    at_y = block * 8 + k
                    carry = extract(
                        rows_x[at, at_x + 1, at_y + 1],
                        32 * at + 16 * at_x + at_y,
                        carry,
                    )
                return carry

            carry = unrolled(0, 2, step, carry)
        return carry

    carry = (none, none)
    for at, source in enumerate((block_a, block_b, block_g)):
        carry = take(loads[at], source, at, carry)
    halo_x.put_edge(*carry, lane)

    pl.semaphore_wait(barrier, count - 1)

    near, rest = halo_x.small()
    waits_x = {volume: halo_x.faces_x(volume) for volume in (1, 0)}
    loads[3].wait()
    loads[4].wait()
    stack_weights(kernel_1, 0, 3)
    stack_weights(kernel_2, 1, 2)
    ok = [lane_keep(side) for side in range(2)]
    halo_x.arrive(near)
    for volume in (1, 0):
        for side in range(2):
            side_x[volume, side] = jnp.where(ok[side], halo_x.own(side, volume, lane), none)
        build_inner(
            taps_x, volume,
            lambda at_x, at_y, volume=volume: rows_x[volume, at_x + 1, at_y + 1],
            (side_x.at[volume, 0], side_x.at[volume, 1]),
        )
    halo_x.arrive(rest)
    for side in range(2):
        for volume in range(3):
            tile = halo_x.merged(side, volume, lane)
            side_x[volume, side] = jnp.where(ok[side], tile, none)

    def both_sums(total, squares):
        return [jnp.sum(total, axis=1, keepdims=True), jnp.sum(squares, axis=1, keepdims=True)]

    def moments(total, squares):
        mean = total / voxels
        scale = lax.rsqrt(squares / voxels - mean * mean + EPSILON)
        return mean, scale

    def first_layer(volume):
        halo_x.arrive(waits_x[volume])
        build_outer(
            taps_x, volume,
            lambda at_x, at_y: rows_x[volume, at_x, at_y],
            (side_x.at[volume, 0], side_x.at[volume, 1]),
        )

        def emit(at_x, at_y, tile, carry):
            total, squares, first, last = carry
            conv_1[volume, at_x, at_y] = tile
            rows_1[volume, at_x + 1, at_y + 1] = tile.astype(BF16)
            first, last = extract(tile, 16 * at_x + at_y, (first, last))
            return total + tile, squares + tile * tile, first, last

        total, squares, first, last = convolve(
            taps_x, volume, 0, emit, (zero, zero, none, none)
        )
        halo_1[volume].put_edge(first, last, lane)
        return both_sums(total, squares)

    def second_layer(volume, mean, scale, waits):
        halo = halo_1[volume]
        slope = jnp.broadcast_to(gain_1 * scale, (C, LANES))
        shift = jnp.broadcast_to(bias_1 - mean * gain_1 * scale, (C, LANES))
        norm_slope = jnp.broadcast_to(scale, (C, LANES))
        norm_shift = jnp.broadcast_to(-mean * scale, (C, LANES))

        def active(value):
            pre = value * slope + shift
            return pre * sigmoid(pre)

        def own_row(at_x, at_y):
            value = conv_1[volume, at_x, at_y]
            if volume == 1:
                norms[at_x, at_y + 2] = (value * norm_slope + norm_shift).astype(BF16)
            return active(value)

        for side in range(2):
            tile = halo.merged(side, 0, lane)
            side_1[volume, side] = tile
            side_h[volume, side] = jnp.where(
                ok[side], active(tile.astype(F32)), 0.0
            ).astype(BF16)
        sides = (side_h.at[volume, 0], side_h.at[volume, 1])
        build_inner(taps_h, volume, own_row, sides)
        halo.arrive(waits)
        build_outer(
            taps_h, volume,
            lambda at_x, at_y: active(rows_1[volume, at_x, at_y].astype(F32)),
            sides,
        )

        def emit(at_x, at_y, tile, carry):
            conv_2[volume, at_x, at_y] = tile
            total, squares, *columns = carry
            if volume == 1:
                rows_2[0, at_x + 1, at_y + 1] = tile.astype(BF16)
                columns = extract(tile, 16 * at_x + at_y, columns)
            return total + tile, squares + tile * tile, *columns

        start = (zero, zero) + ((none, none) if volume == 1 else ())
        total, squares, *columns = convolve(taps_h, volume, 1, emit, start)
        if volume == 1:
            halo_2.put_edge(*columns, lane)
        return both_sums(total, squares)

    sums_b = first_layer(1)
    totals[0].start(pack(sums_b))
    near, rest = halo_b.small()
    face_b = halo_b.faces_x(0)
    sums_a = first_layer(0)
    near_a, rest_a = halo_a.small()
    face_a = halo_a.faces_x(0)
    mean_1, scale_1 = moments(*unpack(totals[0].finish(), 2))
    halo_b.arrive(near + rest)
    waits_g = halo_x.faces_x(2)
    sums_b = second_layer(1, mean_1, scale_1, face_b)
    totals[1].start(pack(sums_b + sums_a))
    near, rest = halo_2.small()
    waits = near + rest + halo_2.faces_x(0)
    kernel_grad(taps_x, 1, [norms], early_out, True)
    fan_out(
        lambda to: early_out.at[to], early_in.at[flat], gw_send.at[0], gw_recv.at[0]
    )
    early_in[flat] = early_out[flat]
    stats = unpack(totals[1].finish(), 4)

    mean_2, scale_2 = moments(stats[0], stats[1])

    def layer_of(mean, scale, gain, bias):
        norm_slope = jnp.broadcast_to(scale, (C, LANES))
        norm_shift = jnp.broadcast_to(-mean * scale, (C, LANES))
        wide_gain = jnp.broadcast_to(gain, (C, LANES))
        wide_bias = jnp.broadcast_to(bias, (C, LANES))

        def slope_of(value, upstream):
            normed = value * norm_slope + norm_shift
            pre = wide_gain * normed + wide_bias
            sigma = sigmoid(pre)
            return upstream * (sigma * (1.0 + pre * (1.0 - sigma))), normed

        return slope_of

    def delta_of(slope_of, sum_d, sum_x, gain, scale):
        wide_d = jnp.broadcast_to(sum_d / voxels, (C, LANES))
        wide_x = jnp.broadcast_to(sum_x / voxels, (C, LANES))
        factor = jnp.broadcast_to(gain * scale, (C, LANES))

        def delta(value, upstream):
            slope, normed = slope_of(value, upstream)
            return factor * (slope - wide_d - normed * wide_x)

        return delta

    slope_2 = layer_of(mean_2, scale_2, gain_2, bias_2)

    def sum_rows(slope_of, value_of, upstream_of):
        carry = (zero, zero)
        for at_x in range(SPAN_X):

            def step(block, carry, at_x=at_x):
                total, weighted = carry
                for k in range(8):
                    at_y = block * 8 + k
                    slope, normed = slope_of(value_of(at_x, at_y), upstream_of(at_x, at_y))
                    slopes_2[at_x, at_y + 2] = slope.astype(BF16)
                    norms_2[at_x, at_y + 2] = normed.astype(BF16)
                    total, weighted = total + slope, weighted + slope * normed
                return total, weighted

            carry = unrolled(0, 2, step, carry)
        return [jnp.sum(part, axis=1, keepdims=True) for part in carry]

    columns = sum_rows(
        slope_2,
        lambda at_x, at_y: conv_2[1, at_x, at_y],
        lambda at_x, at_y: rows_x[2, at_x + 1, at_y + 1].astype(F32),
    )
    totals[2].start(pack(columns))

    kernel_grad(taps_h, 1, [slopes_2, norms_2], mid_out, True)
    fan_out(lambda to: mid_out.at[to], mid_in.at[flat], gw_send.at[1], gw_recv.at[1])
    mid_in[flat] = mid_out[flat]
    halo_a.arrive(near_a + rest_a)
    sums_a = second_layer(0, *moments(stats[2], stats[3]), face_a)
    halo_x.arrive(waits_g)
    halo_2.arrive(waits)
    sum_d2, sum_x2 = unpack(totals[2].finish(), 2)

    delta_2 = delta_of(slope_2, sum_d2, sum_x2, gain_2, scale_2)
    for side in range(2):
        tile = delta_2(
            halo_2.merged(side, 0, lane).astype(F32), side_x[2, side].astype(F32)
        )
        side_2[0, side] = jnp.where(ok[side], tile, 0.0).astype(BF16)
    build(
        taps_d2, 0,
        lambda at_x, at_y: delta_2(
            rows_2[0, at_x, at_y].astype(F32), rows_x[2, at_x, at_y].astype(F32)
        ),
        lambda at_x, at_y: delta_2(
            conv_2[1, at_x, at_y], rows_x[2, at_x + 1, at_y + 1].astype(F32)
        ),
        (side_2.at[0, 0], side_2.at[0, 1]),
    )
    slope_1 = layer_of(mean_1, scale_1, gain_1, bias_1)

    def emit(at_x, at_y, tile, carry):
        total, weighted, first, last = carry
        back_1[at_x, at_y] = tile
        rows_e[0, at_x + 1, at_y + 1] = tile.astype(BF16)
        first, last = extract(tile, 16 * at_x + at_y, (first, last))
        slope, normed = slope_1(conv_1[1, at_x, at_y], tile)
        slopes[at_x, at_y + 2] = slope.astype(BF16)
        return total + slope, weighted + slope * normed, first, last

    total, weighted, first, last = convolve(taps_d2, 0, 2, emit, (zero, zero, none, none))
    halo_e.put_edge(first, last, lane)
    columns = [
        jnp.sum(total, axis=1, keepdims=True), jnp.sum(weighted, axis=1, keepdims=True)
    ]
    totals[3].start(pack(columns + sums_a))
    near, rest = halo_e.small()
    kernel_grad(taps_x, 1, [slopes], late_out, False)
    fan_out(lambda to: late_out.at[to], late_in.at[flat], gw_send.at[2], gw_recv.at[2])
    waits = near + rest + halo_e.faces_x(0)
    late_in[flat] = late_out[flat]
    sum_d1, sum_x1, *sums_a = unpack(totals[3].finish(), 4)

    whole = 1.0 / math.sqrt(voxels)
    for k, factor in enumerate(
        (
            gain_1 * scale_1 * whole, sum_d1 / voxels, sum_x1 / voxels,
            gain_2 * scale_2 * whole, sum_d2 / voxels, sum_x2 / voxels,
        )
    ):
        tile = jnp.broadcast_to(factor, (C, LANES))
        for pair in range(16):
            pairs[k, pair] = tile[2 * pair : 2 * pair + 2]
    fan_in(early_in, gw_recv.at[0])
    early = jnp.sum(early_in[...], axis=0)
    fan_in(mid_in, gw_recv.at[1])
    mid = jnp.sum(mid_in[...], axis=0)
    at = flat // 32 * 4 + lax.rem(flat, 4)
    fan_in(late_in, gw_recv.at[2])
    late = jnp.sum(late_in[...], axis=0)
    gathered[flat, 0:2] = pairs[0, at] * (
        late[0:2] - pairs[1, at] * early[2:3] - pairs[2, at] * early[0:2]
    )
    gathered[flat, 2:4] = pairs[3, at] * (
        mid[0:2] - pairs[4, at] * mid[4:5] - pairs[5, at] * mid[2:4]
    )
    mine = gathered.at[flat]
    fan_out(lambda to: mine, mine, gw_send.at[3], gw_recv.at[3])

    halo_e.arrive(waits)
    delta_1 = delta_of(slope_1, sum_d1, sum_x1, gain_1, scale_1)
    for side in range(2):
        tile = delta_1(
            side_1[1, side].astype(F32), halo_e.merged(side, 0, lane).astype(F32)
        )
        side_e[0, side] = jnp.where(ok[side], tile, 0.0).astype(BF16)
    build(
        taps_d1, 0,
        lambda at_x, at_y: delta_1(
            rows_1[1, at_x, at_y].astype(F32), rows_e[0, at_x, at_y].astype(F32)
        ),
        lambda at_x, at_y: delta_1(conv_1[1, at_x, at_y], back_1[at_x, at_y]),
        (side_e.at[0, 0], side_e.at[0, 1]),
    )
    def emit(at_x, at_y, tile, carry):
        stage[at_x, at_y] = tile
        return carry

    convolve(taps_d1, 0, 3, emit, 0)
    for at_x in range(SPAN_X):
        dx_out[:, at_x] = jnp.swapaxes(stage[at_x], 0, 1).astype(BF16)

    mean_a, scale_a = moments(*sums_a)
    slope_a = jnp.broadcast_to(gain_2 * scale_a, (C, LANES))
    shift_a = jnp.broadcast_to(bias_2 - mean_a * gain_2 * scale_a, (C, LANES))
    for at_x in range(SPAN_X):

        def step(block, carry, at_x=at_x):
            for k in range(8):
                at_y = block * 8 + k
                pre = conv_2[0, at_x, at_y] * slope_a + shift_a
                stage[at_x, at_y] = pre * sigmoid(pre)
            return carry

        unrolled(0, 2, step, 0)
        y_out[:, at_x] = jnp.swapaxes(stage[at_x], 0, 1).astype(BF16)

    for k, total in enumerate((sum_x1, sum_d1, sum_x2, sum_d2)):
        norm_out[k : k + 1] = whole * jnp.sum(
            jnp.where(small_lane == small_row, total, 0.0), axis=0, keepdims=True
        )
    for halo in halos:
        halo.drain()
    for total in totals:
        total.drain()
    for k, chunks in enumerate((early_out, mid_out, late_out)):
        fan_in(chunks, gw_send.at[k])
    fan_in(gathered, gw_recv.at[3])
    for member, out in ((0, gw_first), (1, gw_second)):
        for k in range(7):
            tile = jnp.concatenate(
                [
                    gathered[(pair // 4 * 8 + k) * 4 + pair % 4, 2 * member : 2 * member + 2]
                    for pair in range(16)
                ],
                axis=0,
            )
            for tap in range(4 * k, min(4 * k + 4, 27)):
                out[tap] = tile[:, C * (tap % 4) : C * (tap % 4) + C]

    fan_in(gathered, gw_send.at[3])


def write_out(*refs):
    sources, targets, semaphores = refs[:5], refs[5:10], refs[10]
    copies = [
        pltpu.make_async_copy(source, target, semaphores.at[index])
        for index, (source, target) in enumerate(zip(sources, targets))
    ]
    for copy in copies:
        copy.start()
    for copy in copies:
        copy.wait()


def body(voxels, x_a, x_b, w_first, w_second, gain_first, bias_first, gain_second, bias_second,
         grad_out):
    def sized(*shape, kind=BF16):
        return pltpu.VMEM(shape, kind)

    volumes = (3, 2, 1, 1)
    devices = math.prod(lax.axis_size(axis) for axis in AXES)
    block = (C, SPAN_X, SPAN_Y, LANES)
    scratch = [sized(*block)] * 3 + [sized(27, C, C)] * 2 + [sized(1, C, kind=F32)] * 4
    scratch += [
        sized(4, HEIGHT, DEPTH), sized(SPAN_X, SPAN_Y, C, LANES, kind=F32)
    ]
    scratch += [sized(count, PAD_X, PAD_Y, TAPS, LANES) for count in (2, 2, 1, 1)]
    scratch += [sized(count, PAD_X, PAD_Y, C, LANES) for count in volumes]
    heights = [C if count == 3 else C // 2 for count in volumes]
    pairs = [(2,) if count == 2 else () for count in volumes]
    scratch += [
        sized(*pair, 2, 3, 3, height, LANES) for pair, height in zip(pairs, heights)
    ]
    scratch += [sized(*pair, 2, height, LANES) for pair, height in zip(pairs, heights)]
    scratch += [sized(count, 2, C, LANES) for count in volumes] + [sized(2, 2, C, LANES)]
    scratch += [
        sized(2, SPAN_X, SPAN_Y, C, LANES, kind=F32),
        sized(2, SPAN_X, SPAN_Y, C, LANES, kind=F32),
        sized(SPAN_X, SPAN_Y, C, LANES, kind=F32),
        sized(4, devices, 1, LANES, kind=F32),
        *[sized(SPAN_X, SPAN_Y + 4, C, LANES)] * 4,
        *[sized(devices, 3, LANES, kind=F32)] * 2,
        *[sized(devices, 5, LANES, kind=F32)] * 2,
        *[sized(devices, 2, LANES, kind=F32)] * 2,
        sized(devices, 4, LANES, kind=F32),
        sized(6, 16, 2, LANES, kind=F32),
        pltpu.SemaphoreType.DMA((5, 32)),
        pltpu.SemaphoreType.DMA((5, 32)),
        pltpu.SemaphoreType.DMA((4,)),
        pltpu.SemaphoreType.DMA((4,)),
        pltpu.SemaphoreType.DMA((4,)),
        pltpu.SemaphoreType.DMA((4,)),
        pltpu.SemaphoreType.DMA((9,)),
    ]
    in_vmem = pl.BlockSpec(memory_space=pltpu.VMEM)
    in_hbm = pl.BlockSpec(memory_space=pltpu.HBM)
    taps = jax.ShapeDtypeStruct((27, C, C), F32)
    out_shape = (
        jax.ShapeDtypeStruct(block, BF16),
        jax.ShapeDtypeStruct(block, BF16),
        taps,
        taps,
        jax.ShapeDtypeStruct((4, C), F32),
    )
    results = pl.pallas_call(
        functools.partial(kernel, voxels),
        out_shape=out_shape,
        in_specs=[in_hbm] * 9,
        out_specs=(in_vmem,) * 5,
        scratch_shapes=scratch,
        compiler_params=pltpu.CompilerParams(
            collective_id=0, has_side_effects=True, vmem_limit_bytes=28 * 1024 * 1024
        ),
    )(
        *(pltpu.with_memory_space_constraint(value, pltpu.HBM) for value in (
            x_a, x_b, grad_out, w_first.reshape(27, C, C), w_second.reshape(27, C, C),
            *(row.reshape(1, C) for row in (gain_first, bias_first, gain_second, bias_second)),
        )),
    )
    y_a, dx_b, grad_first, grad_second, norms = pl.pallas_call(
        write_out,
        out_shape=out_shape,
        in_specs=[in_vmem] * 5,
        out_specs=(in_hbm,) * 5,
        scratch_shapes=[pltpu.SemaphoreType.DMA((5,))],
        compiler_params=pltpu.CompilerParams(vmem_limit_bytes=8 * 1024 * 1024),
    )(*results)
    return (
        y_a, dx_b, grad_first.reshape(3, 3, 3, C, C), grad_second.reshape(3, 3, 3, C, C), norms
    )


def solution(mesh):
    split = P(None, "gx", "gy", "gz")
    voxels = float(SPAN_X * SPAN_Y * LANES * mesh.size)
    return jax.shard_map(
        functools.partial(body, voxels),
        mesh=mesh,
        in_specs=(split, split, P(), P(), P(), P(), P(), P(), split),
        out_specs=(split, split, P(), P(), P()),
        check_vma=False,
    )
```
